128 devices in a mesh: local: 16 (over z, y), data: 8 (over x, core).
Axes of the slice: x: 4, y: 4, z: 4, core: 2. Of those that a mesh axis runs over, the one named last changes fastest.
Arguments:
- tokens: bfloat16 [16384, 2048], P(('local', 'data'))
- grad_out: bfloat16 [16384, 2048], P(('local', 'data'))
- w_up: bfloat16 [2, 2048, 8192], P(None, ('local', 'data'))
- w_down: bfloat16 [2, 8192, 2048], P(None, ('local', 'data'))
Outputs:
- output 1: bfloat16 [16384, 2048], P(('local', 'data'))
- output 2: bfloat16 [16384, 2048], P(('local', 'data'))
- output 3: float32 [2, 2048, 8192], P(None, ('local', 'data'))
- output 4: float32 [2, 8192, 2048], P(None, ('local', 'data'))
All inputs are finite; a program needn't handle non-finite values.
Results may differ from the reference program's by a relative error of at most 0.0142873.
Values are sent between devices in bfloat16 or wider.
A program may use at most 1 GiB of HBM per device.

```python
import jax
import jax.numpy as jnp
from jax import lax

HIDDEN = 2048
FFN_DIM = 8192
NUM_LAYERS = 2
TOTAL_TOKENS = 16384
NORM_EPS = 1e-6
BLOCK_ROWS = min(TOTAL_TOKENS, 2048)


def setup_inputs(seed: int = 0) -> dict:
    keys = jax.random.split(jax.random.key(seed), 4)
    tokens = jax.random.normal(keys[0], (TOTAL_TOKENS, HIDDEN), jnp.float32).astype(jnp.bfloat16)
    grad_out = jax.random.normal(keys[1], (TOTAL_TOKENS, HIDDEN), jnp.float32).astype(jnp.bfloat16)
    w_up = (jax.random.normal(keys[2], (NUM_LAYERS, HIDDEN, FFN_DIM), jnp.float32) * HIDDEN ** -0.5).astype(jnp.bfloat16)
    w_down = (jax.random.normal(keys[3], (NUM_LAYERS, FFN_DIM, HIDDEN), jnp.float32) * (1.5 * FFN_DIM ** -0.5)).astype(jnp.bfloat16)
    return {'tokens': tokens, 'grad_out': grad_out, 'w_up': w_up, 'w_down': w_down}


def rms_norm(x_f32):
    return x_f32 * lax.rsqrt(jnp.mean(x_f32 * x_f32, axis=-1, keepdims=True) + NORM_EPS)


def gelu_tanh(values):
    return jax.nn.gelu(values, approximate=True)


def layer_forward(layer_in, up_w, down_w):
    x_f32 = layer_in.astype(jnp.float32)
    normed = rms_norm(x_f32).astype(jnp.bfloat16)
    pre_act = jnp.dot(normed, up_w, preferred_element_type=jnp.float32).astype(jnp.bfloat16)
    hidden = gelu_tanh(pre_act.astype(jnp.float32)).astype(jnp.bfloat16)
    return (x_f32 + jnp.dot(hidden, down_w, preferred_element_type=jnp.float32)).astype(jnp.bfloat16)


def layer_backward(layer_in, cotangent, up_w, down_w):
    x_f32 = layer_in.astype(jnp.float32)
    normed = rms_norm(x_f32).astype(jnp.bfloat16)
    pre_act = jnp.dot(normed, up_w, preferred_element_type=jnp.float32).astype(jnp.bfloat16)
    hidden = gelu_tanh(pre_act.astype(jnp.float32)).astype(jnp.bfloat16)
    grad_down = jnp.dot(hidden.T, cotangent, preferred_element_type=jnp.float32)
    d_hidden = jnp.dot(cotangent, down_w.T, preferred_element_type=jnp.float32).astype(jnp.bfloat16)
    _, gelu_back = jax.vjp(gelu_tanh, pre_act.astype(jnp.float32))
    d_pre = gelu_back(d_hidden.astype(jnp.float32))[0].astype(jnp.bfloat16)
    grad_up = jnp.dot(normed.T, d_pre, preferred_element_type=jnp.float32)
    d_normed = jnp.dot(d_pre, up_w.T, preferred_element_type=jnp.float32)
    _, norm_back = jax.vjp(rms_norm, x_f32)
    d_input = (cotangent.astype(jnp.float32) + norm_back(d_normed)[0]).astype(jnp.bfloat16)
    return d_input, grad_up, grad_down


def reference(tokens, grad_out, w_up, w_down):
    n_blocks = TOTAL_TOKENS // BLOCK_ROWS
    tok_blocks = tokens.reshape(n_blocks, BLOCK_ROWS, HIDDEN)
    grad_blocks = grad_out.reshape(n_blocks, BLOCK_ROWS, HIDDEN)

    def block_step(grad_accum, block_pair):
        accum_up, accum_down = grad_accum
        x_block, g_block = block_pair

        def fwd_step(hidden_state, weights):
            up_w, down_w = weights
            return layer_forward(hidden_state, up_w, down_w), hidden_state

        x_final, layer_inputs = lax.scan(fwd_step, x_block, (w_up, w_down))

        def bwd_step(cotangent, layer_items):
            layer_in, up_w, down_w = layer_items
            d_input, grad_up, grad_down = layer_backward(layer_in, cotangent, up_w, down_w)
            return d_input, (grad_up, grad_down)

        d_tokens, layer_grads = lax.scan(bwd_step, g_block, (layer_inputs, w_up, w_down), reverse=True)
        return (accum_up + layer_grads[0], accum_down + layer_grads[1]), (x_final, d_tokens)

    start_accum = (jnp.zeros((NUM_LAYERS, HIDDEN, FFN_DIM), jnp.float32), jnp.zeros((NUM_LAYERS, FFN_DIM, HIDDEN), jnp.float32))
    total_grads, block_outs = lax.scan(block_step, start_accum, (tok_blocks, grad_blocks))
    x_out = block_outs[0].reshape(TOTAL_TOKENS, HIDDEN)
    dx_in = block_outs[1].reshape(TOTAL_TOKENS, HIDDEN)
    return (x_out, dx_in, total_grads[0], total_grads[1])
```

```python
import jax
import jax.numpy as jnp
from jax import lax
from jax.sharding import PartitionSpec as P

NORM_EPS = 1e-6
BOTH_AXES = ('local', 'data')
CONTRACT_ROWS = (((0,), (0,)), ((), ()))
CONTRACT_COLS = (((1,), (1,)), ((), ()))


def rms_norm(x_f32):
    return x_f32 * lax.rsqrt(jnp.mean(x_f32 * x_f32, axis=-1, keepdims=True) + NORM_EPS)


def gelu_tanh(values):
    return jax.nn.gelu(values, approximate=True)


def solution(mesh):
    nl, nd = mesh.shape['local'], mesh.shape['data']
    tok_spec = P(BOTH_AXES, None)
    w_spec = P(None, BOTH_AXES, None)

    def device_fn(tokens, grad_out, w_up, w_down):
        num_layers, up_rows, ffn = w_up.shape
        down_rows = w_down.shape[1]

        def gather_up(w):
            cols = w.reshape(up_rows, nl, nd, down_rows).transpose(2, 0, 1, 3).reshape(nd, up_rows, nl * down_rows)
            rows = lax.all_to_all(cols, 'data', 0, 0, tiled=True)
            return lax.all_gather(rows.reshape(nd * up_rows, nl * down_rows), 'local', axis=0, tiled=True)

        def gather_down(w):
            return lax.all_gather(w, 'local', axis=0, tiled=True)

        def scatter_up(part):
            mine = lax.psum_scatter(part, 'local', scatter_dimension=0, tiled=True)
            cols = lax.all_to_all(mine.reshape(nd, up_rows, nl * down_rows), 'data', 0, 0, tiled=True)
            return cols.reshape(nd, up_rows, nl, down_rows).transpose(1, 2, 0, 3).reshape(up_rows, ffn)

        def scatter_down(part):
            return lax.psum_scatter(part, 'local', scatter_dimension=0, tiled=True)

        g_full = lax.all_gather(grad_out, 'data', axis=0, tiled=True)
        x = tokens
        saved = []
        for l in range(num_layers):
            up, down = gather_up(w_up[l]), gather_down(w_down[l])
            x_f32 = x.astype(jnp.float32)
            u = rms_norm(x_f32).astype(jnp.bfloat16)
            u_full = lax.all_gather(u, 'data', axis=0, tiled=True)
            a = jnp.dot(u_full, up, preferred_element_type=jnp.float32).astype(jnp.bfloat16)
            s = gelu_tanh(a.astype(jnp.float32)).astype(jnp.bfloat16)
            saved.append((x, u_full, a, s))
            part = jnp.dot(s, down, preferred_element_type=jnp.float32)
            x = (x_f32 + lax.psum_scatter(part, 'data', scatter_dimension=0, tiled=True)).astype(jnp.bfloat16)
        dy, dy_full = grad_out, g_full
        grads_up, grads_down = [None] * num_layers, [None] * num_layers
        for l in reversed(range(num_layers)):
            if l < num_layers - 1:
                w_up, w_down, dy_full = lax.optimization_barrier((w_up, w_down, lax.all_gather(dy, 'data', axis=0, tiled=True)))
                up, down = gather_up(w_up[l]), gather_down(w_down[l])
            x_in, u_full, a, s = saved[l]
            ds = lax.dot_general(dy_full, down, CONTRACT_COLS, preferred_element_type=jnp.float32).astype(jnp.bfloat16)
            _, gelu_back = jax.vjp(gelu_tanh, a.astype(jnp.float32))
            da = gelu_back(ds.astype(jnp.float32))[0].astype(jnp.bfloat16)
            du_part = lax.dot_general(da, up, CONTRACT_COLS, preferred_element_type=jnp.float32)
            down_part = lax.dot_general(s, dy_full, CONTRACT_ROWS, preferred_element_type=jnp.float32)
            up_part = lax.dot_general(u_full, da, CONTRACT_ROWS, preferred_element_type=jnp.float32)
            du = lax.psum_scatter(du_part, 'data', scatter_dimension=0, tiled=True)
            _, norm_back = jax.vjp(rms_norm, x_in.astype(jnp.float32))
            dy = (dy.astype(jnp.float32) + norm_back(du)[0]).astype(jnp.bfloat16)
            grads_up[l] = scatter_up(up_part)
            grads_down[l] = scatter_down(down_part)
        return x, dy, jnp.stack(grads_up), jnp.stack(grads_down)

    return jax.shard_map(device_fn, mesh=mesh, in_specs=(tok_spec, tok_spec, w_spec, w_spec), out_specs=(tok_spec, tok_spec, w_spec, w_spec), check_vma=False)
```

```python
import functools

import jax
import jax.numpy as jnp
from jax import lax
from jax.experimental import pallas as pl
from jax.experimental.pallas import tpu as pltpu
from jax.sharding import PartitionSpec as P

NORM_EPS = 1e-6
BOTH_AXES = ('local', 'data')
CONTRACT_ROWS = (((0,), (0,)), ((), ()))
CONTRACT_COLS = (((1,), (1,)), ((), ()))
MESH = pl.DeviceIdType.MESH
RING = 4
F32, BF16 = jnp.float32, jnp.bfloat16

LINK_RATE = 46.6e3
PAIR_RATE = 600e3
LOCAL_RATE = 3000e3
HOP = 2.2


def gelu_tanh(values):
    return jax.nn.gelu(values, approximate=True)


class Event:
    def __init__(self):
        self.time = None


class Copy:
    def __init__(self, desc, time, remote):
        self.desc, self.time, self.remote = desc, time, remote

    def wait(self):
        if self.remote:
            self.desc.wait_recv()
        else:
            self.desc.wait()


class Net:
    def __init__(self, send_sems, recv_sems, local_sems):
        self.send_sems, self.recv_sems, self.local_sems = send_sems, recv_sems, local_sems
        self.n_remote = self.n_local = 0
        self.now = 0.0
        self.free = {}
        self.sent = []
        self.flows = []
        here = lax.axis_index('local')
        there = lax.axis_index('data')
        self.data = there
        self.pos = {'z': here // RING, 'y': here % RING, 'x': there // 2}
        self.core = there % 2

    def at(self, axis, step):
        return (self.pos[axis] + (step + RING)) % RING

    def device(self, axis, step):
        if axis == 'p':
            return {'data': self.pos['x'] * 2 + (1 - self.core)}
        if axis == 'd':
            return {'data': (self.data + step) % (2 * RING)}
        to = self.at(axis, step)
        if axis == 'x':
            return {'data': to * 2 + self.core}
        if axis == 'y':
            return {'local': self.pos['z'] * RING + to}
        return {'local': to * RING + self.pos['y']}

    def barrier(self, axes):
        peers = [(axis, step) for axis in axes for step in ((1, -1) if axis in 'xyz' else (1,) if axis == 'p' else range(1, 2 * RING))]
        semaphore = pltpu.get_barrier_semaphore()
        for axis, step in peers:
            pl.semaphore_signal(semaphore, inc=1, device_id=self.device(axis, step), device_id_type=MESH)
        pl.semaphore_wait(semaphore, len(peers))

    def send(self, src, dst, axis, step=1):
        k = self.n_remote
        self.n_remote += 1
        desc = pltpu.make_async_remote_copy(
            src_ref=src, dst_ref=dst, send_sem=self.send_sems.at[k], recv_sem=self.recv_sems.at[k],
            device_id=self.device(axis, step), device_id_type=MESH)
        desc.start()
        size = 1
        for n in dst.shape:
            size *= n
        size *= dst.dtype.itemsize
        rate = PAIR_RATE if axis == 'p' else LINK_RATE
        key = (axis, step)
        done = max(self.free.get(key, 0.0), self.now) + size / rate
        self.free[key] = done
        copy = Copy(desc, done + HOP, True)
        self.sent.append(copy)
        return copy

    def load(self, src, dst):
        k = self.n_local
        self.n_local += 1
        desc = pltpu.make_async_copy(src, dst, self.local_sems.at[k])
        desc.start()
        size = 1
        for n in dst.shape:
            size *= n
        return Copy(desc, self.now + 1.0 + size * dst.dtype.itemsize / LOCAL_RATE, False)

    def spend(self, microseconds):
        self.now += microseconds

    def spawn(self, flow):
        self.step(flow)

    def step(self, flow):
        try:
            self.flows.append((flow, next(flow)))
        except StopIteration:
            pass

    def run(self):
        while self.flows:
            best, best_time = None, None
            for k, (_, items) in enumerate(self.flows):
                if any(item.time is None for item in items):
                    continue
                time = max([item.time for item in items] + [0.0])
                if best is None or time < best_time:
                    best, best_time = k, time
            flow, items = self.flows.pop(best)
            for item in items:
                if isinstance(item, Copy):
                    item.wait()
            self.now = max(self.now, best_time)
            self.step(flow)

    def finish(self):
        for copy in self.sent:
            copy.desc.wait_send()


def rows_loop(rows, chunk, body):
    chunk = min(chunk, rows)

    def step(k, carry):
        body(pl.ds(pl.multiple_of(k * chunk, chunk), chunk))
        return carry

    lax.fori_loop(0, rows // chunk, step, 0)


def add_into(net, dst, *others):
    rows, cols = dst.shape

    def body(at):
        total = dst[at, :]
        for other in others:
            total = total + other[at, :]
        dst[at, :] = total

    rows_loop(rows, 16, body)
    net.spend(rows * cols * 4 * (1 + len(others)) / 4e6)


def fire(net, event):
    event.time = net.now


def exchange_back(net, src, dst, done):
    rows = dst.shape[1]

    def block(k):
        return src.at[pl.ds(pl.multiple_of(k * rows, rows), rows)]

    own = net.load(block(net.data), dst.at[net.data])
    copies = [net.send(block((net.data + k) % (2 * RING)), dst.at[net.data], 'd', k) for k in range(1, 2 * RING)]
    yield [own] + copies
    fire(net, done)


def exchange(net, src, dst, done):
    own = net.load(src.at[:, net.data], dst.at[:, net.data])
    copies = [net.send(src.at[:, (net.data + k) % (2 * RING)], dst.at[:, net.data], 'd', k) for k in range(1, 2 * RING)]
    yield [own] + copies
    fire(net, done)


def gather_x(net, full, done):
    half = full.shape[1] // 2
    lo, hi = pl.ds(0, half), pl.ds(half, half)

    def block(step):
        return full.at[net.at('x', step) * 2 + net.core]

    def part(step, rows):
        return full.at[net.at('x', step) * 2 + net.core, rows]

    forth = net.send(block(0), block(0), 'x', 1)
    back = net.send(block(0), block(0), 'x', -1)
    pair = [net.send(block(0), block(0), 'p')]
    yield [forth]
    forth = net.send(part(-1, lo), part(-1, lo), 'x', 1)
    pair.append(net.send(block(-1), block(-1), 'p'))
    yield [back]
    back = net.send(part(1, hi), part(1, hi), 'x', -1)
    pair.append(net.send(block(1), block(1), 'p'))
    yield [forth, back]
    pair.append(net.send(block(2), block(2), 'p'))
    yield pair
    fire(net, done)


def gather_yz(net, own, full, first, done):
    second = 'y' if first == 'z' else 'z'
    half = own.shape[0] // 2
    lo, hi = pl.ds(0, half), pl.ds(half, half)

    def index(one, two):
        at_one, at_two = net.at(first, one), net.at(second, two)
        return (at_one, at_two) if first == 'z' else (at_two, at_one)

    def block(one, two):
        return full.at[index(one, two)]

    def part(one, two, rows):
        return full.at[index(one, two) + (rows,)]

    ends = []

    def relay(one, forth, back, end):
        yield [forth]
        forth = net.send(part(one, -1, lo), part(one, -1, lo), second, 1)
        yield [back]
        back = net.send(part(one, 1, hi), part(one, 1, hi), second, -1)
        yield [forth, back]
        fire(net, end)

    def spread(src, one):
        forth = net.send(src, block(one, 0), second, 1)
        back = net.send(src, block(one, 0), second, -1)
        end = Event()
        ends.append(end)
        net.spawn(relay(one, forth, back, end))

    mine = net.load(own, block(0, 0))
    forth = net.send(own, block(0, 0), first, 1)
    back = net.send(own, block(0, 0), first, -1)
    spread(own, 0)
    yield [forth]
    forth = net.send(part(-1, 0, lo), part(-1, 0, lo), first, 1)
    spread(block(-1, 0), -1)
    yield [back]
    back = net.send(part(1, 0, hi), part(1, 0, hi), first, -1)
    spread(block(1, 0), 1)
    yield [forth, back]
    spread(block(2, 0), 2)
    yield [mine] + ends
    fire(net, done)


def reduce_ring(net, axis, far, ahead, behind, mine, relay_f, relay_b, last_f, last_b, done):
    half = mine.shape[0] // 2
    lo, hi = pl.ds(0, half), pl.ds(half, half)
    first_f = net.send(far.at[lo], relay_f, axis, 1)
    first_b = net.send(far.at[hi], relay_b, axis, -1)
    direct_f = net.send(ahead.at[hi], last_f.at[hi], axis, 1)
    direct_b = net.send(behind.at[lo], last_b.at[lo], axis, -1)
    yield [first_f]
    add_into(net, ahead.at[lo], relay_f)
    summed_f = net.send(ahead.at[lo], last_f.at[lo], axis, 1)
    yield [first_b]
    add_into(net, behind.at[hi], relay_b)
    summed_b = net.send(behind.at[hi], last_b.at[hi], axis, -1)
    yield [direct_f, direct_b, summed_f, summed_b]
    add_into(net, mine, last_f, last_b)
    fire(net, done)


STEPS = (2, 1, -1, 0)


def reduce_x(net, part, acc, other, relay_f, relay_b, last_f, last_b, done):
    half = acc.shape[1] // 2
    lo, hi = pl.ds(0, half), pl.ds(half, half)
    pairs, mine = [], []
    for k, step in enumerate(STEPS):
        pairs.append(net.send(part.at[net.at('x', step) * 2 + (1 - net.core)], other.at[k], 'p'))
        mine.append(net.load(part.at[net.at('x', step) * 2 + net.core], acc.at[k]))
    yield [pairs[0], mine[0]]
    add_into(net, acc.at[0], other.at[0])
    first_f = net.send(acc.at[0, lo], relay_f, 'x', 1)
    first_b = net.send(acc.at[0, hi], relay_b, 'x', -1)
    yield [pairs[1], mine[1]]
    add_into(net, acc.at[1], other.at[1])
    direct_f = net.send(acc.at[1, hi], last_f.at[hi], 'x', 1)
    yield [pairs[2], mine[2]]
    add_into(net, acc.at[2], other.at[2])
    direct_b = net.send(acc.at[2, lo], last_b.at[lo], 'x', -1)
    yield [pairs[3], mine[3]]
    add_into(net, acc.at[3], other.at[3])
    yield [first_f]
    add_into(net, acc.at[1, lo], relay_f)
    summed_f = net.send(acc.at[1, lo], last_f.at[lo], 'x', 1)
    yield [first_b]
    add_into(net, acc.at[2, hi], relay_b)
    summed_b = net.send(acc.at[2, hi], last_b.at[hi], 'x', -1)
    yield [direct_f, direct_b, summed_f, summed_b]
    add_into(net, acc.at[3], last_f, last_b)
    fire(net, done)


def reduce_yz(net, part, first, sums, ahead, behind, relay1, last1, relay2, last2, start, done):
    second = 'y' if first == 'z' else 'z'
    half = sums.shape[1] // 2
    lo, hi = pl.ds(0, half), pl.ds(half, half)

    def index(one, two):
        at_one, at_two = net.at(first, one), net.at(second, two)
        return (at_one, at_two) if first == 'z' else (at_two, at_one)

    def ring(k, end):
        two = STEPS[k]
        loads = [net.load(part.at[index(1, two) + (lo,)], ahead.at[k]),
                 net.load(part.at[index(-1, two) + (hi,)], behind.at[k]),
                 net.load(part.at[index(0, two)], sums.at[k])]
        first_f = net.send(part.at[index(2, two) + (lo,)], relay1.at[0, k], first, 1)
        first_b = net.send(part.at[index(2, two) + (hi,)], relay1.at[1, k], first, -1)
        direct_f = net.send(part.at[index(1, two) + (hi,)], last1.at[0, k, hi], first, 1)
        direct_b = net.send(part.at[index(-1, two) + (lo,)], last1.at[1, k, lo], first, -1)
        yield [first_f, loads[0]]
        add_into(net, ahead.at[k], relay1.at[0, k])
        summed_f = net.send(ahead.at[k], last1.at[0, k, lo], first, 1)
        yield [first_b, loads[1]]
        add_into(net, behind.at[k], relay1.at[1, k])
        summed_b = net.send(behind.at[k], last1.at[1, k, hi], first, -1)
        yield [direct_f, direct_b, summed_f, summed_b, loads[2]]
        add_into(net, sums.at[k], last1.at[0, k], last1.at[1, k])
        fire(net, end)

    if start is not None:
        yield [start]
    ends = [Event() for _ in STEPS]
    for k in range(RING):
        net.spawn(ring(k, ends[k]))
    yield [ends[0]]
    first_f = net.send(sums.at[0, lo], relay2.at[0], second, 1)
    first_b = net.send(sums.at[0, hi], relay2.at[1], second, -1)
    yield [ends[1]]
    direct_f = net.send(sums.at[1, hi], last2.at[0, hi], second, 1)
    yield [ends[2]]
    direct_b = net.send(sums.at[2, lo], last2.at[1, lo], second, -1)
    yield [first_f]
    add_into(net, sums.at[1, lo], relay2.at[0])
    summed_f = net.send(sums.at[1, lo], last2.at[0, lo], second, 1)
    yield [first_b]
    add_into(net, sums.at[2, hi], relay2.at[1])
    summed_b = net.send(sums.at[2, hi], last2.at[1, hi], second, -1)
    yield [ends[3], direct_f, direct_b, summed_f, summed_b]
    add_into(net, sums.at[3], last2.at[0], last2.at[1])
    fire(net, done)


def reduce_yz_scratch(rows, cols):
    return [pltpu.VMEM((RING, rows, cols), F32), pltpu.VMEM((RING, rows // 2, cols), F32), pltpu.VMEM((RING, rows // 2, cols), F32),
            pltpu.VMEM((2, RING, rows // 2, cols), F32), pltpu.VMEM((2, RING, rows, cols), F32),
            pltpu.VMEM((2, rows // 2, cols), F32), pltpu.VMEM((2, rows, cols), F32)]


def reduce_x_scratch(rows, cols):
    return [pltpu.VMEM((RING, rows, cols), F32), pltpu.VMEM((RING, rows, cols), F32), pltpu.VMEM((rows // 2, cols), F32),
            pltpu.VMEM((rows // 2, cols), F32), pltpu.VMEM((rows, cols), F32), pltpu.VMEM((rows, cols), F32)]


def norm_rows(x_ref, u_ref):
    def body(at):
        x = x_ref[at, :].astype(F32)
        u_ref[at, :] = (x * lax.rsqrt(jnp.mean(x * x, axis=-1, keepdims=True) + NORM_EPS)).astype(BF16)

    rows_loop(x_ref.shape[0], 16, body)


def norm_back_rows(x_ref, dy_ref, du_ref, dx_ref):
    def body(at):
        x = x_ref[at, :].astype(F32)
        du = du_ref[at, :]
        r = lax.rsqrt(jnp.mean(x * x, axis=-1, keepdims=True) + NORM_EPS)
        dot = jnp.mean(x * du, axis=-1, keepdims=True)
        dx_ref[at, :] = (dy_ref[at, :].astype(F32) + (r * du - x * (r * r * r * dot))).astype(BF16)

    rows_loop(x_ref.shape[0], 16, body)


def add_rows(x_ref, y_ref, out_ref):
    def body(at):
        out_ref[at, :] = (x_ref[at, :].astype(F32) + y_ref[at, :]).astype(BF16)

    rows_loop(x_ref.shape[0], 16, body)


def call(body, out_shape, out_spaces, in_spaces, scratch, remote, local, collective_id, *args):
    spaces = {'v': pl.BlockSpec(memory_space=pltpu.VMEM), 'h': pl.BlockSpec(memory_space=pl.ANY)}

    def kernel(*refs):
        sems = refs[-3:]
        net = Net(*sems)
        body(net, *refs[:-3])
        net.finish()
        assert net.n_remote <= remote and net.n_local <= local, (net.n_remote, net.n_local)
        if PRINT:
            print(body.__name__, net.n_remote, net.n_local, round(net.now, 1))

    return pl.pallas_call(
        kernel, out_shape=out_shape, in_specs=[spaces[s] for s in in_spaces], out_specs=[spaces[s] for s in out_spaces],
        scratch_shapes=list(scratch) + [pltpu.SemaphoreType.DMA((remote,)), pltpu.SemaphoreType.DMA((remote,)), pltpu.SemaphoreType.DMA((local,))],
        compiler_params=pltpu.CompilerParams(collective_id=collective_id, has_side_effects=True, vmem_limit_bytes=67000000),
        cost_estimate=pl.CostEstimate(flops=10**8, bytes_accessed=10**7, transcendentals=0),
        name=body.__name__)(*args)


PRINT = False


def solution(mesh):
    nl, nd = mesh.shape['local'], mesh.shape['data']
    tok_spec = P(BOTH_AXES, None)
    w_spec = P(None, BOTH_AXES, None)

    def device_fn(tokens, grad_out, w_up, w_down):
        num_layers, ur, ffn = w_up.shape
        dr = w_down.shape[1]
        rows, width = tokens.shape
        hidden = nl * dr
        shape = jax.ShapeDtypeStruct
        cols = w_up.reshape(num_layers, ur, nl, nd, dr).transpose(0, 3, 1, 2, 4).reshape(num_layers, nd, ur, hidden)
        up_full = shape((RING, RING, nd, ur, hidden), BF16)
        down_full = shape((RING, RING, dr, width), BF16)
        act_full = shape((nd, rows, width), BF16)
        own = shape((rows, width), BF16)
        rx = reduce_x_scratch(rows, width)
        ryz_up = reduce_yz_scratch(nd * ur, hidden)
        ryz_down = reduce_yz_scratch(dr, width)

        def prologue(net, x_ref, w_up_ref, w_down_ref, up_ref, down_ref, u_ref, block_ref):
            net.barrier('dyz')
            blocks = Event()
            net.spawn(exchange(net, w_up_ref, block_ref, blocks))
            norm_rows(x_ref, u_ref.at[net.data])
            net.spawn(gather_x(net, u_ref, Event()))
            net.spawn(gather_yz(net, w_down_ref.at[0], down_ref, 'z', Event()))

            def up():
                yield [blocks]
                net.spawn(gather_yz(net, block_ref.at[0], up_ref, 'y', Event()))

            net.spawn(up())
            net.run()

        def forward(net, part_ref, x_ref, g_in_ref, block_ref, w_down_ref, up_ref, down_ref, u_ref, g_ref, next_ref, *scratch):
            net.barrier('pxyz')
            reduced, gathered = Event(), Event()
            net.spawn(reduce_x(net, part_ref, *scratch, reduced))
            net.spawn(gather_yz(net, block_ref.at[1], up_ref, 'y', Event()))
            net.spawn(gather_yz(net, w_down_ref.at[1], down_ref, 'z', Event()))

            def act():
                yield [reduced]
                add_rows(x_ref, scratch[0].at[3], next_ref)
                norm_rows(next_ref, u_ref.at[net.data])
                net.spend(0.5)
                net.spawn(gather_x(net, u_ref, gathered))
                yield [net.load(g_in_ref, g_ref.at[net.data])]
                net.spawn(gather_x(net, g_ref, Event()))

            net.spawn(act())
            net.run()

        def turn(net, du_ref, part_ref, dup_ref, ddown_ref, x_ref, g_ref, block_ref, w_down_ref,
                 out_ref, dy_ref, dy_full_ref, up_ref, down_ref, dw_up_ref, dw_down_ref, *scratch):
            net.barrier('dyz')
            r1, r2, s1, s2 = scratch[:6], scratch[6:12], scratch[12:19], scratch[19:26]
            reduced, gathered, out, summed1, summed2 = (Event() for _ in range(5))
            net.spawn(reduce_x(net, du_ref, *r1, reduced))
            net.spawn(gather_yz(net, block_ref.at[0], up_ref, 'y', Event()))
            net.spawn(gather_yz(net, w_down_ref.at[0], down_ref, 'z', Event()))
            net.spawn(reduce_yz(net, dup_ref, 'y', *s1, None, summed1))
            net.spawn(reduce_yz(net, ddown_ref, 'z', *s2, None, summed2))

            def act():
                yield [reduced]
                norm_back_rows(x_ref, g_ref, r1[0].at[3], dy_ref)
                net.spend(0.7)
                yield [net.load(dy_ref, dy_full_ref.at[net.data])]
                net.spawn(gather_x(net, dy_full_ref, gathered))
                net.spawn(reduce_x(net, part_ref, *r2, out))
                yield [out]
                add_rows(x_ref, r2[0].at[3], out_ref)

            def grads():
                yield [summed1]
                net.spawn(exchange_back(net, s1[0].at[3], dw_up_ref, Event()))
                yield [summed2]
                yield [net.load(s2[0].at[3], dw_down_ref)]

            net.spawn(act())
            net.spawn(grads())
            net.run()

        def last(net, du_ref, dup_ref, ddown_ref, x_ref, g_ref, dx_ref, dw_up_ref, dw_down_ref, *scratch):
            net.barrier('dyz')
            r1, s1, s2 = scratch[:6], scratch[6:13], scratch[13:20]
            reduced, summed1, summed2 = (Event() for _ in range(3))
            net.spawn(reduce_x(net, du_ref, *r1, reduced))
            net.spawn(reduce_yz(net, dup_ref, 'y', *s1, None, summed1))
            net.spawn(reduce_yz(net, ddown_ref, 'z', *s2, None, summed2))

            def act():
                yield [reduced]
                norm_back_rows(x_ref, g_ref, r1[0].at[3], dx_ref)
                net.spend(0.7)

            def grads():
                yield [summed1]
                net.spawn(exchange_back(net, s1[0].at[3], dw_up_ref, Event()))
                yield [summed2]
                yield [net.load(s2[0].at[3], dw_down_ref)]

            net.spawn(act())
            net.spawn(grads())
            net.run()

        def flat_act(full):
            return full.reshape(nd * rows, width)

        def flat_up(full):
            return full.reshape(nl * nd * ur, hidden)

        def flat_down(full):
            return full.reshape(hidden, width)

        def dot(a, b):
            return jnp.dot(a, b, preferred_element_type=F32)

        def hidden_of(u_full, up):
            a = dot(u_full, up).astype(BF16)
            return a, gelu_tanh(a.astype(F32)).astype(BF16)

        def hidden_back(a, dy_full, down):
            ds = lax.dot_general(dy_full, down, CONTRACT_COLS, preferred_element_type=F32).astype(BF16)
            _, back = jax.vjp(gelu_tanh, a.astype(F32))
            return back(ds.astype(F32))[0].astype(BF16)

        def split_part(part):
            return part.reshape(nd, rows, width)

        def grads_of(u_full, s, da, dy_full):
            d_up = lax.dot_general(u_full, da, CONTRACT_ROWS, preferred_element_type=F32)
            d_down = lax.dot_general(s, dy_full, CONTRACT_ROWS, preferred_element_type=F32)
            return d_up.reshape(RING, RING, nd * ur, hidden), d_down.reshape(RING, RING, dr, width)

        def own_up(d_up):
            return d_up.reshape(nd, ur, nl, dr).transpose(1, 2, 0, 3).reshape(ur, ffn)

        d_up_own, d_down_own = shape((nd, ur, hidden), F32), shape((dr, width), F32)

        up0, down0, u0, blocks = call(
            prologue, [up_full, down_full, act_full, shape((num_layers, nd, ur, hidden), BF16)], 'vvvh', 'vhh', [], 64, 8, 0,
            tokens, cols, w_down)
        u0 = flat_act(u0)
        a0, s0 = hidden_of(u0, flat_up(up0))
        part0 = split_part(dot(s0, flat_down(down0)))
        up1, down1, u1, g_full, x1 = call(
            forward, [up_full, down_full, act_full, act_full, own], 'vvvvv', 'hvhhh', rx, 72, 12, 1,
            part0, tokens, grad_out, blocks, w_down)
        u1, g_full, up1, down1 = flat_act(u1), flat_act(g_full), flat_up(up1), flat_down(down1)
        a1, s1 = hidden_of(u1, up1)
        da1 = hidden_back(a1, g_full, down1)
        du1 = split_part(lax.dot_general(da1, up1, CONTRACT_COLS, preferred_element_type=F32))
        part1 = split_part(dot(s1, down1))
        d_up1, d_down1 = grads_of(u1, s1, da1, g_full)
        x_out, dy0, dy_full, up0, down0, dw_up1, dw_down1 = call(
            turn, [own, own, act_full, up_full, down_full, d_up_own, d_down_own], 'vvvvvhh', 'hhhhvvhh', rx + rx + ryz_up + ryz_down, 144, 48, 2,
            du1, part1, d_up1, d_down1, x1, grad_out, blocks, w_down)
        dy_full, up0, down0 = flat_act(dy_full), flat_up(up0), flat_down(down0)
        da0 = hidden_back(a0, dy_full, down0)
        du0 = split_part(lax.dot_general(da0, up0, CONTRACT_COLS, preferred_element_type=F32))
        d_up0, d_down0 = grads_of(u0, s0, da0, dy_full)
        dx, dw_up0, dw_down0 = call(
            last, [own, d_up_own, d_down_own], 'vhh', 'hhhvv', rx + ryz_up + ryz_down, 96, 48, 3,
            du0, d_up0, d_down0, tokens, dy0)
        return x_out, dx, jnp.stack([own_up(dw_up0), own_up(dw_up1)]), jnp.stack([dw_down0, dw_down1])

    return jax.shard_map(device_fn, mesh=mesh, in_specs=(tok_spec, tok_spec, w_spec, w_spec), out_specs=(tok_spec, tok_spec, w_spec, w_spec), check_vma=False)
```

```python
import functools

import jax
import jax.numpy as jnp
from jax import lax
from jax.experimental import pallas as pl
from jax.experimental.pallas import tpu as pltpu
from jax.sharding import PartitionSpec as P

NORM_EPS = 1e-6
BOTH_AXES = ('local', 'data')
CONTRACT_ROWS = (((0,), (0,)), ((), ()))
CONTRACT_COLS = (((1,), (1,)), ((), ()))
MESH = pl.DeviceIdType.MESH
RING = 4
F32, BF16 = jnp.float32, jnp.bfloat16

LINK_RATE = 46.6e3
PAIR_RATE = 600e3
LOCAL_RATE = 3000e3
HOP = 2.2
SLACK = 1.0
GELU_C = 0.7978845608028654


def gelu_tanh(values):
    return jax.nn.gelu(values, approximate=True)


class Event:
    def __init__(self, time=None, rank=0, name=''):
        self.time, self.rank, self.name = time, rank, name


class Copy:
    def __init__(self, desc, time, remote):
        self.desc, self.time, self.remote, self.rank = desc, time, remote, 0

    def wait(self):
        if self.remote:
            self.desc.wait_recv()
        else:
            self.desc.wait()


class Net:
    def __init__(self, send_sems, recv_sems, local_sems):
        self.send_sems, self.recv_sems, self.local_sems = send_sems, recv_sems, local_sems
        self.n_remote = self.n_local = 0
        self.now = 0.0
        self.free = {}
        self.sent = []
        self.flows = []
        here = lax.axis_index('local')
        there = lax.axis_index('data')
        self.data = there
        self.pos = {'z': here // RING, 'y': here % RING, 'x': there // 2}
        self.core = there % 2

    def at(self, axis, step):
        return (self.pos[axis] + (step + RING)) % RING

    def device(self, axis, step):
        if axis == 'p':
            return {'data': self.pos['x'] * 2 + (1 - self.core)}
        if axis == 'd':
            return {'data': (self.data + step) % (2 * RING)}
        to = self.at(axis, step)
        if axis == 'x':
            return {'data': to * 2 + self.core}
        if axis == 'y':
            return {'local': self.pos['z'] * RING + to}
        return {'local': to * RING + self.pos['y']}

    def barrier(self, axes):
        peers = [(axis, step) for axis in axes for step in ((1, -1) if axis in 'xyz' else (1,) if axis == 'p' else range(1, 2 * RING))]
        semaphore = pltpu.get_barrier_semaphore()
        for axis, step in peers:
            pl.semaphore_signal(semaphore, inc=1, device_id=self.device(axis, step), device_id_type=MESH)
        pl.semaphore_wait(semaphore, len(peers))

    def send(self, src, dst, axis, step=1):
        k = self.n_remote
        self.n_remote += 1
        desc = pltpu.make_async_remote_copy(
            src_ref=src, dst_ref=dst, send_sem=self.send_sems.at[k], recv_sem=self.recv_sems.at[k],
            device_id=self.device(axis, step), device_id_type=MESH)
        desc.start()
        size = 1
        for n in dst.shape:
            size *= n
        size *= dst.dtype.itemsize
        rate = PAIR_RATE if axis == 'p' else LINK_RATE
        key = (axis, step)
        done = max(self.free.get(key, 0.0), self.now) + size / rate
        self.free[key] = done
        copy = Copy(desc, done + HOP, True)
        self.sent.append(copy)
        return copy

    def load(self, src, dst):
        k = self.n_local
        self.n_local += 1
        desc = pltpu.make_async_copy(src, dst, self.local_sems.at[k])
        desc.start()
        size = 1
        for n in dst.shape:
            size *= n
        return Copy(desc, self.now + 1.0 + size * dst.dtype.itemsize / LOCAL_RATE, False)

    def spend(self, microseconds):
        self.now += microseconds

    def spawn(self, flow):
        self.step(flow)

    def step(self, flow):
        try:
            self.flows.append((flow, next(flow)))
        except StopIteration:
            pass

    def run(self):
        while self.flows:
            best = None
            for k, (_, items) in enumerate(self.flows):
                if any(item.time is None for item in items):
                    continue
                time = max([item.time for item in items] + [0.0])
                late = max(item.rank for item in items)
                rank = (max(time, self.now) + (SLACK if late else 0.0), late, time)
                if best is None or rank < best[0]:
                    best = (rank, k, time)
            _, k, time = best
            flow, items = self.flows.pop(k)
            for item in items:
                if isinstance(item, Copy):
                    item.wait()
            self.now = max(self.now, time)
            self.step(flow)

    def finish(self):
        for copy in self.sent:
            copy.desc.wait_send()


def rows_loop(rows, chunk, body):
    chunk = min(chunk, rows)

    def step(k, carry):
        body(pl.ds(pl.multiple_of(k * chunk, chunk), chunk))
        return carry

    lax.fori_loop(0, rows // chunk, step, 0)


def add_into(net, dst, *others):
    rows, cols = dst.shape

    def body(at):
        total = dst[at, :]
        for other in others:
            total = total + other[at, :]
        dst[at, :] = total

    rows_loop(rows, 16, body)
    net.spend(rows * cols * 4 * (1 + len(others)) / 4e6)


def fire(net, event):
    event.time = net.now
    if PRINT and event.name:
        print('   %7.1f %s' % (net.now, event.name))


def exchange(net, src, dst, done):
    rows = src.shape[2]

    def mine():
        return dst.at[:, pl.ds(pl.multiple_of(net.data * rows, rows), rows)]

    own = net.load(src.at[:, net.data], mine())
    copies = [net.send(src.at[:, (net.data + k) % (2 * RING)], mine(), 'd', k) for k in range(1, 2 * RING)]
    yield [own] + copies
    fire(net, done)


def exchange_back(net, src, dst, done):
    rows = dst.shape[1]

    def block(k):
        return src.at[pl.ds(pl.multiple_of(k * rows, rows), rows)]

    own = net.load(block(net.data), dst.at[net.data])
    copies = [net.send(block((net.data + k) % (2 * RING)), dst.at[net.data], 'd', k) for k in range(1, 2 * RING)]
    yield [own] + copies
    fire(net, done)


def gather_x(net, full, done, issued=None):
    half = full.shape[1] // 2
    lo, hi = pl.ds(0, half), pl.ds(half, half)

    def block(step):
        return full.at[net.at('x', step) * 2 + net.core]

    def part(step, rows):
        return full.at[net.at('x', step) * 2 + net.core, rows]

    forth = net.send(block(0), block(0), 'x', 1)
    back = net.send(block(0), block(0), 'x', -1)
    pair = [net.send(block(0), block(0), 'p')]
    yield [forth]
    forth = net.send(part(-1, lo), part(-1, lo), 'x', 1)
    pair.append(net.send(block(-1), block(-1), 'p'))
    yield [back]
    back = net.send(part(1, hi), part(1, hi), 'x', -1)
    pair.append(net.send(block(1), block(1), 'p'))
    if issued is not None:
        fire(net, issued)
    yield [forth, back]
    pair.append(net.send(block(2), block(2), 'p'))
    yield pair
    fire(net, done)


def gather_yz(net, own, full, first, done, issued=None):
    second = 'y' if first == 'z' else 'z'
    size = own.shape[0]
    half = size // 2
    all_rows, lo, hi = pl.ds(0, size), pl.ds(0, half), pl.ds(half, half)

    def part(one, two, rows):
        at_one, at_two = net.at(first, one), net.at(second, two)
        return full.at[(at_one * RING + at_two if first == 'z' else at_two * RING + at_one), rows]

    ends = []
    left = [RING]

    def relay(one, forth, back, end):
        yield [forth]
        forth = net.send(part(one, -1, lo), part(one, -1, lo), second, 1)
        yield [back]
        back = net.send(part(one, 1, hi), part(one, 1, hi), second, -1)
        left[0] -= 1
        if left[0] == 0 and issued is not None:
            fire(net, issued)
        yield [forth, back]
        fire(net, end)

    def spread(src, one):
        forth = net.send(src, part(one, 0, all_rows), second, 1)
        back = net.send(src, part(one, 0, all_rows), second, -1)
        end = Event()
        ends.append(end)
        net.spawn(relay(one, forth, back, end))

    mine = net.load(own, part(0, 0, all_rows))
    forth = net.send(own, part(0, 0, all_rows), first, 1)
    back = net.send(own, part(0, 0, all_rows), first, -1)
    spread(own, 0)
    yield [forth]
    forth = net.send(part(-1, 0, lo), part(-1, 0, lo), first, 1)
    spread(part(-1, 0, all_rows), -1)
    yield [back]
    back = net.send(part(1, 0, hi), part(1, 0, hi), first, -1)
    spread(part(1, 0, all_rows), 1)
    yield [forth, back]
    spread(part(2, 0, all_rows), 2)
    yield [mine] + ends
    fire(net, done)


STEPS = (2, 1, -1, 0)


def reduce_x(net, part, made, scratch, done):
    other, relay_f, relay_b, last_f, last_b = scratch
    half = part.shape[2] // 2
    lo, hi = pl.ds(0, half), pl.ds(half, half)

    def acc(k, rows=None):
        return part.at[k, net.core] if rows is None else part.at[k, net.core, rows]

    pairs = [None] * RING
    ready = [Event() for _ in STEPS]

    def pair(k):
        yield [made[k]]
        pairs[k] = net.send(part.at[k, 1 - net.core], other.at[k], 'p')
        yield [pairs[k]]
        add_into(net, acc(k), other.at[k])
        fire(net, ready[k])

    for k in range(RING):
        net.spawn(pair(k))
    yield [ready[0]]
    first_f = net.send(acc(0, lo), relay_f, 'x', 1)
    first_b = net.send(acc(0, hi), relay_b, 'x', -1)
    yield [ready[1]]
    direct_f = net.send(acc(1, hi), last_f.at[hi], 'x', 1)
    yield [ready[2]]
    direct_b = net.send(acc(2, lo), last_b.at[lo], 'x', -1)
    yield [first_f]
    add_into(net, acc(1, lo), relay_f)
    summed_f = net.send(acc(1, lo), last_f.at[lo], 'x', 1)
    yield [first_b]
    add_into(net, acc(2, hi), relay_b)
    summed_b = net.send(acc(2, hi), last_b.at[hi], 'x', -1)
    yield [ready[3], direct_f, direct_b, summed_f, summed_b]
    add_into(net, acc(3), last_f, last_b)
    fire(net, done)


def reduce_x_scratch(rows, cols):
    return [pltpu.VMEM((RING, rows, cols), F32), pltpu.VMEM((rows // 2, cols), F32), pltpu.VMEM((rows // 2, cols), F32),
            pltpu.VMEM((rows, cols), F32), pltpu.VMEM((rows, cols), F32)]


def load_parts(net, src, part, made):
    for k, step in enumerate(STEPS):
        def bring(k=k, step=step):
            yield [net.load(src.at[pl.ds(net.at('x', step) * 2, 2)], part.at[k])]
            fire(net, made[k])

        net.spawn(bring())


def reduce_yz(net, part, first, sums, ahead, behind, relay1, last1, relay2, last2, start, done):
    second = 'y' if first == 'z' else 'z'
    half = sums.shape[1] // 2
    lo, hi = pl.ds(0, half), pl.ds(half, half)

    def index(one, two):
        at_one, at_two = net.at(first, one), net.at(second, two)
        return (at_one, at_two) if first == 'z' else (at_two, at_one)

    def ring(k, end):
        two = STEPS[k]
        loads = [net.load(part.at[index(1, two) + (lo,)], ahead.at[k]),
                 net.load(part.at[index(-1, two) + (hi,)], behind.at[k]),
                 net.load(part.at[index(0, two)], sums.at[k])]
        first_f = net.send(part.at[index(2, two) + (lo,)], relay1.at[0, k], first, 1)
        first_b = net.send(part.at[index(2, two) + (hi,)], relay1.at[1, k], first, -1)
        direct_f = net.send(part.at[index(1, two) + (hi,)], last1.at[0, k, hi], first, 1)
        direct_b = net.send(part.at[index(-1, two) + (lo,)], last1.at[1, k, lo], first, -1)
        yield [first_f, loads[0]]
        add_into(net, ahead.at[k], relay1.at[0, k])
        summed_f = net.send(ahead.at[k], last1.at[0, k, lo], first, 1)
        yield [first_b, loads[1]]
        add_into(net, behind.at[k], relay1.at[1, k])
        summed_b = net.send(behind.at[k], last1.at[1, k, hi], first, -1)
        yield [direct_f, direct_b, summed_f, summed_b, loads[2]]
        add_into(net, sums.at[k], last1.at[0, k], last1.at[1, k])
        fire(net, end)

    if start is not None:
        yield [start]
    ends = [Event() for _ in STEPS]
    for k in range(RING):
        net.spawn(ring(k, ends[k]))
    yield [ends[0]]
    first_f = net.send(sums.at[0, lo], relay2.at[0], second, 1)
    first_b = net.send(sums.at[0, hi], relay2.at[1], second, -1)
    yield [ends[1]]
    direct_f = net.send(sums.at[1, hi], last2.at[0, hi], second, 1)
    yield [ends[2]]
    direct_b = net.send(sums.at[2, lo], last2.at[1, lo], second, -1)
    yield [first_f]
    add_into(net, sums.at[1, lo], relay2.at[0])
    summed_f = net.send(sums.at[1, lo], last2.at[0, lo], second, 1)
    yield [first_b]
    add_into(net, sums.at[2, hi], relay2.at[1])
    summed_b = net.send(sums.at[2, hi], last2.at[1, hi], second, -1)
    yield [ends[3], direct_f, direct_b, summed_f, summed_b]
    add_into(net, sums.at[3], last2.at[0], last2.at[1])
    fire(net, done)


def reduce_yz_scratch(rows, cols):
    return [pltpu.VMEM((RING, rows, cols), F32), pltpu.VMEM((RING, rows // 2, cols), F32), pltpu.VMEM((RING, rows // 2, cols), F32),
            pltpu.VMEM((2, RING, rows // 2, cols), F32), pltpu.VMEM((2, RING, rows, cols), F32),
            pltpu.VMEM((2, rows // 2, cols), F32), pltpu.VMEM((2, rows, cols), F32)]


def norm_rows(x_ref, u_ref):
    def body(at):
        x = x_ref[at, :].astype(F32)
        u_ref[at, :] = (x * lax.rsqrt(jnp.mean(x * x, axis=-1, keepdims=True) + NORM_EPS)).astype(BF16)

    rows_loop(x_ref.shape[0], 16, body)


def norm_back_rows(x_ref, dy_ref, du_ref, dx_ref):
    def body(at):
        x = x_ref[at, :].astype(F32)
        du = du_ref[at, :]
        r = lax.rsqrt(jnp.mean(x * x, axis=-1, keepdims=True) + NORM_EPS)
        dot = jnp.mean(x * du, axis=-1, keepdims=True)
        dx_ref[at, :] = (dy_ref[at, :].astype(F32) + (r * du - x * (r * r * r * dot))).astype(BF16)

    rows_loop(x_ref.shape[0], 16, body)


def add_rows(x_ref, y_ref, out_ref):
    def body(at):
        out_ref[at, :] = (x_ref[at, :].astype(F32) + y_ref[at, :]).astype(BF16)

    rows_loop(x_ref.shape[0], 16, body)


def call(body, out_shape, out_spaces, in_spaces, scratch, remote, local, collective_id, *args):
    spaces = {'v': pl.BlockSpec(memory_space=pltpu.VMEM), 'h': pl.BlockSpec(memory_space=pl.ANY)}

    def kernel(*refs):
        sems = refs[-3:]
        net = Net(*sems)
        body(net, *refs[:-3])
        net.finish()
        assert net.n_remote <= remote and net.n_local <= local, (net.n_remote, net.n_local)
        if PRINT:
            print(body.__name__, net.n_remote, net.n_local, round(net.now, 1))

    return pl.pallas_call(
        kernel, out_shape=out_shape, in_specs=[spaces[s] for s in in_spaces], out_specs=[spaces[s] for s in out_spaces],
        scratch_shapes=list(scratch) + [pltpu.SemaphoreType.DMA((remote,)), pltpu.SemaphoreType.DMA((remote,)), pltpu.SemaphoreType.DMA((local,))],
        compiler_params=pltpu.CompilerParams(collective_id=collective_id, has_side_effects=True, vmem_limit_bytes=67000000),
        cost_estimate=pl.CostEstimate(flops=10**8, bytes_accessed=10**7, transcendentals=0),
        name=body.__name__)(*args)


PRINT = False


WIDE = 512


def wide_loop(total, body):
    wide = min(WIDE, total)

    def step(k, carry):
        body(k, wide, pl.ds(pl.multiple_of(k * wide, wide), wide))
        return carry

    lax.fori_loop(0, total // wide, step, 0)


def flat(value):
    return value.reshape(value.shape[0] * value.shape[1], value.shape[2])


def dot_rows(a, b):
    return jnp.dot(flat(a), flat(b), preferred_element_type=F32)


def dot_cols(a, b):
    return lax.dot_general(flat(a), flat(b), CONTRACT_COLS, preferred_element_type=F32)


def gelu(a):
    return 0.5 * a * (1.0 + jnp.tanh(GELU_C * (a + 0.044715 * a * a * a)))


def hidden_rows(net, chip, u, up, a, s):
    at = pl.ds(chip * 2, 2)

    def body(_, wide, cols):
        pre = dot_rows(u[at], up[:, :, cols]).astype(BF16)
        a[at, :, cols] = pre.reshape(2, -1, wide)
        s[at, :, cols] = gelu(pre.astype(F32)).astype(BF16).reshape(2, -1, wide)

    wide_loop(up.shape[2], body)
    net.spend(2.4)


def down_rows(net, chip, s, down, part):
    at = pl.ds(chip * 2, 2)

    def body(_, wide, cols):
        part[:, :, cols] = dot_rows(s[at], down[:, :, cols]).reshape(2, -1, wide)

    wide_loop(down.shape[2], body)
    net.spend(1.8)


def hidden_back_rows(net, chip, dy, down, ds):
    at = pl.ds(chip * 2, 2)
    rows = down.shape[1]

    def body(k, wide, cols):
        blocks = pl.ds(k * (wide // rows), wide // rows)
        ds[at, :, cols] = dot_cols(dy[at], down[blocks]).astype(BF16).reshape(2, -1, wide)

    wide_loop(down.shape[0] * rows, body)
    net.spend(2.4)


def solution(mesh):
    nl, nd = mesh.shape['local'], mesh.shape['data']
    tok_spec = P(BOTH_AXES, None)
    w_spec = P(None, BOTH_AXES, None)

    def device_fn(tokens, grad_out, w_up, w_down):
        num_layers, ur, ffn = w_up.shape
        dr = w_down.shape[1]
        rows, width = tokens.shape
        hidden = nl * dr
        shape = jax.ShapeDtypeStruct
        cols = w_up.reshape(num_layers, ur, nl, nd, dr).transpose(0, 3, 1, 2, 4).reshape(num_layers, nd, ur, hidden)
        up_full = shape((nl, nd * ur, hidden), BF16)
        down_full = shape((nl, dr, width), BF16)
        act_full = shape((nd, rows, width), BF16)
        hid_full = shape((nd, rows, hidden), BF16)
        own = shape((rows, width), BF16)
        part_vmem = pltpu.VMEM((RING, 2, rows, width), F32)
        rx = [part_vmem] + reduce_x_scratch(rows, width)
        ryz_up = reduce_yz_scratch(nd * ur, hidden)
        ryz_down = reduce_yz_scratch(dr, width)

        def vmem(like):
            return pltpu.VMEM(like.shape, like.dtype)

        def forward(net, x_ref, g_in, cols_in, down_in, block_out, u_out, a_out, s_out, up_out, down_out, next_out, g_out, ds_out, x_out,
                    u, g, u1, up0, down0, up1, down1, a, s, ds, part, *rx_scratch):
            net.barrier('dyz')
            blocks, got_u, got_g, got_u1, got_up0, got_down0, got_up1, got_down1, reduced = (Event() for _ in range(9))
            made = [Event() for _ in STEPS]
            hidden_made = [Event() for _ in STEPS]
            got_up0.rank = 2
            names = dict(blocks=blocks, got_u=got_u, got_g=got_g, got_u1=got_u1, got_up0=got_up0, got_down0=got_down0, got_up1=got_up1,
                         got_down1=got_down1, reduced=reduced)
            for name, event in names.items():
                event.name = name
            for k in range(RING):
                made[k].name, hidden_made[k].name = 'made%d' % k, 'hidden%d' % k
            net.spawn(exchange(net, cols_in, block_out, blocks))
            norm_rows(x_ref, u.at[net.data])
            net.spend(0.5)
            sent_u, sent_up0, sent_down0 = Event(name='sent_u'), Event(name='sent_up0'), Event(name='sent_down0')
            net.spawn(gather_x(net, u, got_u, sent_u))
            net.spawn(gather_yz(net, down_in.at[0], down0, 'z', got_down0, sent_down0))

            def up_first():
                yield [blocks]
                net.spawn(gather_yz(net, block_out.at[0], up0, 'y', got_up0, sent_up0))

            def second():
                yield [sent_up0, sent_down0]
                net.spawn(gather_yz(net, block_out.at[1], up1, 'y', got_up1))
                net.spawn(gather_yz(net, down_in.at[1], down1, 'z', got_down1))

            def grad():
                yield [net.load(g_in, g.at[net.data]), sent_u]
                net.spawn(gather_x(net, g, got_g))

            def save(event, *pairs):
                yield [event]
                yield [net.load(src, dst) for src, dst in pairs]

            def hidden_flow():
                yield [got_u, got_up0]
                for k, step in enumerate(STEPS):
                    hidden_rows(net, net.at('x', step), u, up0, a, s)
                    fire(net, hidden_made[k])
                    yield [Event(net.now, 2)]
                yield [net.load(a, a_out), net.load(s, s_out), net.load(u, u_out)]

            def down_flow():
                for k, step in enumerate(STEPS):
                    yield [hidden_made[k], got_down0, Event(0.0, 1)]
                    down_rows(net, net.at('x', step), s, down0, part.at[k])
                    fire(net, made[k])

            def act():
                yield [reduced]
                add_rows(x_ref, part.at[3, net.core], x_out)
                norm_rows(x_out, u1.at[net.data])
                net.spend(1.0)
                net.spawn(gather_x(net, u1, got_u1))

            def back_flow():
                for k, step in enumerate(STEPS):
                    yield [got_g, got_down1, Event(0.0, 3)]
                    hidden_back_rows(net, net.at('x', step), g, down1, ds)
                yield [net.load(ds, ds_out)]

            for flow in (up_first(), second(), grad(), hidden_flow(), down_flow(), act(), back_flow(),
                         reduce_x(net, part, made, rx_scratch, reduced),
                         save(got_up1, (up1, up_out)), save(got_down1, (down1, down_out)), save(got_u1, (u1, next_out)), save(got_g, (g, g_out))):
                net.spawn(flow)
            net.run()

        def turn(net, du_ref, dup_ref, ddown_ref, x_ref, g_ref, block_ref, w_down_ref,
                 dy_ref, dy_full_ref, up_ref, down_ref, dw_up_ref, dw_down_ref, *scratch):
            net.barrier('dyz')
            r1, s1, s2 = scratch[:6], scratch[6:13], scratch[13:20]
            reduced, gathered, summed1, summed2 = (Event() for _ in range(4))
            made = [Event() for _ in STEPS]
            load_parts(net, du_ref, r1[0], made)
            net.spawn(reduce_x(net, r1[0], made, r1[1:], reduced))
            net.spawn(gather_yz(net, block_ref.at[0], up_ref, 'y', Event()))
            net.spawn(gather_yz(net, w_down_ref.at[0], down_ref, 'z', Event()))
            net.spawn(reduce_yz(net, dup_ref, 'y', *s1, None, summed1))
            net.spawn(reduce_yz(net, ddown_ref, 'z', *s2, None, summed2))

            def act():
                yield [reduced]
                norm_back_rows(x_ref, g_ref, r1[0].at[3, net.core], dy_ref)
                net.spend(0.7)
                yield [net.load(dy_ref, dy_full_ref.at[net.data])]
                net.spawn(gather_x(net, dy_full_ref, gathered))

            def grads():
                yield [summed1]
                net.spawn(exchange_back(net, s1[0].at[3], dw_up_ref, Event()))
                yield [summed2]
                yield [net.load(s2[0].at[3], dw_down_ref)]

            net.spawn(act())
            net.spawn(grads())
            net.run()

        def last(net, du_ref, part_ref, dup_ref, ddown_ref, x_ref, dy_ref, x1_ref, dx_ref, out_ref, dw_up_ref, dw_down_ref, *scratch):
            net.barrier('dyz')
            r1, r2, s1, s2 = scratch[:6], scratch[6:12], scratch[12:19], scratch[19:26]
            reduced, out, summed1, summed2 = (Event() for _ in range(4))
            made1, made2 = [Event() for _ in STEPS], [Event() for _ in STEPS]
            load_parts(net, du_ref, r1[0], made1)
            net.spawn(reduce_x(net, r1[0], made1, r1[1:], reduced))
            net.spawn(reduce_yz(net, dup_ref, 'y', *s1, None, summed1))
            net.spawn(reduce_yz(net, ddown_ref, 'z', *s2, None, summed2))

            def act():
                yield [reduced]
                norm_back_rows(x_ref, dy_ref, r1[0].at[3, net.core], dx_ref)
                net.spend(0.7)

            def forward_out():
                yield [Event(20.0)]
                load_parts(net, part_ref, r2[0], made2)
                net.spawn(reduce_x(net, r2[0], made2, r2[1:], out))
                yield [out]
                add_rows(x1_ref, r2[0].at[3, net.core], out_ref)

            def grads():
                yield [summed1]
                net.spawn(exchange_back(net, s1[0].at[3], dw_up_ref, Event()))
                yield [summed2]
                yield [net.load(s2[0].at[3], dw_down_ref)]

            net.spawn(act())
            net.spawn(forward_out())
            net.spawn(grads())
            net.run()

        def flat_act(full):
            return full.reshape(nd * rows, width)

        def flat_up(full):
            return full.reshape(nl * nd * ur, hidden)

        def flat_down(full):
            return full.reshape(hidden, width)

        def dot(a, b):
            return jnp.dot(a, b, preferred_element_type=F32)

        def hidden_of(u_full, up):
            a = dot(u_full, up).astype(BF16)
            return a, gelu_tanh(a.astype(F32)).astype(BF16)

        def pre_back(a, ds):
            _, back = jax.vjp(gelu_tanh, a.astype(F32))
            return back(ds.astype(F32))[0].astype(BF16)

        def split_part(part):
            return part.reshape(nd, rows, width)

        def grads_of(u_full, s, da, dy_full):
            d_up = lax.dot_general(u_full, da, CONTRACT_ROWS, preferred_element_type=F32)
            d_down = lax.dot_general(s, dy_full, CONTRACT_ROWS, preferred_element_type=F32)
            return d_up.reshape(RING, RING, nd * ur, hidden), d_down.reshape(RING, RING, dr, width)

        def own_up(d_up):
            return d_up.reshape(nd, ur, nl, dr).transpose(1, 2, 0, 3).reshape(ur, ffn)

        d_up_own, d_down_own = shape((nd, ur, hidden), F32), shape((dr, width), F32)

        blocks, u0, a0, s0, up1, down1, u1, g_full, ds1, x1 = call(
            forward, [shape((num_layers, nd * ur, hidden), BF16), act_full, hid_full, hid_full, up_full, down_full, act_full, act_full, hid_full, own],
            'hhhhhhhhhv', 'vhhh',
            [vmem(act_full)] * 3 + [vmem(up_full), vmem(down_full)] * 2 + [vmem(hid_full)] * 3 + rx, 128, 32, 0,
            tokens, grad_out, cols, w_down)
        u0, u1, g_full = flat_act(u0), flat_act(u1), flat_act(g_full)
        a0, s0, ds1 = (t.reshape(nd * rows, hidden) for t in (a0, s0, ds1))
        up1, down1 = flat_up(up1), flat_down(down1)
        a1, s1 = hidden_of(u1, up1)
        da1 = pre_back(a1, ds1)
        du1 = split_part(lax.dot_general(da1, up1, CONTRACT_COLS, preferred_element_type=F32))
        part1 = split_part(dot(s1, down1))
        d_up1, d_down1 = grads_of(u1, s1, da1, g_full)
        dy0, dy_full, up0, down0, dw_up1, dw_down1 = call(
            turn, [own, act_full, up_full, down_full, d_up_own, d_down_own], 'vvvvhh', 'hhhvvhh', rx + ryz_up + ryz_down, 144, 48, 1,
            du1, d_up1, d_down1, x1, grad_out, blocks, w_down)
        dy_full, up0, down0 = flat_act(dy_full), flat_up(up0), flat_down(down0)
        da0 = pre_back(a0, lax.dot_general(dy_full, down0, CONTRACT_COLS, preferred_element_type=F32).astype(BF16))
        du0 = split_part(lax.dot_general(da0, up0, CONTRACT_COLS, preferred_element_type=F32))
        d_up0, d_down0 = grads_of(u0, s0, da0, dy_full)
        dx, x_out, dw_up0, dw_down0 = call(
            last, [own, own, d_up_own, d_down_own], 'vvhh', 'hhhhvvv', rx + rx + ryz_up + ryz_down, 96, 56, 2,
            du0, part1, d_up0, d_down0, tokens, dy0, x1)
        return x_out, dx, jnp.stack([own_up(dw_up0), own_up(dw_up1)]), jnp.stack([dw_down0, dw_down1])

    return jax.shard_map(device_fn, mesh=mesh, in_specs=(tok_spec, tok_spec, w_spec, w_spec), out_specs=(tok_spec, tok_spec, w_spec, w_spec), check_vma=False)
```

```python
import functools

import jax
import jax.numpy as jnp
from jax import lax
from jax.experimental import pallas as pl
from jax.experimental.pallas import tpu as pltpu
from jax.sharding import PartitionSpec as P

NORM_EPS = 1e-6
BOTH_AXES = ('local', 'data')
CONTRACT_ROWS = (((0,), (0,)), ((), ()))
CONTRACT_COLS = (((1,), (1,)), ((), ()))
MESH = pl.DeviceIdType.MESH
RING = 4
F32, BF16 = jnp.float32, jnp.bfloat16

LINK_RATE = 46.6e3
PAIR_RATE = 600e3
LOCAL_RATE = 3000e3
HOP = 2.2
SLACK = 1.0
GELU_C = 0.7978845608028654


class Event:
    def __init__(self, time=None, rank=0, name=''):
        self.time, self.rank, self.name = time, rank, name


class Copy:
    def __init__(self, desc, time, remote):
        self.desc, self.time, self.remote, self.rank = desc, time, remote, 0

    def wait(self):
        if self.remote:
            self.desc.wait_recv()
        else:
            self.desc.wait()


class Credit:
    def __init__(self, semaphore, count, time):
        self.semaphore, self.count, self.time, self.rank = semaphore, count, time, 0

    def wait(self):
        pl.semaphore_wait(self.semaphore, self.count)


class Net:
    def __init__(self, send_sems, recv_sems, local_sems, credit_sems):
        self.send_sems, self.recv_sems, self.local_sems, self.credit_sems = send_sems, recv_sems, local_sems, credit_sems
        self.n_remote = self.n_local = 0
        self.now = 0.0
        self.free = {}
        self.sent = []
        self.flows = []
        here = lax.axis_index('local')
        there = lax.axis_index('data')
        self.data = there
        self.pos = {'z': here // RING, 'y': here % RING, 'x': there // 2}
        self.core = there % 2

    def at(self, axis, step):
        return (self.pos[axis] + (step + RING)) % RING

    def device(self, axis, step):
        if axis == 'p':
            return {'data': self.pos['x'] * 2 + (1 - self.core)}
        if axis == 'd':
            return {'data': (self.data + step) % (2 * RING)}
        to = self.at(axis, step)
        if axis == 'x':
            return {'data': to * 2 + self.core}
        if axis == 'y':
            return {'local': self.pos['z'] * RING + to}
        return {'local': to * RING + self.pos['y']}

    def peers(self, axes):
        return [(axis, step) for axis in axes for step in ((1, -1) if axis in 'xyz' else (1,) if axis == 'p' else range(1, 2 * RING))]

    def signal(self, semaphore, axes):
        for axis, step in self.peers(axes):
            pl.semaphore_signal(semaphore, inc=1, device_id=self.device(axis, step), device_id_type=MESH)

    def barrier(self, axes):
        semaphore = pltpu.get_barrier_semaphore()
        self.signal(semaphore, axes)
        pl.semaphore_wait(semaphore, len(self.peers(axes)))

    def grant(self, k, axes):
        self.signal(self.credit_sems.at[k], axes)
        return Credit(self.credit_sems.at[k], len(self.peers(axes)), self.now + HOP)

    def drain(self, copies):
        for copy in copies:
            copy.desc.wait_send()
            self.sent.remove(copy)

    def send(self, src, dst, axis, step=1):
        k = self.n_remote
        self.n_remote += 1
        desc = pltpu.make_async_remote_copy(
            src_ref=src, dst_ref=dst, send_sem=self.send_sems.at[k], recv_sem=self.recv_sems.at[k],
            device_id=self.device(axis, step), device_id_type=MESH)
        desc.start()
        size = 1
        for n in dst.shape:
            size *= n
        size *= dst.dtype.itemsize
        rate = PAIR_RATE if axis == 'p' else LINK_RATE
        key = (axis, step)
        done = max(self.free.get(key, 0.0), self.now) + size / rate
        self.free[key] = done
        copy = Copy(desc, done + HOP, True)
        self.sent.append(copy)
        return copy

    def load(self, src, dst):
        k = self.n_local
        self.n_local += 1
        desc = pltpu.make_async_copy(src, dst, self.local_sems.at[k])
        desc.start()
        size = 1
        for n in dst.shape:
            size *= n
        return Copy(desc, self.now + 1.0 + size * dst.dtype.itemsize / LOCAL_RATE, False)

    def spend(self, microseconds):
        self.now += microseconds

    def spawn(self, flow):
        self.step(flow)

    def step(self, flow):
        try:
            self.flows.append((flow, next(flow)))
        except StopIteration:
            pass

    def run(self):
        while self.flows:
            best = None
            for k, (_, items) in enumerate(self.flows):
                if any(item.time is None for item in items):
                    continue
                time = max([item.time for item in items] + [0.0])
                late = max(item.rank for item in items)
                rank = (max(time, self.now) + (SLACK if late else 0.0), late, time)
                if best is None or rank < best[0]:
                    best = (rank, k, time)
            _, k, time = best
            flow, items = self.flows.pop(k)
            for item in items:
                if not isinstance(item, Event):
                    item.wait()
            self.now = max(self.now, time)
            self.step(flow)

    def finish(self):
        for copy in self.sent:
            copy.desc.wait_send()


def rows_loop(rows, chunk, body):
    chunk = min(chunk, rows)

    def step(k, carry):
        body(pl.ds(pl.multiple_of(k * chunk, chunk), chunk))
        return carry

    lax.fori_loop(0, rows // chunk, step, 0)


def add_into(net, dst, *others):
    rows, cols = dst.shape

    def body(at):
        total = dst[at, :]
        for other in others:
            total = total + other[at, :]
        dst[at, :] = total

    rows_loop(rows, 16, body)
    net.spend(rows * cols * 4 * (1 + len(others)) / 4e6)


def fire(net, event):
    event.time = net.now
    if PRINT and event.name:
        print('   %7.1f %s' % (net.now, event.name))


def exchange(net, src, dst, done):
    rows = src.shape[2]

    def mine():
        return dst.at[:, pl.ds(pl.multiple_of(net.data * rows, rows), rows)]

    own = net.load(src.at[:, net.data], mine())
    copies = [net.send(src.at[:, (net.data + k) % (2 * RING)], mine(), 'd', k) for k in range(1, 2 * RING)]
    yield [own] + copies
    fire(net, done)


def exchange_back(net, src, dst, done):
    rows = dst.shape[1]

    def block(k):
        return src.at[pl.ds(pl.multiple_of(k * rows, rows), rows)]

    own = net.load(block(net.data), dst.at[net.data])
    copies = [net.send(block((net.data + k) % (2 * RING)), dst.at[net.data], 'd', k) for k in range(1, 2 * RING)]
    yield [own] + copies
    fire(net, done)


def gather_x(net, full, done, issued=None):
    half = full.shape[1] // 2
    lo, hi = pl.ds(0, half), pl.ds(half, half)

    def block(step):
        return full.at[net.at('x', step) * 2 + net.core]

    def part(step, rows):
        return full.at[net.at('x', step) * 2 + net.core, rows]

    forth = net.send(block(0), block(0), 'x', 1)
    back = net.send(block(0), block(0), 'x', -1)
    pair = [net.send(block(0), block(0), 'p')]
    yield [forth]
    forth = net.send(part(-1, lo), part(-1, lo), 'x', 1)
    pair.append(net.send(block(-1), block(-1), 'p'))
    yield [back]
    back = net.send(part(1, hi), part(1, hi), 'x', -1)
    pair.append(net.send(block(1), block(1), 'p'))
    if issued is not None:
        fire(net, issued)
    yield [forth, back]
    pair.append(net.send(block(2), block(2), 'p'))
    yield pair
    fire(net, done)


def gather_yz(net, own, full, first, done, issued=None):
    second = 'y' if first == 'z' else 'z'
    size = own.shape[0]
    half = size // 2
    all_rows, lo, hi = pl.ds(0, size), pl.ds(0, half), pl.ds(half, half)

    def part(one, two, rows):
        at_one, at_two = net.at(first, one), net.at(second, two)
        return full.at[(at_one * RING + at_two if first == 'z' else at_two * RING + at_one), rows]

    ends = []
    left = [RING]

    def relay(one, forth, back, end):
        yield [forth]
        forth = net.send(part(one, -1, lo), part(one, -1, lo), second, 1)
        yield [back]
        back = net.send(part(one, 1, hi), part(one, 1, hi), second, -1)
        left[0] -= 1
        if left[0] == 0 and issued is not None:
            fire(net, issued)
        yield [forth, back]
        fire(net, end)

    def spread(src, one):
        forth = net.send(src, part(one, 0, all_rows), second, 1)
        back = net.send(src, part(one, 0, all_rows), second, -1)
        end = Event()
        ends.append(end)
        net.spawn(relay(one, forth, back, end))

    mine = net.load(own, part(0, 0, all_rows))
    forth = net.send(own, part(0, 0, all_rows), first, 1)
    back = net.send(own, part(0, 0, all_rows), first, -1)
    spread(own, 0)
    yield [forth]
    forth = net.send(part(-1, 0, lo), part(-1, 0, lo), first, 1)
    spread(part(-1, 0, all_rows), -1)
    yield [back]
    back = net.send(part(1, 0, hi), part(1, 0, hi), first, -1)
    spread(part(1, 0, all_rows), 1)
    yield [forth, back]
    spread(part(2, 0, all_rows), 2)
    yield [mine] + ends
    fire(net, done)


STEPS = (2, 1, -1, 0)


def reduce_x(net, part, made, scratch, done):
    other, relay_f, relay_b, last_f, last_b = scratch
    half = part.shape[2] // 2
    lo, hi = pl.ds(0, half), pl.ds(half, half)

    def acc(k, rows=None):
        return part.at[k, net.core] if rows is None else part.at[k, net.core, rows]

    pairs = [None] * RING
    ready = [Event() for _ in STEPS]

    def pair(k):
        yield [made[k]]
        pairs[k] = net.send(part.at[k, 1 - net.core], other.at[k], 'p')
        yield [pairs[k]]
        add_into(net, acc(k), other.at[k])
        fire(net, ready[k])

    for k in range(RING):
        net.spawn(pair(k))
    yield [ready[0]]
    first_f = net.send(acc(0, lo), relay_f, 'x', 1)
    first_b = net.send(acc(0, hi), relay_b, 'x', -1)
    yield [ready[1]]
    direct_f = net.send(acc(1, hi), last_f.at[hi], 'x', 1)
    yield [ready[2]]
    direct_b = net.send(acc(2, lo), last_b.at[lo], 'x', -1)
    yield [first_f]
    add_into(net, acc(1, lo), relay_f)
    summed_f = net.send(acc(1, lo), last_f.at[lo], 'x', 1)
    yield [first_b]
    add_into(net, acc(2, hi), relay_b)
    summed_b = net.send(acc(2, hi), last_b.at[hi], 'x', -1)
    yield [ready[3], direct_f, direct_b, summed_f, summed_b]
    add_into(net, acc(3), last_f, last_b)
    done.copies = pairs + [first_f, first_b, direct_f, direct_b, summed_f, summed_b]
    fire(net, done)


def reduce_x_scratch(rows, cols):
    return [pltpu.VMEM((RING, rows, cols), F32), pltpu.VMEM((rows // 2, cols), F32), pltpu.VMEM((rows // 2, cols), F32),
            pltpu.VMEM((rows, cols), F32), pltpu.VMEM((rows, cols), F32)]


def load_parts(net, src, part, made):
    for k, step in enumerate(STEPS):
        def bring(k=k, step=step):
            yield [net.load(src.at[pl.ds(net.at('x', step) * 2, 2)], part.at[k])]
            fire(net, made[k])

        net.spawn(bring())


def reduce_yz(net, part, first, scratch, start, done):
    ahead, behind, mine, relay1, last1, relay2, last2 = scratch
    second = 'y' if first == 'z' else 'z'
    half = mine.shape[0] // 2
    lo, hi, all_rows = pl.ds(0, half), pl.ds(half, half), pl.ds(0, 2 * half)

    def term(one, two, rows=all_rows):
        at_one, at_two = net.at(first, one), net.at(second, two)
        return part.at[(at_one * RING + at_two if first == 'z' else at_two * RING + at_one), rows]

    def bring(gate, src, dst, got):
        yield [gate]
        yield [net.load(src, dst)]
        fire(net, got)

    free = [[Event() for _ in range(RING + 1)] for _ in range(3)]
    got = [[Event() for _ in range(RING)] for _ in range(3)]
    ends = [Event() for _ in STEPS]

    def ring(k):
        two = STEPS[k]
        net.spawn(bring(free[0][k], term(1, two, lo), ahead, got[0][k]))
        net.spawn(bring(free[1][k], term(-1, two, hi), behind, got[1][k]))
        net.spawn(bring(free[2][k], term(0, two), mine, got[2][k]))
        first_f = net.send(term(2, two, lo), relay1.at[0, k], first, 1)
        first_b = net.send(term(2, two, hi), relay1.at[1, k], first, -1)
        direct_f = net.send(term(1, two, hi), last1.at[0, k, hi], first, 1)
        direct_b = net.send(term(-1, two, lo), last1.at[1, k, lo], first, -1)
        yield [first_f, got[0][k]]
        add_into(net, relay1.at[0, k], ahead)
        fire(net, free[0][k + 1])
        summed_f = net.send(relay1.at[0, k], last1.at[0, k, lo], first, 1)
        yield [first_b, got[1][k]]
        add_into(net, relay1.at[1, k], behind)
        fire(net, free[1][k + 1])
        summed_b = net.send(relay1.at[1, k], last1.at[1, k, hi], first, -1)
        yield [direct_f, direct_b, summed_f, summed_b, got[2][k]]
        add_into(net, last1.at[0, k], last1.at[1, k], mine)
        fire(net, free[2][k + 1])
        fire(net, ends[k])

    def sums(k, rows=all_rows):
        return last1.at[0, k, rows]

    if start is not None:
        yield [start]
    for events in free:
        fire(net, events[0])
    for k in range(RING):
        net.spawn(ring(k))
    yield [ends[0]]
    first_f = net.send(sums(0, lo), relay2.at[0], second, 1)
    first_b = net.send(sums(0, hi), relay2.at[1], second, -1)
    yield [ends[1]]
    direct_f = net.send(sums(1, hi), last2.at[0, hi], second, 1)
    yield [ends[2]]
    direct_b = net.send(sums(2, lo), last2.at[1, lo], second, -1)
    yield [first_f]
    add_into(net, sums(1, lo), relay2.at[0])
    summed_f = net.send(sums(1, lo), last2.at[0, lo], second, 1)
    yield [first_b]
    add_into(net, sums(2, hi), relay2.at[1])
    summed_b = net.send(sums(2, hi), last2.at[1, hi], second, -1)
    yield [ends[3], direct_f, direct_b, summed_f, summed_b]
    add_into(net, sums(3), last2.at[0], last2.at[1])
    done.total = sums(3)
    fire(net, done)


def reduce_yz_scratch(rows, cols):
    return [pltpu.VMEM((rows // 2, cols), F32), pltpu.VMEM((rows // 2, cols), F32), pltpu.VMEM((rows, cols), F32),
            pltpu.VMEM((2, RING, rows // 2, cols), F32), pltpu.VMEM((2, RING, rows, cols), F32),
            pltpu.VMEM((2, rows // 2, cols), F32), pltpu.VMEM((2, rows, cols), F32)]


def norm_rows(x_ref, u_ref):
    def body(at):
        x = x_ref[at, :].astype(F32)
        u_ref[at, :] = (x * lax.rsqrt(jnp.mean(x * x, axis=-1, keepdims=True) + NORM_EPS)).astype(BF16)

    rows_loop(x_ref.shape[0], 16, body)


def norm_back_rows(x_ref, dy_ref, du_ref, dx_ref):
    def body(at):
        x = x_ref[at, :].astype(F32)
        du = du_ref[at, :]
        r = lax.rsqrt(jnp.mean(x * x, axis=-1, keepdims=True) + NORM_EPS)
        xr = x * r
        dx_ref[at, :] = (dy_ref[at, :].astype(F32) + r * (du - xr * jnp.mean(xr * du, axis=-1, keepdims=True))).astype(BF16)

    rows_loop(x_ref.shape[0], 16, body)


def add_rows(x_ref, y_ref, out_ref):
    def body(at):
        out_ref[at, :] = (x_ref[at, :].astype(F32) + y_ref[at, :]).astype(BF16)

    rows_loop(x_ref.shape[0], 16, body)


def call(body, out_shape, out_spaces, in_spaces, scratch, remote, local, collective_id, *args):
    spaces = {'v': pl.BlockSpec(memory_space=pltpu.VMEM), 'h': pl.BlockSpec(memory_space=pl.ANY)}

    def kernel(*refs):
        net = Net(*refs[-5:-1])
        net.tile_sems = refs[-1]
        body(net, *refs[:-5])
        net.finish()
        assert net.n_remote <= remote and net.n_local <= local, (net.n_remote, net.n_local)
        if PRINT:
            print(body.__name__, net.n_remote, net.n_local, round(net.now, 1))

    return pl.pallas_call(
        kernel, out_shape=out_shape, in_specs=[spaces[s] for s in in_spaces], out_specs=[spaces[s] for s in out_spaces],
        scratch_shapes=list(scratch) + [pltpu.SemaphoreType.DMA((remote,)), pltpu.SemaphoreType.DMA((remote,)), pltpu.SemaphoreType.DMA((local,)),
                                               pltpu.SemaphoreType.REGULAR((2,)), pltpu.SemaphoreType.DMA((2,))],
        compiler_params=pltpu.CompilerParams(collective_id=collective_id, has_side_effects=True, vmem_limit_bytes=67000000),
        cost_estimate=pl.CostEstimate(flops=10**8, bytes_accessed=10**7, transcendentals=0),
        name=body.__name__)(*args)


PRINT = False


WIDE = 512


def wide_loop(total, body):
    wide = min(WIDE, total)

    def step(k, carry):
        body(k, wide, pl.ds(pl.multiple_of(k * wide, wide), wide))
        return carry

    lax.fori_loop(0, total // wide, step, 0)


def flat(value):
    return value.reshape(value.shape[0] * value.shape[1], value.shape[2])


def dot_rows(a, b):
    return jnp.dot(flat(a), flat(b), preferred_element_type=F32)


def dot_cols(a, b):
    return lax.dot_general(flat(a), flat(b), CONTRACT_COLS, preferred_element_type=F32)


def gelu(a):
    return 0.5 * a * (1.0 + jnp.tanh(GELU_C * (a + 0.044715 * a * a * a)))


def hidden_rows(net, chip, u, up, a, s):
    at = pl.ds(chip * 2, 2)

    def body(_, wide, cols):
        pre = dot_rows(u[at], up[:, :, cols]).astype(BF16)
        a[at, :, cols] = pre.reshape(2, -1, wide)
        s[at, :, cols] = gelu(pre.astype(F32)).astype(BF16).reshape(2, -1, wide)

    wide_loop(up.shape[2], body)
    net.spend(2.4)


def down_rows(net, chip, s, down, part):
    at = pl.ds(chip * 2, 2)

    def body(_, wide, cols):
        part[:, :, cols] = dot_rows(s[at], down[:, :, cols]).reshape(2, -1, wide)

    wide_loop(down.shape[2], body)
    net.spend(1.8)


def hidden_back_rows(net, chip, dy, down, ds):
    at = pl.ds(chip * 2, 2)
    rows = down.shape[1]

    def body(k, wide, cols):
        blocks = pl.ds(k * (wide // rows), wide // rows)
        ds[at, :, cols] = dot_cols(dy[at], down[blocks]).astype(BF16).reshape(2, -1, wide)

    wide_loop(down.shape[0] * rows, body)
    net.spend(2.4)


def gelu_both(a):
    t = jnp.tanh(GELU_C * (a + 0.044715 * a * a * a))
    return 0.5 * a * (1.0 + t), 0.5 * (1.0 + t) + 0.5 * a * (1.0 - t * t) * (GELU_C * (1.0 + 3 * 0.044715 * a * a))


def hidden_turn_rows(net, chip, u, up, s, ds):
    at = pl.ds(chip * 2, 2)

    def body(_, wide, cols):
        pre = dot_rows(u[at], up[:, :, cols]).astype(BF16).astype(F32)
        value, slope = gelu_both(pre)
        s[at, :, cols] = value.astype(BF16).reshape(2, -1, wide)
        ds[at, :, cols] = (ds[at, :, cols].astype(F32) * slope.reshape(2, -1, wide)).astype(BF16)

    wide_loop(up.shape[2], body)
    net.spend(2.8)


def pre_back_rows(net, chip, dy, down, a, da):
    at = pl.ds(chip * 2, 2)
    rows = down.shape[1]

    def body(k, wide, cols):
        blocks = pl.ds(k * (wide // rows), wide // rows)
        ds = dot_cols(dy[at], down[blocks]).astype(BF16).astype(F32).reshape(2, -1, wide)
        da[at, :, cols] = (ds * gelu_both(a[at, :, cols].astype(F32))[1]).astype(BF16)

    wide_loop(down.shape[0] * rows, body)
    net.spend(2.8)


def input_back_rows(net, chip, da, up, part):
    at = pl.ds(chip * 2, 2)
    rows = up.shape[1]

    def body(k, wide, cols):
        blocks = pl.ds(k * (wide // rows), wide // rows)
        part[:, :, cols] = dot_cols(da[at], up[blocks]).reshape(2, -1, wide)

    wide_loop(up.shape[0] * rows, body)
    net.spend(2.2)


def stored_tiles(net, count, compute, stage, out):
    def store(t):
        return pltpu.make_async_copy(stage.at[t % 2], out(t), net.tile_sems.at[t % 2])

    def step(t, carry):
        @pl.when(t >= 2)
        def _():
            store(t - 2).wait()

        compute(t, stage.at[t % 2])
        store(t).start()
        return carry

    lax.fori_loop(0, count, step, 0)
    for t in range(max(count - 2, 0), count):
        store(t).wait()


def dot_tokens(a, b):
    return lax.dot_general(flat(a), flat(b), CONTRACT_ROWS, preferred_element_type=F32)


def grad_tiles(net, lhs, rhs, stage, out):
    _, blocks, rows, cols = stage.shape
    wide = blocks * rows

    def compute(t, slot):
        slot[...] = dot_tokens(lhs[:, :, pl.ds(pl.multiple_of(t * wide, wide), wide)], rhs[...]).reshape(blocks, rows, cols)

    stored_tiles(net, lhs.shape[2] // wide, compute, stage, lambda t: out.at[pl.ds(t * blocks, blocks)])
    net.spend(3.6 * lhs.shape[2] / 1024)


def solution(mesh):
    nl, nd = mesh.shape['local'], mesh.shape['data']
    tok_spec = P(BOTH_AXES, None)
    w_spec = P(None, BOTH_AXES, None)

    def device_fn(tokens, grad_out, w_up, w_down):
        num_layers, ur, ffn = w_up.shape
        dr = w_down.shape[1]
        rows, width = tokens.shape
        hidden = nl * dr
        shape = jax.ShapeDtypeStruct
        cols = w_up.reshape(num_layers, ur, nl, nd, dr).transpose(0, 3, 1, 2, 4).reshape(num_layers, nd, ur, hidden)
        up_full = shape((nl, nd * ur, hidden), BF16)
        down_full = shape((nl, dr, width), BF16)
        act_full = shape((nd, rows, width), BF16)
        hid_full = shape((nd, rows, hidden), BF16)
        own = shape((rows, width), BF16)
        part_vmem = pltpu.VMEM((RING, 2, rows, width), F32)
        rx = [part_vmem] + reduce_x_scratch(rows, width)
        ryz_up = reduce_yz_scratch(nd * ur, hidden)
        ryz_down = reduce_yz_scratch(dr, width)

        def vmem(like):
            return pltpu.VMEM(like.shape, like.dtype)

        def forward(net, x_ref, g_in, cols_in, down_in, block_out, u_out, a_out, s_out, up_out, down_out, next_out, g_out, ds_out, x_out,
                    u, g, u1, up0, down0, up1, down1, a, s, ds, part, *rx_scratch):
            net.barrier('dyz')
            blocks, got_u, got_g, got_u1, got_up0, got_down0, got_up1, got_down1, reduced = (Event() for _ in range(9))
            made = [Event() for _ in STEPS]
            hidden_made = [Event() for _ in STEPS]
            got_up0.rank = 2
            names = dict(blocks=blocks, got_u=got_u, got_g=got_g, got_u1=got_u1, got_up0=got_up0, got_down0=got_down0, got_up1=got_up1,
                         got_down1=got_down1, reduced=reduced)
            for name, event in names.items():
                event.name = name
            for k in range(RING):
                made[k].name, hidden_made[k].name = 'made%d' % k, 'hidden%d' % k
            net.spawn(exchange(net, cols_in, block_out, blocks))
            norm_rows(x_ref, u.at[net.data])
            net.spend(0.5)
            sent_u, sent_up0, sent_down0 = Event(name='sent_u'), Event(name='sent_up0'), Event(name='sent_down0')
            net.spawn(gather_x(net, u, got_u, sent_u))
            net.spawn(gather_yz(net, down_in.at[0], down0, 'z', got_down0, sent_down0))

            def up_first():
                yield [blocks]
                net.spawn(gather_yz(net, block_out.at[0], up0, 'y', got_up0, sent_up0))

            def second():
                yield [sent_up0, sent_down0]
                net.spawn(gather_yz(net, block_out.at[1], up1, 'y', got_up1))
                net.spawn(gather_yz(net, down_in.at[1], down1, 'z', got_down1))

            def grad():
                yield [net.load(g_in, g.at[net.data]), sent_u]
                net.spawn(gather_x(net, g, got_g))

            def save(event, *pairs):
                yield [event]
                yield [net.load(src, dst) for src, dst in pairs]

            def hidden_flow():
                yield [got_u, got_up0]
                for k, step in enumerate(STEPS):
                    hidden_rows(net, net.at('x', step), u, up0, a, s)
                    fire(net, hidden_made[k])
                    yield [Event(net.now, 2)]
                yield [net.load(a, a_out), net.load(s, s_out), net.load(u, u_out)]

            def down_flow():
                for k, step in enumerate(STEPS):
                    yield [hidden_made[k], got_down0, Event(0.0, 1)]
                    down_rows(net, net.at('x', step), s, down0, part.at[k])
                    fire(net, made[k])

            def act():
                yield [reduced]
                add_rows(x_ref, part.at[3, net.core], x_out)
                norm_rows(x_out, u1.at[net.data])
                net.spend(1.0)
                net.spawn(gather_x(net, u1, got_u1))

            def back_flow():
                for k, step in enumerate(STEPS):
                    yield [got_g, got_down1, Event(0.0, 3)]
                    hidden_back_rows(net, net.at('x', step), g, down1, ds)
                yield [net.load(ds, ds_out)]

            for flow in (up_first(), second(), grad(), hidden_flow(), down_flow(), act(), back_flow(),
                         reduce_x(net, part, made, rx_scratch, reduced),
                         save(got_up1, (up1, up_out)), save(got_down1, *[(down1.at[:, :, pl.ds(h * down_out.shape[3], down_out.shape[3])], down_out.at[h]) for h in range(2)]), save(got_u1, (u1, next_out)), save(got_g, (g, g_out))):
                net.spawn(flow)
            net.run()

        def turn(net, u_in, up_in, down_in, ds_in, g_in, u0_in, a0_in, s0_in, x_ref, g_own, block_in, w_down_in,
                 dy_ref, y_out, du_out, d_up0, d_down0, d_up1, d_down1, dw_up, dw_down,
                 u, up1, up0, down0, half_in, ds, s, stage_up, stage_down, part, *scratch):
            net.barrier('dyz')
            rx_scratch, s_up, s_down = scratch[:5], scratch[5:12], scratch[12:19]
            names = ('inputs', 'hidden', 'du_sent', 'reduced', 'got_dy', 'got_up0', 'got_down0', 'd_down1', 'd_up1', 'y_made', 'acts', 'd_down0', 'da0', 'd_up0', 'summed_up', 'summed_down', 'all_du')
            ev = {name: Event(name=name) for name in names}
            made = [Event(name='made%d' % k) for k in range(RING)]
            wide = half_in.shape[2]

            def columns(h):
                return pl.ds(h * wide, wide)

            net.spawn(gather_yz(net, w_down_in.at[0], down0, 'z', ev['got_down0']))
            net.spawn(gather_yz(net, block_in.at[0], up0, 'y', ev['got_up0']))
            net.spawn(reduce_x(net, part, made, rx_scratch, ev['reduced']))
            net.spawn(reduce_yz(net, d_up1, 'y', s_up, ev['d_up1'], ev['summed_up']))
            net.spawn(reduce_yz(net, d_down1, 'z', s_down, ev['d_down1'], ev['summed_down']))

            def layer1():
                yield [net.load(ds_in, ds), net.load(up_in, up1), net.load(u_in, u)]
                for k, step in enumerate(STEPS):
                    hidden_turn_rows(net, net.at('x', step), u, up1, s, ds)
                    if k == RING - 1:
                        fire(net, ev['hidden'])
                    yield [Event(net.now, 1)]
                    input_back_rows(net, net.at('x', step), ds, up1, part.at[k])
                    fire(net, made[k])
                    yield [Event(net.now, 1)]
                fire(net, ev['all_du'])

            def grads1():
                for h in range(2):
                    yield [net.load(g_in.at[:, :, columns(h)], half_in), Event(0.0, 2), ev['hidden']]
                    grad_tiles(net, s, half_in, stage_down, d_down1.at[:, :, columns(h)])
                fire(net, ev['d_down1'])
                yield [Event(net.now, 2)]
                for h in range(2):
                    grad_tiles(net, u.at[:, :, columns(h)], ds, stage_up, d_up1.at[pl.ds(h * (nl // 2), nl // 2)])
                    yield [Event(net.now, 2)]
                fire(net, ev['d_up1'])

            def layer1_out():
                yield [ev['all_du'], ev['d_up1']]
                yield [net.load(down_in.at[h], up1.at[:, pl.ds(h * dr, dr)]) for h in range(2)]
                for h in range(2):
                    def compute(chip, slot, h=h):
                        slot[...] = dot_rows(s[pl.ds(chip * 2, 2)], up1[:, pl.ds(h * dr, dr)]).reshape(2, rows, wide)

                    stored_tiles(net, RING, compute, stage_up, lambda chip, h=h: y_out.at[pl.ds(chip * 2, 2), :, columns(h)])
                    net.spend(3.6)
                    yield [Event(net.now, 3)]
                fire(net, ev['y_made'])
                yield [net.load(a0_in, up1.at[pl.ds(0, nd)]), net.load(s0_in, up1.at[pl.ds(nd, nd)])]
                fire(net, ev['acts'])

            def act():
                yield [ev['d_up1']]
                credit = net.grant(0, 'xp')
                yield [ev['reduced'], credit]
                norm_back_rows(x_ref, g_own, part.at[3, net.core], dy_ref)
                net.spend(0.7)
                yield [net.load(dy_ref, u.at[net.data])]
                net.spawn(gather_x(net, u, ev['got_dy']))

            def layer0():
                a0, s0 = up1.at[pl.ds(0, nd)], up1.at[pl.ds(nd, nd)]
                yield [ev['got_dy'], ev['acts'], Event(0.0, 2)]
                for h in range(2):
                    grad_tiles(net, s0, u.at[:, :, columns(h)], stage_down, d_down0.at[:, :, columns(h)])
                    yield [Event(net.now, 2)]
                yield [ev['got_down0'], Event(0.0, 2)]
                for step in STEPS:
                    pre_back_rows(net, net.at('x', step), u, down0, a0, ds)
                    yield [Event(net.now, 2)]
                fire(net, ev['da0'])
                for h in range(2):
                    yield [net.load(u0_in.at[:, :, columns(h)], half_in), Event(0.0, 2)]
                    grad_tiles(net, half_in, ds, stage_up, d_up0.at[pl.ds(h * (nl // 2), nl // 2)])
                net.drain(ev['reduced'].copies)
                copies = []
                for k, step in enumerate(STEPS):
                    yield [ev['got_up0'], Event(0.0, 2)]
                    input_back_rows(net, net.at('x', step), ds, up0, part.at[k])
                    copies.append(net.load(part.at[k], du_out.at[pl.ds(net.at('x', step) * 2, 2)]))
                yield copies

            def sums():
                yield [ev['summed_down']]
                yield [net.load(ev['summed_down'].total, dw_down)]

            def sums_up():
                yield [ev['summed_up']]
                net.spawn(exchange_back(net, ev['summed_up'].total, dw_up, Event()))

            for flow in (layer1(), grads1(), layer1_out(), act(), layer0(), sums(), sums_up()):
                net.spawn(flow)
            net.run()

        def last(net, du_ref, part_ref, dup_ref, ddown_ref, x_ref, dy_ref, x1_ref, dx_ref, out_ref, dw_up_ref, dw_down_ref, *scratch):
            net.barrier('dyz')
            r1, r2, s1, s2 = scratch[:6], scratch[6:12], scratch[12:19], scratch[19:26]
            reduced, out, summed1, summed2 = (Event() for _ in range(4))
            made1, made2 = [Event() for _ in STEPS], [Event() for _ in STEPS]
            load_parts(net, du_ref, r1[0], made1)
            net.spawn(reduce_x(net, r1[0], made1, r1[1:], reduced))
            net.spawn(reduce_yz(net, dup_ref, 'y', s1, None, summed1))
            net.spawn(reduce_yz(net, ddown_ref, 'z', s2, None, summed2))

            def act():
                yield [reduced]
                norm_back_rows(x_ref, dy_ref, r1[0].at[3, net.core], dx_ref)
                net.spend(0.7)

            def forward_out():
                yield [Event(20.0)]
                load_parts(net, part_ref, r2[0], made2)
                net.spawn(reduce_x(net, r2[0], made2, r2[1:], out))
                yield [out]
                add_rows(x1_ref, r2[0].at[3, net.core], out_ref)

            def grads():
                yield [summed1]
                net.spawn(exchange_back(net, summed1.total, dw_up_ref, Event()))
                yield [summed2]
                yield [net.load(summed2.total, dw_down_ref)]

            net.spawn(act())
            net.spawn(forward_out())
            net.spawn(grads())
            net.run()

        def own_up(d_up):
            return d_up.reshape(nd, ur, nl, dr).transpose(1, 2, 0, 3).reshape(ur, ffn)

        d_up_own, d_down_own = shape((nd, ur, hidden), F32), shape((dr, width), F32)

        blocks, u0, a0, s0, up1, down1, u1, g_full, ds1, x1 = call(
            forward, [shape((num_layers, nd * ur, hidden), BF16), act_full, hid_full, hid_full, up_full, shape((2, nl, dr, width // 2), BF16),
                      act_full, act_full, hid_full, own],
            'hhhhhhhhhv', 'vhhh',
            [vmem(act_full)] * 3 + [vmem(up_full), vmem(down_full)] * 2 + [vmem(hid_full)] * 3 + rx, 128, 32, 0,
            tokens, grad_out, cols, w_down)
        part_full = shape((nd, rows, width), F32)
        d_up_full, d_down_full = shape((nl, nd * ur, hidden), F32), shape((nl, dr, width), F32)
        dy0, part1, du0, d_up0, d_down0, _, _, dw_up1, dw_down1 = call(
            turn, [own, part_full, part_full, d_up_full, d_down_full, d_up_full, d_down_full, d_up_own, d_down_own], 'vhhhhhhhh', 'hhhhhhhhvvhh',
            [vmem(act_full), vmem(up_full), vmem(up_full), vmem(down_full), pltpu.VMEM((nd, rows, width // 2), BF16), vmem(hid_full), vmem(hid_full),
             pltpu.VMEM((2, 2, nd * ur, hidden), F32), pltpu.VMEM((2, nl // RING, dr, width // 2), F32)] + rx + ryz_up + ryz_down, 144, 64, 1,
            u1, up1, down1, ds1, g_full, u0, a0, s0, x1, grad_out, blocks, w_down)
        dx, x_out, dw_up0, dw_down0 = call(
            last, [own, own, d_up_own, d_down_own], 'vvhh', 'hhhhvvv', rx + rx + ryz_up + ryz_down, 96, 56, 2,
            du0, part1, d_up0, d_down0, tokens, dy0, x1)
        return x_out, dx, jnp.stack([own_up(dw_up0), own_up(dw_up1)]), jnp.stack([dw_down0, dw_down1])

    return jax.shard_map(device_fn, mesh=mesh, in_specs=(tok_spec, tok_spec, w_spec, w_spec), out_specs=(tok_spec, tok_spec, w_spec, w_spec), check_vma=False)
```

```python
import functools

import jax
import jax.numpy as jnp
from jax import lax
from jax.experimental import pallas as pl
from jax.experimental.pallas import tpu as pltpu
from jax.sharding import PartitionSpec as P

NORM_EPS = 1e-6
BOTH_AXES = ('local', 'data')
CONTRACT_ROWS = (((0,), (0,)), ((), ()))
CONTRACT_COLS = (((1,), (1,)), ((), ()))
MESH = pl.DeviceIdType.MESH
RING = 4
F32, BF16 = jnp.float32, jnp.bfloat16

LINK_RATE = 43.0e3
PAIR_RATE = 600e3
LOCAL_RATE = 3000e3
HOP = 2.5
SLACK = 1.0
GELU_C = 0.7978845608028654


class Event:
    def __init__(self, time=None, rank=0, name=''):
        self.time, self.rank, self.name = time, rank, name


class Copy:
    def __init__(self, desc, time, remote):
        self.desc, self.time, self.remote, self.rank = desc, time, remote, 0

    def wait(self):
        if self.remote:
            self.desc.wait_recv()
        else:
            self.desc.wait()


class Credit:
    def __init__(self, semaphore, count, time):
        self.semaphore, self.count, self.time, self.rank = semaphore, count, time, 0

    def wait(self):
        pl.semaphore_wait(self.semaphore, self.count)


class Net:
    def __init__(self, send_sems, recv_sems, local_sems, credit_sems):
        self.send_sems, self.recv_sems, self.local_sems, self.credit_sems = send_sems, recv_sems, local_sems, credit_sems
        self.n_remote = self.n_local = 0
        self.now = 0.0
        self.free = {}
        self.sent = []
        self.flows = []
        here = lax.axis_index('local')
        there = lax.axis_index('data')
        self.data = there
        self.pos = {'z': here // RING, 'y': here % RING, 'x': there // 2}
        self.core = there % 2

    def at(self, axis, step):
        return (self.pos[axis] + (step + RING)) % RING

    def device(self, axis, step):
        if axis == 'p':
            return {'data': self.pos['x'] * 2 + (1 - self.core)}
        if axis == 'd':
            return {'data': (self.data + step) % (2 * RING)}
        to = self.at(axis, step)
        if axis == 'x':
            return {'data': to * 2 + self.core}
        if axis == 'y':
            return {'local': self.pos['z'] * RING + to}
        return {'local': to * RING + self.pos['y']}

    def peers(self, axes):
        return [(axis, step) for axis in axes for step in ((1, -1) if axis in 'xyz' else (1,) if axis == 'p' else range(1, 2 * RING))]

    def signal(self, semaphore, axes):
        for axis, step in self.peers(axes):
            pl.semaphore_signal(semaphore, inc=1, device_id=self.device(axis, step), device_id_type=MESH)

    def barrier(self, axes):
        semaphore = pltpu.get_barrier_semaphore()
        self.signal(semaphore, axes)
        pl.semaphore_wait(semaphore, len(self.peers(axes)))

    def grant(self, k, axes):
        self.signal(self.credit_sems.at[k], axes)
        return Credit(self.credit_sems.at[k], len(self.peers(axes)), self.now + HOP)

    def drain(self, copies):
        for copy in copies:
            copy.desc.wait_send()
            self.sent.remove(copy)

    def send(self, src, dst, axis, step=1):
        k = self.n_remote
        self.n_remote += 1
        desc = pltpu.make_async_remote_copy(
            src_ref=src, dst_ref=dst, send_sem=self.send_sems.at[k], recv_sem=self.recv_sems.at[k],
            device_id=self.device(axis, step), device_id_type=MESH)
        desc.start()
        size = 1
        for n in dst.shape:
            size *= n
        size *= dst.dtype.itemsize
        rate = PAIR_RATE if axis == 'p' else LINK_RATE
        key = (axis, step)
        done = max(self.free.get(key, 0.0), self.now) + size / rate
        self.free[key] = done
        copy = Copy(desc, done + HOP, True)
        self.sent.append(copy)
        return copy

    def load(self, src, dst):
        k = self.n_local
        self.n_local += 1
        desc = pltpu.make_async_copy(src, dst, self.local_sems.at[k])
        desc.start()
        size = 1
        for n in dst.shape:
            size *= n
        return Copy(desc, self.now + 1.0 + size * dst.dtype.itemsize / LOCAL_RATE, False)

    def spend(self, microseconds):
        self.now += microseconds

    def spawn(self, flow):
        self.step(flow)

    def step(self, flow):
        try:
            self.flows.append((flow, next(flow)))
        except StopIteration:
            pass

    def run(self):
        while self.flows:
            best = None
            for k, (_, items) in enumerate(self.flows):
                if any(item.time is None for item in items):
                    continue
                time = max([item.time for item in items] + [0.0])
                late = max(item.rank for item in items)
                rank = (max(time, self.now) + (SLACK if late else 0.0), late, time)
                if best is None or rank < best[0]:
                    best = (rank, k, time)
            _, k, time = best
            flow, items = self.flows.pop(k)
            for item in items:
                if not isinstance(item, Event):
                    item.wait()
            self.now = max(self.now, time)
            self.step(flow)

    def finish(self):
        for copy in self.sent:
            copy.desc.wait_send()


def rows_loop(rows, chunk, body):
    chunk = min(chunk, rows)

    def step(k, carry):
        body(pl.ds(pl.multiple_of(k * chunk, chunk), chunk))
        return carry

    lax.fori_loop(0, rows // chunk, step, 0)


def add_into(net, dst, *others):
    rows, cols = dst.shape

    def body(at):
        total = dst[at, :]
        for other in others:
            total = total + other[at, :]
        dst[at, :] = total

    rows_loop(rows, 16, body)
    net.spend(rows * cols * 4 * (1 + len(others)) / 4e6)


def fire(net, event):
    event.time = net.now
    if PRINT and event.name:
        print('   %7.1f %s' % (net.now, event.name))


def exchange(net, src, dst, done):
    rows = src.shape[2]

    def mine():
        return dst.at[:, pl.ds(pl.multiple_of(net.data * rows, rows), rows)]

    own = net.load(src.at[:, net.data], mine())
    copies = [net.send(src.at[:, (net.data + k) % (2 * RING)], mine(), 'd', k) for k in range(1, 2 * RING)]
    yield [own] + copies
    fire(net, done)


def exchange_back(net, src, dst, done):
    rows = dst.shape[1]

    def block(k):
        return src.at[pl.ds(pl.multiple_of(k * rows, rows), rows)]

    own = net.load(block(net.data), dst.at[net.data])
    done.copies = [net.send(block((net.data + k) % (2 * RING)), dst.at[net.data], 'd', k) for k in range(1, 2 * RING)]
    yield [own] + done.copies
    fire(net, done)


def gather_x(net, full, done, issued=None):
    half = full.shape[1] // 2
    lo, hi = pl.ds(0, half), pl.ds(half, half)

    def block(step):
        return full.at[net.at('x', step) * 2 + net.core]

    def part(step, rows):
        return full.at[net.at('x', step) * 2 + net.core, rows]

    forth = net.send(block(0), block(0), 'x', 1)
    back = net.send(block(0), block(0), 'x', -1)
    pair = [net.send(block(0), block(0), 'p')]
    yield [forth]
    forth = net.send(part(-1, lo), part(-1, lo), 'x', 1)
    pair.append(net.send(block(-1), block(-1), 'p'))
    yield [back]
    back = net.send(part(1, hi), part(1, hi), 'x', -1)
    pair.append(net.send(block(1), block(1), 'p'))
    if issued is not None:
        fire(net, issued)
    yield [forth, back]
    pair.append(net.send(block(2), block(2), 'p'))
    yield pair
    fire(net, done)


def gather_yz(net, own, full, first, done, issued=None, offset=0, near=False):
    second = 'y' if first == 'z' else 'z'
    size = own.shape[0]
    half = size // 2
    all_rows, lo, hi = pl.ds(offset, size), pl.ds(offset, half), pl.ds(offset + half, half)

    def part(one, two, rows):
        return full.at[yz_index(net, first, one, two), rows]

    ends = []
    left = [3 if near else RING]

    def relay(one, forth, back, end):
        if not near:
            yield [forth]
            forth = net.send(part(one, -1, lo), part(one, -1, lo), second, 1)
            yield [back]
            back = net.send(part(one, 1, hi), part(one, 1, hi), second, -1)
        left[0] -= 1
        if left[0] == 0 and issued is not None:
            fire(net, issued)
        yield [forth, back]
        fire(net, end)

    def spread(src, one):
        forth = net.send(src, part(one, 0, all_rows), second, 1)
        back = net.send(src, part(one, 0, all_rows), second, -1)
        end = Event()
        ends.append(end)
        net.spawn(relay(one, forth, back, end))

    mine = net.load(own, part(0, 0, all_rows))
    forth = net.send(own, part(0, 0, all_rows), first, 1)
    back = net.send(own, part(0, 0, all_rows), first, -1)
    spread(own, 0)
    yield [forth]
    if not near:
        forth = net.send(part(-1, 0, lo), part(-1, 0, lo), first, 1)
    spread(part(-1, 0, all_rows), -1)
    yield [back]
    if not near:
        back = net.send(part(1, 0, hi), part(1, 0, hi), first, -1)
    spread(part(1, 0, all_rows), 1)
    if not near:
        yield [forth, back]
        spread(part(2, 0, all_rows), 2)
    yield [mine] + ends
    fire(net, done)


def yz_index(net, first, one, two):
    at_one, at_two = net.at(first, one), net.at('y' if first == 'z' else 'z', two)
    return at_one * RING + at_two if first == 'z' else at_two * RING + at_one


FAR = [(2, 0), (2, 1), (2, -1), (2, 2), (0, 2), (1, 2), (-1, 2)]


STEPS = (2, 1, -1, 0)


def reduce_x(net, part, made, scratch, done):
    other, relay_f, relay_b, last_f, last_b = scratch
    half = part.shape[2] // 2
    lo, hi = pl.ds(0, half), pl.ds(half, half)

    def acc(k, rows=None):
        return part.at[k, net.core] if rows is None else part.at[k, net.core, rows]

    pairs = [None] * RING
    ready = [Event() for _ in STEPS]

    def pair(k):
        yield [made[k]]
        pairs[k] = net.send(part.at[k, 1 - net.core], other.at[k], 'p')
        yield [pairs[k]]
        add_into(net, acc(k), other.at[k])
        fire(net, ready[k])

    for k in range(RING):
        net.spawn(pair(k))
    yield [ready[0]]
    first_f = net.send(acc(0, lo), relay_f, 'x', 1)
    first_b = net.send(acc(0, hi), relay_b, 'x', -1)
    yield [ready[1]]
    direct_f = net.send(acc(1, hi), last_f.at[hi], 'x', 1)
    yield [ready[2]]
    direct_b = net.send(acc(2, lo), last_b.at[lo], 'x', -1)
    yield [first_f]
    add_into(net, acc(1, lo), relay_f)
    summed_f = net.send(acc(1, lo), last_f.at[lo], 'x', 1)
    yield [first_b]
    add_into(net, acc(2, hi), relay_b)
    summed_b = net.send(acc(2, hi), last_b.at[hi], 'x', -1)
    yield [ready[3], direct_f, direct_b, summed_f, summed_b]
    add_into(net, acc(3), last_f, last_b)
    done.copies = pairs + [first_f, first_b, direct_f, direct_b, summed_f, summed_b]
    fire(net, done)


def reduce_x_scratch(rows, cols):
    return [pltpu.VMEM((RING, rows, cols), F32), pltpu.VMEM((rows // 2, cols), F32), pltpu.VMEM((rows // 2, cols), F32),
            pltpu.VMEM((rows, cols), F32), pltpu.VMEM((rows, cols), F32)]


def load_parts(net, src, part, made):
    for k, step in enumerate(STEPS):
        def bring(k=k, step=step):
            yield [net.load(src.at[pl.ds(net.at('x', step) * 2, 2)], part.at[k])]
            fire(net, made[k])

        net.spawn(bring())


class Sums:
    def __init__(self, net, first, scratch):
        self.net, self.first, self.scratch = net, first, scratch
        self.second = 'y' if first == 'z' else 'z'
        self.free = [Event(0.0) for _ in range(3)]
        self.relays_free, self.all_free = Event(0.0), Event(0.0)
        self.phase1 = []
        self.phase2 = []

    def release(self, credit, axes, copies, event):
        self.net.drain(copies)
        yield [self.net.grant(credit, axes)]
        fire(self.net, event)

    def run(self, part, start, done, credit=None):
        net, first, second = self.net, self.first, self.second
        ahead, behind, mine, relay1, last1, relay2, last2 = self.scratch
        relays_free, all_free = self.relays_free, self.all_free
        half = mine.shape[0] // 2
        lo, hi, all_rows = pl.ds(0, half), pl.ds(half, half), pl.ds(0, 2 * half)

        def term(one, two, rows=all_rows):
            return part.at[yz_index(net, first, one, two), rows]

        def bring(gate, src, dst, got):
            yield [gate, start]
            yield [net.load(src, dst)]
            fire(net, got)

        free = [[gate] + [Event() for _ in range(RING)] for gate in self.free]
        self.free = [events[RING] for events in free]
        got = [[Event() for _ in range(RING)] for _ in range(3)]
        ends = [Event() for _ in STEPS]
        relay_copies = []

        def ring(k):
            two = STEPS[k]
            net.spawn(bring(free[0][k], term(1, two, lo), ahead, got[0][k]))
            net.spawn(bring(free[1][k], term(-1, two, hi), behind, got[1][k]))
            net.spawn(bring(free[2][k], term(0, two), mine, got[2][k]))
            first_f = net.send(term(2, two, lo), relay1.at[0, k], first, 1)
            first_b = net.send(term(2, two, hi), relay1.at[1, k], first, -1)
            direct, sent = [], Event()

            def directs():
                yield [all_free]
                direct.append(net.send(term(1, two, hi), last1.at[0, k, hi], first, 1))
                direct.append(net.send(term(-1, two, lo), last1.at[1, k, lo], first, -1))
                fire(net, sent)

            net.spawn(directs())
            yield [first_f, got[0][k]]
            add_into(net, relay1.at[0, k], ahead)
            fire(net, free[0][k + 1])
            yield [all_free]
            summed_f = net.send(relay1.at[0, k], last1.at[0, k, lo], first, 1)
            yield [first_b, got[1][k]]
            add_into(net, relay1.at[1, k], behind)
            fire(net, free[1][k + 1])
            summed_b = net.send(relay1.at[1, k], last1.at[1, k, hi], first, -1)
            relay_copies.extend([summed_f, summed_b])
            yield [sent]
            yield direct + [summed_f, summed_b, got[2][k]]
            add_into(net, last1.at[0, k], last1.at[1, k], mine)
            fire(net, free[2][k + 1])
            fire(net, ends[k])

        def sums(k, rows=all_rows):
            return last1.at[0, k, rows]

        yield [start, relays_free]
        for k in range(RING):
            net.spawn(ring(k))
        if credit is not None:
            self.relays_free = Event()

            def relays():
                yield ends
                yield from self.release(credit, first, relay_copies, self.relays_free)

            net.spawn(relays())
        yield [ends[0]]
        first_f = net.send(sums(0, lo), relay2.at[0], second, 1)
        first_b = net.send(sums(0, hi), relay2.at[1], second, -1)
        yield [ends[1]]
        direct_f = net.send(sums(1, hi), last2.at[0, hi], second, 1)
        yield [ends[2]]
        direct_b = net.send(sums(2, lo), last2.at[1, lo], second, -1)
        yield [first_f]
        add_into(net, sums(1, lo), relay2.at[0])
        summed_f = net.send(sums(1, lo), last2.at[0, lo], second, 1)
        yield [first_b]
        add_into(net, sums(2, hi), relay2.at[1])
        summed_b = net.send(sums(2, hi), last2.at[1, hi], second, -1)
        yield [ends[3], direct_f, direct_b, summed_f, summed_b]
        add_into(net, sums(3), last2.at[0], last2.at[1])
        done.total = sums(3)
        done.copies = [first_f, first_b, direct_f, direct_b, summed_f, summed_b]
        fire(net, done)


def reduce_yz_scratch(rows, cols):
    return [pltpu.VMEM((rows // 2, cols), F32), pltpu.VMEM((rows // 2, cols), F32), pltpu.VMEM((rows, cols), F32),
            pltpu.VMEM((2, RING, rows // 2, cols), F32), pltpu.VMEM((2, RING, rows, cols), F32),
            pltpu.VMEM((2, rows // 2, cols), F32), pltpu.VMEM((2, rows, cols), F32)]


def norm_rows(x_ref, u_ref):
    def body(at):
        x = x_ref[at, :].astype(F32)
        u_ref[at, :] = (x * lax.rsqrt(jnp.mean(x * x, axis=-1, keepdims=True) + NORM_EPS)).astype(BF16)

    rows_loop(x_ref.shape[0], 16, body)


def norm_back_rows(x_ref, dy_ref, du_ref, dx_ref):
    def body(at):
        x = x_ref[at, :].astype(F32)
        du = du_ref[at, :]
        r = lax.rsqrt(jnp.mean(x * x, axis=-1, keepdims=True) + NORM_EPS)
        xr = x * r
        dx_ref[at, :] = (dy_ref[at, :].astype(F32) + r * (du - xr * jnp.mean(xr * du, axis=-1, keepdims=True))).astype(BF16)

    rows_loop(x_ref.shape[0], 16, body)


def add_rows(x_ref, y_ref, out_ref):
    def body(at):
        out_ref[at, :] = (x_ref[at, :].astype(F32) + y_ref[at, :]).astype(BF16)

    rows_loop(x_ref.shape[0], 16, body)


def swap_halves(even, odd):
    low = lax.broadcasted_iota(jnp.int32, even.shape, len(even.shape) - 1) < even.shape[-1] // 2
    shift = even.shape[-1] // 2
    axis = len(even.shape) - 1
    return jnp.where(low, even, pltpu.roll(odd, shift, axis)), jnp.where(low, pltpu.roll(even, shift, axis), odd)


def split_columns(w_ref, cols_ref):
    tile = w_ref.shape[2] // (4 * RING * RING)
    for l in range(w_ref.shape[0]):
        for x in range(RING):
            for p in range(cols_ref.shape[3] // tile):
                pair = [w_ref[l, :, pl.ds((i * RING + x) * tile, tile)].astype(F32) for i in (2 * p, 2 * p + 1)]
                for c, value in enumerate(swap_halves(*pair)):
                    cols_ref[l, 2 * x + c, :, pl.ds(p * tile, tile)] = value.astype(cols_ref.dtype)


def join_columns(cols_ref, w_ref):
    tile = w_ref.shape[1] // (4 * RING * RING)
    for x in range(RING):
        for p in range(cols_ref.shape[2] // tile):
            pair = [cols_ref[2 * x + c, :, pl.ds(p * tile, tile)] for c in range(2)]
            for i, value in zip((2 * p, 2 * p + 1), swap_halves(*pair)):
                w_ref[:, pl.ds((i * RING + x) * tile, tile)] = value


def call(body, out_shape, out_spaces, in_spaces, scratch, remote, local, collective_id, *args):
    spaces = {'v': pl.BlockSpec(memory_space=pltpu.VMEM), 'h': pl.BlockSpec(memory_space=pl.ANY)}

    def kernel(*refs):
        net = Net(*refs[-5:-1])
        net.tile_sems = refs[-1]
        body(net, *refs[:-5])
        net.finish()
        assert net.n_remote <= remote and net.n_local <= local, (net.n_remote, net.n_local)
        if PRINT:
            print(body.__name__, net.n_remote, net.n_local, round(net.now, 1))

    return pl.pallas_call(
        kernel, out_shape=out_shape, in_specs=[spaces[s] for s in in_spaces], out_specs=[spaces[s] for s in out_spaces],
        scratch_shapes=list(scratch) + [pltpu.SemaphoreType.DMA((remote,)), pltpu.SemaphoreType.DMA((remote,)), pltpu.SemaphoreType.DMA((local,)),
                                               pltpu.SemaphoreType.REGULAR((8,)), pltpu.SemaphoreType.DMA((2,))],
        compiler_params=pltpu.CompilerParams(collective_id=collective_id, has_side_effects=True, vmem_limit_bytes=67000000),
        cost_estimate=pl.CostEstimate(flops=10**8, bytes_accessed=10**7, transcendentals=0),
        name=body.__name__)(*args)


PRINT = False


WIDE = 512


def wide_loop(total, body):
    wide = min(WIDE, total)

    def step(k, carry):
        body(k, wide, pl.ds(pl.multiple_of(k * wide, wide), wide))
        return carry

    lax.fori_loop(0, total // wide, step, 0)


def flat(value):
    return value.reshape(value.shape[0] * value.shape[1], value.shape[2])


def dot_rows(a, b):
    return jnp.dot(flat(a), flat(b), preferred_element_type=F32)


def dot_cols(a, b):
    return lax.dot_general(flat(a), flat(b), CONTRACT_COLS, preferred_element_type=F32)


def gelu(a):
    return 0.5 * a * (1.0 + jnp.tanh(GELU_C * (a + 0.044715 * a * a * a)))


def hidden_rows(net, chip, u, up, a, s):
    at = pl.ds(chip * 2, 2)

    def body(_, wide, cols):
        pre = dot_rows(u[at], up[:, :, cols]).astype(BF16)
        a[at, :, cols] = pre.reshape(2, -1, wide)
        s[at, :, cols] = gelu(pre.astype(F32)).astype(BF16).reshape(2, -1, wide)

    wide_loop(up.shape[2], body)
    net.spend(1.4)


def down_rows(net, chip, s, down, part):
    at = pl.ds(chip * 2, 2)

    def body(_, wide, cols):
        part[:, :, cols] = dot_rows(s[at], down[:, :, cols]).reshape(2, -1, wide)

    wide_loop(down.shape[2], body)
    net.spend(1.5)


def hidden_back_rows(net, chip, dy, down, ds):
    at = pl.ds(chip * 2, 2)
    rows = down.shape[1]

    def body(k, wide, cols):
        blocks = pl.ds(k * (wide // rows), wide // rows)
        ds[at, :, cols] = dot_cols(dy[at], down[blocks]).astype(BF16).reshape(2, -1, wide)

    wide_loop(down.shape[0] * rows, body)
    net.spend(1.4)


def gelu_both(a):
    t = jnp.tanh(GELU_C * (a + 0.044715 * a * a * a))
    return 0.5 * a * (1.0 + t), 0.5 * (1.0 + t) + 0.5 * a * (1.0 - t * t) * (GELU_C * (1.0 + 3 * 0.044715 * a * a))


def hidden_turn_rows(net, chip, u, up, s, ds):
    at = pl.ds(chip * 2, 2)

    def body(_, wide, cols):
        pre = dot_rows(u[at], up[:, :, cols]).astype(BF16).astype(F32)
        value, slope = gelu_both(pre)
        s[at, :, cols] = value.astype(BF16).reshape(2, -1, wide)
        ds[at, :, cols] = (ds[at, :, cols].astype(F32) * slope.reshape(2, -1, wide)).astype(BF16)

    wide_loop(up.shape[2], body)
    net.spend(1.8)


def pre_back_rows(net, chip, dy, down, a, da):
    at = pl.ds(chip * 2, 2)
    rows = down.shape[1]

    def body(k, wide, cols):
        blocks = pl.ds(k * (wide // rows), wide // rows)
        ds = dot_cols(dy[at], down[blocks]).astype(BF16).astype(F32).reshape(2, -1, wide)
        da[at, :, cols] = (ds * gelu_both(a[at, :, cols].astype(F32))[1]).astype(BF16)

    wide_loop(down.shape[0] * rows, body)
    net.spend(1.9)


def input_back_rows(net, chip, da, up, part):
    at = pl.ds(chip * 2, 2)
    rows = up.shape[1]

    def body(k, wide, cols):
        blocks = pl.ds(k * (wide // rows), wide // rows)
        part[:, :, cols] = dot_cols(da[at], up[blocks]).reshape(2, -1, wide)

    wide_loop(up.shape[0] * rows, body)
    net.spend(1.6)


def stored_tiles(net, count, compute, stage, out):
    def store(t):
        return pltpu.make_async_copy(stage.at[t % 2], out(t), net.tile_sems.at[t % 2])

    def step(t, carry):
        @pl.when(t >= 2)
        def _():
            store(t - 2).wait()

        compute(t, stage.at[t % 2])
        store(t).start()
        return carry

    lax.fori_loop(0, count, step, 0)
    for t in range(max(count - 2, 0), count):
        store(t).wait()


def dot_tokens(a, b):
    return lax.dot_general(flat(a), flat(b), CONTRACT_ROWS, preferred_element_type=F32)


def grad_tiles(net, lhs, rhs, stage, out):
    _, blocks, rows, cols = stage.shape
    wide = blocks * rows

    def compute(t, slot):
        slot[...] = dot_tokens(lhs[:, :, pl.ds(pl.multiple_of(t * wide, wide), wide)], rhs[...]).reshape(blocks, rows, cols)

    stored_tiles(net, lhs.shape[2] // wide, compute, stage, lambda t: out.at[pl.ds(t * blocks, blocks)])
    net.spend(3.2 * lhs.shape[2] / 1024)


def solution(mesh):
    nl, nd = mesh.shape['local'], mesh.shape['data']
    tok_spec = P(BOTH_AXES, None)
    w_spec = P(None, BOTH_AXES, None)

    def device_fn(tokens, grad_out, w_up, w_down):
        num_layers, ur, ffn = w_up.shape
        dr = w_down.shape[1]
        rows, width = tokens.shape
        hidden = nl * dr
        shape = jax.ShapeDtypeStruct
        up_full = shape((nl, nd * ur, hidden), BF16)
        down_full = shape((nl, dr, width), BF16)
        act_full = shape((nd, rows, width), BF16)
        hid_full = shape((nd, rows, hidden), BF16)
        own = shape((rows, width), BF16)
        part_vmem = pltpu.VMEM((RING, 2, rows, width), F32)
        rx = [part_vmem] + reduce_x_scratch(rows, width)
        ryz_up = reduce_yz_scratch(nd * ur, hidden)
        ryz_down = reduce_yz_scratch(dr, width)

        def vmem(like):
            return pltpu.VMEM(like.shape, like.dtype)

        def forward(net, x_ref, g_in, w_up_ref, down_in, block_out, u_out, a_out, s_out, up_out, down_out, next_out, g_out, ds_out, keep_out, x_out,
                    cols, u, g, u1, up0, down0, up1, down1, a, s, ds, part, *rx_scratch):
            net.barrier('dyz')
            blocks, got_u, got_g, got_u1, got_up0, got_down0, got_up1, got_down1, reduced = (Event() for _ in range(9))
            made = [Event() for _ in STEPS]
            hidden_made = [Event() for _ in STEPS]
            got_up0.rank = 2
            names = dict(blocks=blocks, got_u=got_u, got_g=got_g, got_u1=got_u1, got_up0=got_up0, got_down0=got_down0, got_up1=got_up1,
                         got_down1=got_down1, reduced=reduced)
            for name, event in names.items():
                event.name = name
            for k in range(RING):
                made[k].name, hidden_made[k].name = 'made%d' % k, 'hidden%d' % k
            split_columns(w_up_ref, cols)
            net.spawn(exchange(net, cols, block_out, blocks))
            norm_rows(x_ref, u.at[net.data])
            net.spend(0.5)
            sent_u, sent_up0, sent_down0 = Event(name='sent_u'), Event(name='sent_up0'), Event(name='sent_down0')
            net.spawn(gather_x(net, u, got_u, sent_u))
            net.spawn(gather_yz(net, down_in.at[0], down0, 'z', got_down0, sent_down0))

            def up_first():
                yield [blocks]
                net.spawn(gather_yz(net, block_out.at[0], up0, 'y', got_up0, sent_up0))

            def second():
                yield [sent_up0, sent_down0]
                net.spawn(gather_yz(net, block_out.at[1], up1, 'y', got_up1))
                net.spawn(gather_yz(net, down_in.at[1], down1, 'z', got_down1))

            def grad():
                yield [net.load(g_in, g.at[net.data]), sent_u]
                net.spawn(gather_x(net, g, got_g))

            def save(event, *pairs):
                yield [event]
                yield [net.load(src, dst) for src, dst in pairs]

            def hidden_flow():
                yield [got_u, got_up0]
                for k, step in enumerate(STEPS):
                    hidden_rows(net, net.at('x', step), u, up0, a, s)
                    fire(net, hidden_made[k])
                    yield [Event(net.now, 2)]
                yield [net.load(a, a_out), net.load(s, s_out), net.load(u, u_out)]

            def down_flow():
                for k, step in enumerate(STEPS):
                    yield [hidden_made[k], got_down0, Event(0.0, 1)]
                    down_rows(net, net.at('x', step), s, down0, part.at[k])
                    fire(net, made[k])
                yield [net.load(down0.at[yz_index(net, 'z', *far)], keep_out.at[k]) for k, far in enumerate(FAR)]

            def act():
                yield [reduced]
                add_rows(x_ref, part.at[3, net.core], x_out)
                norm_rows(x_out, u1.at[net.data])
                net.spend(1.0)
                net.spawn(gather_x(net, u1, got_u1))

            def back_flow():
                for k, step in enumerate(STEPS):
                    yield [got_g, got_down1, Event(0.0, 3)]
                    hidden_back_rows(net, net.at('x', step), g, down1, ds)
                yield [net.load(ds, ds_out)]

            for flow in (up_first(), second(), grad(), hidden_flow(), down_flow(), act(), back_flow(),
                         reduce_x(net, part, made, rx_scratch, reduced),
                         save(got_up1, (up1, up_out)), save(got_down1, *[(down1.at[:, :, pl.ds(h * down_out.shape[3], down_out.shape[3])], down_out.at[h]) for h in range(2)]), save(got_u1, (u1, next_out)), save(got_g, (g, g_out))):
                net.spawn(flow)
            net.run()

        def turn(net, u_in, up_in, down_in, ds_in, g_in, u0_in, a0_in, s0_in, keep_in, x_ref, x0_ref, g_own, block_in, w_down_in,
                 x_out, dx_out, d_up0, d_down0, d_up1, d_down1, dw_up1, dw_down1, dw_up0, dw_down0,
                 dy, u, up1, up0, down0, half_in, ds, s, stage_up, stage_down, part, *scratch):
            net.barrier('dyz')
            rx_scratch = scratch[:5]
            sums_up, sums_down = Sums(net, 'y', scratch[5:12]), Sums(net, 'z', scratch[12:19])
            names = ('hidden', 'all_du', 'reduced', 'sent_dy', 'got_dy', 'got_up0', 'got_up0_rest', 'got_down0', 'd_down1', 'd_up1', 'y_reduced', 'acts',
                     'd_down0', 'd_up0', 'du_reduced', 'sum_up1', 'sum_down1', 'sum_up0', 'sum_down0', 'out_up1', 'out_up0')
            ev = {name: Event(name=name) for name in names}
            made, y_made, du_made = ([Event(name='%s%d' % (name, k)) for k in range(RING)] for name in ('made', 'y_made', 'du_made'))
            wide = half_in.shape[2]
            top = nd * ur * 3 // 4

            def columns(h):
                return pl.ds(h * wide, wide)

            net.spawn(gather_yz(net, w_down_in.at[0], down0, 'z', ev['got_down0'], near=True))
            net.spawn(gather_yz(net, block_in.at[0, pl.ds(0, top)], up0, 'y', ev['got_up0']))
            net.spawn(gather_yz(net, block_in.at[0, pl.ds(top, nd * ur - top)], up0, 'z', ev['got_up0_rest'], offset=top))
            net.spawn(reduce_x(net, part, made, rx_scratch, ev['reduced']))
            net.spawn(sums_up.run(d_up1, ev['d_up1'], ev['sum_up1'], 3))
            net.spawn(sums_down.run(d_down1, ev['d_down1'], ev['sum_down1'], 4))

            def layer1():
                yield [net.load(ds_in, ds), net.load(up_in, up1), net.load(u_in, u)]
                for k, step in enumerate(STEPS):
                    hidden_turn_rows(net, net.at('x', step), u, up1, s, ds)
                    if k == RING - 1:
                        fire(net, ev['hidden'])
                    yield [Event(net.now, 1)]
                    input_back_rows(net, net.at('x', step), ds, up1, part.at[k])
                    fire(net, made[k])
                    yield [Event(net.now, 1)]
                fire(net, ev['all_du'])

            def grads1():
                for h in range(2):
                    yield [net.load(g_in.at[:, :, columns(h)], half_in), Event(0.0, 2), ev['hidden']]
                    grad_tiles(net, s, half_in, stage_down, d_down1.at[:, :, columns(h)])
                fire(net, ev['d_down1'])
                yield [Event(net.now, 2)]
                for h in range(2):
                    grad_tiles(net, u.at[:, :, columns(h)], ds, stage_up, d_up1.at[pl.ds(h * (nl // 2), nl // 2)])
                    yield [Event(net.now, 2)]
                fire(net, ev['d_up1'])

            def act():
                yield [ev['d_up1']]
                credit = net.grant(0, 'xp')
                yield [ev['reduced'], credit]
                norm_back_rows(x_ref, g_own, part.at[3, net.core], dy)
                net.spend(0.7)
                yield [net.load(dy, u.at[net.data])]
                net.spawn(gather_x(net, u, ev['got_dy'], ev['sent_dy']))

            def layer1_out():
                yield [ev['all_du'], ev['d_up1']]
                yield [net.load(down_in.at[h], up1.at[:, pl.ds(h * dr, dr)]) for h in range(2)]
                yield [ev['reduced'], ev['sent_dy']]
                net.drain(ev['reduced'].copies)
                yield [net.grant(1, 'xp')]
                net.spawn(reduce_x(net, part, y_made, rx_scratch, ev['y_reduced']))
                for k, step in enumerate(STEPS):
                    chip = net.at('x', step)
                    for h in range(2):
                        net.spend(-0.7)
                        down_rows(net, chip, s, up1.at[:, pl.ds(h * dr, dr)], part.at[k, :, :, columns(h)])
                    fire(net, y_made[k])
                    yield [Event(net.now, 2)]
                yield [net.load(a0_in, up1.at[pl.ds(0, nd)]), net.load(s0_in, up1.at[pl.ds(nd, nd)])]
                fire(net, ev['acts'])
                yield [ev['y_reduced']]
                add_rows(x_ref, part.at[3, net.core], x_out)

            def layer0():
                a0, s0 = up1.at[pl.ds(0, nd)], up1.at[pl.ds(nd, nd)]
                yield [ev['got_dy'], ev['acts'], Event(0.0, 2)]
                for h in range(2):
                    grad_tiles(net, s0, u.at[:, :, columns(h)], stage_down, d_down0.at[:, :, columns(h)])
                    yield [Event(net.now, 2)]
                fire(net, ev['d_down0'])
                yield [ev['got_down0'], Event(0.0, 2)] + [net.load(keep_in.at[k], down0.at[yz_index(net, 'z', *far)]) for k, far in enumerate(FAR)]
                for step in STEPS:
                    pre_back_rows(net, net.at('x', step), u, down0, a0, ds)
                    yield [Event(net.now, 2)]
                for h in range(2):
                    yield [net.load(u0_in.at[:, :, columns(h)], half_in), Event(0.0, 2)]
                    grad_tiles(net, half_in, ds, stage_up, d_up0.at[pl.ds(h * (nl // 2), nl // 2)])
                fire(net, ev['d_up0'])
                yield [ev['y_reduced'], ev['got_up0'], ev['got_up0_rest'], Event(0.0, 2)]
                net.drain(ev['y_reduced'].copies)
                yield [net.grant(2, 'xp')]
                net.spawn(reduce_x(net, part, du_made, rx_scratch, ev['du_reduced']))
                for k, step in enumerate(STEPS):
                    input_back_rows(net, net.at('x', step), ds, up0, part.at[k])
                    fire(net, du_made[k])
                    yield [Event(net.now, 2)]
                yield [ev['du_reduced']]
                norm_back_rows(x0_ref, dy, part.at[3, net.core], dx_out)

            def out_down1():
                yield [ev['sum_down1']]
                yield [net.load(ev['sum_down1'].total, dw_down1)]
                sums_down.all_free = free = Event()
                net.spawn(sums_down.run(d_down0, ev['d_down0'], ev['sum_down0']))
                yield from sums_down.release(6, 'yz', ev['sum_down1'].copies, free)

            def out_up1():
                yield [ev['sum_up1']]
                net.spawn(exchange_back(net, ev['sum_up1'].total, dw_up1, ev['out_up1']))
                yield [ev['out_up1']]
                sums_up.all_free = free = Event()
                net.spawn(sums_up.run(d_up0, ev['d_up0'], ev['sum_up0']))
                yield from sums_up.release(5, 'yz', ev['sum_up1'].copies + ev['out_up1'].copies, free)

            def out_down0():
                yield [ev['sum_down0']]
                yield [net.load(ev['sum_down0'].total, dw_down0)]

            def out_up0():
                yield [ev['sum_up0']]
                net.spawn(exchange_back(net, ev['sum_up0'].total, dw_up0, ev['out_up0']))

            for flow in (layer1(), grads1(), act(), layer1_out(), layer0(), out_down1(), out_up1(), out_down0(), out_up0()):
                net.spawn(flow)
            net.run()

        def finish(up1_ref, up0_ref, down1_ref, down0_ref, x_ref, dx_ref, x_out, dx_out, up_out, down_out):
            for l, (up_ref, down_ref) in enumerate(((up0_ref, down0_ref), (up1_ref, down1_ref))):
                join_columns(up_ref, up_out.at[l])
                rows_loop(dr, 16, lambda at: down_out.at[l].__setitem__((at, slice(None)), down_ref[at, :]))
            rows_loop(rows, 16, lambda at: x_out.__setitem__((at, slice(None)), x_ref[at, :]))
            rows_loop(rows, 16, lambda at: dx_out.__setitem__((at, slice(None)), dx_ref[at, :]))

        d_up_own, d_down_own = shape((nd, ur, hidden), F32), shape((dr, width), F32)

        blocks, u0, a0, s0, up1, down1, u1, g_full, ds1, keep, x1 = call(
            forward, [shape((num_layers, nd * ur, hidden), BF16), act_full, hid_full, hid_full, up_full, shape((2, nl, dr, width // 2), BF16),
                      act_full, act_full, hid_full, shape((len(FAR), dr, width), BF16), own],
            'hhhhhhhhhhv', 'vhvh',
            [pltpu.VMEM((num_layers, nd, ur, hidden), BF16)] + [vmem(act_full)] * 3 + [vmem(up_full), vmem(down_full)] * 2 + [vmem(hid_full)] * 3 + rx,
            128, 40, 0, tokens, grad_out, w_up, w_down)
        d_up_full, d_down_full = shape((nl, nd * ur, hidden), F32), shape((nl, dr, width), F32)
        x_out, dx, _, _, _, _, *grads = call(
            turn, [own, own] + [d_up_full, d_down_full] * 2 + [d_up_own, d_down_own] * 2, 'vv' + 'h' * 8, 'hhhhhhhhhvvvhh',
            [vmem(own), vmem(act_full), vmem(up_full), vmem(up_full), vmem(down_full), pltpu.VMEM((nd, rows, width // 2), BF16), vmem(hid_full), vmem(hid_full),
             pltpu.VMEM((2, 2, nd * ur, hidden), F32), pltpu.VMEM((2, nl // RING, dr, width // 2), F32)] + rx + ryz_up + ryz_down, 240, 96, 1,
            u1, up1, down1, ds1, g_full, u0, a0, s0, keep, x1, tokens, grad_out, blocks, w_down)
        up1_own, down1_own, up0_own, down0_own = grads
        return pl.pallas_call(
            finish, out_shape=[own, own, shape(w_up.shape, F32), shape(w_down.shape, F32)], name='finish',
            in_specs=[pl.BlockSpec(memory_space=pltpu.VMEM)] * 6, out_specs=[pl.BlockSpec(memory_space=pltpu.VMEM)] * 4,
        )(up1_own, up0_own, down1_own, down0_own, x_out, dx)

    return jax.shard_map(device_fn, mesh=mesh, in_specs=(tok_spec, tok_spec, w_spec, w_spec), out_specs=(tok_spec, tok_spec, w_spec, w_spec), check_vma=False)
```

```python
import contextlib

import jax
import jax.numpy as jnp
from jax import lax
from jax.experimental import pallas as pl
from jax.experimental.pallas import tpu as pltpu
from jax.sharding import PartitionSpec as P

NORM_EPS = 1e-6
BOTH_AXES = ('local', 'data')
CONTRACT_ROWS = (((0,), (0,)), ((), ()))
CONTRACT_COLS = (((1,), (1,)), ((), ()))
MESH = pl.DeviceIdType.MESH
RING = 4
F32, BF16 = jnp.float32, jnp.bfloat16

LINK_RATE = 46.0e3
PAIR_RATE = 600e3
LOCAL_RATE = 3000e3
HOP = 2.4
PAIR_HOP = 1.0
ENTRY = 3.0
SLACK = 0.1
GELU_C = 0.7978845608028654


def scope(label):
    return jax.named_scope(label) if SCOPES else contextlib.nullcontext()


class Event:
    def __init__(self, time=None, rank=0, name=''):
        self.time, self.rank, self.name = time, rank, name


class Copy:
    def __init__(self, desc, time, remote):
        self.desc, self.time, self.remote, self.rank, self.waited = desc, time, remote, 0, False

    def wait(self):
        if self.remote:
            self.desc.wait_recv()
        else:
            self.desc.wait()


class Credit:
    def __init__(self, semaphore, count, time):
        self.semaphore, self.count, self.time, self.rank, self.waited = semaphore, count, time, 0, False

    def wait(self):
        pl.semaphore_wait(self.semaphore, self.count)


class Net:
    def __init__(self, send_sems, recv_sems, local_sems, credit_sems):
        self.send_sems, self.recv_sems, self.local_sems, self.credit_sems = send_sems, recv_sems, local_sems, credit_sems
        self.n_remote = self.n_local = 0
        self.now = 0.0
        self.free = {}
        self.sent = []
        self.flows = []
        self.labels = {}
        here = lax.axis_index('local')
        there = lax.axis_index('data')
        self.data = there
        self.pos = {'z': here // RING, 'y': here % RING, 'x': there // 2}
        self.core = there % 2

    def at(self, axis, step):
        return (self.pos[axis] + (step + RING)) % RING

    def device(self, axis, step):
        if axis == 'p':
            return {'data': self.pos['x'] * 2 + (1 - self.core)}
        if axis == 'd':
            return {'data': (self.data + step) % (2 * RING)}
        to = self.at(axis, step)
        if axis == 'x':
            return {'data': to * 2 + self.core}
        if axis == 'y':
            return {'local': self.pos['z'] * RING + to}
        return {'local': to * RING + self.pos['y']}

    def peers(self, axes):
        return [(axis, step) for axis in axes for step in ((1, -1) if axis in 'xyz' else (1,) if axis == 'p' else range(1, 2 * RING))]

    def signal(self, semaphore, axes):
        for axis, step in self.peers(axes):
            pl.semaphore_signal(semaphore, inc=1, device_id=self.device(axis, step), device_id_type=MESH)

    def arrive(self, axes):
        self.entry, self.entered = pltpu.get_barrier_semaphore(), len(self.peers(axes))
        self.signal(self.entry, axes)

    def enter(self):
        pl.semaphore_wait(self.entry, self.entered)
        self.now = max(self.now, ENTRY)

    def grant(self, k, axes):
        self.signal(self.credit_sems.at[k], axes)
        return Credit(self.credit_sems.at[k], len(self.peers(axes)), self.now + HOP)

    def drain(self, copies):
        for copy in copies:
            copy.desc.wait_send()
            self.sent.remove(copy)

    def send(self, src, dst, axis, step=1):
        k = self.n_remote
        self.n_remote += 1
        desc = pltpu.make_async_remote_copy(
            src_ref=src, dst_ref=dst, send_sem=self.send_sems.at[k], recv_sem=self.recv_sems.at[k],
            device_id=self.device(axis, step), device_id_type=MESH)
        desc.start()
        size = 1
        for n in dst.shape:
            size *= n
        size *= dst.dtype.itemsize
        rate = PAIR_RATE if axis == 'p' else LINK_RATE
        if axis == 'd':
            axis, step, size = ('p', 1, size) if step == 1 else ('x', 1 if step < RING + 2 else -1, size)
        key = (axis, step)
        done = max(self.free.get(key, 0.0), self.now) + size / rate
        self.free[key] = done
        copy = Copy(desc, done + (PAIR_HOP if axis == 'p' else HOP), True)
        self.sent.append(copy)
        return copy

    def load(self, src, dst):
        k = self.n_local
        self.n_local += 1
        desc = pltpu.make_async_copy(src, dst, self.local_sems.at[k])
        desc.start()
        size = 1
        for n in dst.shape:
            size *= n
        done = max(self.free.get('hbm', 0.0), self.now) + size * dst.dtype.itemsize / LOCAL_RATE
        self.free['hbm'] = done
        return Copy(desc, done + 0.9, False)

    def save(self, src, dst):
        copy = self.load(src, dst)
        copy.time += 4.0
        return copy

    def spend(self, microseconds):
        self.now += microseconds

    def spawn(self, flow):
        self.step(flow)

    def step(self, flow):
        try:
            if flow not in self.labels:
                self.labels[flow] = [flow.__name__, len(self.labels), 0]
            self.labels[flow][2] += 1
            self.flows.append((flow, next(flow)))
        except StopIteration:
            pass

    def run(self):
        while self.flows:
            best = None
            for k, (_, items) in enumerate(self.flows):
                if any(item.time is None for item in items):
                    continue
                time = max([item.time for item in items] + [0.0])
                late = max(item.rank for item in items)
                rank = (max(time, self.now) + (SLACK if late else 0.0), late, time)
                if best is None or rank < best[0]:
                    best = (rank, k, time)
            _, k, time = best
            flow, items = self.flows.pop(k)
            label = '%s_%d_%d' % tuple(self.labels[flow])
            with scope('w_' + label):
                for item in items:
                    if not isinstance(item, Event) and not item.waited:
                        item.wait()
                        item.waited = True
            before = self.now
            self.now = max(self.now, time)
            if PRINT:
                print('STEP', label, round(before, 2), round(self.now, 2))
            with scope('s_' + label):
                self.step(flow)

    def finish(self):
        for copy in self.sent:
            copy.desc.wait_send()


def rows_loop(rows, chunk, body):
    chunk = min(chunk, rows)

    def step(k, carry):
        body(pl.ds(pl.multiple_of(k * chunk, chunk), chunk))
        return carry

    lax.fori_loop(0, rows // chunk, step, 0)


def add_into(net, dst, *others):
    rows, cols = dst.shape

    def body(at):
        total = dst[at, :]
        for other in others:
            total = total + other[at, :]
        dst[at, :] = total

    rows_loop(rows, 16, body)
    net.spend(rows * cols * 4 * (1 + len(others)) / 4e6)


def fire(net, event):
    event.time = net.now
    if PRINT and event.name:
        print('   %7.1f %s' % (net.now, event.name))


def exchange(net, src, dst, done):
    rows = src.shape[1]

    def mine():
        return dst.at[pl.ds(pl.multiple_of(net.data * rows, rows), rows)]

    own = net.load(src.at[net.data], mine())
    copies = [net.send(src.at[(net.data + k) % (2 * RING)], mine(), 'd', k) for k in (4, 5, 2, 3, 6, 7, 1)]
    yield [own] + copies
    fire(net, done)


def exchange_back(net, src, dst, done):
    rows = dst.shape[1]

    def block(k):
        return src.at[pl.ds(pl.multiple_of(k * rows, rows), rows)]

    own = net.load(block(net.data), dst.at[net.data])
    copies = [net.send(block((net.data + k) % (2 * RING)), dst.at[net.data], 'd', k) for k in (4, 5, 2, 3, 6, 7, 1)]
    yield [own] + copies
    fire(net, done)


def copy_rows(net, src, dst):
    def body(at):
        dst[at, :] = src[at, :]

    rows_loop(src.shape[0], 16, body)
    net.spend(0.2)


def gather_x(net, full, done, issued=None, chips=None):
    half = full.shape[1] // 2
    lo, hi = pl.ds(0, half), pl.ds(half, half)
    chips = chips or {step: Event() for step in STEPS}
    left = [2]
    done.copies = []

    def send(*args):
        done.copies.append(net.send(*args))
        return done.copies[-1]

    def block(step):
        return full.at[net.at('x', step) * 2 + net.core]

    def part(step, rows):
        return full.at[net.at('x', step) * 2 + net.core, rows]

    relays = []

    def side(step, first, second, mine):
        yield [mine[0]]
        relays.append(send(part(step, first), part(step, first), 'x', -step))
        left[0] -= 1
        if left[0] == 0:
            net.spawn(far())
            if issued is not None:
                fire(net, issued)
        yield [mine[1]]
        pair = send(block(step), block(step), 'p')
        yield [pair]
        fire(net, chips[step])

    def far():
        yield relays
        pair = send(block(2), block(2), 'p')
        yield [pair]
        fire(net, chips[2])

    forth = [send(part(0, rows), part(0, rows), 'x', 1) for rows in (lo, hi)]
    back = [send(part(0, rows), part(0, rows), 'x', -1) for rows in (hi, lo)]
    pair = send(block(0), block(0), 'p')
    net.spawn(side(-1, lo, hi, forth))
    net.spawn(side(1, hi, lo, back))
    yield [pair]
    fire(net, chips[0])
    yield [chips[step] for step in STEPS]
    fire(net, done)


def gather_yz(net, own, full, first, done, issued=None, offset=0, near=False):
    second = 'y' if first == 'z' else 'z'
    size = own.shape[0]
    half = size // 2
    lo, hi = pl.ds(offset, half), pl.ds(offset + half, half)
    source = {True: own.at[pl.ds(0, half)], False: own.at[pl.ds(half, half)]}

    def part(one, two, rows):
        return full.at[yz_index(net, first, one, two), rows]

    left = [3 if near else RING, 3 if near else RING]

    def arrived(which):
        left[which] -= 1
        if left[which] == 0 and (done, issued)[which] is not None:
            fire(net, (done, issued)[which])

    def send(one, rows, axis, step):
        src = source[rows is lo] if one == 0 else part(one, 0, rows)
        return net.send(src, part(one, 0, rows), axis, step)

    def column(one):
        forth = [send(one, rows, second, 1) for rows in (lo, hi)]
        back = [send(one, rows, second, -1) for rows in (hi, lo)]

        def finish():
            if near:
                arrived(1)
                yield forth + back
            else:
                yield [forth[0]]
                relays = [net.send(part(one, -1, lo), part(one, -1, lo), second, 1)]
                yield [back[0]]
                relays.append(net.send(part(one, 1, hi), part(one, 1, hi), second, -1))
                arrived(1)
                yield [forth[1], back[1]] + relays
            arrived(0)

        net.spawn(finish())

    relays = []

    def side(step, first_half, mine):
        yield [mine[0]]
        if not near:
            relays.append(net.send(part(step, 0, first_half), part(step, 0, first_half), first, -step))
            if len(relays) == 2:
                net.spawn(far())
        yield [mine[1]]
        column(step)

    def far():
        yield relays
        column(2)

    mine = [net.load(source[True], part(0, 0, lo)), net.load(source[False], part(0, 0, hi))]
    forth = [send(0, rows, first, 1) for rows in (lo, hi)]
    back = [send(0, rows, first, -1) for rows in (hi, lo)]
    column(0)
    net.spawn(side(-1, lo, forth))
    net.spawn(side(1, hi, back))
    left[0] += 1
    yield mine
    arrived(0)


def yz_index(net, first, one, two):
    at_one, at_two = net.at(first, one), net.at('y' if first == 'z' else 'z', two)
    return at_one * RING + at_two if first == 'z' else at_two * RING + at_one


FAR = [(2, 0), (2, 1), (2, -1), (2, 2), (0, 2), (1, 2), (-1, 2)]


STEPS = (2, 1, -1, 0)
WUP = 1
WDOWN = 1


def reduce_x(net, part, made, scratch, done):
    other, relay_f, relay_b, last_f, last_b = scratch
    half = part.shape[2] // 2
    lo, hi = pl.ds(0, half), pl.ds(half, half)

    def acc(k, rows=None):
        return part.at[k, net.core] if rows is None else part.at[k, net.core, rows]

    pairs = [None] * RING
    ready = [Event() for _ in STEPS]

    def pair(k):
        yield [made[k]]
        pairs[k] = net.send(part.at[k, 1 - net.core], other.at[k], 'p')
        yield [pairs[k]]
        add_into(net, acc(k), other.at[k])
        fire(net, ready[k])

    for k in range(RING):
        net.spawn(pair(k))
    sent = {}
    started = Event()

    def part_flow(k):
        yield [ready[k]]
        if k == 0:
            sent['first_f'] = net.send(acc(0, lo), relay_f, 'x', 1)
            sent['first_b'] = net.send(acc(0, hi), relay_b, 'x', -1)
        elif k == 1:
            sent['direct_f'] = net.send(acc(1, hi), last_f.at[hi], 'x', 1)
        else:
            sent['direct_b'] = net.send(acc(2, lo), last_b.at[lo], 'x', -1)
        if len(sent) == 4:
            fire(net, started)

    for k in range(3):
        net.spawn(part_flow(k))
    yield [started]
    yield [sent['first_f']]
    add_into(net, acc(1, lo), relay_f)
    summed_f = net.send(acc(1, lo), last_f.at[lo], 'x', 1)
    yield [sent['first_b']]
    add_into(net, acc(2, hi), relay_b)
    summed_b = net.send(acc(2, hi), last_b.at[hi], 'x', -1)
    yield [ready[3], sent['direct_f'], sent['direct_b'], summed_f, summed_b]
    add_into(net, acc(3), last_f, last_b)
    done.copies = pairs + list(sent.values()) + [summed_f, summed_b]
    fire(net, done)


def reduce_x_scratch(rows, cols):
    return [pltpu.VMEM((RING, rows, cols), F32), pltpu.VMEM((rows // 2, cols), F32), pltpu.VMEM((rows // 2, cols), F32),
            pltpu.VMEM((rows, cols), F32), pltpu.VMEM((rows, cols), F32)]


def load_parts(net, src, part, made):
    for k, step in enumerate(STEPS):
        def bring(k=k, step=step):
            yield [net.load(src.at[pl.ds(net.at('x', step) * 2, 2)], part.at[k])]
            fire(net, made[k])

        net.spawn(bring())


class Sums:
    def __init__(self, net, first, scratch, window):
        self.window = window
        self.net, self.first, self.scratch = net, first, scratch
        self.second = 'y' if first == 'z' else 'z'
        self.free = [Event(0.0) for _ in range(3)]
        self.relays_free, self.all_free = Event(0.0), Event(0.0)
        self.phase1 = []
        self.phase2 = []

    def release(self, credit, axes, copies, event):
        self.net.drain(copies)
        yield [self.net.grant(credit, axes)]
        fire(self.net, event)

    def run(self, part, start, done, credit=None, mark=None, hold=None):
        net, first, second = self.net, self.first, self.second
        ahead, behind, mine, relay1, last1, relay2, last2 = self.scratch
        relays_free, all_free = self.relays_free, self.all_free
        half = mine.shape[0] // 2
        lo, hi, all_rows = pl.ds(0, half), pl.ds(half, half), pl.ds(0, 2 * half)

        def term(one, two, rows=all_rows):
            start = yz_index(net, first, one, two) * (2 * half) + rows.start
            return part.at[pl.ds(pl.multiple_of(start, half), rows.size)]

        def bring(gate, src, dst, got):
            yield [gate, start]
            yield [net.load(src, dst)]
            fire(net, got)

        free = [[gate] + [Event() for _ in range(RING)] for gate in self.free]
        self.free = [events[RING] for events in free]
        got = [[Event() for _ in range(RING)] for _ in range(3)]
        ends = [Event() for _ in STEPS]
        passed = [Event() for _ in STEPS]
        relay_copies = []

        def ring(k):
            two = STEPS[k]
            if k >= self.window:
                yield [passed[k - self.window]]
            net.spawn(bring(free[0][k], term(1, two, lo), ahead, got[0][k]))
            net.spawn(bring(free[1][k], term(-1, two, hi), behind, got[1][k]))
            net.spawn(bring(free[2][k], term(0, two), mine, got[2][k]))
            first_f = net.send(term(2, two, lo), relay1.at[0, k], first, 1)
            first_b = net.send(term(2, two, hi), relay1.at[1, k], first, -1)
            direct, sent = [], Event()

            def directs():
                yield [all_free]
                direct.append(net.send(term(1, two, hi), last1.at[0, k, hi], first, 1))
                direct.append(net.send(term(-1, two, lo), last1.at[1, k, lo], first, -1))
                fire(net, sent)

            net.spawn(directs())
            yield [first_f, got[0][k]]
            add_into(net, relay1.at[0, k], ahead)
            fire(net, free[0][k + 1])
            yield [all_free]
            summed_f = net.send(relay1.at[0, k], last1.at[0, k, lo], first, 1)
            yield [first_b, got[1][k]]
            add_into(net, relay1.at[1, k], behind)
            fire(net, free[1][k + 1])
            summed_b = net.send(relay1.at[1, k], last1.at[1, k, hi], first, -1)
            relay_copies.extend([summed_f, summed_b])
            fire(net, passed[k])
            if k == RING - 1 and mark is not None:
                fire(net, mark)
            yield [sent]
            yield direct + [summed_f, summed_b, got[2][k]]
            add_into(net, last1.at[0, k], last1.at[1, k], mine)
            fire(net, free[2][k + 1])
            fire(net, ends[k])

        def sums(k, rows=all_rows):
            return last1.at[0, k, rows]

        yield [start, relays_free]
        for k in range(RING):
            net.spawn(ring(k))
        if credit is not None:
            self.relays_free = Event()

            def relays():
                yield ends
                yield from self.release(credit, first, relay_copies, self.relays_free)

            net.spawn(relays())
        yield [ends[0]] + ([hold] if hold else [])
        first_f = net.send(sums(0, lo), relay2.at[0], second, 1)
        first_b = net.send(sums(0, hi), relay2.at[1], second, -1)
        yield [ends[1]]
        direct_f = net.send(sums(1, hi), last2.at[0, hi], second, 1)
        yield [ends[2]]
        direct_b = net.send(sums(2, lo), last2.at[1, lo], second, -1)
        yield [first_f]
        add_into(net, sums(1, lo), relay2.at[0])
        summed_f = net.send(sums(1, lo), last2.at[0, lo], second, 1)
        yield [first_b]
        add_into(net, sums(2, hi), relay2.at[1])
        summed_b = net.send(sums(2, hi), last2.at[1, hi], second, -1)
        yield [ends[3], direct_f, direct_b, summed_f, summed_b]
        add_into(net, sums(3), last2.at[0], last2.at[1])
        done.total = sums(3)
        done.copies = [first_f, first_b, direct_f, direct_b, summed_f, summed_b]
        fire(net, done)


def reduce_yz_scratch(rows, cols):
    return [pltpu.VMEM((rows // 2, cols), F32), pltpu.VMEM((rows // 2, cols), F32), pltpu.VMEM((rows, cols), F32),
            pltpu.VMEM((2, RING, rows // 2, cols), F32), pltpu.VMEM((2, RING, rows, cols), F32),
            pltpu.VMEM((2, rows // 2, cols), F32), pltpu.VMEM((2, rows, cols), F32)]


def norm_rows(x_ref, u_ref):
    def body(at):
        x = x_ref[at, :].astype(F32)
        u_ref[at, :] = (x * lax.rsqrt(jnp.mean(x * x, axis=-1, keepdims=True) + NORM_EPS)).astype(BF16)

    rows_loop(x_ref.shape[0], 16, body)


def norm_back_rows(x_ref, dy_ref, du_ref, dx_ref):
    def body(at):
        x = x_ref[at, :].astype(F32)
        du = du_ref[at, :]
        r = lax.rsqrt(jnp.mean(x * x, axis=-1, keepdims=True) + NORM_EPS)
        xr = x * r
        dx_ref[at, :] = (dy_ref[at, :].astype(F32) + r * (du - xr * jnp.mean(xr * du, axis=-1, keepdims=True))).astype(BF16)

    rows_loop(x_ref.shape[0], 16, body)


def add_rows(x_ref, y_ref, out_ref):
    def body(at):
        out_ref[at, :] = (x_ref[at, :].astype(F32) + y_ref[at, :]).astype(BF16)

    rows_loop(x_ref.shape[0], 16, body)


def swap_halves(even, odd):
    low = lax.broadcasted_iota(jnp.int32, even.shape, len(even.shape) - 1) < even.shape[-1] // 2
    shift = even.shape[-1] // 2
    axis = len(even.shape) - 1
    return jnp.where(low, even, pltpu.roll(odd, shift, axis)), jnp.where(low, pltpu.roll(even, shift, axis), odd)


def split_columns(w_ref, cols_ref):
    tile = w_ref.shape[2] // (4 * RING * RING)
    for l in range(w_ref.shape[0]):
        for x in range(RING):
            for p in range(cols_ref.shape[3] // tile):
                pair = [w_ref[l, :, pl.ds((i * RING + x) * tile, tile)].astype(F32) for i in (2 * p, 2 * p + 1)]
                for c, value in enumerate(swap_halves(*pair)):
                    cols_ref[l, 2 * x + c, :, pl.ds(p * tile, tile)] = value.astype(cols_ref.dtype)


def join_columns(cols_ref, w_ref):
    tile = w_ref.shape[1] // (4 * RING * RING)
    for x in range(RING):
        for p in range(cols_ref.shape[2] // tile):
            pair = [cols_ref[2 * x + c, :, pl.ds(p * tile, tile)] for c in range(2)]
            for i, value in zip((2 * p, 2 * p + 1), swap_halves(*pair)):
                w_ref[:, pl.ds((i * RING + x) * tile, tile)] = value


def call(body, out_shape, out_spaces, in_spaces, scratch, remote, local, collective_id, *args):
    spaces = {'v': pl.BlockSpec(memory_space=pltpu.VMEM), 'h': pl.BlockSpec(memory_space=pl.ANY)}

    def kernel(*refs):
        net = Net(*refs[-5:-1])
        net.tile_sems = refs[-1]
        body(net, *refs[:-5])
        net.finish()
        assert net.n_remote <= remote and net.n_local <= local, (net.n_remote, net.n_local)
        if PRINT:
            print(body.__name__, net.n_remote, net.n_local, round(net.now, 1))

    return pl.pallas_call(
        kernel, out_shape=out_shape, in_specs=[spaces[s] for s in in_spaces], out_specs=[spaces[s] for s in out_spaces],
        scratch_shapes=list(scratch) + [pltpu.SemaphoreType.DMA((remote,)), pltpu.SemaphoreType.DMA((remote,)), pltpu.SemaphoreType.DMA((local,)),
                                               pltpu.SemaphoreType.REGULAR((8,)), pltpu.SemaphoreType.DMA((2,))],
        compiler_params=pltpu.CompilerParams(collective_id=collective_id, has_side_effects=True, vmem_limit_bytes=67000000),
        cost_estimate=pl.CostEstimate(flops=10**8, bytes_accessed=10**7, transcendentals=0),
        name=body.__name__)(*args)


PRINT = False
SCOPES = False


WIDE = 512
GR = 2
DU = 3


def wide_loop(total, body):
    wide = min(WIDE, total)

    def step(k, carry):
        body(k, wide, pl.ds(pl.multiple_of(k * wide, wide), wide))
        return carry

    lax.fori_loop(0, total // wide, step, 0)


def flat(value):
    return value.reshape(value.shape[0] * value.shape[1], value.shape[2])


def dot_rows(a, b):
    return jnp.dot(flat(a), flat(b), preferred_element_type=F32)


def dot_cols(a, b):
    return lax.dot_general(flat(a), flat(b), CONTRACT_COLS, preferred_element_type=F32)


def gelu(a):
    return 0.5 * a * (1.0 + jnp.tanh(GELU_C * (a + 0.044715 * a * a * a)))


def hidden_rows(net, chip, u, up, a, s):
    at = pl.ds(chip * 2, 2)

    def body(_, wide, cols):
        pre = dot_rows(u[at], up[:, :, cols]).astype(BF16)
        a[at, :, cols] = pre.reshape(2, -1, wide)
        s[at, :, cols] = gelu(pre.astype(F32)).astype(BF16).reshape(2, -1, wide)

    wide_loop(up.shape[2], body)
    net.spend(1.7)


def down_rows(net, chip, s, down, part):
    at = pl.ds(chip * 2, 2)

    def body(_, wide, cols):
        part[:, :, cols] = dot_rows(s[at], down[:, :, cols]).reshape(2, -1, wide)

    wide_loop(down.shape[2], body)
    net.spend(1.76)


def hidden_back_rows(net, chip, dy, down, ds):
    at = pl.ds(chip * 2, 2)
    rows = down.shape[1]

    def body(k, wide, cols):
        blocks = pl.ds(k * (wide // rows), wide // rows)
        ds[at, :, cols] = dot_cols(dy[at], down[blocks]).astype(BF16).reshape(2, -1, wide)

    wide_loop(down.shape[0] * rows, body)
    net.spend(1.5)


def gelu_both(a):
    t = jnp.tanh(GELU_C * (a + 0.044715 * a * a * a))
    return 0.5 * a * (1.0 + t), 0.5 * (1.0 + t) + 0.5 * a * (1.0 - t * t) * (GELU_C * (1.0 + 3 * 0.044715 * a * a))


def hidden_turn_rows(net, chip, u, up, s, ds):
    at = pl.ds(chip * 2, 2)

    def body(_, wide, cols):
        pre = dot_rows(u[at], up[:, :, cols]).astype(BF16).astype(F32)
        value, slope = gelu_both(pre)
        s[at, :, cols] = value.astype(BF16).reshape(2, -1, wide)
        ds[at, :, cols] = (ds[at, :, cols].astype(F32) * slope.reshape(2, -1, wide)).astype(BF16)

    wide_loop(up.shape[2], body)
    net.spend(2.1)


def pre_back_rows(net, chip, dy, down, a, da):
    at = pl.ds(chip * 2, 2)
    rows = down.shape[1]

    def body(k, wide, cols):
        blocks = pl.ds(k * (wide // rows), wide // rows)
        ds = dot_cols(dy[at], down[blocks]).astype(BF16).astype(F32).reshape(2, -1, wide)
        da[at, :, cols] = (ds * gelu_both(a[at, :, cols].astype(F32))[1]).astype(BF16)

    wide_loop(down.shape[0] * rows, body)
    net.spend(1.95)


def input_back_rows(net, chip, da, up, part):
    at = pl.ds(chip * 2, 2)
    rows = up.shape[1]

    def body(k, wide, cols):
        blocks = pl.ds(k * (wide // rows), wide // rows)
        part[:, :, cols] = dot_cols(da[at], up[blocks]).reshape(2, -1, wide)

    wide_loop(up.shape[0] * rows, body)
    net.spend(1.9)


def stored_tiles(net, count, compute, stage, out):
    def store(t):
        return pltpu.make_async_copy(stage.at[t % 2], out(t), net.tile_sems.at[t % 2])

    def step(t, carry):
        @pl.when(t >= 2)
        def _():
            store(t - 2).wait()

        compute(t, stage.at[t % 2])
        store(t).start()
        return carry

    lax.fori_loop(0, count, step, 0)
    for t in range(max(count - 2, 0), count):
        store(t).wait()


def dot_tokens(a, b):
    return lax.dot_general(flat(a), flat(b), CONTRACT_ROWS, preferred_element_type=F32)


def grad_tiles(net, lhs, rhs, stage, out):
    wide = stage.shape[1]

    def compute(t, slot):
        slot[...] = dot_tokens(lhs[:, :, pl.ds(pl.multiple_of(t * wide, wide), wide)], rhs[...])

    stored_tiles(net, lhs.shape[2] // wide, compute, stage, lambda t: out.at[pl.ds(pl.multiple_of(t * wide, wide), wide)])
    net.spend(3.2 * lhs.shape[2] / 1024)


def solution(mesh):
    nl, nd = mesh.shape['local'], mesh.shape['data']
    tok_spec = P(BOTH_AXES, None)
    w_spec = P(None, BOTH_AXES, None)

    def device_fn(tokens, grad_out, w_up, w_down):
        num_layers, ur, ffn = w_up.shape
        dr = w_down.shape[1]
        rows, width = tokens.shape
        hidden = nl * dr
        shape = jax.ShapeDtypeStruct
        up_full = shape((nl, nd * ur, hidden), BF16)
        down_full = shape((nl, dr, width), BF16)
        act_full = shape((nd, rows, width), BF16)
        hid_full = shape((nd, rows, hidden), BF16)
        own = shape((rows, width), BF16)
        part_vmem = pltpu.VMEM((RING, 2, rows, width), F32)
        rx = [part_vmem] + reduce_x_scratch(rows, width)
        ryz_up = reduce_yz_scratch(nd * ur, hidden)
        ryz_down = reduce_yz_scratch(dr, width)

        def vmem(like):
            return pltpu.VMEM(like.shape, like.dtype)

        def forward(net, x_ref, g_in, w_up_ref, down_in, block_out, u_out, a_out, s_out, up_out, down_out, next_out, g_out, ds_out, keep_out, x_out,
                    cols, next_own, u, g, up0, down0, up1, down1, a, s, ds, part, *rx_scratch):
            net.arrive('dyz')
            names = ('blocks', 'blocks1', 'sent_u', 'got_u', 'got_g', 'sent_up0', 'sent_down0', 'got_up0', 'got_down0', 'got_up1', 'got_down1', 'reduced')
            ev = {name: Event(name=name) for name in names}
            ev['got_up0'].rank = 2
            made = [Event(name='made%d' % k) for k in range(RING)]
            hidden_made = [Event(name='hidden%d' % k) for k in range(RING)]
            grad = net.load(g_in, g.at[net.data])
            split_columns(w_up_ref, cols)
            norm_rows(x_ref, u.at[net.data])
            net.enter()
            net.spawn(exchange(net, cols.at[0], block_out.at[0], ev['blocks']))
            net.spawn(gather_yz(net, down_in.at[0], down0, 'z', ev['got_down0'], ev['sent_down0']))
            net.spawn(gather_x(net, u, ev['got_u'], ev['sent_u']))

            def up_first():
                yield [ev['blocks']]
                net.spawn(gather_yz(net, block_out.at[0], up0, 'y', ev['got_up0'], ev['sent_up0']))
                yield [ev['sent_u']]
                net.spawn(exchange(net, cols.at[1], block_out.at[1], ev['blocks1']))
                yield [grad]
                net.spawn(gather_x(net, g, ev['got_g']))

            def second():
                yield [ev['sent_up0'], ev['sent_down0'], ev['blocks1']]
                net.spawn(gather_yz(net, block_out.at[1], up1, 'y', ev['got_up1']))
                net.spawn(gather_yz(net, down_in.at[1], down1, 'z', ev['got_down1']))

            def save(event, *pairs):
                yield [ev[event]]
                yield [net.save(src, dst) for src, dst in pairs]

            def hidden_flow():
                yield [ev['got_u'], ev['got_up0']]
                for k, step in enumerate(STEPS):
                    hidden_rows(net, net.at('x', step), u, up0, a, s)
                    fire(net, hidden_made[k])
                    yield [Event(net.now, 2)]
                yield [net.save(a, a_out), net.save(s, s_out), net.save(u, u_out)]

            def down_flow():
                for k, step in enumerate(STEPS):
                    yield [hidden_made[k], ev['got_down0'], Event(0.0, 1)]
                    down_rows(net, net.at('x', step), s, down0, part.at[k])
                    fire(net, made[k])
                yield [net.save(down0.at[yz_index(net, 'z', *far)], keep_out.at[k]) for k, far in enumerate(FAR)]

            def act():
                yield [ev['reduced']]
                add_rows(x_ref, part.at[3, net.core], x_out)
                norm_rows(x_out, next_own)
                net.spend(1.0)
                yield [net.load(next_own, next_out)]

            def back_flow():
                for k, step in enumerate(STEPS):
                    yield [ev['got_g'], ev['got_down1'], Event(0.0, 3)]
                    hidden_back_rows(net, net.at('x', step), g, down1, ds)
                yield [net.load(ds, ds_out)]

            half = down_out.shape[3]
            for flow in (up_first(), second(), hidden_flow(), down_flow(), act(), back_flow(), reduce_x(net, part, made, rx_scratch, ev['reduced']),
                         save('got_up1', (up1, up_out)), save('got_down1', *[(down1.at[:, :, pl.ds(h * half, half)], down_out.at[h]) for h in range(2)]),
                         save('got_g', (g, g_out))):
                net.spawn(flow)
            net.run()

        def turn(net, u_in, up_in, down_in, ds_in, g_in, u0_in, a0_in, s0_in, keep_in, x_ref, x0_ref, g_own, block_in, w_down_in,
                 x_out, dx_out, d_up0, d_down0, d_up1, d_down1, dw_up1, dw_down1, dw_up0, dw_down0,
                 own_up, u, up1, up0, down0, half_in, ds, s, stage, part, *scratch):
            net.arrive('dyz')
            inputs = [net.load(u_in, u.at[net.data]), net.load(up_in, up1), net.load(ds_in, ds)]
            inputs[0].wait()
            inputs[0].waited = True
            net.enter()
            rx_scratch = scratch[:5]
            sums_up, sums_down = Sums(net, 'y', scratch[5:12], WUP), Sums(net, 'z', scratch[12:19], WDOWN)
            names = ('got_u', 'hidden', 'all_du', 'reduced', 'sent_dy', 'got_dy', 'got_up0', 'got_up0_rest', 'got_down0', 'd_down1', 'd_up1', 'y_reduced', 'acts',
                     'd_down0', 'da0', 'd_up0', 'du_reduced', 'sum_up1', 'sum_down1', 'sum_up0', 'sum_down0', 'up0_passed', 'out_up1', 'out_up0')
            ev = {name: Event(name=name) for name in names}
            made, y_made, du_made = ([Event(name='%s%d' % (name, k)) for k in range(RING)] for name in ('made', 'y_made', 'du_made'))
            wide = half_in.shape[2]
            top = nd * ur * 3 // 4

            def columns(h):
                return pl.ds(h * wide, wide)

            here = {step: Event(name='u%d' % step) for step in STEPS}
            dy_here = {step: Event() for step in STEPS}
            net.spawn(gather_x(net, u, ev['got_u'], chips=here))
            net.spawn(gather_yz(net, w_down_in.at[0], down0, 'z', ev['got_down0'], near=True))
            net.spawn(gather_yz(net, block_in.at[0, pl.ds(0, top)], up0, 'y', ev['got_up0']))
            net.spawn(gather_yz(net, block_in.at[0, pl.ds(top, nd * ur - top)], up0, 'z', ev['got_up0_rest'], offset=top))
            net.spawn(reduce_x(net, part, made, rx_scratch, ev['reduced']))
            net.spawn(sums_up.run(d_up1, ev['d_up1'], ev['sum_up1'], 3))
            net.spawn(sums_down.run(d_down1, ev['d_down1'], ev['sum_down1'], 4))

            left = [RING, RING]

            def layer1(k, step):
                yield [here[step], Event(0.0, 1)] + inputs[1:]
                hidden_turn_rows(net, net.at('x', step), u, up1, s, ds)
                left[0] -= 1
                if left[0] == 0:
                    fire(net, ev['hidden'])
                yield [Event(net.now, DU)]
                input_back_rows(net, net.at('x', step), ds, up1, part.at[k])
                fire(net, made[k])
                left[1] -= 1
                if left[1] == 0:
                    fire(net, ev['all_du'])

            def grads1():
                for h in range(2):
                    yield [net.load(g_in.at[:, :, columns(h)], half_in), Event(0.0, GR), ev['hidden']]
                    grad_tiles(net, s, half_in, stage, d_down1.at[:, columns(h)])
                fire(net, ev['d_down1'])
                for h in range(2):
                    yield [Event(net.now, GR)]
                    grad_tiles(net, u.at[:, :, columns(h)], ds, stage, d_up1.at[columns(h)])
                fire(net, ev['d_up1'])

            def act():
                yield [ev['d_up1'], ev['got_u']]
                net.drain(ev['got_u'].copies)
                credit = net.grant(0, 'xp')
                yield [ev['reduced'], credit]
                norm_back_rows(x_ref, g_own, part.at[3, net.core], u.at[net.data])
                net.spend(0.7)
                net.spawn(gather_x(net, u, ev['got_dy'], ev['sent_dy'], dy_here))

            def layer1_out():
                yield [ev['all_du'], ev['d_up1']]
                yield [net.load(down_in.at[h], up1.at[:, pl.ds(h * dr, dr)]) for h in range(2)]
                yield [ev['reduced'], Event(0.0, 2)]
                net.drain(ev['reduced'].copies)
                credit = net.grant(1, 'xp')
                for k, step in enumerate(STEPS):
                    for h in range(2):
                        net.spend(-0.88)
                        down_rows(net, net.at('x', step), s, up1.at[:, pl.ds(h * dr, dr)], part.at[k, :, :, columns(h)])
                    yield [Event(net.now, 2)]
                loads = [net.load(a0_in, up1.at[pl.ds(0, nd)]), net.load(s0_in, up1.at[pl.ds(nd, nd)])]
                loads += [net.load(keep_in.at[k], down0.at[yz_index(net, 'z', *far)]) for k, far in enumerate(FAR)]
                yield loads
                fire(net, ev['acts'])
                yield [ev['sent_dy'], credit]
                net.spawn(reduce_x(net, part, y_made, rx_scratch, ev['y_reduced']))
                for k in range(RING):
                    fire(net, y_made[k])
                yield [ev['y_reduced']]
                add_rows(x_ref, part.at[3, net.core], x_out)

            a0, s0 = up1.at[pl.ds(0, nd)], up1.at[pl.ds(nd, nd)]
            backs = [RING]

            def layer0_hidden(step):
                yield [dy_here[step], ev['acts'], ev['got_down0'], Event(0.0, 2)]
                pre_back_rows(net, net.at('x', step), u, down0, a0, ds)
                backs[0] -= 1
                if backs[0] == 0:
                    fire(net, ev['da0'])

            def layer0():
                yield [ev['d_down1']]
                first = net.load(u0_in.at[:, :, columns(0)], half_in)
                for h in range(2):
                    yield [ev['got_dy'], ev['acts'], Event(0.0, 3)]
                    grad_tiles(net, s0, u.at[:, :, columns(h)], stage, d_down0.at[:, columns(h)])
                fire(net, ev['d_down0'])
                for h in range(2):
                    yield [net.load(u0_in.at[:, :, columns(h)], half_in) if h else first]
                    yield [ev['da0'], Event(0.0, 3)]
                    grad_tiles(net, half_in, ds, stage, d_up0.at[columns(h)])
                fire(net, ev['d_up0'])
                yield [ev['y_reduced'], ev['got_up0'], ev['got_up0_rest'], Event(0.0, 2)]
                net.drain(ev['y_reduced'].copies)
                yield [net.grant(2, 'xp')]
                net.spawn(reduce_x(net, part, du_made, rx_scratch, ev['du_reduced']))
                for k, step in enumerate(STEPS):
                    input_back_rows(net, net.at('x', step), ds, up0, part.at[k])
                    fire(net, du_made[k])
                    yield [Event(net.now, 2)]
                yield [ev['du_reduced']]
                norm_back_rows(x0_ref, u.at[net.data], part.at[3, net.core], dx_out)

            def out_down1():
                yield [ev['sum_down1']]
                yield [net.load(ev['sum_down1'].total, dw_down1)]
                sums_down.all_free = free = Event()
                net.spawn(sums_down.run(d_down0, ev['d_up0'], ev['sum_down0'], hold=ev['up0_passed']))
                yield from sums_down.release(6, 'yz', ev['sum_down1'].copies, free)

            def out_up1():
                yield [ev['sum_up1']]
                copy_rows(net, ev['sum_up1'].total, own_up)
                sums_up.all_free = free = Event()
                net.spawn(sums_up.run(d_up0, ev['d_up0'], ev['sum_up0'], mark=ev['up0_passed']))
                yield from sums_up.release(5, 'yz', ev['sum_up1'].copies, free)
                net.spawn(exchange_back(net, own_up, dw_up1, Event(name='out_up1')))

            def out_down0():
                yield [ev['sum_down0']]
                yield [net.load(ev['sum_down0'].total, dw_down0)]

            def out_up0():
                yield [ev['sum_up0']]
                net.spawn(exchange_back(net, ev['sum_up0'].total, dw_up0, ev['out_up0']))

            for k in (3, 2, 1, 0):
                net.spawn(layer1(k, STEPS[k]))
            for step in (0, -1, 1, 2):
                net.spawn(layer0_hidden(step))
            for flow in (grads1(), act(), layer1_out(), layer0(), out_down1(), out_up1(), out_down0(), out_up0()):
                net.spawn(flow)
            net.run()

        def finish(up1_ref, up0_ref, down1_ref, down0_ref, x_ref, dx_ref, x_out, dx_out, up_out, down_out):
            for l, (up_ref, down_ref) in enumerate(((up0_ref, down0_ref), (up1_ref, down1_ref))):
                join_columns(up_ref, up_out.at[l])
                rows_loop(dr, 16, lambda at: down_out.at[l].__setitem__((at, slice(None)), down_ref[at, :]))
            rows_loop(rows, 16, lambda at: x_out.__setitem__((at, slice(None)), x_ref[at, :]))
            rows_loop(rows, 16, lambda at: dx_out.__setitem__((at, slice(None)), dx_ref[at, :]))

        d_up_own, d_down_own = shape((nd, ur, hidden), F32), shape((dr, width), F32)

        blocks, u0, a0, s0, up1, down1, u1, g_full, ds1, keep, x1 = call(
            forward, [shape((num_layers, nd * ur, hidden), BF16), act_full, hid_full, hid_full, up_full, shape((2, nl, dr, width // 2), BF16),
                      own, act_full, hid_full, shape((len(FAR), dr, width), BF16), own],
            'hhhhhhhhhhv', 'vhvh',
            [pltpu.VMEM((num_layers, nd, ur, hidden), BF16), vmem(own)] + [vmem(act_full)] * 2 + [vmem(up_full), vmem(down_full)] * 2 + [vmem(hid_full)] * 3 + rx,
            176, 48, 0, tokens, grad_out, w_up, w_down)
        d_up_full, d_down_full = shape((width, hidden), F32), shape((hidden, width), F32)
        x_out, dx, _, _, _, _, *grads = call(
            turn, [own, own] + [d_up_full, d_down_full] * 2 + [d_up_own, d_down_own] * 2, 'vv' + 'h' * 8, 'hhhhhhhhhvvvhh',
            [pltpu.VMEM((nd * ur, hidden), F32), vmem(act_full), vmem(up_full), vmem(up_full), vmem(down_full), pltpu.VMEM((nd, rows, width // 2), BF16), vmem(hid_full), vmem(hid_full),
             pltpu.VMEM((2, hidden // 2, width // 2), F32)] + rx + ryz_up + ryz_down, 288, 104, 1,
            u1, up1, down1, ds1, g_full, u0, a0, s0, keep, x1, tokens, grad_out, blocks, w_down)
        up1_own, down1_own, up0_own, down0_own = grads
        return pl.pallas_call(
            finish, out_shape=[own, own, shape(w_up.shape, F32), shape(w_down.shape, F32)], name='finish',
            in_specs=[pl.BlockSpec(memory_space=pltpu.VMEM)] * 6, out_specs=[pl.BlockSpec(memory_space=pltpu.VMEM)] * 4,
        )(up1_own, up0_own, down1_own, down0_own, x_out, dx)

    return jax.shard_map(device_fn, mesh=mesh, in_specs=(tok_spec, tok_spec, w_spec, w_spec), out_specs=(tok_spec, tok_spec, w_spec, w_spec), check_vma=False)
```

```python
import contextlib

import jax
import jax.numpy as jnp
from jax import lax
from jax.experimental import pallas as pl
from jax.experimental.pallas import tpu as pltpu
from jax.sharding import PartitionSpec as P

NORM_EPS = 1e-6
BOTH_AXES = ('local', 'data')
CONTRACT_ROWS = (((0,), (0,)), ((), ()))
CONTRACT_COLS = (((1,), (1,)), ((), ()))
MESH = pl.DeviceIdType.MESH
RING = 4
F32, BF16 = jnp.float32, jnp.bfloat16

LINK_RATE = 46.0e3
PAIR_RATE = 600e3
LOCAL_RATE = 3000e3
HOP = 2.4
PAIR_HOP = 1.0
ENTRY = 3.0
SLACK = 0.1
GELU_C = 0.7978845608028654


def scope(label):
    return jax.named_scope(label) if SCOPES else contextlib.nullcontext()


class Event:
    def __init__(self, time=None, rank=0, name=''):
        self.time, self.rank, self.name = time, rank, name


class Copy:
    def __init__(self, desc, time, remote):
        self.desc, self.time, self.remote, self.rank, self.waited = desc, time, remote, 0, False

    def wait(self):
        if self.remote:
            self.desc.wait_recv()
        else:
            self.desc.wait()


class Credit:
    def __init__(self, semaphore, count, time):
        self.semaphore, self.count, self.time, self.rank, self.waited = semaphore, count, time, 0, False

    def wait(self):
        pl.semaphore_wait(self.semaphore, self.count)


class Net:
    def __init__(self, send_sems, recv_sems, local_sems, credit_sems):
        self.send_sems, self.recv_sems, self.local_sems, self.credit_sems = send_sems, recv_sems, local_sems, credit_sems
        self.n_remote = self.n_local = 0
        self.now = 0.0
        self.free = {}
        self.sent = []
        self.flows = []
        self.labels = {}
        here = lax.axis_index('local')
        there = lax.axis_index('data')
        self.data = there
        self.pos = {'z': here // RING, 'y': here % RING, 'x': there // 2}
        self.core = there % 2

    def at(self, axis, step):
        return (self.pos[axis] + (step + RING)) % RING

    def device(self, axis, step):
        if axis == 'p':
            return {'data': self.pos['x'] * 2 + (1 - self.core)}
        if axis == 'd':
            return {'data': (self.data + step) % (2 * RING)}
        to = self.at(axis, step)
        if axis == 'x':
            return {'data': to * 2 + self.core}
        if axis == 'y':
            return {'local': self.pos['z'] * RING + to}
        return {'local': to * RING + self.pos['y']}

    def peers(self, axes):
        return [(axis, step) for axis in axes for step in ((1, -1) if axis in 'xyz' else (1,) if axis == 'p' else range(1, 2 * RING))]

    def signal(self, semaphore, axes):
        for axis, step in self.peers(axes):
            pl.semaphore_signal(semaphore, inc=1, device_id=self.device(axis, step), device_id_type=MESH)

    def arrive(self, axes):
        self.entry, self.entered = pltpu.get_barrier_semaphore(), len(self.peers(axes))
        self.signal(self.entry, axes)

    def enter(self):
        pl.semaphore_wait(self.entry, self.entered)
        self.now = max(self.now, ENTRY)

    def grant(self, k, axes):
        self.signal(self.credit_sems.at[k], axes)
        return Credit(self.credit_sems.at[k], len(self.peers(axes)), self.now + HOP)

    def drain(self, copies):
        for copy in copies:
            if copy in self.sent:
                copy.desc.wait_send()
                self.sent.remove(copy)

    def idle(self, gap):
        over = [copy for copy in self.sent if copy.time + 4.0 < self.now]
        self.drain(over[:int(gap / 0.05)])

    def send(self, src, dst, axis, step=1):
        k = self.n_remote
        self.n_remote += 1
        desc = pltpu.make_async_remote_copy(
            src_ref=src, dst_ref=dst, send_sem=self.send_sems.at[k], recv_sem=self.recv_sems.at[k],
            device_id=self.device(axis, step), device_id_type=MESH)
        desc.start()
        size = 1
        for n in dst.shape:
            size *= n
        size *= dst.dtype.itemsize
        rate = PAIR_RATE if axis == 'p' else LINK_RATE
        if axis == 'd':
            axis, step, size = ('p', 1, size) if step == 1 else ('x', 1 if step < RING + 2 else -1, size)
        key = (axis, step)
        done = max(self.free.get(key, 0.0), self.now) + size / rate
        self.free[key] = done
        copy = Copy(desc, done + (PAIR_HOP if axis == 'p' else HOP), True)
        self.sent.append(copy)
        return copy

    def load(self, src, dst):
        k = self.n_local
        self.n_local += 1
        desc = pltpu.make_async_copy(src, dst, self.local_sems.at[k])
        desc.start()
        size = 1
        for n in dst.shape:
            size *= n
        done = max(self.free.get('hbm', 0.0), self.now) + size * dst.dtype.itemsize / LOCAL_RATE
        self.free['hbm'] = done
        return Copy(desc, done + 0.9, False)

    def save(self, src, dst):
        copy = self.load(src, dst)
        copy.time += 4.0
        return copy

    def spend(self, microseconds):
        self.now += microseconds

    def spawn(self, flow):
        self.step(flow)

    def step(self, flow):
        try:
            if flow not in self.labels:
                self.labels[flow] = [flow.__name__, len(self.labels), 0]
            self.labels[flow][2] += 1
            self.flows.append((flow, next(flow)))
        except StopIteration:
            pass

    def run(self):
        while self.flows:
            best = None
            for k, (_, items) in enumerate(self.flows):
                if any(item.time is None for item in items):
                    continue
                time = max([item.time for item in items] + [0.0])
                late = max([item.rank for item in items] + [0])
                rank = (max(time, self.now) + (SLACK if late else 0.0), late, time)
                if best is None or rank < best[0]:
                    best = (rank, k, time)
            _, k, time = best
            flow, items = self.flows.pop(k)
            self.idle(time - self.now)
            label = '%s_%d_%d' % tuple(self.labels[flow])
            with scope('w_' + label):
                for item in items:
                    if not isinstance(item, Event) and not item.waited:
                        item.wait()
                        item.waited = True
            before = self.now
            self.now = max(self.now, time)
            if PRINT:
                print('STEP', label, round(before, 2), round(self.now, 2))
            with scope('s_' + label):
                self.step(flow)

    def finish(self):
        for copy in self.sent:
            copy.desc.wait_send()


def rows_loop(rows, chunk, body):
    chunk = min(chunk, rows)

    def step(k, carry):
        body(pl.ds(pl.multiple_of(k * chunk, chunk), chunk))
        return carry

    lax.fori_loop(0, rows // chunk, step, 0)


def add_into(net, dst, *others):
    rows, cols = dst.shape

    def body(at):
        total = dst[at, :]
        for other in others:
            total = total + other[at, :]
        dst[at, :] = total

    rows_loop(rows, 16, body)
    net.spend(rows * cols * 4 * (1 + len(others)) / 4e6)


def fire(net, event):
    event.time = net.now
    if PRINT and event.name:
        print('   %7.1f %s' % (net.now, event.name))


def exchange(net, src, dst, done):
    rows = src.shape[1]

    def mine():
        return dst.at[pl.ds(pl.multiple_of(net.data * rows, rows), rows)]

    own = net.load(src.at[net.data], mine())
    copies = [net.send(src.at[(net.data + k) % (2 * RING)], mine(), 'd', k) for k in (4, 5, 2, 3, 6, 7, 1)]
    yield [own] + copies
    fire(net, done)


def exchange_back(net, src, dst, done):
    rows = dst.shape[1]

    def block(k):
        return src.at[pl.ds(pl.multiple_of(k * rows, rows), rows)]

    own = net.load(block(net.data), dst.at[net.data])
    copies = [net.send(block((net.data + k) % (2 * RING)), dst.at[net.data], 'd', k) for k in (4, 5, 2, 3, 6, 7, 1)]
    yield [own] + copies
    net.drain(copies)
    fire(net, done)


def copy_rows(net, src, dst):
    def body(at):
        dst[at, :] = src[at, :]

    rows_loop(src.shape[0], 16, body)
    net.spend(0.2)


def gather_x(net, full, done, issued=None, chips=None):
    half = full.shape[1] // 2
    lo, hi = pl.ds(0, half), pl.ds(half, half)
    chips = chips or {step: Event() for step in STEPS}
    left = [2]
    done.copies = []

    def send(*args):
        done.copies.append(net.send(*args))
        return done.copies[-1]

    def block(step):
        return full.at[net.at('x', step) * 2 + net.core]

    def part(step, rows):
        return full.at[net.at('x', step) * 2 + net.core, rows]

    relays = []

    def side(step, first, second, mine):
        yield [mine[0]]
        relays.append(send(part(step, first), part(step, first), 'x', -step))
        left[0] -= 1
        if left[0] == 0:
            net.spawn(far())
            if issued is not None:
                fire(net, issued)
        yield [mine[1]]
        pair = send(block(step), block(step), 'p')
        yield [pair]
        fire(net, chips[step])

    def far():
        yield relays
        pair = send(block(2), block(2), 'p')
        yield [pair]
        fire(net, chips[2])

    forth = [send(part(0, rows), part(0, rows), 'x', 1) for rows in (lo, hi)]
    back = [send(part(0, rows), part(0, rows), 'x', -1) for rows in (hi, lo)]
    pair = send(block(0), block(0), 'p')
    net.spawn(side(-1, lo, hi, forth))
    net.spawn(side(1, hi, lo, back))
    yield [pair]
    fire(net, chips[0])
    yield [chips[step] for step in STEPS]
    fire(net, done)


def gather_yz(net, own, full, first, done, issued=None, offset=0, near=False, split=True):
    second = 'y' if first == 'z' else 'z'
    size = own.shape[0]
    half = size // 2
    lo, hi, both = pl.ds(offset, half), pl.ds(offset + half, half), pl.ds(offset, size)
    forward, backward = ((lo, hi), (hi, lo)) if split and not near else ((both,), (both,))

    def part(one, two, rows):
        return full.at[yz_index(net, first, one, two), rows]

    left = [3 if near else RING, 3 if near else RING]

    def arrived(which):
        left[which] -= 1
        if left[which] == 0 and (done, issued)[which] is not None:
            fire(net, (done, issued)[which])

    def send(one, rows, axis, step):
        src = own.at[pl.ds(rows.start - offset, rows.size)] if one == 0 else part(one, 0, rows)
        return net.send(src, part(one, 0, rows), axis, step)

    def column(one):
        forth = [send(one, rows, second, 1) for rows in forward]
        back = [send(one, rows, second, -1) for rows in backward]

        def finish():
            if near:
                arrived(1)
                yield forth + back
            else:
                yield [forth[0]]
                relays = [net.send(part(one, -1, lo), part(one, -1, lo), second, 1)]
                yield [back[0]]
                relays.append(net.send(part(one, 1, hi), part(one, 1, hi), second, -1))
                arrived(1)
                yield forth[1:] + back[1:] + relays
            arrived(0)

        net.spawn(finish())

    relays = []

    def side(step, first_half, mine):
        yield [mine[0]]
        if not near:
            relays.append(net.send(part(step, 0, first_half), part(step, 0, first_half), first, -step))
            if len(relays) == 2:
                net.spawn(far())
        yield mine[1:]
        column(step)

    def far():
        yield relays
        column(2)

    mine = [net.load(own, part(0, 0, both))]
    forth = [send(0, rows, first, 1) for rows in forward]
    back = [send(0, rows, first, -1) for rows in backward]
    column(0)
    net.spawn(side(-1, lo, forth))
    net.spawn(side(1, hi, back))
    left[0] += 1
    yield mine
    arrived(0)


def yz_index(net, first, one, two):
    at_one, at_two = net.at(first, one), net.at('y' if first == 'z' else 'z', two)
    return at_one * RING + at_two if first == 'z' else at_two * RING + at_one


FAR = [(2, 0), (2, 1), (2, -1), (2, 2), (0, 2), (1, 2), (-1, 2)]


STEPS = (2, 1, -1, 0)
WINDOW = 2


def reduce_x(net, part, made, scratch, done):
    other, relay_f, relay_b, last_f, last_b = scratch
    half = part.shape[2] // 2
    lo, hi = pl.ds(0, half), pl.ds(half, half)

    def acc(k, rows=None):
        return part.at[k, net.core] if rows is None else part.at[k, net.core, rows]

    pairs = [None] * RING
    ready = [Event() for _ in STEPS]

    def pair(k):
        yield [made[k]]
        pairs[k] = net.send(part.at[k, 1 - net.core], other.at[k], 'p')
        yield [pairs[k]]
        add_into(net, acc(k), other.at[k])
        fire(net, ready[k])

    for k in range(RING):
        net.spawn(pair(k))
    sent = {}
    started = Event()

    def part_flow(k):
        yield [ready[k]]
        if k == 0:
            sent['first_f'] = net.send(acc(0, lo), relay_f, 'x', 1)
            sent['first_b'] = net.send(acc(0, hi), relay_b, 'x', -1)
        elif k == 1:
            sent['direct_f'] = net.send(acc(1, hi), last_f.at[hi], 'x', 1)
        else:
            sent['direct_b'] = net.send(acc(2, lo), last_b.at[lo], 'x', -1)
        if len(sent) == 4:
            fire(net, started)

    for k in range(3):
        net.spawn(part_flow(k))
    yield [started]
    yield [sent['first_f']]
    add_into(net, acc(1, lo), relay_f)
    summed_f = net.send(acc(1, lo), last_f.at[lo], 'x', 1)
    yield [sent['first_b']]
    add_into(net, acc(2, hi), relay_b)
    summed_b = net.send(acc(2, hi), last_b.at[hi], 'x', -1)
    yield [ready[3], sent['direct_f'], sent['direct_b'], summed_f, summed_b]
    add_into(net, acc(3), last_f, last_b)
    done.copies = pairs + list(sent.values()) + [summed_f, summed_b]
    fire(net, done)


def reduce_x_scratch(rows, cols):
    return [pltpu.VMEM((RING, rows, cols), F32), pltpu.VMEM((rows // 2, cols), F32), pltpu.VMEM((rows // 2, cols), F32),
            pltpu.VMEM((rows, cols), F32), pltpu.VMEM((rows, cols), F32)]


def load_parts(net, src, part, made):
    for k, step in enumerate(STEPS):
        def bring(k=k, step=step):
            yield [net.load(src.at[pl.ds(net.at('x', step) * 2, 2)], part.at[k])]
            fire(net, made[k])

        net.spawn(bring())


class Sums:
    def __init__(self, net, first, scratch, stage):
        self.net, self.first, self.scratch, self.stage = net, first, scratch, stage
        self.second = 'y' if first == 'z' else 'z'

    def run(self, place, start, done, free, passed_all):
        net, first, second = self.net, self.first, self.second
        relay1, last1, relay2, last2 = self.scratch
        ahead, behind, mine = self.stage
        half = mine.shape[0] // 2
        lo, hi, all_rows = pl.ds(0, half), pl.ds(half, half), pl.ds(0, 2 * half)
        done.copies = []

        def send(*args):
            done.copies.append(net.send(*args))
            return done.copies[-1]

        def term(one, two, rows=all_rows):
            return place(yz_index(net, first, one, two), rows)

        def bring(gate, src, dst, got):
            yield [gate, start]
            yield [net.load(src, dst)]
            fire(net, got)

        chain = [[gate] + [Event() for _ in range(RING)] for gate in free]
        free[:] = [events[RING] for events in chain]
        got = [[Event() for _ in range(RING)] for _ in range(3)]
        ends = [Event() for _ in STEPS]
        passed = [Event() for _ in range(RING - 1)] + [passed_all]

        def ring(k):
            two = STEPS[k]
            if k >= WINDOW:
                yield [passed[k - WINDOW]]
            net.spawn(bring(chain[0][k], term(1, two, lo), ahead, got[0][k]))
            net.spawn(bring(chain[1][k], term(-1, two, hi), behind, got[1][k]))
            net.spawn(bring(chain[2][k], term(0, two), mine, got[2][k]))
            first_f = send(term(2, two, lo), relay1.at[0, k], first, 1)
            first_b = send(term(2, two, hi), relay1.at[1, k], first, -1)
            direct_f = send(term(1, two, hi), last1.at[0, k, hi], first, 1)
            direct_b = send(term(-1, two, lo), last1.at[1, k, lo], first, -1)
            yield [first_f, got[0][k]]
            add_into(net, relay1.at[0, k], ahead)
            fire(net, chain[0][k + 1])
            summed_f = send(relay1.at[0, k], last1.at[0, k, lo], first, 1)
            yield [first_b, got[1][k]]
            add_into(net, relay1.at[1, k], behind)
            fire(net, chain[1][k + 1])
            summed_b = send(relay1.at[1, k], last1.at[1, k, hi], first, -1)
            fire(net, passed[k])
            yield [direct_f, direct_b, summed_f, summed_b, got[2][k]]
            add_into(net, last1.at[0, k], last1.at[1, k], mine)
            fire(net, chain[2][k + 1])
            fire(net, ends[k])

        def sums(k, rows=all_rows):
            return last1.at[0, k, rows]

        yield [start]
        for k in range(RING):
            net.spawn(ring(k))
        yield [ends[0]]
        first_f = send(sums(0, lo), relay2.at[0], second, 1)
        first_b = send(sums(0, hi), relay2.at[1], second, -1)
        yield [ends[1]]
        direct_f = send(sums(1, hi), last2.at[0, hi], second, 1)
        yield [ends[2]]
        direct_b = send(sums(2, lo), last2.at[1, lo], second, -1)
        yield [first_f]
        add_into(net, sums(1, lo), relay2.at[0])
        summed_f = send(sums(1, lo), last2.at[0, lo], second, 1)
        yield [first_b]
        add_into(net, sums(2, hi), relay2.at[1])
        summed_b = send(sums(2, hi), last2.at[1, hi], second, -1)
        yield [ends[3], direct_f, direct_b, summed_f, summed_b]
        add_into(net, sums(3), last2.at[0], last2.at[1])
        done.total = sums(3)
        fire(net, done)


def sums_scratch(rows, cols):
    return [pltpu.VMEM((2, RING, rows // 2, cols), F32), pltpu.VMEM((2, RING, rows, cols), F32),
            pltpu.VMEM((2, rows // 2, cols), F32), pltpu.VMEM((2, rows, cols), F32)]


def sums_stage(rows, cols):
    return [pltpu.VMEM((rows // 2, cols), F32), pltpu.VMEM((rows // 2, cols), F32), pltpu.VMEM((rows, cols), F32)]


def norm_rows(x_ref, u_ref):
    def body(at):
        x = x_ref[at, :].astype(F32)
        u_ref[at, :] = (x * lax.rsqrt(jnp.mean(x * x, axis=-1, keepdims=True) + NORM_EPS)).astype(BF16)

    rows_loop(x_ref.shape[0], 16, body)


def norm_back_rows(x_ref, dy_ref, du_ref, dx_ref):
    def body(at):
        x = x_ref[at, :].astype(F32)
        du = du_ref[at, :]
        r = lax.rsqrt(jnp.mean(x * x, axis=-1, keepdims=True) + NORM_EPS)
        xr = x * r
        dx_ref[at, :] = (dy_ref[at, :].astype(F32) + r * (du - xr * jnp.mean(xr * du, axis=-1, keepdims=True))).astype(BF16)

    rows_loop(x_ref.shape[0], 16, body)


def add_rows(x_ref, y_ref, out_ref):
    def body(at):
        out_ref[at, :] = (x_ref[at, :].astype(F32) + y_ref[at, :]).astype(BF16)

    rows_loop(x_ref.shape[0], 16, body)


def swap_halves(even, odd):
    low = lax.broadcasted_iota(jnp.int32, even.shape, len(even.shape) - 1) < even.shape[-1] // 2
    shift = even.shape[-1] // 2
    axis = len(even.shape) - 1
    return jnp.where(low, even, pltpu.roll(odd, shift, axis)), jnp.where(low, pltpu.roll(even, shift, axis), odd)


def split_columns(w_ref, cols_ref):
    tile = w_ref.shape[2] // (4 * RING * RING)
    for l in range(w_ref.shape[0]):
        for x in range(RING):
            for p in range(cols_ref.shape[3] // tile):
                pair = [w_ref[l, :, pl.ds((i * RING + x) * tile, tile)].astype(F32) for i in (2 * p, 2 * p + 1)]
                for c, value in enumerate(swap_halves(*pair)):
                    cols_ref[l, 2 * x + c, :, pl.ds(p * tile, tile)] = value.astype(cols_ref.dtype)


def join_columns(cols_ref, w_ref):
    tile = w_ref.shape[1] // (4 * RING * RING)
    for x in range(RING):
        for p in range(cols_ref.shape[2] // tile):
            pair = [cols_ref[2 * x + c, :, pl.ds(p * tile, tile)] for c in range(2)]
            for i, value in zip((2 * p, 2 * p + 1), swap_halves(*pair)):
                w_ref[:, pl.ds((i * RING + x) * tile, tile)] = value


def call(body, out_shape, out_spaces, in_spaces, scratch, remote, local, collective_id, *args):
    spaces = {'v': pl.BlockSpec(memory_space=pltpu.VMEM), 'h': pl.BlockSpec(memory_space=pl.ANY)}

    def kernel(*refs):
        net = Net(*refs[-5:-1])
        net.tile_sems = refs[-1]
        body(net, *refs[:-5])
        net.finish()
        assert net.n_remote <= remote and net.n_local <= local, (net.n_remote, net.n_local)
        if PRINT:
            print(body.__name__, net.n_remote, net.n_local, round(net.now, 1))

    return pl.pallas_call(
        kernel, out_shape=out_shape, in_specs=[spaces[s] for s in in_spaces], out_specs=[spaces[s] for s in out_spaces],
        scratch_shapes=list(scratch) + [pltpu.SemaphoreType.DMA((remote,)), pltpu.SemaphoreType.DMA((remote,)), pltpu.SemaphoreType.DMA((local,)),
                                               pltpu.SemaphoreType.REGULAR((8,)), pltpu.SemaphoreType.DMA((2,))],
        compiler_params=pltpu.CompilerParams(collective_id=collective_id, has_side_effects=True, vmem_limit_bytes=67000000),
        cost_estimate=pl.CostEstimate(flops=10**8, bytes_accessed=10**7, transcendentals=0),
        name=body.__name__)(*args)


PRINT = False
SCOPES = False


WIDE = 512
GR = 2
DU = 3


def wide_loop(total, body):
    wide = min(WIDE, total)

    def step(k, carry):
        body(k, wide, pl.ds(pl.multiple_of(k * wide, wide), wide))
        return carry

    lax.fori_loop(0, total // wide, step, 0)


def flat(value):
    return value.reshape(value.shape[0] * value.shape[1], value.shape[2])


def dot_rows(a, b):
    return jnp.dot(flat(a), flat(b), preferred_element_type=F32)


def dot_cols(a, b):
    return lax.dot_general(flat(a), flat(b), CONTRACT_COLS, preferred_element_type=F32)


def gelu(a):
    return 0.5 * a * (1.0 + jnp.tanh(GELU_C * (a + 0.044715 * a * a * a)))


def hidden_rows(net, chip, u, up, a, s):
    at = pl.ds(chip * 2, 2)

    def body(_, wide, cols):
        pre = dot_rows(u[at], up[:, :, cols]).astype(BF16)
        a[at, :, cols] = pre.reshape(2, -1, wide)
        s[at, :, cols] = gelu(pre.astype(F32)).astype(BF16).reshape(2, -1, wide)

    wide_loop(up.shape[2], body)
    net.spend(1.7)


def down_rows(net, chip, s, down, part):
    at = pl.ds(chip * 2, 2)

    def body(_, wide, cols):
        part[:, :, cols] = dot_rows(s[at], down[:, :, cols]).reshape(2, -1, wide)

    wide_loop(down.shape[2], body)
    net.spend(1.76)


def hidden_back_rows(net, chip, dy, down, ds):
    at = pl.ds(chip * 2, 2)
    rows = down.shape[1]

    def body(k, wide, cols):
        blocks = pl.ds(k * (wide // rows), wide // rows)
        ds[at, :, cols] = dot_cols(dy[at], down[blocks]).astype(BF16).reshape(2, -1, wide)

    wide_loop(down.shape[0] * rows, body)
    net.spend(1.5)


def gelu_both(a):
    t = jnp.tanh(GELU_C * (a + 0.044715 * a * a * a))
    return 0.5 * a * (1.0 + t), 0.5 * (1.0 + t) + 0.5 * a * (1.0 - t * t) * (GELU_C * (1.0 + 3 * 0.044715 * a * a))


def hidden_turn_rows(net, chip, u, up, s, ds):
    at = pl.ds(chip * 2, 2)

    def body(_, wide, cols):
        pre = dot_rows(u[at], up[:, :, cols]).astype(BF16).astype(F32)
        value, slope = gelu_both(pre)
        s[at, :, cols] = value.astype(BF16).reshape(2, -1, wide)
        ds[at, :, cols] = (ds[at, :, cols].astype(F32) * slope.reshape(2, -1, wide)).astype(BF16)

    wide_loop(up.shape[2], body)
    net.spend(2.1)


def pre_back_rows(net, chip, dy, down, a, da):
    at = pl.ds(chip * 2, 2)
    rows = down.shape[1]

    def body(k, wide, cols):
        blocks = pl.ds(k * (wide // rows), wide // rows)
        ds = dot_cols(dy[at], down[blocks]).astype(BF16).astype(F32).reshape(2, -1, wide)
        da[at, :, cols] = (ds * gelu_both(a[at, :, cols].astype(F32))[1]).astype(BF16)

    wide_loop(down.shape[0] * rows, body)
    net.spend(1.95)


def input_back_rows(net, chip, da, up, part):
    at = pl.ds(chip * 2, 2)
    rows = up.shape[1]

    def body(k, wide, cols):
        blocks = pl.ds(k * (wide // rows), wide // rows)
        part[:, :, cols] = dot_cols(da[at], up[blocks]).reshape(2, -1, wide)

    wide_loop(up.shape[0] * rows, body)
    net.spend(1.9)


def stored_tiles(net, count, compute, stage, out):
    def store(t):
        return pltpu.make_async_copy(stage.at[t % 2], out(t), net.tile_sems.at[t % 2])

    def step(t, carry):
        @pl.when(t >= 2)
        def _():
            store(t - 2).wait()

        compute(t, stage.at[t % 2])
        store(t).start()
        return carry

    lax.fori_loop(0, count, step, 0)
    for t in range(max(count - 2, 0), count):
        store(t).wait()


def dot_tokens(a, b):
    return lax.dot_general(flat(a), flat(b), CONTRACT_ROWS, preferred_element_type=F32)


def grad_tiles(net, lhs, rhs, stage, out):
    wide = stage.shape[1]

    def compute(t, slot):
        slot[...] = dot_tokens(lhs[:, :, pl.ds(pl.multiple_of(t * wide, wide), wide)], rhs[...])

    stored_tiles(net, lhs.shape[2] // wide, compute, stage, lambda t: out.at[pl.ds(pl.multiple_of(t * wide, wide), wide)])
    net.spend(3.9 * lhs.shape[2] / 1024)


def solution(mesh):
    nl, nd = mesh.shape['local'], mesh.shape['data']
    tok_spec = P(BOTH_AXES, None)
    w_spec = P(None, BOTH_AXES, None)

    def device_fn(tokens, grad_out, w_up, w_down):
        num_layers, ur, ffn = w_up.shape
        dr = w_down.shape[1]
        rows, width = tokens.shape
        hidden = nl * dr
        shape = jax.ShapeDtypeStruct
        up_full = shape((nl, nd * ur, hidden), BF16)
        down_full = shape((nl, dr, width), BF16)
        act_full = shape((nd, rows, width), BF16)
        hid_full = shape((nd, rows, hidden), BF16)
        own = shape((rows, width), BF16)
        part_vmem = pltpu.VMEM((RING, 2, rows, width), F32)
        rx = [part_vmem] + reduce_x_scratch(rows, width)
        sums = sums_scratch(dr, hidden) * 4 + sums_stage(dr, hidden) * 2

        def vmem(like):
            return pltpu.VMEM(like.shape, like.dtype)

        def forward(net, x_ref, g_in, w_up_ref, down_in, block_out, u_out, a_out, s_out, up_out, down_out, next_out, g_out, ds_out, keep_out, x_out,
                    cols, next_own, u, g, up0, down0, up1, down1, a, s, ds, part, *rx_scratch):
            net.arrive('dyz')
            names = ('blocks', 'blocks1', 'sent_u', 'got_u', 'got_g', 'sent_up0', 'sent_down0', 'sent_up1', 'sent_down1', 'got_up0', 'got_down0', 'got_up1', 'got_down1', 'reduced')
            ev = {name: Event(name=name) for name in names}
            ev['got_up0'].rank = 2
            made = [Event(name='made%d' % k) for k in range(RING)]
            hidden_made = [Event(name='hidden%d' % k) for k in range(RING)]
            def gather(name, own, full, split):
                size = own.shape[0] // 2

                def join(kind, events):
                    yield events
                    fire(net, ev[kind + name])

                got, sent = [Event(), Event()], [Event(), Event()]
                for k, first in enumerate('yz'):
                    net.spawn(gather_yz(net, own.at[pl.ds(k * size, size)], full, first, got[k], sent[k], k * size, split=split))
                net.spawn(join('got_', got))
                net.spawn(join('sent_', sent))

            net.enter()
            gather('down0', down_in.at[0], down0, False)
            split_columns(w_up_ref, cols)
            net.spend(0.5)
            net.spawn(exchange(net, cols.at[0], block_out.at[0], ev['blocks']))
            norm_rows(x_ref, u.at[net.data])
            net.spend(0.7)
            net.spawn(gather_x(net, u, ev['got_u'], ev['sent_u']))
            grad = net.load(g_in, g.at[net.data])

            def up_first():
                yield [ev['blocks']]
                gather('up0', block_out.at[0], up0, True)
                yield [ev['sent_u']]
                net.spawn(exchange(net, cols.at[1], block_out.at[1], ev['blocks1']))
                yield [grad]
                net.spawn(gather_x(net, g, ev['got_g']))

            def second():
                yield [ev['sent_up0'], ev['sent_down0'], ev['blocks1']]
                gather('down1', down_in.at[1], down1, False)
                yield [ev['sent_down1']]
                gather('up1', block_out.at[1], up1, True)

            def save(event, *pairs):
                yield [ev[event]]
                yield [net.save(src, dst) for src, dst in pairs]

            def hidden_flow():
                yield [ev['got_u'], ev['got_up0']]
                for k, step in enumerate(STEPS):
                    hidden_rows(net, net.at('x', step), u, up0, a, s)
                    fire(net, hidden_made[k])
                    yield [Event(net.now, 2)]
                yield [net.save(a, a_out), net.save(s, s_out), net.save(u, u_out)]

            def down_flow():
                for k, step in enumerate(STEPS):
                    yield [hidden_made[k], ev['got_down0'], Event(0.0, 1)]
                    down_rows(net, net.at('x', step), s, down0, part.at[k])
                    fire(net, made[k])
                yield [net.save(down0.at[yz_index(net, 'z', *far)], keep_out.at[k]) for k, far in enumerate(FAR)]

            def act():
                yield [ev['reduced']]
                add_rows(x_ref, part.at[3, net.core], x_out)
                norm_rows(x_out, next_own)
                net.spend(1.0)
                yield [net.load(next_own, next_out)]

            def back_flow():
                for k, step in enumerate(STEPS):
                    yield [ev['got_g'], ev['got_down1'], Event(0.0, 3)]
                    hidden_back_rows(net, net.at('x', step), g, down1, ds)
                yield [net.load(ds, ds_out)]

            half = down_out.shape[3]
            for flow in (up_first(), second(), hidden_flow(), down_flow(), act(), back_flow(), reduce_x(net, part, made, rx_scratch, ev['reduced']),
                         save('got_up1', (up1, up_out)), save('got_down1', *[(down1.at[:, :, pl.ds(h * half, half)], down_out.at[h]) for h in range(2)]),
                         save('got_g', (g, g_out))):
                net.spawn(flow)
            net.run()

        def turn(net, u_in, up_in, down_in, ds_in, g_in, u0_in, a0_in, s0_in, keep_in, x_ref, x0_ref, g_own, block_in, w_down_in,
                 x_out, dx_out, d_up0, d_down0, d_up1, d_down1, dw_up1, dw_down1, dw_up0, dw_down0,
                 own_up, u, up1, up0, down0, half_in, ds, s, stage, part, *scratch):
            net.arrive('dyz')
            inputs = [net.load(u_in, u.at[net.data]), net.load(up_in, up1), net.load(ds_in, ds)]
            inputs[0].wait()
            inputs[0].waited = True
            net.enter()
            rx_scratch = scratch[:5]
            stages = (scratch[21:24], scratch[24:27])
            jobs = [[Sums(net, first, scratch[5 + 8 * n + 4 * k:9 + 8 * n + 4 * k], stages[k]) for k, first in enumerate('yz')] for n in range(2)]
            names = ('got_u', 'hidden', 'all_du', 'reduced', 'sent_dy', 'got_dy', 'got_up0', 'got_up0_rest', 'got_down0', 'd_down1', 'd_up1', 'y_reduced', 'acts',
                     'd_down0', 'da0', 'd_up0', 'du_reduced', 'out_up1', 'out_up0') + tuple(
                'sum_%s%d%d' % (kind, layer, k) for kind in ('up', 'down') for layer in range(2) for k in range(2))
            ev = {name: Event(name=name) for name in names}
            made, y_made, du_made = ([Event(name='%s%d' % (name, k)) for k in range(RING)] for name in ('made', 'y_made', 'du_made'))
            wide = half_in.shape[2]
            top = nd * ur * 3 // 4

            def columns(h):
                return pl.ds(h * wide, wide)

            here = {step: Event(name='u%d' % step) for step in STEPS}
            dy_here = {step: Event() for step in STEPS}
            net.spawn(gather_x(net, u, ev['got_u'], chips=here))
            net.spawn(gather_yz(net, w_down_in.at[0], down0, 'z', ev['got_down0'], near=True))
            net.spawn(gather_yz(net, block_in.at[0, pl.ds(0, top)], up0, 'y', ev['got_up0']))
            net.spawn(gather_yz(net, block_in.at[0, pl.ds(top, nd * ur - top)], up0, 'z', ev['got_up0_rest'], offset=top))
            net.spawn(reduce_x(net, part, made, rx_scratch, ev['reduced']))
            frees = [[Event(0.0) for _ in range(3)] for _ in range(2)]

            def up_place(ref, k):
                half = nd * ur // 2
                return lambda block, rows: ref.at[pl.ds(pl.multiple_of(block * (2 * half) + k * half + rows.start, rows.size), rows.size)]

            def down_place(ref, k):
                return lambda block, rows: ref.at[pl.ds(pl.multiple_of(block * dr + rows.start, rows.size), rows.size), columns(k)]

            def sum_job(n, place, ref, ready, name, credits=()):
                passed = [Event(), Event()]
                for k in range(2):
                    start = Event()
                    ev['start_%s%d' % (name, k)] = start
                    net.spawn(gate(start, ready + ([credits[k]] if credits else [])))
                    net.spawn(jobs[n][k].run(place(ref, k), start, ev['sum_%s%d' % (name, k)], frees[k], passed[k]))
                return passed

            def gate(event, items):
                yield items
                fire(net, event)

            left = [RING, RING]

            def layer1(k, step):
                yield [here[step], Event(0.0, 1)] + inputs[1:]
                hidden_turn_rows(net, net.at('x', step), u, up1, s, ds)
                left[0] -= 1
                if left[0] == 0:
                    fire(net, ev['hidden'])
                yield [Event(net.now, DU)]
                input_back_rows(net, net.at('x', step), ds, up1, part.at[k])
                fire(net, made[k])
                left[1] -= 1
                if left[1] == 0:
                    fire(net, ev['all_du'])

            def grads1():
                for h in range(2):
                    yield [net.load(g_in.at[:, :, columns(h)], half_in), Event(0.0, GR), ev['hidden']]
                    grad_tiles(net, s, half_in, stage, d_down1.at[:, columns(h)])
                fire(net, ev['d_down1'])
                for h in range(2):
                    yield [Event(net.now, GR)]
                    grad_tiles(net, u.at[:, :, columns(h)], ds, stage, d_up1.at[columns(h)])
                fire(net, ev['d_up1'])

            def act():
                yield [ev['d_up1'], ev['got_u']]
                net.drain(ev['got_u'].copies)
                credit = net.grant(0, 'xp')
                yield [ev['reduced'], credit]
                norm_back_rows(x_ref, g_own, part.at[3, net.core], u.at[net.data])
                net.spend(0.7)
                net.spawn(gather_x(net, u, ev['got_dy'], ev['sent_dy'], dy_here))

            def layer1_out():
                yield [ev['all_du'], ev['d_up1']]
                yield [net.load(down_in.at[h], up1.at[:, pl.ds(h * dr, dr)]) for h in range(2)]
                yield [ev['reduced'], Event(0.0, 2)]
                net.drain(ev['reduced'].copies)
                credit = net.grant(1, 'xp')
                for k, step in enumerate(STEPS):
                    for h in range(2):
                        net.spend(-0.88)
                        down_rows(net, net.at('x', step), s, up1.at[:, pl.ds(h * dr, dr)], part.at[k, :, :, columns(h)])
                    yield [Event(net.now, 2)]
                loads = [net.load(a0_in, up1.at[pl.ds(0, nd)]), net.load(s0_in, up1.at[pl.ds(nd, nd)])]
                loads += [net.load(keep_in.at[k], down0.at[yz_index(net, 'z', *far)]) for k, far in enumerate(FAR)]
                yield loads
                fire(net, ev['acts'])
                yield [ev['sent_dy'], credit]
                net.spawn(reduce_x(net, part, y_made, rx_scratch, ev['y_reduced']))
                for k in range(RING):
                    fire(net, y_made[k])
                yield [ev['y_reduced']]
                add_rows(x_ref, part.at[3, net.core], x_out)

            a0, s0 = up1.at[pl.ds(0, nd)], up1.at[pl.ds(nd, nd)]
            backs = [RING]

            def layer0_hidden(step):
                yield [dy_here[step], ev['acts'], ev['got_down0'], Event(0.0, 2)]
                pre_back_rows(net, net.at('x', step), u, down0, a0, ds)
                backs[0] -= 1
                if backs[0] == 0:
                    fire(net, ev['da0'])

            def layer0():
                yield [ev['d_down1']]
                first = net.load(u0_in.at[:, :, columns(0)], half_in)
                for h in range(2):
                    yield [net.load(u0_in.at[:, :, columns(h)], half_in) if h else first]
                    yield [ev['da0'], Event(0.0, 3)]
                    grad_tiles(net, half_in, ds, stage, d_up0.at[columns(h)])
                fire(net, ev['d_up0'])
                for h in range(2):
                    yield [ev['got_dy'], ev['acts'], Event(0.0, 3)]
                    grad_tiles(net, s0, u.at[:, :, columns(h)], stage, d_down0.at[:, columns(h)])
                fire(net, ev['d_down0'])
                yield [ev['y_reduced'], ev['got_up0'], ev['got_up0_rest'], Event(0.0, 2)]
                net.drain(ev['y_reduced'].copies)
                yield [net.grant(2, 'xp')]
                net.spawn(reduce_x(net, part, du_made, rx_scratch, ev['du_reduced']))
                for k, step in enumerate(STEPS):
                    input_back_rows(net, net.at('x', step), ds, up0, part.at[k])
                    fire(net, du_made[k])
                    yield [Event(net.now, 2)]
                yield [ev['du_reduced']]
                norm_back_rows(x0_ref, u.at[net.data], part.at[3, net.core], dx_out)

            def out_down(layer, dw_down, credit):
                def one(k):
                    done = ev['sum_down%d%d' % (layer, k)]
                    yield [done]
                    yield [net.load(done.total, dw_down.at[:, columns(k)])]
                    if credit is not None:
                        net.drain(done.copies)
                        yield [net.grant(credit + k, 'yz')]
                        fire(net, freed[credit + k])

                for k in range(2):
                    net.spawn(one(k))

            def out_up(layer, dw_up, credit):
                copied = [Event(), Event()]

                def one(k):
                    done = ev['sum_up%d%d' % (layer, k)]
                    yield [done]
                    copy_rows(net, done.total, own_up.at[pl.ds(k * (nd * ur // 2), nd * ur // 2)])
                    fire(net, copied[k])
                    if credit is not None:
                        net.drain(done.copies)
                        yield [net.grant(credit + k, 'yz')]
                        fire(net, freed[credit + k])

                def both():
                    yield copied + ([ev['out_up1']] if layer == 0 else [])
                    net.spawn(exchange_back(net, own_up, dw_up, ev['out_up%d' % layer]))

                for k in range(2):
                    net.spawn(one(k))
                net.spawn(both())

            freed = {k: Event() for k in range(3, 7)}
            passed = sum_job(0, down_place, d_down1, [ev['d_down1']], 'down1')
            passed = sum_job(1, up_place, d_up1, [ev['d_up1']] + passed, 'up1')
            passed = sum_job(0, up_place, d_up0, [ev['d_up0']] + passed, 'up0', [freed[3], freed[4]])
            sum_job(1, down_place, d_down0, [ev['d_down0']] + passed, 'down0', [freed[5], freed[6]])
            out_down(1, dw_down1, 3)
            out_up(1, dw_up1, 5)
            out_up(0, dw_up0, None)
            out_down(0, dw_down0, None)

            for k in (3, 2, 1, 0):
                net.spawn(layer1(k, STEPS[k]))
            for step in (0, -1, 1, 2):
                net.spawn(layer0_hidden(step))
            for flow in (grads1(), act(), layer1_out(), layer0()):
                net.spawn(flow)
            net.run()

        def finish(up1_ref, up0_ref, down1_ref, down0_ref, x_ref, dx_ref, x_out, dx_out, up_out, down_out):
            for l, (up_ref, down_ref) in enumerate(((up0_ref, down0_ref), (up1_ref, down1_ref))):
                join_columns(up_ref, up_out.at[l])
                rows_loop(dr, 16, lambda at: down_out.at[l].__setitem__((at, slice(None)), down_ref[at, :]))
            rows_loop(rows, 16, lambda at: x_out.__setitem__((at, slice(None)), x_ref[at, :]))
            rows_loop(rows, 16, lambda at: dx_out.__setitem__((at, slice(None)), dx_ref[at, :]))

        d_up_own, d_down_own = shape((nd, ur, hidden), F32), shape((dr, width), F32)

        blocks, u0, a0, s0, up1, down1, u1, g_full, ds1, keep, x1 = call(
            forward, [shape((num_layers, nd * ur, hidden), BF16), act_full, hid_full, hid_full, up_full, shape((2, nl, dr, width // 2), BF16),
                      own, act_full, hid_full, shape((len(FAR), dr, width), BF16), own],
            'hhhhhhhhhhv', 'vhvh',
            [pltpu.VMEM((num_layers, nd, ur, hidden), BF16), vmem(own)] + [vmem(act_full)] * 2 + [vmem(up_full), vmem(down_full)] * 2 + [vmem(hid_full)] * 3 + rx,
            320, 64, 0, tokens, grad_out, w_up, w_down)
        d_up_full, d_down_full = shape((width, hidden), F32), shape((hidden, width), F32)
        x_out, dx, _, _, _, _, *grads = call(
            turn, [own, own] + [d_up_full, d_down_full] * 2 + [d_up_own, d_down_own] * 2, 'vv' + 'h' * 8, 'hhhhhhhhhvvvhh',
            [pltpu.VMEM((nd * ur, hidden), F32), vmem(act_full), vmem(up_full), vmem(up_full), vmem(down_full), pltpu.VMEM((nd, rows, width // 2), BF16), vmem(hid_full), vmem(hid_full),
             pltpu.VMEM((2, hidden // 2, width // 2), F32)] + rx + sums, 400, 160, 1,
            u1, up1, down1, ds1, g_full, u0, a0, s0, keep, x1, tokens, grad_out, blocks, w_down)
        up1_own, down1_own, up0_own, down0_own = grads
        return pl.pallas_call(
            finish, out_shape=[own, own, shape(w_up.shape, F32), shape(w_down.shape, F32)], name='finish',
            in_specs=[pl.BlockSpec(memory_space=pltpu.VMEM)] * 6, out_specs=[pl.BlockSpec(memory_space=pltpu.VMEM)] * 4,
        )(up1_own, up0_own, down1_own, down0_own, x_out, dx)

    return jax.shard_map(device_fn, mesh=mesh, in_specs=(tok_spec, tok_spec, w_spec, w_spec), out_specs=(tok_spec, tok_spec, w_spec, w_spec), check_vma=False)
```

```python
import contextlib

import jax
import jax.numpy as jnp
from jax import lax
from jax.experimental import pallas as pl
from jax.experimental.pallas import tpu as pltpu
from jax.sharding import PartitionSpec as P

NORM_EPS = 1e-6
BOTH_AXES = ('local', 'data')
CONTRACT_ROWS = (((0,), (0,)), ((), ()))
CONTRACT_COLS = (((1,), (1,)), ((), ()))
MESH = pl.DeviceIdType.MESH
RING = 4
F32, BF16 = jnp.float32, jnp.bfloat16

LINK_RATE = 46.0e3
PAIR_RATE = 600e3
LOCAL_RATE = 3000e3
HOP = 2.4
PAIR_HOP = 1.0
ENTRY = 3.0
SLACK = 0.1
GELU_C = 0.7978845608028654


def scope(label):
    return jax.named_scope(label) if SCOPES else contextlib.nullcontext()


class Event:
    def __init__(self, time=None, rank=0, name=''):
        self.time, self.rank, self.name = time, rank, name


class Copy:
    def __init__(self, desc, time, remote):
        self.desc, self.time, self.remote, self.rank, self.waited = desc, time, remote, 0, False

    def wait(self):
        if self.remote:
            self.desc.wait_recv()
        else:
            self.desc.wait()


class Credit:
    def __init__(self, semaphore, count, time):
        self.semaphore, self.count, self.time, self.rank, self.waited = semaphore, count, time, 0, False

    def wait(self):
        pl.semaphore_wait(self.semaphore, self.count)


class Pool:
    def __init__(self):
        self.slots, self.next = [], 0

    def again(self):
        self.next = 0
        return self


class Net:
    def __init__(self, send_sems, recv_sems, local_sems, credit_sems):
        self.send_sems, self.recv_sems, self.local_sems, self.credit_sems = send_sems, recv_sems, local_sems, credit_sems
        self.n_remote = self.n_local = 0
        self.free_sends = list(range(send_sems.shape[0]))
        self.free_locals = []
        self.now = 0.0
        self.free = {}
        self.sent = []
        self.flows = []
        self.labels = {}
        here = lax.axis_index('local')
        there = lax.axis_index('data')
        self.data = there
        self.pos = {'z': here // RING, 'y': here % RING, 'x': there // 2}
        self.core = there % 2

    def at(self, axis, step):
        return (self.pos[axis] + (step + RING)) % RING

    def device(self, axis, step):
        if axis == 'p':
            return {'data': self.pos['x'] * 2 + (1 - self.core)}
        if axis == 'd':
            return {'data': (self.data + step) % (2 * RING)}
        to = self.at(axis, step)
        if axis == 'x':
            return {'data': to * 2 + self.core}
        if axis == 'y':
            return {'local': self.pos['z'] * RING + to}
        return {'local': to * RING + self.pos['y']}

    def peers(self, axes):
        return [(axis, step) for axis in axes for step in ((1, -1) if axis in 'xyz' else (1,) if axis == 'p' else range(1, 2 * RING))]

    def signal(self, semaphore, axes):
        for axis, step in self.peers(axes):
            pl.semaphore_signal(semaphore, inc=1, device_id=self.device(axis, step), device_id_type=MESH)

    def arrive(self, axes):
        self.entry, self.entered = pltpu.get_barrier_semaphore(), len(self.peers(axes))
        self.signal(self.entry, axes)

    def enter(self):
        pl.semaphore_wait(self.entry, self.entered)
        self.now = max(self.now, ENTRY)

    def grant(self, k, axes):
        self.signal(self.credit_sems.at[k], axes)
        return Credit(self.credit_sems.at[k], len(self.peers(axes)), self.now + HOP)

    def drain(self, copies):
        for copy in copies:
            if copy in self.sent:
                copy.desc.wait_send()
                self.sent.remove(copy)
                self.free_sends.append(copy.slot)

    def idle(self, gap):
        over = [copy for copy in self.sent if copy.time + 1.5 < self.now]
        self.drain(over[:int(gap / 0.05)])

    def send(self, src, dst, axis, step=1, pool=None):
        if pool is not None and pool.next < len(pool.slots):
            k = pool.slots[pool.next]
        else:
            k = self.n_remote
            self.n_remote += 1
            if pool is not None:
                pool.slots.append(k)
        if pool is not None:
            pool.next += 1
        if not self.free_sends:
            if PRINT:
                print('EXHAUSTED', round(self.now, 1))
            self.drain([min(self.sent, key=lambda copy: copy.time)])
        send_slot = self.free_sends.pop()
        desc = pltpu.make_async_remote_copy(
            src_ref=src, dst_ref=dst, send_sem=self.send_sems.at[send_slot], recv_sem=self.recv_sems.at[k],
            device_id=self.device(axis, step), device_id_type=MESH)
        desc.start()
        size = 1
        for n in dst.shape:
            size *= n
        size *= dst.dtype.itemsize
        rate = PAIR_RATE if axis == 'p' else LINK_RATE
        if axis == 'd':
            axis, step, size = ('p', 1, size) if step == 1 else ('x', 1 if step < RING + 2 else -1, size)
        key = (axis, step)
        done = max(self.free.get(key, 0.0), self.now) + size / rate
        self.free[key] = done
        copy = Copy(desc, done + (PAIR_HOP if axis == 'p' else HOP), True)
        copy.slot = send_slot
        self.sent.append(copy)
        return copy

    def load(self, src, dst):
        if not self.free_locals:
            self.free_locals.append(self.n_local)
            self.n_local += 1
        k = self.free_locals.pop()
        desc = pltpu.make_async_copy(src, dst, self.local_sems.at[k])
        desc.start()
        size = 1
        for n in dst.shape:
            size *= n
        done = max(self.free.get('hbm', 0.0), self.now) + size * dst.dtype.itemsize / LOCAL_RATE
        self.free['hbm'] = done
        copy = Copy(desc, done + 0.9, False)
        copy.slot = k
        return copy

    def save(self, src, dst):
        copy = self.load(src, dst)
        copy.time += 4.0
        return copy

    def spend(self, microseconds):
        self.now += microseconds

    def spawn(self, flow):
        self.step(flow)

    def step(self, flow):
        try:
            if flow not in self.labels:
                self.labels[flow] = [flow.__name__, len(self.labels), 0]
            self.labels[flow][2] += 1
            self.flows.append((flow, next(flow)))
        except StopIteration:
            pass

    def run(self):
        while self.flows:
            best = None
            for k, (_, items) in enumerate(self.flows):
                if any(item.time is None for item in items):
                    continue
                time = max([item.time for item in items] + [0.0])
                late = max([item.rank for item in items] + [0])
                rank = (max(time, self.now) + (SLACK if late else 0.0), late, time)
                if best is None or rank < best[0]:
                    best = (rank, k, time)
            _, k, time = best
            flow, items = self.flows.pop(k)
            self.idle(time - self.now)
            label = '%s_%d_%d' % tuple(self.labels[flow])
            with scope('w_' + label):
                for item in items:
                    if not isinstance(item, Event) and not item.waited:
                        item.wait()
                        item.waited = True
                        if isinstance(item, Copy) and not item.remote:
                            self.free_locals.append(item.slot)
            before = self.now
            self.now = max(self.now, time)
            if PRINT:
                print('STEP', label, round(before, 2), round(self.now, 2))
            with scope('s_' + label):
                self.step(flow)

    def finish(self):
        for copy in self.sent:
            copy.desc.wait_send()


def rows_loop(rows, chunk, body):
    chunk = min(chunk, rows)

    def step(k, carry):
        body(pl.ds(pl.multiple_of(k * chunk, chunk), chunk))
        return carry

    lax.fori_loop(0, rows // chunk, step, 0)


def add_into(net, dst, *others):
    rows, cols = dst.shape

    def body(at):
        total = dst[at, :]
        for other in others:
            total = total + other[at, :]
        dst[at, :] = total

    rows_loop(rows, 16, body)
    net.spend(rows * cols * 4 * (1 + len(others)) / 4e6)


def fire(net, event):
    event.time = net.now
    if PRINT and event.name:
        print('   %7.1f %s' % (net.now, event.name))


def exchange(net, src, dst, done):
    rows = src.shape[1]

    def mine():
        return dst.at[pl.ds(pl.multiple_of(net.data * rows, rows), rows)]

    own = net.load(src.at[net.data], mine())
    copies = [net.send(src.at[(net.data + k) % (2 * RING)], mine(), 'd', k) for k in (4, 5, 2, 3, 6, 7, 1)]
    yield [own] + copies
    fire(net, done)


def exchange_back(net, src, dst, done):
    rows = dst.shape[1]

    def block(k):
        return src.at[pl.ds(pl.multiple_of(k * rows, rows), rows)]

    own = net.load(block(net.data), dst.at[net.data])
    copies = [net.send(block((net.data + k) % (2 * RING)), dst.at[net.data], 'd', k) for k in (4, 5, 2, 3, 6, 7, 1)]
    yield [own] + copies
    net.drain(copies)
    fire(net, done)


def copy_rows(net, src, dst):
    def body(at):
        dst[at, :] = src[at, :]

    rows_loop(src.shape[0], 16, body)
    net.spend(0.2)


def gather_x(net, full, done, issued=None, chips=None, pool=None):
    half = full.shape[1] // 2
    lo, hi = pl.ds(0, half), pl.ds(half, half)
    chips = chips or {step: Event() for step in STEPS}
    left = [2]
    done.copies = []

    def send(*args):
        done.copies.append(net.send(*args, pool=pool))
        return done.copies[-1]

    def block(step):
        return full.at[net.at('x', step) * 2 + net.core]

    def part(step, rows):
        return full.at[net.at('x', step) * 2 + net.core, rows]

    relays = []

    def side(step, first, second, mine):
        yield [mine[0]]
        relays.append(send(part(step, first), part(step, first), 'x', -step))
        left[0] -= 1
        if left[0] == 0:
            net.spawn(far())
            if issued is not None:
                fire(net, issued)
        yield [mine[1]]
        pair = send(block(step), block(step), 'p')
        yield [pair]
        fire(net, chips[step])

    def far():
        yield relays
        pair = send(block(2), block(2), 'p')
        yield [pair]
        fire(net, chips[2])

    forth = [send(part(0, rows), part(0, rows), 'x', 1) for rows in (lo, hi)]
    back = [send(part(0, rows), part(0, rows), 'x', -1) for rows in (hi, lo)]
    pair = send(block(0), block(0), 'p')
    net.spawn(side(-1, lo, hi, forth))
    net.spawn(side(1, hi, lo, back))
    yield [pair]
    fire(net, chips[0])
    yield [chips[step] for step in STEPS]
    fire(net, done)


def gather_yz(net, own, full, first, done, issued=None, offset=0, near=False, split=True, pool=None):
    second = 'y' if first == 'z' else 'z'
    size = own.shape[0]
    half = size // 2
    lo, hi, both = pl.ds(offset, half), pl.ds(offset + half, half), pl.ds(offset, size)
    forward, backward = ((lo, hi), (hi, lo)) if split and not near else ((both,), (both,))

    def part(one, two, rows):
        return full.at[yz_index(net, first, one, two), rows]

    left = [3 if near else RING, 3 if near else RING]

    def arrived(which):
        left[which] -= 1
        if left[which] == 0 and (done, issued)[which] is not None:
            fire(net, (done, issued)[which])

    def send(one, rows, axis, step):
        src = own.at[pl.ds(rows.start - offset, rows.size)] if one == 0 else part(one, 0, rows)
        return net.send(src, part(one, 0, rows), axis, step, pool)

    def column(one):
        forth = [send(one, rows, second, 1) for rows in forward]
        back = [send(one, rows, second, -1) for rows in backward]

        def finish():
            if near:
                arrived(1)
                yield forth + back
            else:
                yield [forth[0]]
                relays = [net.send(part(one, -1, lo), part(one, -1, lo), second, 1, pool)]
                yield [back[0]]
                relays.append(net.send(part(one, 1, hi), part(one, 1, hi), second, -1, pool))
                arrived(1)
                yield forth[1:] + back[1:] + relays
            arrived(0)

        net.spawn(finish())

    relays = []

    def side(step, first_half, mine):
        yield [mine[0]]
        if not near:
            relays.append(net.send(part(step, 0, first_half), part(step, 0, first_half), first, -step, pool))
            if len(relays) == 2:
                net.spawn(far())
        yield mine[1:]
        column(step)

    def far():
        yield relays
        column(2)

    mine = [net.load(own, part(0, 0, both))]
    forth = [send(0, rows, first, 1) for rows in forward]
    back = [send(0, rows, first, -1) for rows in backward]
    column(0)
    net.spawn(side(-1, lo, forth))
    net.spawn(side(1, hi, back))
    left[0] += 1
    yield mine
    arrived(0)


def yz_index(net, first, one, two):
    at_one, at_two = net.at(first, one), net.at('y' if first == 'z' else 'z', two)
    return at_one * RING + at_two if first == 'z' else at_two * RING + at_one


FAR = [(2, 0), (2, 1), (2, -1), (2, 2), (0, 2), (1, 2), (-1, 2)]


STEPS = (2, 1, -1, 0)
WINDOW = 2


def reduce_x(net, part, made, scratch, done, pool=None):
    other, relay_f, relay_b, last_f, last_b = scratch
    half = part.shape[2] // 2
    lo, hi = pl.ds(0, half), pl.ds(half, half)

    def acc(k, rows=None):
        return part.at[k, net.core] if rows is None else part.at[k, net.core, rows]

    pairs = [None] * RING
    ready = [Event() for _ in STEPS]

    def pair(k):
        yield [made[k]]
        pairs[k] = net.send(part.at[k, 1 - net.core], other.at[k], 'p', pool=pool)
        yield [pairs[k]]
        add_into(net, acc(k), other.at[k])
        fire(net, ready[k])

    for k in range(RING):
        net.spawn(pair(k))
    sent = {}
    started = Event()

    def part_flow(k):
        yield [ready[k]]
        if k == 0:
            sent['first_f'] = net.send(acc(0, lo), relay_f, 'x', 1, pool=pool)
            sent['first_b'] = net.send(acc(0, hi), relay_b, 'x', -1, pool=pool)
        elif k == 1:
            sent['direct_f'] = net.send(acc(1, hi), last_f.at[hi], 'x', 1, pool=pool)
        else:
            sent['direct_b'] = net.send(acc(2, lo), last_b.at[lo], 'x', -1, pool=pool)
        if len(sent) == 4:
            fire(net, started)

    for k in range(3):
        net.spawn(part_flow(k))
    yield [started]
    yield [sent['first_f']]
    add_into(net, acc(1, lo), relay_f)
    summed_f = net.send(acc(1, lo), last_f.at[lo], 'x', 1, pool=pool)
    yield [sent['first_b']]
    add_into(net, acc(2, hi), relay_b)
    summed_b = net.send(acc(2, hi), last_b.at[hi], 'x', -1, pool=pool)
    yield [ready[3], sent['direct_f'], sent['direct_b'], summed_f, summed_b]
    add_into(net, acc(3), last_f, last_b)
    done.copies = pairs + list(sent.values()) + [summed_f, summed_b]
    fire(net, done)


def reduce_x_scratch(rows, cols):
    return [pltpu.VMEM((RING, rows, cols), F32), pltpu.VMEM((rows // 2, cols), F32), pltpu.VMEM((rows // 2, cols), F32),
            pltpu.VMEM((rows, cols), F32), pltpu.VMEM((rows, cols), F32)]


def load_parts(net, src, part, made):
    for k, step in enumerate(STEPS):
        def bring(k=k, step=step):
            yield [net.load(src.at[pl.ds(net.at('x', step) * 2, 2)], part.at[k])]
            fire(net, made[k])

        net.spawn(bring())


class Sums:
    def __init__(self, net, first, scratch, stage):
        self.net, self.first, self.scratch, self.stage = net, first, scratch, stage
        self.second = 'y' if first == 'z' else 'z'

    def run(self, place, start, done, free, passed_all, pool):
        net, first, second = self.net, self.first, self.second
        relay1, last1, relay2, last2 = self.scratch
        ahead, behind, mine = self.stage
        half = mine.shape[0] // 2
        lo, hi, all_rows = pl.ds(0, half), pl.ds(half, half), pl.ds(0, 2 * half)
        done.copies = []

        def send(*args):
            done.copies.append(net.send(*args, pool=pool))
            return done.copies[-1]

        def term(one, two, rows=all_rows):
            return place(yz_index(net, first, one, two), rows)

        def bring(gate, src, dst, got):
            yield [gate, start]
            yield [net.load(src, dst)]
            fire(net, got)

        chain = [[gate] + [Event() for _ in range(RING)] for gate in free]
        free[:] = [events[RING] for events in chain]
        got = [[Event() for _ in range(RING)] for _ in range(3)]
        ends = [Event() for _ in STEPS]
        passed = [Event() for _ in range(RING - 1)] + [passed_all]

        def ring(k):
            two = STEPS[k]
            if k >= WINDOW:
                yield [passed[k - WINDOW]]
            net.spawn(bring(chain[0][k], term(1, two, lo), ahead, got[0][k]))
            net.spawn(bring(chain[1][k], term(-1, two, hi), behind, got[1][k]))
            net.spawn(bring(chain[2][k], term(0, two), mine, got[2][k]))
            first_f = send(term(2, two, lo), relay1.at[0, k], first, 1)
            first_b = send(term(2, two, hi), relay1.at[1, k], first, -1)
            direct_f = send(term(1, two, hi), last1.at[0, k, hi], first, 1)
            direct_b = send(term(-1, two, lo), last1.at[1, k, lo], first, -1)
            yield [first_f, got[0][k]]
            add_into(net, relay1.at[0, k], ahead)
            fire(net, chain[0][k + 1])
            summed_f = send(relay1.at[0, k], last1.at[0, k, lo], first, 1)
            yield [first_b, got[1][k]]
            add_into(net, relay1.at[1, k], behind)
            fire(net, chain[1][k + 1])
            summed_b = send(relay1.at[1, k], last1.at[1, k, hi], first, -1)
            fire(net, passed[k])
            yield [direct_f, direct_b, summed_f, summed_b, got[2][k]]
            add_into(net, last1.at[0, k], last1.at[1, k], mine)
            fire(net, chain[2][k + 1])
            fire(net, ends[k])

        def sums(k, rows=all_rows):
            return last1.at[0, k, rows]

        yield [start]
        for k in range(RING):
            net.spawn(ring(k))
        yield [ends[0]]
        first_f = send(sums(0, lo), relay2.at[0], second, 1)
        first_b = send(sums(0, hi), relay2.at[1], second, -1)
        yield [ends[1]]
        direct_f = send(sums(1, hi), last2.at[0, hi], second, 1)
        yield [ends[2]]
        direct_b = send(sums(2, lo), last2.at[1, lo], second, -1)
        yield [first_f]
        add_into(net, sums(1, lo), relay2.at[0])
        summed_f = send(sums(1, lo), last2.at[0, lo], second, 1)
        yield [first_b]
        add_into(net, sums(2, hi), relay2.at[1])
        summed_b = send(sums(2, hi), last2.at[1, hi], second, -1)
        yield [ends[3], direct_f, direct_b, summed_f, summed_b]
        add_into(net, sums(3), last2.at[0], last2.at[1])
        done.total = sums(3)
        fire(net, done)


def sums_scratch(rows, cols):
    return [pltpu.VMEM((2, RING, rows // 2, cols), F32), pltpu.VMEM((2, RING, rows, cols), F32),
            pltpu.VMEM((2, rows // 2, cols), F32), pltpu.VMEM((2, rows, cols), F32)]


def sums_stage(rows, cols):
    return [pltpu.VMEM((rows // 2, cols), F32), pltpu.VMEM((rows // 2, cols), F32), pltpu.VMEM((rows, cols), F32)]


def norm_rows(x_ref, u_ref):
    def body(at):
        x = x_ref[at, :].astype(F32)
        u_ref[at, :] = (x * lax.rsqrt(jnp.mean(x * x, axis=-1, keepdims=True) + NORM_EPS)).astype(BF16)

    rows_loop(x_ref.shape[0], 16, body)


def norm_back_rows(x_ref, dy_ref, du_ref, dx_ref):
    def body(at):
        x = x_ref[at, :].astype(F32)
        du = du_ref[at, :]
        r = lax.rsqrt(jnp.mean(x * x, axis=-1, keepdims=True) + NORM_EPS)
        xr = x * r
        dx_ref[at, :] = (dy_ref[at, :].astype(F32) + r * (du - xr * jnp.mean(xr * du, axis=-1, keepdims=True))).astype(BF16)

    rows_loop(x_ref.shape[0], 16, body)


def add_rows(x_ref, y_ref, out_ref):
    def body(at):
        out_ref[at, :] = (x_ref[at, :].astype(F32) + y_ref[at, :]).astype(BF16)

    rows_loop(x_ref.shape[0], 16, body)


def swap_halves(even, odd):
    low = lax.broadcasted_iota(jnp.int32, even.shape, len(even.shape) - 1) < even.shape[-1] // 2
    shift = even.shape[-1] // 2
    axis = len(even.shape) - 1
    return jnp.where(low, even, pltpu.roll(odd, shift, axis)), jnp.where(low, pltpu.roll(even, shift, axis), odd)


def split_columns(w_ref, cols_ref):
    tile = w_ref.shape[2] // (4 * RING * RING)
    for l in range(w_ref.shape[0]):
        for x in range(RING):
            for p in range(cols_ref.shape[3] // tile):
                pair = [w_ref[l, :, pl.ds((i * RING + x) * tile, tile)].astype(F32) for i in (2 * p, 2 * p + 1)]
                for c, value in enumerate(swap_halves(*pair)):
                    cols_ref[l, 2 * x + c, :, pl.ds(p * tile, tile)] = value.astype(cols_ref.dtype)


def join_columns(cols_ref, w_ref):
    tile = w_ref.shape[1] // (4 * RING * RING)
    for x in range(RING):
        for p in range(cols_ref.shape[2] // tile):
            pair = [cols_ref[2 * x + c, :, pl.ds(p * tile, tile)] for c in range(2)]
            for i, value in zip((2 * p, 2 * p + 1), swap_halves(*pair)):
                w_ref[:, pl.ds((i * RING + x) * tile, tile)] = value


def call(body, out_shape, out_spaces, in_spaces, scratch, remote, sends, local, collective_id, *args):
    spaces = {'v': pl.BlockSpec(memory_space=pltpu.VMEM), 'h': pl.BlockSpec(memory_space=pl.ANY)}

    def kernel(*refs):
        net = Net(*refs[-5:-1])
        net.tile_sems = refs[-1]
        body(net, *refs[:-5])
        net.finish()
        assert net.n_remote <= remote and net.n_local <= local, (body.__name__, net.n_remote, net.n_local)
        if PRINT:
            print(body.__name__, net.n_remote, net.n_local, round(net.now, 1))

    return pl.pallas_call(
        kernel, out_shape=out_shape, in_specs=[spaces[s] for s in in_spaces], out_specs=[spaces[s] for s in out_spaces],
        scratch_shapes=list(scratch) + [pltpu.SemaphoreType.DMA((sends,)), pltpu.SemaphoreType.DMA((remote,)), pltpu.SemaphoreType.DMA((local,)),
                                               pltpu.SemaphoreType.REGULAR((8,)), pltpu.SemaphoreType.DMA((2,))],
        compiler_params=pltpu.CompilerParams(collective_id=collective_id, has_side_effects=True, vmem_limit_bytes=67000000),
        cost_estimate=pl.CostEstimate(flops=10**8, bytes_accessed=10**7, transcendentals=0),
        name=body.__name__)(*args)


PRINT = False
SCOPES = False


WIDE = 512
KR, KS, KL = 134, 64, 10
TR, TS, TL = 222, 64, 13
GR = 2
DU = 3


def wide_loop(total, body):
    wide = min(WIDE, total)

    def step(k, carry):
        body(k, wide, pl.ds(pl.multiple_of(k * wide, wide), wide))
        return carry

    lax.fori_loop(0, total // wide, step, 0)


def flat(value):
    return value.reshape(value.shape[0] * value.shape[1], value.shape[2])


def dot_rows(a, b):
    return jnp.dot(flat(a), flat(b), preferred_element_type=F32)


def dot_cols(a, b):
    return lax.dot_general(flat(a), flat(b), CONTRACT_COLS, preferred_element_type=F32)


def gelu(a):
    return 0.5 * a * (1.0 + jnp.tanh(GELU_C * (a + 0.044715 * a * a * a)))


def hidden_rows(net, chip, u, up, a, s):
    at = pl.ds(chip * 2, 2)

    def body(_, wide, cols):
        pre = dot_rows(u[at], up[:, :, cols]).astype(BF16)
        a[at, :, cols] = pre.reshape(2, -1, wide)
        s[at, :, cols] = gelu(pre.astype(F32)).astype(BF16).reshape(2, -1, wide)

    wide_loop(up.shape[2], body)
    net.spend(1.7)


def down_rows(net, chip, s, down, part):
    at = pl.ds(chip * 2, 2)

    def body(_, wide, cols):
        part[:, :, cols] = dot_rows(s[at], down[:, :, cols]).reshape(2, -1, wide)

    wide_loop(down.shape[2], body)
    net.spend(1.76)


def hidden_back_rows(net, chip, dy, down, ds):
    at = pl.ds(chip * 2, 2)
    rows = down.shape[1]

    def body(k, wide, cols):
        blocks = pl.ds(k * (wide // rows), wide // rows)
        ds[at, :, cols] = dot_cols(dy[at], down[blocks]).astype(BF16).reshape(2, -1, wide)

    wide_loop(down.shape[0] * rows, body)
    net.spend(1.5)


def gelu_both(a):
    t = jnp.tanh(GELU_C * (a + 0.044715 * a * a * a))
    return 0.5 * a * (1.0 + t), 0.5 * (1.0 + t) + 0.5 * a * (1.0 - t * t) * (GELU_C * (1.0 + 3 * 0.044715 * a * a))


def hidden_turn_rows(net, chip, u, up, s, ds):
    at = pl.ds(chip * 2, 2)

    def body(_, wide, cols):
        pre = dot_rows(u[at], up[:, :, cols]).astype(BF16).astype(F32)
        value, slope = gelu_both(pre)
        s[at, :, cols] = value.astype(BF16).reshape(2, -1, wide)
        ds[at, :, cols] = (ds[at, :, cols].astype(F32) * slope.reshape(2, -1, wide)).astype(BF16)

    wide_loop(up.shape[2], body)
    net.spend(2.1)


def pre_back_rows(net, chip, dy, down, a, da):
    at = pl.ds(chip * 2, 2)
    rows = down.shape[1]

    def body(k, wide, cols):
        blocks = pl.ds(k * (wide // rows), wide // rows)
        ds = dot_cols(dy[at], down[blocks]).astype(BF16).astype(F32).reshape(2, -1, wide)
        da[at, :, cols] = (ds * gelu_both(a[at, :, cols].astype(F32))[1]).astype(BF16)

    wide_loop(down.shape[0] * rows, body)
    net.spend(1.95)


def input_back_rows(net, chip, da, up, part):
    at = pl.ds(chip * 2, 2)
    rows = up.shape[1]

    def body(k, wide, cols):
        blocks = pl.ds(k * (wide // rows), wide // rows)
        part[:, :, cols] = dot_cols(da[at], up[blocks]).reshape(2, -1, wide)

    wide_loop(up.shape[0] * rows, body)
    net.spend(1.9)


def stored_tiles(net, count, compute, stage, out):
    def store(t):
        return pltpu.make_async_copy(stage.at[t % 2], out(t), net.tile_sems.at[t % 2])

    def step(t, carry):
        @pl.when(t >= 2)
        def _():
            store(t - 2).wait()

        compute(t, stage.at[t % 2])
        store(t).start()
        return carry

    lax.fori_loop(0, count, step, 0)
    for t in range(max(count - 2, 0), count):
        store(t).wait()


def dot_tokens(a, b):
    return lax.dot_general(flat(a), flat(b), CONTRACT_ROWS, preferred_element_type=F32)


def grad_tiles(net, lhs, rhs, stage, out):
    wide = stage.shape[1]

    def compute(t, slot):
        slot[...] = dot_tokens(lhs[:, :, pl.ds(pl.multiple_of(t * wide, wide), wide)], rhs[...])

    stored_tiles(net, lhs.shape[2] // wide, compute, stage, lambda t: out.at[pl.ds(pl.multiple_of(t * wide, wide), wide)])
    net.spend(3.9 * lhs.shape[2] / 1024)


def solution(mesh):
    nl, nd = mesh.shape['local'], mesh.shape['data']
    tok_spec = P(BOTH_AXES, None)
    w_spec = P(None, BOTH_AXES, None)

    def device_fn(tokens, grad_out, w_up, w_down):
        num_layers, ur, ffn = w_up.shape
        dr = w_down.shape[1]
        rows, width = tokens.shape
        hidden = nl * dr
        shape = jax.ShapeDtypeStruct
        up_full = shape((nl, nd * ur, hidden), BF16)
        down_full = shape((nl, dr, width), BF16)
        act_full = shape((nd, rows, width), BF16)
        hid_full = shape((nd, rows, hidden), BF16)
        own = shape((rows, width), BF16)
        part_vmem = pltpu.VMEM((RING, 2, rows, width), F32)
        rx = [part_vmem] + reduce_x_scratch(rows, width)
        sums = sums_scratch(dr, hidden) * 4 + sums_stage(dr, hidden) * 2

        def vmem(like):
            return pltpu.VMEM(like.shape, like.dtype)

        def forward(net, x_ref, g_in, w_up_ref, down_in, block_out, u_out, a_out, s_out, up_out, down_out, next_out, g_out, ds_out, keep_out, x_out,
                    cols, next_own, u, g, up0, down0, up1, down1, a, s, ds, part, *rx_scratch):
            net.arrive('dyz')
            names = ('blocks', 'blocks1', 'sent_u', 'got_u', 'got_g', 'sent_up0', 'sent_down0', 'sent_up1', 'sent_down1', 'got_up0', 'got_down0', 'got_up1', 'got_down1', 'reduced')
            ev = {name: Event(name=name) for name in names}
            ev['got_up0'].rank = 2
            made = [Event(name='made%d' % k) for k in range(RING)]
            hidden_made = [Event(name='hidden%d' % k) for k in range(RING)]
            pools = {name: [Pool(), Pool()] for name in ('up', 'down')}
            act_pool = Pool()

            def gather(name, own, full, split):
                size = own.shape[0] // 2

                def join(kind, events):
                    yield events
                    fire(net, ev[kind + name])

                got, sent = [Event(), Event()], [Event(), Event()]
                for k, first in enumerate('yz'):
                    net.spawn(gather_yz(net, own.at[pl.ds(k * size, size)], full, first, got[k], sent[k], k * size, split=split, pool=pools[name[:-1]][k].again()))
                net.spawn(join('got_', got))
                net.spawn(join('sent_', sent))

            net.enter()
            gather('down0', down_in.at[0], down0, False)
            split_columns(w_up_ref, cols)
            net.spend(0.5)
            net.spawn(exchange(net, cols.at[0], block_out.at[0], ev['blocks']))
            norm_rows(x_ref, u.at[net.data])
            net.spend(0.7)
            grad = net.load(g_in, g.at[net.data])

            def up_first():
                yield [ev['blocks']]
                gather('up0', block_out.at[0], up0, True)
                net.spawn(gather_x(net, u, ev['got_u'], ev['sent_u'], pool=act_pool))
                yield [ev['sent_u']]
                net.spawn(exchange(net, cols.at[1], block_out.at[1], ev['blocks1']))
                yield [ev['got_u'], grad]
                yield [net.grant(0, 'xp')]
                net.spawn(gather_x(net, g, ev['got_g'], pool=act_pool.again()))

            def second():
                yield [ev['got_down0']]
                credit = net.grant(1, 'yz')
                yield [ev['sent_up0'], ev['sent_down0'], ev['blocks1'], credit]
                gather('down1', down_in.at[1], down1, False)
                yield [ev['got_up0']]
                credit = net.grant(2, 'yz')
                yield [ev['sent_down1'], credit]
                gather('up1', block_out.at[1], up1, True)

            def save(event, *pairs):
                yield [ev[event]]
                yield [net.save(src, dst) for src, dst in pairs]

            def hidden_flow():
                yield [ev['got_u'], ev['got_up0']]
                for k, step in enumerate(STEPS):
                    hidden_rows(net, net.at('x', step), u, up0, a, s)
                    fire(net, hidden_made[k])
                    yield [Event(net.now, 2)]
                yield [net.save(a, a_out), net.save(s, s_out), net.save(u, u_out)]

            def down_flow():
                for k, step in enumerate(STEPS):
                    yield [hidden_made[k], ev['got_down0'], Event(0.0, 1)]
                    down_rows(net, net.at('x', step), s, down0, part.at[k])
                    fire(net, made[k])
                yield [net.save(down0.at[yz_index(net, 'z', *far)], keep_out.at[k]) for k, far in enumerate(FAR)]

            def act():
                yield [ev['reduced']]
                add_rows(x_ref, part.at[3, net.core], x_out)
                norm_rows(x_out, next_own)
                net.spend(1.0)
                yield [net.load(next_own, next_out)]

            def back_flow():
                for k, step in enumerate(STEPS):
                    yield [ev['got_g'], ev['got_down1'], Event(0.0, 3)]
                    hidden_back_rows(net, net.at('x', step), g, down1, ds)
                yield [net.load(ds, ds_out)]

            half = down_out.shape[3]
            for flow in (up_first(), second(), hidden_flow(), down_flow(), act(), back_flow(), reduce_x(net, part, made, rx_scratch, ev['reduced']),
                         save('got_up1', (up1, up_out)), save('got_down1', *[(down1.at[:, :, pl.ds(h * half, half)], down_out.at[h]) for h in range(2)]),
                         save('got_g', (g, g_out))):
                net.spawn(flow)
            net.run()

        def turn(net, u_in, up_in, down_in, ds_in, g_in, u0_in, a0_in, s0_in, keep_in, x_ref, x0_ref, g_own, block_in, w_down_in,
                 x_out, dx_out, d_up0, d_down0, d_up1, d_down1, dw_up1, dw_down1, dw_up0, dw_down0,
                 own_up, u, up1, up0, down0, half_in, ds, s, stage, part, *scratch):
            net.arrive('dyz')
            inputs = [net.load(u_in, u.at[net.data]), net.load(up_in, up1), net.load(ds_in, ds)]
            inputs[0].wait()
            inputs[0].waited = True
            net.free_locals.append(inputs[0].slot)
            net.enter()
            rx_scratch = scratch[:5]
            stages = (scratch[21:24], scratch[24:27])
            jobs = [[Sums(net, first, scratch[5 + 8 * n + 4 * k:9 + 8 * n + 4 * k], stages[k]) for k, first in enumerate('yz')] for n in range(2)]
            names = ('got_u', 'hidden', 'all_du', 'reduced', 'sent_dy', 'got_dy', 'got_up0', 'got_up0_rest', 'got_down0', 'd_down1', 'd_up1', 'y_reduced', 'acts',
                     'd_down0', 'da0', 'd_up0', 'du_reduced', 'out_up1', 'out_up0') + tuple(
                'sum_%s%d%d' % (kind, layer, k) for kind in ('up', 'down') for layer in range(2) for k in range(2))
            ev = {name: Event(name=name) for name in names}
            made, y_made, du_made = ([Event(name='%s%d' % (name, k)) for k in range(RING)] for name in ('made', 'y_made', 'du_made'))
            wide = half_in.shape[2]
            top = nd * ur * 3 // 4

            def columns(h):
                return pl.ds(h * wide, wide)

            here = {step: Event(name='u%d' % step) for step in STEPS}
            dy_here = {step: Event() for step in STEPS}
            ag_pool, rs_pool = Pool(), Pool()
            job_pools = [[Pool(), Pool()], [Pool(), Pool()]]
            net.spawn(gather_x(net, u, ev['got_u'], chips=here, pool=ag_pool))
            net.spawn(gather_yz(net, w_down_in.at[0], down0, 'z', ev['got_down0'], near=True))
            net.spawn(gather_yz(net, block_in.at[0, pl.ds(0, top)], up0, 'y', ev['got_up0']))
            net.spawn(gather_yz(net, block_in.at[0, pl.ds(top, nd * ur - top)], up0, 'z', ev['got_up0_rest'], offset=top))
            net.spawn(reduce_x(net, part, made, rx_scratch, ev['reduced'], rs_pool))
            frees = [[Event(0.0) for _ in range(3)] for _ in range(2)]

            def up_place(ref, k):
                half = nd * ur // 2
                return lambda block, rows: ref.at[pl.ds(pl.multiple_of(block * (2 * half) + k * half + rows.start, rows.size), rows.size)]

            def down_place(ref, k):
                return lambda block, rows: ref.at[pl.ds(pl.multiple_of(block * dr + rows.start, rows.size), rows.size), columns(k)]

            def sum_job(n, place, ref, ready, name, credits=()):
                passed = [Event(), Event()]
                for k in range(2):
                    start = Event()
                    ev['start_%s%d' % (name, k)] = start
                    net.spawn(gate(start, ready + ([credits[k]] if credits else []), job_pools[n][k]))
                    net.spawn(jobs[n][k].run(place(ref, k), start, ev['sum_%s%d' % (name, k)], frees[k], passed[k], job_pools[n][k]))
                return passed

            def gate(event, items, pool):
                yield items
                pool.again()
                fire(net, event)

            left = [RING, RING]

            def layer1(k, step):
                yield [here[step], Event(0.0, 1)] + inputs[1:]
                hidden_turn_rows(net, net.at('x', step), u, up1, s, ds)
                left[0] -= 1
                if left[0] == 0:
                    fire(net, ev['hidden'])
                yield [Event(net.now, DU)]
                input_back_rows(net, net.at('x', step), ds, up1, part.at[k])
                fire(net, made[k])
                left[1] -= 1
                if left[1] == 0:
                    fire(net, ev['all_du'])

            def grads1():
                for h in range(2):
                    yield [net.load(g_in.at[:, :, columns(h)], half_in), Event(0.0, GR), ev['hidden']]
                    grad_tiles(net, s, half_in, stage, d_down1.at[:, columns(h)])
                fire(net, ev['d_down1'])
                for h in range(2):
                    yield [Event(net.now, GR)]
                    grad_tiles(net, u.at[:, :, columns(h)], ds, stage, d_up1.at[columns(h)])
                fire(net, ev['d_up1'])

            def act():
                yield [ev['d_up1'], ev['got_u']]
                net.drain(ev['got_u'].copies)
                credit = net.grant(0, 'xp')
                yield [ev['reduced'], credit]
                norm_back_rows(x_ref, g_own, part.at[3, net.core], u.at[net.data])
                net.spend(0.7)
                net.spawn(gather_x(net, u, ev['got_dy'], ev['sent_dy'], dy_here, pool=ag_pool.again()))

            def layer1_out():
                yield [ev['all_du'], ev['d_up1']]
                yield [net.load(down_in.at[h], up1.at[:, pl.ds(h * dr, dr)]) for h in range(2)]
                yield [ev['reduced'], Event(0.0, 2)]
                net.drain(ev['reduced'].copies)
                credit = net.grant(1, 'xp')
                for k, step in enumerate(STEPS):
                    for h in range(2):
                        net.spend(-0.88)
                        down_rows(net, net.at('x', step), s, up1.at[:, pl.ds(h * dr, dr)], part.at[k, :, :, columns(h)])
                    yield [Event(net.now, 2)]
                loads = [net.load(a0_in, up1.at[pl.ds(0, nd)]), net.load(s0_in, up1.at[pl.ds(nd, nd)])]
                loads += [net.load(keep_in.at[k], down0.at[yz_index(net, 'z', *far)]) for k, far in enumerate(FAR)]
                yield loads
                fire(net, ev['acts'])
                yield [ev['sent_dy'], credit]
                net.spawn(reduce_x(net, part, y_made, rx_scratch, ev['y_reduced'], rs_pool.again()))
                for k in range(RING):
                    fire(net, y_made[k])
                yield [ev['y_reduced']]
                add_rows(x_ref, part.at[3, net.core], x_out)

            a0, s0 = up1.at[pl.ds(0, nd)], up1.at[pl.ds(nd, nd)]
            backs = [RING]

            def layer0_hidden(step):
                yield [dy_here[step], ev['acts'], ev['got_down0'], Event(0.0, 2)]
                pre_back_rows(net, net.at('x', step), u, down0, a0, ds)
                backs[0] -= 1
                if backs[0] == 0:
                    fire(net, ev['da0'])

            def layer0():
                yield [ev['d_down1']]
                first = net.load(u0_in.at[:, :, columns(0)], half_in)
                for h in range(2):
                    yield [net.load(u0_in.at[:, :, columns(h)], half_in) if h else first]
                    yield [ev['da0'], Event(0.0, 3)]
                    grad_tiles(net, half_in, ds, stage, d_up0.at[columns(h)])
                fire(net, ev['d_up0'])
                for h in range(2):
                    yield [ev['got_dy'], ev['acts'], Event(0.0, 3)]
                    grad_tiles(net, s0, u.at[:, :, columns(h)], stage, d_down0.at[:, columns(h)])
                fire(net, ev['d_down0'])
                yield [ev['y_reduced'], ev['got_up0'], ev['got_up0_rest'], Event(0.0, 2)]
                net.drain(ev['y_reduced'].copies)
                yield [net.grant(2, 'xp')]
                net.spawn(reduce_x(net, part, du_made, rx_scratch, ev['du_reduced'], rs_pool.again()))
                for k, step in enumerate(STEPS):
                    input_back_rows(net, net.at('x', step), ds, up0, part.at[k])
                    fire(net, du_made[k])
                    yield [Event(net.now, 2)]
                yield [ev['du_reduced']]
                norm_back_rows(x0_ref, u.at[net.data], part.at[3, net.core], dx_out)

            def out_down(layer, dw_down, credit):
                def one(k):
                    done = ev['sum_down%d%d' % (layer, k)]
                    yield [done]
                    yield [net.load(done.total, dw_down.at[:, columns(k)])]
                    if credit is not None:
                        net.drain(done.copies)
                        yield [net.grant(credit + k, 'yz')]
                        fire(net, freed[credit + k])

                for k in range(2):
                    net.spawn(one(k))

            def out_up(layer, dw_up, credit):
                copied = [Event(), Event()]

                def one(k):
                    done = ev['sum_up%d%d' % (layer, k)]
                    yield [done]
                    copy_rows(net, done.total, own_up.at[pl.ds(k * (nd * ur // 2), nd * ur // 2)])
                    fire(net, copied[k])
                    if credit is not None:
                        net.drain(done.copies)
                        yield [net.grant(credit + k, 'yz')]
                        fire(net, freed[credit + k])

                def both():
                    yield copied + ([ev['out_up1']] if layer == 0 else [])
                    net.spawn(exchange_back(net, own_up, dw_up, ev['out_up%d' % layer]))

                for k in range(2):
                    net.spawn(one(k))
                net.spawn(both())

            freed = {k: Event() for k in range(3, 7)}
            passed = sum_job(0, down_place, d_down1, [ev['d_down1']], 'down1')
            passed = sum_job(1, up_place, d_up1, [ev['d_up1']] + passed, 'up1')
            passed = sum_job(0, up_place, d_up0, [ev['d_up0']] + passed, 'up0', [freed[3], freed[4]])
            sum_job(1, down_place, d_down0, [ev['d_down0']] + passed, 'down0', [freed[5], freed[6]])
            out_down(1, dw_down1, 3)
            out_up(1, dw_up1, 5)
            out_up(0, dw_up0, None)
            out_down(0, dw_down0, None)

            for k in (3, 2, 1, 0):
                net.spawn(layer1(k, STEPS[k]))
            for step in (0, -1, 1, 2):
                net.spawn(layer0_hidden(step))
            for flow in (grads1(), act(), layer1_out(), layer0()):
                net.spawn(flow)
            net.run()

        def finish(up1_ref, up0_ref, down1_ref, down0_ref, x_ref, dx_ref, x_out, dx_out, up_out, down_out):
            for l, (up_ref, down_ref) in enumerate(((up0_ref, down0_ref), (up1_ref, down1_ref))):
                join_columns(up_ref, up_out.at[l])
                rows_loop(dr, 16, lambda at: down_out.at[l].__setitem__((at, slice(None)), down_ref[at, :]))
            rows_loop(rows, 16, lambda at: x_out.__setitem__((at, slice(None)), x_ref[at, :]))
            rows_loop(rows, 16, lambda at: dx_out.__setitem__((at, slice(None)), dx_ref[at, :]))

        d_up_own, d_down_own = shape((nd, ur, hidden), F32), shape((dr, width), F32)

        blocks, u0, a0, s0, up1, down1, u1, g_full, ds1, keep, x1 = call(
            forward, [shape((num_layers, nd * ur, hidden), BF16), act_full, hid_full, hid_full, up_full, shape((2, nl, dr, width // 2), BF16),
                      own, act_full, hid_full, shape((len(FAR), dr, width), BF16), own],
            'hhhhhhhhhhv', 'vhvh',
            [pltpu.VMEM((num_layers, nd, ur, hidden), BF16), vmem(own)] + [vmem(act_full)] * 2 + [vmem(up_full), vmem(down_full)] * 2 + [vmem(hid_full)] * 3 + rx,
            KR, KS, KL, 0, tokens, grad_out, w_up, w_down)
        d_up_full, d_down_full = shape((width, hidden), F32), shape((hidden, width), F32)
        x_out, dx, _, _, _, _, *grads = call(
            turn, [own, own] + [d_up_full, d_down_full] * 2 + [d_up_own, d_down_own] * 2, 'vv' + 'h' * 8, 'hhhhhhhhhvvvhh',
            [pltpu.VMEM((nd * ur, hidden), F32), vmem(act_full), vmem(up_full), vmem(up_full), vmem(down_full), pltpu.VMEM((nd, rows, width // 2), BF16), vmem(hid_full), vmem(hid_full),
             pltpu.VMEM((2, hidden // 2, width // 2), F32)] + rx + sums, TR, TS, TL, 1,
            u1, up1, down1, ds1, g_full, u0, a0, s0, keep, x1, tokens, grad_out, blocks, w_down)
        up1_own, down1_own, up0_own, down0_own = grads
        return pl.pallas_call(
            finish, out_shape=[own, own, shape(w_up.shape, F32), shape(w_down.shape, F32)], name='finish',
            in_specs=[pl.BlockSpec(memory_space=pltpu.VMEM)] * 6, out_specs=[pl.BlockSpec(memory_space=pltpu.VMEM)] * 4,
        )(up1_own, up0_own, down1_own, down0_own, x_out, dx)

    return jax.shard_map(device_fn, mesh=mesh, in_specs=(tok_spec, tok_spec, w_spec, w_spec), out_specs=(tok_spec, tok_spec, w_spec, w_spec), check_vma=False)
```

```python
import contextlib

import jax
import jax.numpy as jnp
from jax import lax
from jax.experimental import pallas as pl
from jax.experimental.pallas import tpu as pltpu
from jax.sharding import PartitionSpec as P

NORM_EPS = 1e-6
BOTH_AXES = ('local', 'data')
CONTRACT_ROWS = (((0,), (0,)), ((), ()))
CONTRACT_COLS = (((1,), (1,)), ((), ()))
MESH = pl.DeviceIdType.MESH
RING = 4
F32, BF16 = jnp.float32, jnp.bfloat16

LINK_RATE = 46.0e3
PAIR_RATE = 600e3
LOCAL_RATE = 3000e3
HOP = 2.4
PAIR_HOP = 1.0
ENTRY = 3.0
SLACK = 0.1
GELU_C = 0.7978845608028654


def scope(label):
    return jax.named_scope(label) if SCOPES else contextlib.nullcontext()


class Event:
    def __init__(self, time=None, rank=0, name=''):
        self.time, self.rank, self.name = time, rank, name


class Copy:
    def __init__(self, desc, time, remote):
        self.desc, self.time, self.remote, self.rank, self.waited = desc, time, remote, 0, False

    def wait(self):
        if self.remote:
            self.desc.wait_recv()
        else:
            self.desc.wait()


class Credit:
    def __init__(self, semaphore, count, time):
        self.semaphore, self.count, self.time, self.rank, self.waited = semaphore, count, time, 0, False

    def wait(self):
        pl.semaphore_wait(self.semaphore, self.count)


class Pool:
    def __init__(self):
        self.slots, self.next = [], 0

    def again(self):
        self.next = 0
        return self


class Net:
    def __init__(self, send_sems, recv_sems, local_sems, credit_sems):
        self.send_sems, self.recv_sems, self.local_sems, self.credit_sems = send_sems, recv_sems, local_sems, credit_sems
        self.n_remote = self.n_local = 0
        self.free_sends = list(range(send_sems.shape[0]))
        self.free_locals = []
        self.now = 0.0
        self.free = {}
        self.sent = []
        self.flows = []
        self.labels = {}
        here, there = lax.axis_index('local'), lax.axis_index('data')
        pos = {'z': here // RING, 'y': lax.rem(here, RING), 'x': there // 2}
        self.data, self.core = there, lax.rem(there, 2)
        self.ring = {axis: [at] + [lax.rem(at + step, RING) for step in range(1, RING)] for axis, at in pos.items()}
        self.hops = [there] + [lax.rem(there + step, 2 * RING) for step in range(1, 2 * RING)]
        self.blocks = [at * 2 + self.core for at in self.ring['x']]
        self.places = [[z * RING + y for y in self.ring['y']] for z in self.ring['z']]
        self.partner = pos['x'] * 2 + (1 - self.core)
        self.other = 1 - self.core

    def at(self, axis, step):
        return self.ring[axis][step % RING]

    def block(self, step):
        return self.blocks[step % RING]

    def device(self, axis, step):
        if axis == 'p':
            return {'data': self.partner}
        if axis == 'd':
            return {'data': self.hops[step % (2 * RING)]}
        if axis == 'x':
            return {'data': self.block(step)}
        if axis == 'y':
            return {'local': self.places[0][step % RING]}
        return {'local': self.places[step % RING][0]}

    def peers(self, axes):
        return [(axis, step) for axis in axes for step in ((1, -1) if axis in 'xyz' else (1,) if axis == 'p' else range(1, 2 * RING))]

    def signal(self, semaphore, axes):
        for axis, step in self.peers(axes):
            pl.semaphore_signal(semaphore, inc=1, device_id=self.device(axis, step), device_id_type=MESH)

    def arrive(self, axes):
        self.entry, self.entered = pltpu.get_barrier_semaphore(), len(self.peers(axes))
        self.signal(self.entry, axes)

    def enter(self):
        pl.semaphore_wait(self.entry, self.entered)
        self.now = max(self.now, ENTRY)

    def take(self, copies):
        for copy in copies:
            copy.wait()
            copy.waited = True
            self.free_locals.append(copy.slot)
            self.now = max(self.now, copy.time)

    def grant(self, k, axes):
        self.signal(self.credit_sems.at[k], axes)
        return Credit(self.credit_sems.at[k], len(self.peers(axes)), self.now + HOP)

    def drain(self, copies):
        for copy in copies:
            if copy in self.sent:
                copy.desc.wait_send()
                self.sent.remove(copy)
                self.free_sends.append(copy.slot)

    def idle(self, gap):
        over = [copy for copy in self.sent if copy.time + 1.5 < self.now]
        self.drain(over[:int(gap / 0.05)])

    def send(self, src, dst, axis, step=1, pool=None):
        if pool is not None and pool.next < len(pool.slots):
            k = pool.slots[pool.next]
        else:
            k = self.n_remote
            self.n_remote += 1
            if pool is not None:
                pool.slots.append(k)
        if pool is not None:
            pool.next += 1
        if not self.free_sends:
            if PRINT:
                print('EXHAUSTED', round(self.now, 1))
            self.drain([min(self.sent, key=lambda copy: copy.time)])
        send_slot = self.free_sends.pop()
        desc = pltpu.make_async_remote_copy(
            src_ref=src, dst_ref=dst, send_sem=self.send_sems.at[send_slot], recv_sem=self.recv_sems.at[k],
            device_id=self.device(axis, step), device_id_type=MESH)
        desc.start()
        size = 1
        for n in dst.shape:
            size *= n
        size *= dst.dtype.itemsize
        rate = PAIR_RATE if axis == 'p' else LINK_RATE
        if axis == 'd':
            axis, step, size = ('p', 1, size) if step == 1 else ('x', 1 if step < RING + 2 else -1, size)
        key = (axis, step)
        done = max(self.free.get(key, 0.0), self.now) + size / rate
        self.free[key] = done
        copy = Copy(desc, done + (PAIR_HOP if axis == 'p' else HOP), True)
        copy.slot = send_slot
        self.sent.append(copy)
        return copy

    def load(self, src, dst):
        if not self.free_locals:
            self.free_locals.append(self.n_local)
            self.n_local += 1
        k = self.free_locals.pop()
        desc = pltpu.make_async_copy(src, dst, self.local_sems.at[k])
        desc.start()
        size = 1
        for n in dst.shape:
            size *= n
        done = max(self.free.get('hbm', 0.0), self.now) + size * dst.dtype.itemsize / LOCAL_RATE
        self.free['hbm'] = done
        copy = Copy(desc, done + 0.9, False)
        copy.slot = k
        return copy

    def save(self, src, dst):
        copy = self.load(src, dst)
        copy.time += 4.0
        return copy

    def spend(self, microseconds):
        self.now += microseconds

    def spawn(self, flow):
        self.step(flow)

    def step(self, flow):
        try:
            if flow not in self.labels:
                self.labels[flow] = [flow.__name__, len(self.labels), 0]
            self.labels[flow][2] += 1
            self.flows.append((flow, next(flow)))
        except StopIteration:
            pass

    def run(self):
        while self.flows:
            best = None
            for k, (_, items) in enumerate(self.flows):
                if any(item.time is None for item in items):
                    continue
                time = max([item.time for item in items] + [0.0])
                late = max([item.rank for item in items] + [0])
                rank = (max(time, self.now) + (SLACK if late else 0.0), late, time)
                if best is None or rank < best[0]:
                    best = (rank, k, time)
            _, k, time = best
            flow, items = self.flows.pop(k)
            self.idle(time - self.now)
            label = '%s_%d_%d' % tuple(self.labels[flow])
            with scope('w_' + label):
                for item in items:
                    if not isinstance(item, Event) and not item.waited:
                        item.wait()
                        item.waited = True
                        if isinstance(item, Copy) and not item.remote:
                            self.free_locals.append(item.slot)
            before = self.now
            self.now = max(self.now, time)
            if PRINT:
                print('STEP', label, round(before, 2), round(self.now, 2))
            with scope('s_' + label):
                self.step(flow)

    def finish(self):
        for copy in self.sent:
            copy.desc.wait_send()


def rows_loop(rows, chunk, body):
    chunk = min(chunk, rows)

    def step(k, carry):
        body(pl.ds(pl.multiple_of(k * chunk, chunk), chunk))
        return carry

    lax.fori_loop(0, rows // chunk, step, 0)


def add_into(net, dst, *others):
    rows, cols = dst.shape

    def body(at):
        total = dst[at, :]
        for other in others:
            total = total + other[at, :]
        dst[at, :] = total

    rows_loop(rows, 16, body)
    net.spend(rows * cols * 4 * (1 + len(others)) / 4e6)


def fire(net, event):
    event.time = net.now
    if PRINT and event.name:
        print('   %7.1f %s' % (net.now, event.name))


def exchange(net, source, dst, done):
    rows = dst.shape[0] // (2 * RING)

    def mine():
        return dst.at[pl.ds(pl.multiple_of(net.data * rows, rows), rows)]

    own = net.load(source(net.data), mine())
    copies = [net.send(source(net.hops[k]), mine(), 'd', k) for k in (4, 5, 2, 3, 6, 7, 1)]
    yield [own] + copies
    net.drain(copies)
    fire(net, done)


def exchange_back(net, src, dst, done):
    rows = dst.shape[1]
    per = src.shape[1] // rows

    def block(k):
        return src.at[lax.div(k, per), pl.ds(pl.multiple_of(lax.rem(k, per) * rows, rows), rows)]

    own = net.load(block(net.data), dst.at[net.data])
    copies = [net.send(block(net.hops[k]), dst.at[net.data], 'd', k) for k in (4, 5, 2, 3, 6, 7, 1)]
    yield [own] + copies
    net.drain(copies)
    fire(net, done)


def copy_rows(net, src, dst):
    def body(at):
        dst[at, :] = src[at, :]

    rows_loop(src.shape[0], 16, body)
    net.spend(0.2)


def gather_x(net, full, done, issued=None, chips=None, pool=None):
    half = full.shape[1] // 2
    lo, hi = pl.ds(0, half), pl.ds(half, half)
    chips = chips or {step: Event() for step in STEPS}
    left = [2]
    done.copies = []

    def send(*args):
        done.copies.append(net.send(*args, pool=pool))
        return done.copies[-1]

    def block(step):
        return full.at[net.block(step)]

    def part(step, rows):
        return full.at[net.block(step), rows]

    relays = []

    def side(step, first, second, mine):
        yield [mine[0]]
        relays.append(send(part(step, first), part(step, first), 'x', -step))
        left[0] -= 1
        if left[0] == 0:
            net.spawn(far())
            if issued is not None:
                fire(net, issued)
        yield [mine[1]]
        pair = send(block(step), block(step), 'p')
        yield [pair]
        fire(net, chips[step])

    def far():
        yield relays
        pair = send(block(2), block(2), 'p')
        yield [pair]
        fire(net, chips[2])

    forth = [send(part(0, rows), part(0, rows), 'x', 1) for rows in (lo, hi)]
    back = [send(part(0, rows), part(0, rows), 'x', -1) for rows in (hi, lo)]
    pair = send(block(0), block(0), 'p')
    net.spawn(side(-1, lo, hi, forth))
    net.spawn(side(1, hi, lo, back))
    yield [pair]
    fire(net, chips[0])
    yield [chips[step] for step in STEPS]
    fire(net, done)


def gather_yz(net, own, full, first, done, issued=None, offset=0, near=False, split=True, pool=None):
    second = 'y' if first == 'z' else 'z'
    done.copies = []

    def emit(*args):
        done.copies.append(net.send(*args, pool=pool))
        return done.copies[-1]

    size = own.shape[0]
    half = size // 2
    lo, hi, both = pl.ds(offset, half), pl.ds(offset + half, half), pl.ds(offset, size)
    forward, backward = ((lo, hi), (hi, lo)) if split and not near else ((both,), (both,))

    def part(one, two, rows):
        return full.at[yz_index(net, first, one, two), rows]

    left = [3 if near else RING, 3 if near else RING]

    def arrived(which):
        left[which] -= 1
        if left[which] == 0 and (done, issued)[which] is not None:
            fire(net, (done, issued)[which])

    def send(one, rows, axis, step):
        src = own.at[pl.ds(rows.start - offset, rows.size)] if one == 0 else part(one, 0, rows)
        return emit(src, part(one, 0, rows), axis, step)

    def column(one):
        forth = [send(one, rows, second, 1) for rows in forward]
        back = [send(one, rows, second, -1) for rows in backward]

        def finish():
            if near:
                arrived(1)
                yield forth + back
            else:
                yield [forth[0]]
                relays = [emit(part(one, -1, lo), part(one, -1, lo), second, 1)]
                yield [back[0]]
                relays.append(emit(part(one, 1, hi), part(one, 1, hi), second, -1))
                arrived(1)
                yield forth[1:] + back[1:] + relays
            arrived(0)

        net.spawn(finish())

    relays = []

    def side(step, first_half, mine):
        yield [mine[0]]
        if not near:
            relays.append(emit(part(step, 0, first_half), part(step, 0, first_half), first, -step))
            if len(relays) == 2:
                net.spawn(far())
        yield mine[1:]
        column(step)

    def far():
        yield relays
        column(2)

    mine = [net.load(own, part(0, 0, both))]
    forth = [send(0, rows, first, 1) for rows in forward]
    back = [send(0, rows, first, -1) for rows in backward]
    column(0)
    net.spawn(side(-1, lo, forth))
    net.spawn(side(1, hi, back))
    left[0] += 1
    yield mine
    arrived(0)


def yz_index(net, first, one, two):
    return net.places[one % RING][two % RING] if first == 'z' else net.places[two % RING][one % RING]


FAR = [(2, 0), (2, 1), (2, -1), (2, 2), (0, 2), (1, 2), (-1, 2)]


STEPS = (2, 1, -1, 0)
WINDOW = 2


def reduce_x(net, part, made, scratch, done, pool=None):
    other, relay_f, relay_b, last_f, last_b = scratch
    half = part.shape[2] // 2
    lo, hi = pl.ds(0, half), pl.ds(half, half)

    def acc(k, rows=None):
        return part.at[k, net.core] if rows is None else part.at[k, net.core, rows]

    pairs = [None] * RING
    ready = [Event() for _ in STEPS]

    def pair(k):
        yield [made[k]]
        pairs[k] = net.send(part.at[k, net.other], other.at[k], 'p', pool=pool)
        yield [pairs[k]]
        add_into(net, acc(k), other.at[k])
        fire(net, ready[k])

    for k in range(RING):
        net.spawn(pair(k))
    sent = {}
    started = Event()

    def part_flow(k):
        yield [ready[k]]
        if k == 0:
            sent['first_f'] = net.send(acc(0, lo), relay_f, 'x', 1, pool=pool)
            sent['first_b'] = net.send(acc(0, hi), relay_b, 'x', -1, pool=pool)
        elif k == 1:
            sent['direct_f'] = net.send(acc(1, hi), last_f.at[hi], 'x', 1, pool=pool)
        else:
            sent['direct_b'] = net.send(acc(2, lo), last_b.at[lo], 'x', -1, pool=pool)
        if len(sent) == 4:
            fire(net, started)

    for k in range(3):
        net.spawn(part_flow(k))
    yield [started]
    yield [sent['first_f']]
    add_into(net, acc(1, lo), relay_f)
    summed_f = net.send(acc(1, lo), last_f.at[lo], 'x', 1, pool=pool)
    yield [sent['first_b']]
    add_into(net, acc(2, hi), relay_b)
    summed_b = net.send(acc(2, hi), last_b.at[hi], 'x', -1, pool=pool)
    yield [ready[3], sent['direct_f'], sent['direct_b'], summed_f, summed_b]
    add_into(net, acc(3), last_f, last_b)
    done.copies = pairs + list(sent.values()) + [summed_f, summed_b]
    fire(net, done)


def reduce_x_scratch(rows, cols):
    return [pltpu.VMEM((RING, rows, cols), F32), pltpu.VMEM((rows // 2, cols), F32), pltpu.VMEM((rows // 2, cols), F32),
            pltpu.VMEM((rows, cols), F32), pltpu.VMEM((rows, cols), F32)]


def load_parts(net, src, part, made):
    for k, step in enumerate(STEPS):
        def bring(k=k, step=step):
            yield [net.load(src.at[pl.ds(net.at('x', step) * 2, 2)], part.at[k])]
            fire(net, made[k])

        net.spawn(bring())


class Sums:
    def __init__(self, net, first, scratch, stage):
        self.net, self.first, self.scratch, self.stage = net, first, scratch, stage
        self.second = 'y' if first == 'z' else 'z'

    def run(self, place, start, done, free, passed_all, pool):
        net, first, second = self.net, self.first, self.second
        relay1, last1, relay2, last2 = self.scratch
        ahead, behind, mine = self.stage
        half = mine.shape[0] // 2
        lo, hi, all_rows = pl.ds(0, half), pl.ds(half, half), pl.ds(0, 2 * half)
        done.copies = []

        def send(*args):
            done.copies.append(net.send(*args, pool=pool))
            return done.copies[-1]

        def term(one, two, rows=all_rows):
            return place(yz_index(net, first, one, two), rows)

        def bring(gate, src, dst, got):
            yield [gate, start]
            yield [net.load(src, dst)]
            fire(net, got)

        chain = [[gate] + [Event() for _ in range(RING)] for gate in free]
        free[:] = [events[RING] for events in chain]
        got = [[Event() for _ in range(RING)] for _ in range(3)]
        ends = [Event() for _ in STEPS]
        passed = [Event() for _ in range(RING - 1)] + [passed_all]

        def ring(k):
            two = STEPS[k]
            if k >= WINDOW:
                yield [passed[k - WINDOW]]
            net.spawn(bring(chain[0][k], term(1, two, lo), ahead, got[0][k]))
            net.spawn(bring(chain[1][k], term(-1, two, hi), behind, got[1][k]))
            net.spawn(bring(chain[2][k], term(0, two), mine, got[2][k]))
            first_f = send(term(2, two, lo), relay1.at[0, k], first, 1)
            first_b = send(term(2, two, hi), relay1.at[1, k], first, -1)
            direct_f = send(term(1, two, hi), last1.at[0, k, hi], first, 1)
            direct_b = send(term(-1, two, lo), last1.at[1, k, lo], first, -1)
            yield [first_f, got[0][k]]
            add_into(net, relay1.at[0, k], ahead)
            fire(net, chain[0][k + 1])
            summed_f = send(relay1.at[0, k], last1.at[0, k, lo], first, 1)
            yield [first_b, got[1][k]]
            add_into(net, relay1.at[1, k], behind)
            fire(net, chain[1][k + 1])
            summed_b = send(relay1.at[1, k], last1.at[1, k, hi], first, -1)
            fire(net, passed[k])
            yield [direct_f, direct_b, summed_f, summed_b, got[2][k]]
            add_into(net, last1.at[0, k], last1.at[1, k], mine)
            fire(net, chain[2][k + 1])
            fire(net, ends[k])

        def sums(k, rows=all_rows):
            return last1.at[0, k, rows]

        yield [start]
        for k in range(RING):
            net.spawn(ring(k))
        yield [ends[0]]
        first_f = send(sums(0, lo), relay2.at[0], second, 1)
        first_b = send(sums(0, hi), relay2.at[1], second, -1)
        yield [ends[1]]
        direct_f = send(sums(1, hi), last2.at[0, hi], second, 1)
        yield [ends[2]]
        direct_b = send(sums(2, lo), last2.at[1, lo], second, -1)
        yield [first_f]
        add_into(net, sums(1, lo), relay2.at[0])
        summed_f = send(sums(1, lo), last2.at[0, lo], second, 1)
        yield [first_b]
        add_into(net, sums(2, hi), relay2.at[1])
        summed_b = send(sums(2, hi), last2.at[1, hi], second, -1)
        yield [ends[3], direct_f, direct_b, summed_f, summed_b]
        add_into(net, sums(3), last2.at[0], last2.at[1])
        done.total = sums(3)
        fire(net, done)


def sums_scratch(rows, cols):
    return [pltpu.VMEM((2, RING, rows // 2, cols), F32), pltpu.VMEM((2, RING, rows, cols), F32),
            pltpu.VMEM((2, rows // 2, cols), F32), pltpu.VMEM((2, rows, cols), F32)]


def sums_stage(rows, cols):
    return [pltpu.VMEM((rows // 2, cols), F32), pltpu.VMEM((rows // 2, cols), F32), pltpu.VMEM((rows, cols), F32)]


def norm_rows(x_ref, u_ref):
    def body(at):
        x = x_ref[at, :].astype(F32)
        u_ref[at, :] = (x * lax.rsqrt(jnp.mean(x * x, axis=-1, keepdims=True) + NORM_EPS)).astype(BF16)

    rows_loop(x_ref.shape[0], 16, body)


def norm_back_rows(x_ref, dy_of, du_ref, dx_ref):
    def body(at):
        x = x_ref[at, :].astype(F32)
        du = du_ref[at, :]
        r = lax.rsqrt(jnp.mean(x * x, axis=-1, keepdims=True) + NORM_EPS)
        xr = x * r
        dx_ref[at, :] = (dy_of(at).astype(F32) + r * (du - xr * jnp.mean(xr * du, axis=-1, keepdims=True))).astype(BF16)

    rows_loop(x_ref.shape[0], 16, body)


def add_rows(x_ref, y_ref, out_ref):
    def body(at):
        out_ref[at, :] = (x_ref[at, :].astype(F32) + y_ref[at, :]).astype(BF16)

    rows_loop(x_ref.shape[0], 16, body)


def swap_halves(even, odd):
    low = lax.broadcasted_iota(jnp.int32, even.shape, len(even.shape) - 1) < even.shape[-1] // 2
    shift = even.shape[-1] // 2
    axis = len(even.shape) - 1
    return jnp.where(low, even, pltpu.roll(odd, shift, axis)), jnp.where(low, pltpu.roll(even, shift, axis), odd)


def split_columns(w_ref, cols_ref, layers):
    pieces, _, wide = w_ref.shape
    rows = layers
    tile = pieces * wide // (4 * RING * RING)
    for x in range(RING):
        for p in range(wide // tile):
            pair = []
            for i in (2 * p, 2 * p + 1):
                at = (i * RING + x) * tile
                pair.append(w_ref[at // wide, pl.ds(0, rows), pl.ds(at % wide, tile)].astype(F32))
            for c, value in enumerate(swap_halves(*pair)):
                cols_ref[2 * x + c, pl.ds(0, rows), pl.ds(p * tile, tile)] = value.astype(cols_ref.dtype)


def join_columns(cols_ref, w_ref):
    tile = w_ref.shape[1] // (4 * RING * RING)
    for x in range(RING):
        for p in range(cols_ref.shape[2] // tile):
            pair = [cols_ref[2 * x + c, :, pl.ds(p * tile, tile)] for c in range(2)]
            for i, value in zip((2 * p, 2 * p + 1), swap_halves(*pair)):
                w_ref[:, pl.ds((i * RING + x) * tile, tile)] = value


def call(body, out_shape, out_spaces, in_spaces, scratch, remote, sends, local, collective_id, *args):
    spaces = {'v': pl.BlockSpec(memory_space=pltpu.VMEM), 'h': pl.BlockSpec(memory_space=pl.ANY)}

    def kernel(*refs):
        net = Net(*refs[-5:-1])
        net.tile_sems = refs[-1]
        body(net, *refs[:-5])
        net.finish()
        assert net.n_remote <= remote and net.n_local <= local, (body.__name__, net.n_remote, net.n_local)
        if PRINT:
            print(body.__name__, net.n_remote, net.n_local, round(net.now, 1))

    return pl.pallas_call(
        kernel, out_shape=out_shape, in_specs=[spaces[s] for s in in_spaces], out_specs=[spaces[s] for s in out_spaces],
        scratch_shapes=list(scratch) + [pltpu.SemaphoreType.DMA((sends,)), pltpu.SemaphoreType.DMA((remote,)), pltpu.SemaphoreType.DMA((local,)),
                                               pltpu.SemaphoreType.REGULAR((14,)), pltpu.SemaphoreType.DMA((2,))],
        compiler_params=pltpu.CompilerParams(collective_id=collective_id, has_side_effects=True, vmem_limit_bytes=67000000),
        cost_estimate=pl.CostEstimate(flops=10**8, bytes_accessed=10**7, transcendentals=0),
        name=body.__name__)(*args)


PRINT = False
SCOPES = False


WIDE = 512
TR, TS, TL = 268, 64, 19
GR = 2
DU = 3


def wide_loop(total, body):
    wide = min(WIDE, total)

    def step(k, carry):
        body(k, wide, pl.ds(pl.multiple_of(k * wide, wide), wide))
        return carry

    lax.fori_loop(0, total // wide, step, 0)


def flat(value):
    return value.reshape(value.shape[0] * value.shape[1], value.shape[2])


def dot_rows(a, b):
    return jnp.dot(flat(a), flat(b), preferred_element_type=F32)


def dot_cols(a, b):
    return lax.dot_general(flat(a), flat(b), CONTRACT_COLS, preferred_element_type=F32)


def gelu(a):
    return 0.5 * a * (1.0 + jnp.tanh(GELU_C * (a + 0.044715 * a * a * a)))


def hidden_rows(net, chip, u, up, a, s):
    at = pl.ds(chip * 2, 2)

    def body(_, wide, cols):
        pre = dot_rows(u[at], up[:, :, cols]).astype(BF16)
        a[at, :, cols] = pre.reshape(2, -1, wide)
        s[at, :, cols] = gelu(pre.astype(F32)).astype(BF16).reshape(2, -1, wide)

    wide_loop(up.shape[2], body)
    net.spend(1.7)


def down_rows(net, chip, s, down, part):
    at = pl.ds(chip * 2, 2)

    def body(_, wide, cols):
        part[:, :, cols] = dot_rows(s[at], down[:, :, cols]).reshape(2, -1, wide)

    wide_loop(down.shape[2], body)
    net.spend(1.76)


def hidden_back_rows(net, chip, dy, down, ds):
    at = pl.ds(chip * 2, 2)
    rows = down.shape[1]

    def body(k, wide, cols):
        blocks = pl.ds(k * (wide // rows), wide // rows)
        ds[at, :, cols] = dot_cols(dy[at], down[blocks]).astype(BF16).reshape(2, -1, wide)

    wide_loop(down.shape[0] * rows, body)
    net.spend(1.5)


def gelu_both(a):
    t = jnp.tanh(GELU_C * (a + 0.044715 * a * a * a))
    return 0.5 * a * (1.0 + t), 0.5 * (1.0 + t) + 0.5 * a * (1.0 - t * t) * (GELU_C * (1.0 + 3 * 0.044715 * a * a))


def hidden_turn_rows(net, chip, u, up, s, ds):
    at = pl.ds(chip * 2, 2)

    def body(_, wide, cols):
        pre = dot_rows(u[at], up[:, :, cols]).astype(BF16).astype(F32)
        value, slope = gelu_both(pre)
        s[at, :, cols] = value.astype(BF16).reshape(2, -1, wide)
        ds[at, :, cols] = (ds[at, :, cols].astype(F32) * slope.reshape(2, -1, wide)).astype(BF16)

    wide_loop(up.shape[2], body)
    net.spend(2.1)


def pre_back_rows(net, chip, dy, down, a, da):
    at = pl.ds(chip * 2, 2)
    rows = down.shape[1]

    def body(k, wide, cols):
        blocks = pl.ds(k * (wide // rows), wide // rows)
        ds = dot_cols(dy[at], down[blocks]).astype(BF16).astype(F32).reshape(2, -1, wide)
        da[at, :, cols] = (ds * gelu_both(a[at, :, cols].astype(F32))[1]).astype(BF16)

    wide_loop(down.shape[0] * rows, body)
    net.spend(1.95)


def input_back_rows(net, chip, da, up, part):
    at = pl.ds(chip * 2, 2)
    rows = up.shape[1]

    def body(k, wide, cols):
        blocks = pl.ds(k * (wide // rows), wide // rows)
        part[:, :, cols] = dot_cols(da[at], up[blocks]).reshape(2, -1, wide)

    wide_loop(up.shape[0] * rows, body)
    net.spend(1.9)


def stored_tiles(net, count, compute, stage, out):
    def store(t):
        return pltpu.make_async_copy(stage.at[lax.rem(t, 2)], out(t), net.tile_sems.at[lax.rem(t, 2)])

    def step(t, carry):
        @pl.when(t >= 2)
        def _():
            store(t - 2).wait()

        compute(t, stage.at[lax.rem(t, 2)])
        store(t).start()
        return carry

    lax.fori_loop(0, count, step, 0)
    for t in range(max(count - 2, 0), count):
        store(jnp.int32(t)).wait()


def dot_tokens(a, b):
    return lax.dot_general(flat(a), flat(b), CONTRACT_ROWS, preferred_element_type=F32)


def grad_tiles(net, lhs, rhs, stage, out):
    wide = stage.shape[1]

    def compute(t, slot):
        slot[...] = dot_tokens(lhs[:, :, pl.ds(pl.multiple_of(t * wide, wide), wide)], rhs[...])

    stored_tiles(net, lhs.shape[2] // wide, compute, stage, lambda t: out.at[pl.ds(pl.multiple_of(t * wide, wide), wide)])
    net.spend(3.9 * lhs.shape[2] / 1024)


def solution(mesh):
    nl, nd = mesh.shape['local'], mesh.shape['data']
    tok_spec = P(BOTH_AXES, None)
    w_spec = P(None, BOTH_AXES, None)

    def device_fn(tokens, grad_out, w_up, w_down):
        num_layers, ur, ffn = w_up.shape
        dr = w_down.shape[1]
        rows, width = tokens.shape
        hidden = nl * dr
        shape = jax.ShapeDtypeStruct
        up_full = shape((nl, nd * ur, hidden), BF16)
        down_full = shape((nl, dr, width), BF16)
        act_full = shape((nd, rows, width), BF16)
        hid_full = shape((nd, rows, hidden), BF16)
        own = shape((rows, width), BF16)
        part_vmem = pltpu.VMEM((RING, 2, rows, width), F32)
        rx = [part_vmem] + reduce_x_scratch(rows, width)
        sums = sums_scratch(dr, hidden) * 4 + sums_stage(dr, hidden) * 2

        def vmem(like):
            return pltpu.VMEM(like.shape, like.dtype)

        def step(net, x_in, x_halves, g_in, w_up_in, w_down_in,
                 x_out, dx_out, block_out, u_out, a_out, s_out, d_up0, d_down0, d_up1, d_down1, dw_up1, dw_down1, dw_up0, dw_down0,
                 x, u, g, up0, up1, down0, down1, ds, s, stage, part, *scratch):
            net.arrive('dyz')
            rx_scratch = scratch[:5]
            names = ('blocks', 'blocks1', 'sent_u', 'got_u', 'got_g', 'sent_up0', 'sent_down0', 'sent_up1', 'sent_down1', 'got_up0', 'got_down0',
                     'got_up1', 'got_down1', 'saved', 'free0', 'reduced0', 'ds_made', 'got_u1', 'hidden', 'all_du', 'reduced1', 'sent_dy', 'got_dy',
                     'back_up0', 'back_up0_rest', 'back_down0', 'd_down1', 'd_up1', 'y_reduced', 'acts', 'd_down0', 'da0', 'd_up0', 'du_reduced',
                     'out_up1', 'out_up0', 'got_u0', 'y_made', 'x_saved')
            ev = {name: Event(name=name) for name in names}
            for kind in ('up', 'down'):
                for layer in range(2):
                    for k in range(2):
                        ev['sum_%s%d%d' % (kind, layer, k)] = Event(name='sum_%s%d%d' % (kind, layer, k))
            ev['got_up0'].rank = 2
            hidden_made, made0, made1, y_made, du_made = ([Event(name='%s%d' % (name, k)) for k in range(RING)]
                                                          for name in ('hidden_', 'made0_', 'made1_', 'y_made_', 'du_made_'))
            wide = width // 2
            half_up = nd * ur // 2
            pools = {name: [Pool(), Pool()] for name in ('up', 'down')}
            act_pool, rs_pool = Pool(), Pool()
            job_pools = [[Pool(), Pool()], [Pool(), Pool()]]
            stages = (scratch[21:24], scratch[24:27])
            jobs = [[Sums(net, first, scratch[5 + 8 * n + 4 * k:9 + 8 * n + 4 * k], stages[k]) for k, first in enumerate('yz')] for n in range(2)]
            frees = [[Event(0.0) for _ in range(3)] for _ in range(2)]
            freed = {k: Event() for k in range(10, 14)}

            def columns(h):
                return pl.ds(h * wide, wide)

            inputs = [net.load(x_in, x)]
            inputs += [net.load(w_up_in.at[l, :, pl.ds(k * hidden, hidden)], ds.at[k, pl.ds(l * ur, ur)]) for l in range(num_layers) for k in range(nd)]

            def gather(name, own, full, split):
                size = own.shape[0] // 2

                def join(kind, events):
                    yield events
                    if kind == 'got_':
                        ev[kind + name].copies = events[0].copies + events[1].copies
                    fire(net, ev[kind + name])

                got, sent = [Event(), Event()], [Event(), Event()]
                for k, first in enumerate('yz'):
                    net.spawn(gather_yz(net, own.at[pl.ds(k * size, size)], full, first, got[k], sent[k], k * size, split=split, pool=pools[name[:-1]][k].again()))
                net.spawn(join('got_', got))
                net.spawn(join('sent_', sent))

            net.enter()
            gather('down0', w_down_in.at[0], down0, False)
            net.take(inputs)
            split_columns(ds, s, num_layers * ur)
            net.spend(0.5)
            net.spawn(exchange(net, lambda k: s.at[k, pl.ds(0, ur)], block_out.at[0], ev['blocks']))
            norm_rows(x, u.at[net.data])
            net.spend(0.7)
            own_grads = net.load(g_in, g.at[net.data])

            def up_first():
                yield [ev['blocks']]
                gather('up0', block_out.at[0], up0, True)
                net.spawn(gather_x(net, u, ev['got_u'], ev['sent_u'], pool=act_pool))
                yield [ev['sent_u']]
                net.spawn(exchange(net, lambda k: s.at[k, pl.ds(ur, ur)], block_out.at[1], ev['blocks1']))
                yield [ev['got_u'], own_grads]
                yield [net.grant(0, 'xp')]
                net.spawn(gather_x(net, g, ev['got_g'], pool=act_pool.again()))

            def second():
                yield [ev['got_down0']]
                credit = net.grant(1, 'yz')
                yield [ev['sent_up0'], ev['sent_down0'], ev['blocks1'], credit]
                gather('down1', w_down_in.at[1], down1, False)
                yield [ev['got_up0']]
                credit = net.grant(2, 'yz')
                yield [ev['sent_down1'], credit]
                gather('up1', block_out.at[1], up1, True)

            def hidden_flow():
                yield [ev['got_u'], ev['got_up0'], ev['blocks1']]
                for k, step in enumerate(STEPS):
                    hidden_rows(net, net.at('x', step), u, up0, ds, s)
                    fire(net, hidden_made[k])
                    yield [Event(net.now, 2)]
                yield [net.load(ds, a_out), net.load(s, s_out), net.load(u, u_out)]
                fire(net, ev['saved'])

            def down_flow():
                for k, step in enumerate(STEPS):
                    yield [hidden_made[k], ev['got_down0'], Event(0.0, 1)]
                    down_rows(net, net.at('x', step), s, down0, part.at[k])
                    fire(net, made0[k])
                fire(net, ev['free0'])

            net.spawn(reduce_x(net, part, made0, rx_scratch, ev['reduced0'], rs_pool))
            here = {step: Event(name='u%d' % step) for step in STEPS}
            dy_here = {step: Event() for step in STEPS}

            def next_layer():
                yield [ev['saved'], ev['got_g']]
                net.drain(ev['got_u'].copies + ev['got_g'].copies)
                credit = net.grant(3, 'xp')
                yield [ev['reduced0'], credit]
                add_rows(x, part.at[3, net.core], x)
                norm_rows(x, u.at[net.data])
                net.spend(1.0)
                net.spawn(gather_x(net, u, ev['got_u1'], chips=here, pool=act_pool.again()))
                net.drain(ev['reduced0'].copies)
                yield [net.grant(4, 'xp')]
                net.spawn(reduce_x(net, part, made1, rx_scratch, ev['reduced1'], rs_pool.again()))

            def back_flow():
                for k, step in enumerate(STEPS):
                    yield [ev['got_g'], ev['got_down1'], ev['saved'], Event(0.0, 3)]
                    hidden_back_rows(net, net.at('x', step), g, down1, ds)
                fire(net, ev['ds_made'])

            def again():
                top = nd * ur * 3 // 4
                yield [ev['free0'], ev['got_down1'], ev['ds_made']]
                net.drain(ev['got_up0'].copies + ev['got_down0'].copies)
                credit = net.grant(6, 'yz')
                yield [ev['sent_up1'], credit]
                net.spawn(gather_yz(net, w_down_in.at[0], down0, 'z', ev['back_down0'], near=True, pool=pools['down'][1].again()))
                yield [ev['got_up1']]
                yield [net.grant(7, 'yz')]
                net.spawn(gather_yz(net, block_out.at[0, pl.ds(0, top)], up0, 'y', ev['back_up0'], pool=pools['up'][0].again()))
                net.spawn(gather_yz(net, block_out.at[0, pl.ds(top, nd * ur - top)], up0, 'z', ev['back_up0_rest'], offset=top, pool=pools['up'][1].again()))

            left = [RING, RING]

            def layer1(k, step):
                yield [here[step], ev['ds_made'], ev['got_up1'], Event(0.0, 1)]
                hidden_turn_rows(net, net.at('x', step), u, up1, s, ds)
                left[0] -= 1
                if left[0] == 0:
                    fire(net, ev['hidden'])
                yield [Event(net.now, DU)]
                input_back_rows(net, net.at('x', step), ds, up1, part.at[k])
                fire(net, made1[k])
                left[1] -= 1
                if left[1] == 0:
                    fire(net, ev['all_du'])

            def grads1():
                for h in range(2):
                    yield [Event(0.0, GR), ev['hidden']]
                    grad_tiles(net, s, g.at[:, :, columns(h)], stage, d_down1.at[:, columns(h)])
                fire(net, ev['d_down1'])
                for h in range(2):
                    yield [Event(net.now, GR)]
                    grad_tiles(net, u.at[:, :, columns(h)], ds, stage, d_up1.at[columns(h)])
                fire(net, ev['d_up1'])

            def act():
                yield [ev['d_up1'], ev['all_du'], ev['got_u1']]
                own_g = [net.load(g_in.at[:, columns(h)], ds.at[h]) for h in range(2)]
                net.drain(ev['got_u1'].copies)
                credit = net.grant(5, 'xp')
                yield [ev['reduced1'], credit] + own_g
                norm_back_rows(x, lambda at: jnp.concatenate([ds[h, at, :] for h in range(2)], axis=-1), part.at[3, net.core], u.at[net.data])
                net.spend(0.7)
                net.spawn(gather_x(net, u, ev['got_dy'], ev['sent_dy'], dy_here, pool=act_pool.again()))

            def layer1_out():
                yield [ev['reduced1'], Event(0.0, 2)]
                net.drain(ev['reduced1'].copies)
                credit = net.grant(8, 'xp')
                for k, step in enumerate(STEPS):
                    down_rows(net, net.at('x', step), s, down1, part.at[k])
                    yield [Event(net.now, 2)]
                fire(net, ev['y_made'])
                yield [ev['sent_dy'], credit]
                net.spawn(reduce_x(net, part, y_made, rx_scratch, ev['y_reduced'], rs_pool.again()))
                for k in range(RING):
                    fire(net, y_made[k])
                yield [ev['y_reduced']]
                add_rows(x, part.at[3, net.core], x)
                yield [net.load(x, x_out)]
                fire(net, ev['x_saved'])

            a0, s0 = up1.at[pl.ds(0, nd)], up1.at[pl.ds(nd, nd)]
            backs = [RING]

            def bring_back():
                yield [ev['d_down1']]
                yield [net.load(u_out, g)]
                fire(net, ev['got_u0'])

            def bring_acts():
                yield [ev['all_du']]
                net.drain(ev['got_up1'].copies)
                yield [net.load(a_out, a0), net.load(s_out, s0)]
                fire(net, ev['acts'])

            def layer0_hidden(step):
                yield [dy_here[step], ev['acts'], ev['back_down0'], ev['d_up1'], Event(0.0, 2)]
                pre_back_rows(net, net.at('x', step), u, down0, a0, ds)
                backs[0] -= 1
                if backs[0] == 0:
                    fire(net, ev['da0'])

            def layer0():
                for h in range(2):
                    yield [ev['da0'], ev['got_u0'], Event(0.0, 3)]
                    grad_tiles(net, g.at[:, :, columns(h)], ds, stage, d_up0.at[columns(h)])
                fire(net, ev['d_up0'])
                for h in range(2):
                    yield [ev['got_dy'], ev['acts'], Event(0.0, 3)]
                    grad_tiles(net, s0, u.at[:, :, columns(h)], stage, d_down0.at[:, columns(h)])
                fire(net, ev['d_down0'])
                yield [ev['y_reduced'], ev['back_up0'], ev['back_up0_rest'], Event(0.0, 2)]
                net.drain(ev['y_reduced'].copies + ev['got_down1'].copies)
                x0 = down1.at[pl.ds(0, x_halves.shape[0])]
                yield [net.grant(9, 'xp'), net.load(x_halves, x0)]
                net.spawn(reduce_x(net, part, du_made, rx_scratch, ev['du_reduced'], rs_pool.again()))
                for k, step in enumerate(STEPS):
                    input_back_rows(net, net.at('x', step), ds, up0, part.at[k])
                    fire(net, du_made[k])
                    yield [Event(net.now, 2)]
                yield [ev['du_reduced'], ev['x_saved']]
                for q in range(x_halves.shape[0]):
                    rows_q = pl.ds(q * dr, dr)
                    dy_q = u.at[net.data, rows_q]
                    norm_back_rows(x0.at[q], lambda at, dy_q=dy_q: dy_q[at, :], part.at[3, net.core, rows_q], x.at[rows_q])
                yield [net.load(x, dx_out)]

            def up_place(ref, k):
                return lambda block, rows: ref.at[pl.ds(pl.multiple_of(block * (2 * half_up) + k * half_up + rows.start, rows.size), rows.size)]

            def down_place(ref, k):
                return lambda block, rows: ref.at[pl.ds(pl.multiple_of(block * dr + rows.start, rows.size), rows.size), columns(k)]

            def gate(event, items, pool):
                yield items
                pool.again()
                fire(net, event)

            def sum_job(n, place, ref, ready, name, credits=()):
                passed = [Event(), Event()]
                for k in range(2):
                    start = Event()
                    net.spawn(gate(start, ready + ([credits[k]] if credits else []), job_pools[n][k]))
                    net.spawn(jobs[n][k].run(place(ref, k), start, ev['sum_%s%d' % (name, k)], frees[k], passed[k], job_pools[n][k]))
                return passed

            def out_down(layer, dw_down, credit):
                def one(k):
                    done = ev['sum_down%d%d' % (layer, k)]
                    yield [done]
                    yield [net.load(done.total, dw_down.at[:, columns(k)])]
                    if credit is not None:
                        net.drain(done.copies)
                        yield [net.grant(credit + k, 'yz')]
                        fire(net, freed[credit + k])

                for k in range(2):
                    net.spawn(one(k))

            def out_up(n, layer, dw_up, credit):
                totals = [ev['sum_up%d%d' % (layer, k)] for k in range(2)]
                yield totals
                net.drain(totals[0].copies + totals[1].copies)
                spare = jobs[n][0].scratch[0].at[0]
                for k, done in enumerate(totals):
                    for q in range(2):
                        copy_rows(net, done.total.at[pl.ds(q * spare.shape[1], spare.shape[1])], spare.at[2 * k + q])
                done = ev['out_up%d' % layer]
                net.spawn(exchange_back(net, spare, dw_up, done))
                if credit is not None:
                    yield [done]
                    for k in range(2):
                        yield [net.grant(credit + k, 'yz')]
                        fire(net, freed[credit + k])

            passed = sum_job(0, down_place, d_down1, [ev['d_down1']], 'down1')
            passed = sum_job(1, up_place, d_up1, [ev['d_up1']] + passed, 'up1')
            passed = sum_job(0, up_place, d_up0, [ev['d_up0']] + passed, 'up0', [freed[10], freed[11]])
            sum_job(1, down_place, d_down0, [ev['d_down0']] + passed, 'down0', [freed[12], freed[13]])
            out_down(1, dw_down1, 10)
            net.spawn(out_up(1, 1, dw_up1, 12))
            net.spawn(out_up(0, 0, dw_up0, None))
            out_down(0, dw_down0, None)
            for k in (3, 2, 1, 0):
                net.spawn(layer1(k, STEPS[k]))
            for step in (0, -1, 1, 2):
                net.spawn(layer0_hidden(step))
            for flow in (up_first(), second(), hidden_flow(), down_flow(), next_layer(), back_flow(), again(), grads1(), act(), layer1_out(),
                         bring_back(), bring_acts(), layer0()):
                net.spawn(flow)
            net.run()

        def finish(up1_ref, up0_ref, down1_ref, down0_ref, x_ref, dx_ref, x_out, dx_out, up_out, down_out):
            for l, (up_ref, down_ref) in enumerate(((up0_ref, down0_ref), (up1_ref, down1_ref))):
                join_columns(up_ref, up_out.at[l])
                rows_loop(dr, 16, lambda at: down_out.at[l].__setitem__((at, slice(None)), down_ref[at, :]))
            rows_loop(rows, 16, lambda at: x_out.__setitem__((at, slice(None)), x_ref[at, :]))
            rows_loop(rows, 16, lambda at: dx_out.__setitem__((at, slice(None)), dx_ref[at, :]))

        d_up_own, d_down_own = shape((nd, ur, hidden), F32), shape((dr, width), F32)

        d_up_full, d_down_full = shape((width, hidden), F32), shape((hidden, width), F32)
        x_out, dx, _, _, _, _, _, _, _, _, *grads = call(
            step, [own, own, shape((num_layers, nd * ur, hidden), BF16), act_full, hid_full, hid_full] + [d_up_full, d_down_full] * 2
            + [d_up_own, d_down_own] * 2, 'h' * 14, 'hhhhh',
            [vmem(own)] + [vmem(act_full)] * 2 + [vmem(up_full)] * 2 + [vmem(down_full)] * 2 + [vmem(hid_full)] * 2
            + [pltpu.VMEM((2, hidden // 4, width // 2), F32)] + rx + sums, TR, TS, TL, 0,
            tokens, tokens.reshape(rows // dr, dr, width), grad_out, w_up, w_down)
        up1_own, down1_own, up0_own, down0_own = grads
        return pl.pallas_call(
            finish, out_shape=[own, own, shape(w_up.shape, F32), shape(w_down.shape, F32)], name='finish',
            in_specs=[pl.BlockSpec(memory_space=pltpu.VMEM)] * 6, out_specs=[pl.BlockSpec(memory_space=pltpu.VMEM)] * 4,
        )(up1_own, up0_own, down1_own, down0_own, x_out, dx)

    return jax.shard_map(device_fn, mesh=mesh, in_specs=(tok_spec, tok_spec, w_spec, w_spec), out_specs=(tok_spec, tok_spec, w_spec, w_spec), check_vma=False)
```

```python
import contextlib

import jax
import jax.numpy as jnp
from jax import lax
from jax.experimental import pallas as pl
from jax.experimental.pallas import tpu as pltpu
from jax.sharding import PartitionSpec as P

NORM_EPS = 1e-6
BOTH_AXES = ('local', 'data')
CONTRACT_ROWS = (((0,), (0,)), ((), ()))
CONTRACT_COLS = (((1,), (1,)), ((), ()))
MESH = pl.DeviceIdType.MESH
RING = 4
F32, BF16 = jnp.float32, jnp.bfloat16

LINK_RATE = 46.0e3
PAIR_RATE = 600e3
LOCAL_RATE = 3000e3
HOP = 2.4
PAIR_HOP = 1.0
ENTRY = 4.0
GELU_C = 0.7978845608028654


def scope(label):
    return jax.named_scope(label) if SCOPES else contextlib.nullcontext()


class Event:
    def __init__(self, time=None, rank=0, name=''):
        self.time, self.rank, self.name = time, rank, name


class Copy:
    def __init__(self, desc, time, remote):
        self.desc, self.time, self.remote, self.rank, self.waited = desc, time, remote, 0, False

    def wait(self):
        if self.remote:
            self.desc.wait_recv()
        else:
            self.desc.wait()


class Credit:
    def __init__(self, semaphore, count, time):
        self.semaphore, self.count, self.time, self.rank, self.waited = semaphore, count, time, 0, False

    def wait(self):
        pl.semaphore_wait(self.semaphore, self.count)


class Pool:
    def __init__(self):
        self.slots, self.next = [], 0

    def again(self):
        self.next = 0
        return self


class Net:
    def __init__(self, send_sems, recv_sems, local_sems, credit_sems):
        self.send_sems, self.recv_sems, self.local_sems, self.credit_sems = send_sems, recv_sems, local_sems, credit_sems
        self.n_remote = self.n_local = 0
        self.free_sends = list(range(send_sems.shape[0]))
        self.free_locals = []
        self.now = 0.0
        self.free = {}
        self.sent = []
        self.flows = []
        self.labels = {}
        here, there = lax.axis_index('local'), lax.axis_index('data')
        pos = {'z': here // RING, 'y': lax.rem(here, RING), 'x': there // 2}
        self.data, self.core = there, lax.rem(there, 2)
        self.ring = {axis: [at] + [lax.rem(at + step, RING) for step in range(1, RING)] for axis, at in pos.items()}
        self.hops = [there] + [lax.rem(there + step, 2 * RING) for step in range(1, 2 * RING)]
        self.blocks = [at * 2 + self.core for at in self.ring['x']]
        self.places = [[z * RING + y for y in self.ring['y']] for z in self.ring['z']]
        self.partner = pos['x'] * 2 + (1 - self.core)
        self.other = 1 - self.core

    def at(self, axis, step):
        return self.ring[axis][step % RING]

    def block(self, step):
        return self.blocks[step % RING]

    def device(self, axis, step):
        if axis == 'p':
            return {'data': self.partner}
        if axis == 'd':
            return {'data': self.hops[step % (2 * RING)]}
        if axis == 'x':
            return {'data': self.block(step)}
        if axis == 'y':
            return {'local': self.places[0][step % RING]}
        return {'local': self.places[step % RING][0]}

    def peers(self, axes):
        return [(axis, step) for axis in axes for step in ((1, -1) if axis in 'xyz' else (1,) if axis == 'p' else range(1, 2 * RING))]

    def signal(self, semaphore, axes):
        for axis, step in self.peers(axes):
            pl.semaphore_signal(semaphore, inc=1, device_id=self.device(axis, step), device_id_type=MESH)

    def arrive(self, axes):
        self.entry, self.entered = pltpu.get_barrier_semaphore(), len(self.peers(axes))
        self.signal(self.entry, axes)

    def enter(self):
        pl.semaphore_wait(self.entry, self.entered)
        self.now = max(self.now, ENTRY)

    def take(self, copies):
        for copy in copies:
            copy.wait()
            copy.waited = True
            self.free_locals.append(copy.slot)
            self.now = max(self.now, copy.time)

    def grant(self, k, axes):
        self.signal(self.credit_sems.at[k], axes)
        return Credit(self.credit_sems.at[k], len(self.peers(axes)), self.now + HOP)

    def drain(self, copies):
        for copy in copies:
            if copy in self.sent:
                copy.desc.wait_send()
                self.sent.remove(copy)
                self.free_sends.append(copy.slot)

    def idle(self, gap):
        over = [copy for copy in self.sent if copy.time + 1.5 < self.now]
        self.drain(over[:int(gap / 0.05)])

    def send(self, src, dst, axis, step=1, pool=None):
        if pool is not None and pool.next < len(pool.slots):
            k = pool.slots[pool.next]
        else:
            k = self.n_remote
            self.n_remote += 1
            if pool is not None:
                pool.slots.append(k)
        if pool is not None:
            pool.next += 1
        if not self.free_sends:
            if PRINT:
                print('EXHAUSTED', round(self.now, 1))
            self.drain([min(self.sent, key=lambda copy: copy.time)])
        send_slot = self.free_sends.pop()
        desc = pltpu.make_async_remote_copy(
            src_ref=src, dst_ref=dst, send_sem=self.send_sems.at[send_slot], recv_sem=self.recv_sems.at[k],
            device_id=self.device(axis, step), device_id_type=MESH)
        desc.start()
        size = 1
        for n in dst.shape:
            size *= n
        size *= dst.dtype.itemsize
        rate = PAIR_RATE if axis == 'p' else LINK_RATE
        extra = 2.0 if axis == 'd' else 0.0
        if axis == 'd':
            axis, step, size = ('p', 1, size) if step == 1 else ('x', 1 if step < RING + 2 else -1, size)
        key = (axis, step)
        done = max(self.free.get(key, 0.0), self.now) + size / rate
        self.free[key] = done
        copy = Copy(desc, done + extra + (PAIR_HOP if axis == 'p' else HOP), True)
        copy.slot = send_slot
        self.sent.append(copy)
        return copy

    def load(self, src, dst):
        if not self.free_locals:
            self.free_locals.append(self.n_local)
            self.n_local += 1
        k = self.free_locals.pop()
        desc = pltpu.make_async_copy(src, dst, self.local_sems.at[k])
        desc.start()
        size = 1
        for n in dst.shape:
            size *= n
        done = max(self.free.get('hbm', 0.0), self.now) + size * dst.dtype.itemsize / LOCAL_RATE
        self.free['hbm'] = done
        copy = Copy(desc, done + 0.9, False)
        copy.slot = k
        return copy

    def save(self, src, dst):
        copy = self.load(src, dst)
        copy.time += 4.0
        return copy

    def spend(self, microseconds):
        self.now += microseconds

    def spawn(self, flow):
        self.step(flow)

    def step(self, flow):
        try:
            if flow not in self.labels:
                self.labels[flow] = [flow.__name__, len(self.labels), 0]
            self.labels[flow][2] += 1
            self.flows.append((flow, next(flow)))
        except StopIteration:
            pass

    def run(self):
        while self.flows:
            best = None
            for k, (_, items) in enumerate(self.flows):
                if any(item.time is None for item in items):
                    continue
                time = max([item.time for item in items] + [0.0])
                late = max([item.rank for item in items] + [0])
                rank = (max(time, self.now) + (SLACK if late else 0.0), late, time)
                if best is None or rank < best[0]:
                    best = (rank, k, time)
            _, k, time = best
            flow, items = self.flows.pop(k)
            self.idle(time - self.now)
            label = '%s_%d_%d' % tuple(self.labels[flow])
            with scope('w_' + label):
                for item in items:
                    if not isinstance(item, Event) and not item.waited:
                        item.wait()
                        item.waited = True
                        if isinstance(item, Copy) and not item.remote:
                            self.free_locals.append(item.slot)
            before = self.now
            self.now = max(self.now, time)
            if PRINT:
                print('STEP', label, round(before, 2), round(self.now, 2))
            with scope('s_' + label):
                self.step(flow)

    def finish(self):
        for copy in self.sent:
            copy.desc.wait_send()


def rows_loop(rows, chunk, body):
    chunk = min(chunk, rows)

    def step(k, carry):
        body(pl.ds(pl.multiple_of(k * chunk, chunk), chunk))
        return carry

    lax.fori_loop(0, rows // chunk, step, 0)


def add_into(net, dst, *others):
    rows, cols = dst.shape

    def body(at):
        total = dst[at, :]
        for other in others:
            total = total + other[at, :]
        dst[at, :] = total

    rows_loop(rows, 16, body)
    net.spend(rows * cols * 4 * (1 + len(others)) / 4e6)


def fire(net, event):
    event.time = net.now
    if PRINT and event.name:
        print('   %7.1f %s' % (net.now, event.name))


def exchange(net, source, dst, done):
    rows = dst.shape[0] // (2 * RING)

    def mine():
        return dst.at[pl.ds(pl.multiple_of(net.data * rows, rows), rows)]

    own = net.load(source(net.data), mine())
    copies = [net.send(source(net.hops[k]), mine(), 'd', k) for k in (4, 5, 2, 3, 6, 7, 1)]
    yield [own] + copies
    net.drain(copies)
    fire(net, done)


def exchange_back(net, src, dst, done):
    rows = dst.shape[1]
    per = src.shape[1] // rows

    def block(k):
        return src.at[lax.div(k, per), pl.ds(pl.multiple_of(lax.rem(k, per) * rows, rows), rows)]

    own = net.load(block(net.data), dst.at[net.data])
    copies = [net.send(block(net.hops[k]), dst.at[net.data], 'd', k) for k in (4, 5, 2, 3, 6, 7, 1)]
    yield [own] + copies
    net.drain(copies)
    fire(net, done)


def copy_rows(net, src, dst):
    def body(at):
        dst[at, :] = src[at, :]

    rows_loop(src.shape[0], 16, body)
    net.spend(0.2)


def gather_x(net, full, done, issued=None, chips=None, pool=None):
    half = full.shape[1] // 2
    lo, hi = pl.ds(0, half), pl.ds(half, half)
    chips = chips or {step: Event() for step in STEPS}
    left = [2]
    done.copies = []

    def send(*args):
        done.copies.append(net.send(*args, pool=pool))
        return done.copies[-1]

    def block(step):
        return full.at[net.block(step)]

    def part(step, rows):
        return full.at[net.block(step), rows]

    relays = []

    def side(step, first, second, mine):
        yield [mine[0]]
        relays.append(send(part(step, first), part(step, first), 'x', -step))
        left[0] -= 1
        if left[0] == 0:
            net.spawn(far())
            if issued is not None:
                fire(net, issued)
        yield [mine[1]]
        pair = send(block(step), block(step), 'p')
        yield [pair]
        fire(net, chips[step])

    def far():
        yield relays
        pair = send(block(2), block(2), 'p')
        yield [pair]
        fire(net, chips[2])

    forth = [send(part(0, rows), part(0, rows), 'x', 1) for rows in (lo, hi)]
    back = [send(part(0, rows), part(0, rows), 'x', -1) for rows in (hi, lo)]
    pair = send(block(0), block(0), 'p')
    net.spawn(side(-1, lo, hi, forth))
    net.spawn(side(1, hi, lo, back))
    yield [pair]
    fire(net, chips[0])
    yield [chips[step] for step in STEPS]
    fire(net, done)


def gather_yz(net, own, full, first, done, issued=None, offset=0, near=False, split=True, pool=None):
    second = 'y' if first == 'z' else 'z'
    done.copies = []

    def emit(*args):
        done.copies.append(net.send(*args, pool=pool))
        return done.copies[-1]

    size = own.shape[0]
    half = size // 2
    lo, hi, both = pl.ds(offset, half), pl.ds(offset + half, half), pl.ds(offset, size)
    forward, backward = ((lo, hi), (hi, lo)) if split and not near else ((both,), (both,))

    def part(one, two, rows):
        return full.at[yz_index(net, first, one, two), rows]

    left = [3 if near else RING, 3 if near else RING]

    def arrived(which):
        left[which] -= 1
        if left[which] == 0 and (done, issued)[which] is not None:
            fire(net, (done, issued)[which])

    def send(one, rows, axis, step):
        src = own.at[pl.ds(rows.start - offset, rows.size)] if one == 0 else part(one, 0, rows)
        return emit(src, part(one, 0, rows), axis, step)

    def column(one):
        forth = [send(one, rows, second, 1) for rows in forward]
        back = [send(one, rows, second, -1) for rows in backward]

        def finish():
            if near:
                arrived(1)
                yield forth + back
            else:
                yield [forth[0]]
                relays = [emit(part(one, -1, lo), part(one, -1, lo), second, 1)]
                yield [back[0]]
                relays.append(emit(part(one, 1, hi), part(one, 1, hi), second, -1))
                arrived(1)
                yield forth[1:] + back[1:] + relays
            arrived(0)

        net.spawn(finish())

    relays = []

    def side(step, first_half, mine):
        yield [mine[0]]
        if not near:
            relays.append(emit(part(step, 0, first_half), part(step, 0, first_half), first, -step))
            if len(relays) == 2:
                net.spawn(far())
        yield mine[1:]
        column(step)

    def far():
        yield relays
        column(2)

    mine = [net.load(own, part(0, 0, both))]
    forth = [send(0, rows, first, 1) for rows in forward]
    back = [send(0, rows, first, -1) for rows in backward]
    column(0)
    net.spawn(side(-1, lo, forth))
    net.spawn(side(1, hi, back))
    left[0] += 1
    yield mine
    arrived(0)


def yz_index(net, first, one, two):
    return net.places[one % RING][two % RING] if first == 'z' else net.places[two % RING][one % RING]


FAR = [(2, 0), (2, 1), (2, -1), (2, 2), (0, 2), (1, 2), (-1, 2)]


STEPS = (2, 1, -1, 0)


def reduce_x(net, part, made, scratch, done, pool=None):
    other, relay_f, relay_b, last_f, last_b = scratch
    half = part.shape[2] // 2
    lo, hi = pl.ds(0, half), pl.ds(half, half)

    def acc(k, rows=None):
        return part.at[k, net.core] if rows is None else part.at[k, net.core, rows]

    pairs = [None] * RING
    ready = [Event() for _ in STEPS]

    def pair(k):
        yield [made[k]]
        pairs[k] = net.send(part.at[k, net.other], other.at[k], 'p', pool=pool)
        yield [pairs[k]]
        add_into(net, acc(k), other.at[k])
        fire(net, ready[k])

    for k in range(RING):
        net.spawn(pair(k))
    sent = {}
    started = Event()

    def part_flow(k):
        yield [ready[k]]
        if k == 0:
            sent['first_f'] = net.send(acc(0, lo), relay_f, 'x', 1, pool=pool)
            sent['first_b'] = net.send(acc(0, hi), relay_b, 'x', -1, pool=pool)
        elif k == 1:
            sent['direct_f'] = net.send(acc(1, hi), last_f.at[hi], 'x', 1, pool=pool)
        else:
            sent['direct_b'] = net.send(acc(2, lo), last_b.at[lo], 'x', -1, pool=pool)
        if len(sent) == 4:
            fire(net, started)

    for k in range(3):
        net.spawn(part_flow(k))
    yield [started]
    yield [sent['first_f']]
    add_into(net, acc(1, lo), relay_f)
    summed_f = net.send(acc(1, lo), last_f.at[lo], 'x', 1, pool=pool)
    yield [sent['first_b']]
    add_into(net, acc(2, hi), relay_b)
    summed_b = net.send(acc(2, hi), last_b.at[hi], 'x', -1, pool=pool)
    yield [ready[3], sent['direct_f'], sent['direct_b'], summed_f, summed_b]
    add_into(net, acc(3), last_f, last_b)
    done.copies = pairs + list(sent.values()) + [summed_f, summed_b]
    fire(net, done)


def reduce_x_scratch(rows, cols):
    return [pltpu.VMEM((RING, rows, cols), F32), pltpu.VMEM((rows // 2, cols), F32), pltpu.VMEM((rows // 2, cols), F32),
            pltpu.VMEM((rows, cols), F32), pltpu.VMEM((rows, cols), F32)]


def load_parts(net, src, part, made):
    for k, step in enumerate(STEPS):
        def bring(k=k, step=step):
            yield [net.load(src.at[pl.ds(net.at('x', step) * 2, 2)], part.at[k])]
            fire(net, made[k])

        net.spawn(bring())


class Sums:
    def __init__(self, net, first, scratch, stage):
        self.net, self.first, self.scratch, self.stage = net, first, scratch, stage
        self.second = 'y' if first == 'z' else 'z'

    def run(self, place, start, done, free, passed_all, pool, window, lead):
        net, first, second = self.net, self.first, self.second
        relay1, last1, relay2, last2 = self.scratch
        ahead, behind, mine = self.stage
        half = mine.shape[0] // 2
        lo, hi, all_rows = pl.ds(0, half), pl.ds(half, half), pl.ds(0, 2 * half)
        done.copies = []

        def send(*args):
            done.copies.append(net.send(*args, pool=pool))
            return done.copies[-1]

        def term(one, two, rows=all_rows):
            return place(yz_index(net, first, one, two), rows)

        def bring(gate, src, dst, got):
            yield [gate, start]
            yield [net.load(src, dst)]
            fire(net, got)

        chain = [[gate] + [Event() for _ in range(RING)] for gate in free]
        free[:] = [events[RING] for events in chain]
        got = [[Event() for _ in range(RING)] for _ in range(3)]
        ends = [Event() for _ in STEPS]
        passed = [Event() for _ in range(RING)]
        passed[lead] = passed_all

        def ring(k):
            two = STEPS[k]
            if k >= window:
                yield [passed[k - window]]
            net.spawn(bring(chain[0][k], term(1, two, lo), ahead, got[0][k]))
            net.spawn(bring(chain[1][k], term(-1, two, hi), behind, got[1][k]))
            net.spawn(bring(chain[2][k], term(0, two), mine, got[2][k]))
            first_f = send(term(2, two, lo), relay1.at[0, k], first, 1)
            first_b = send(term(2, two, hi), relay1.at[1, k], first, -1)
            direct_f = send(term(1, two, hi), last1.at[0, k, hi], first, 1)
            direct_b = send(term(-1, two, lo), last1.at[1, k, lo], first, -1)
            yield [first_f, got[0][k]]
            add_into(net, relay1.at[0, k], ahead)
            fire(net, chain[0][k + 1])
            summed_f = send(relay1.at[0, k], last1.at[0, k, lo], first, 1)
            yield [first_b, got[1][k]]
            add_into(net, relay1.at[1, k], behind)
            fire(net, chain[1][k + 1])
            summed_b = send(relay1.at[1, k], last1.at[1, k, hi], first, -1)
            fire(net, passed[k])
            yield [direct_f, direct_b, summed_f, summed_b, got[2][k]]
            add_into(net, last1.at[0, k], last1.at[1, k], mine)
            fire(net, chain[2][k + 1])
            fire(net, ends[k])

        def sums(k, rows=all_rows):
            return last1.at[0, k, rows]

        yield [start]
        for k in range(RING):
            net.spawn(ring(k))
        yield [ends[0]]
        first_f = send(sums(0, lo), relay2.at[0], second, 1)
        first_b = send(sums(0, hi), relay2.at[1], second, -1)
        yield [ends[1]]
        direct_f = send(sums(1, hi), last2.at[0, hi], second, 1)
        yield [ends[2]]
        direct_b = send(sums(2, lo), last2.at[1, lo], second, -1)
        yield [first_f]
        add_into(net, sums(1, lo), relay2.at[0])
        summed_f = send(sums(1, lo), last2.at[0, lo], second, 1)
        yield [first_b]
        add_into(net, sums(2, hi), relay2.at[1])
        summed_b = send(sums(2, hi), last2.at[1, hi], second, -1)
        yield [ends[3], direct_f, direct_b, summed_f, summed_b]
        add_into(net, sums(3), last2.at[0], last2.at[1])
        done.total = sums(3)
        fire(net, done)


def sums_scratch(rows, cols):
    return [pltpu.VMEM((2, RING, rows // 2, cols), F32), pltpu.VMEM((2, RING, rows, cols), F32),
            pltpu.VMEM((2, rows // 2, cols), F32), pltpu.VMEM((2, rows, cols), F32)]


def sums_stage(rows, cols):
    return [pltpu.VMEM((rows // 2, cols), F32), pltpu.VMEM((rows // 2, cols), F32), pltpu.VMEM((rows, cols), F32)]


def norm_rows(x_ref, u_ref):
    def body(at):
        x = x_ref[at, :].astype(F32)
        u_ref[at, :] = (x * lax.rsqrt(jnp.mean(x * x, axis=-1, keepdims=True) + NORM_EPS)).astype(BF16)

    rows_loop(x_ref.shape[0], 16, body)


def norm_back_rows(x_ref, dy_of, du_ref, dx_ref):
    def body(at):
        x = x_ref[at, :].astype(F32)
        du = du_ref[at, :]
        r = lax.rsqrt(jnp.mean(x * x, axis=-1, keepdims=True) + NORM_EPS)
        xr = x * r
        dx_ref[at, :] = (dy_of(at).astype(F32) + r * (du - xr * jnp.mean(xr * du, axis=-1, keepdims=True))).astype(BF16)

    rows_loop(x_ref.shape[0], 16, body)


def add_rows(x_ref, y_ref, out_ref):
    def body(at):
        out_ref[at, :] = (x_ref[at, :].astype(F32) + y_ref[at, :]).astype(BF16)

    rows_loop(x_ref.shape[0], 16, body)


def swap_halves(even, odd):
    low = lax.broadcasted_iota(jnp.int32, even.shape, len(even.shape) - 1) < even.shape[-1] // 2
    shift = even.shape[-1] // 2
    axis = len(even.shape) - 1
    return jnp.where(low, even, pltpu.roll(odd, shift, axis)), jnp.where(low, pltpu.roll(even, shift, axis), odd)


def split_columns(w_ref, cols_ref, layers):
    pieces, _, wide = w_ref.shape
    rows = layers
    tile = pieces * wide // (4 * RING * RING)
    for x in range(RING):
        for p in range(wide // tile):
            pair = []
            for i in (2 * p, 2 * p + 1):
                at = (i * RING + x) * tile
                pair.append(w_ref[at // wide, pl.ds(0, rows), pl.ds(at % wide, tile)].astype(F32))
            for c, value in enumerate(swap_halves(*pair)):
                cols_ref[2 * x + c, pl.ds(0, rows), pl.ds(p * tile, tile)] = value.astype(cols_ref.dtype)


def join_columns(cols_ref, w_ref):
    tile = w_ref.shape[1] // (4 * RING * RING)
    for x in range(RING):
        for p in range(cols_ref.shape[2] // tile):
            pair = [cols_ref[2 * x + c, :, pl.ds(p * tile, tile)] for c in range(2)]
            for i, value in zip((2 * p, 2 * p + 1), swap_halves(*pair)):
                w_ref[:, pl.ds((i * RING + x) * tile, tile)] = value


def call(body, out_shape, out_spaces, in_spaces, scratch, remote, sends, local, collective_id, *args):
    spaces = {'v': pl.BlockSpec(memory_space=pltpu.VMEM), 'h': pl.BlockSpec(memory_space=pl.ANY)}

    def kernel(*refs):
        net = Net(*refs[-5:-1])
        net.tile_sems = refs[-1]
        body(net, *refs[:-5])
        net.finish()
        assert net.n_remote <= remote and net.n_local <= local, (body.__name__, net.n_remote, net.n_local)
        if PRINT:
            print(body.__name__, net.n_remote, net.n_local, round(net.now, 1))

    return pl.pallas_call(
        kernel, out_shape=out_shape, in_specs=[spaces[s] for s in in_spaces], out_specs=[spaces[s] for s in out_spaces],
        scratch_shapes=list(scratch) + [pltpu.SemaphoreType.DMA((sends,)), pltpu.SemaphoreType.DMA((remote,)), pltpu.SemaphoreType.DMA((local,)),
                                               pltpu.SemaphoreType.REGULAR((14,)), pltpu.SemaphoreType.DMA((2,))],
        compiler_params=pltpu.CompilerParams(collective_id=collective_id, has_side_effects=True, vmem_limit_bytes=67000000),
        cost_estimate=pl.CostEstimate(flops=10**8, bytes_accessed=10**7, transcendentals=0),
        name=body.__name__)(*args)


PRINT = False
SCOPES = False


WIDE = 512
EARLY = 3
SLACK = 0.1
R_HIDDEN, R_DOWN, R_BACK, R_TURN, R_DU, R_DDOWN, R_DDOWN2, R_DUP, R_OUT, R_PRE, R_GUP, R_GDOWN, R_DX = 2, 1, 3, 1, 3, 2, 2, 4, 2, 2, 3, 3, 2
WINDOWS = (2, 2, 2, 2, 2, 2, 2, 2)
AXES = ('yz', 'yz', 'yz', 'yz')
TOP = 6
NEAR = 'z'
LEAD = (3, 3, 3)
TR, TS, TL = 278, 64, 19


def wide_loop(total, body):
    wide = min(WIDE, total)

    def step(k, carry):
        body(k, wide, pl.ds(pl.multiple_of(k * wide, wide), wide))
        return carry

    lax.fori_loop(0, total // wide, step, 0)


def flat(value):
    return value.reshape(value.shape[0] * value.shape[1], value.shape[2])


def dot_rows(a, b):
    return jnp.dot(flat(a), flat(b), preferred_element_type=F32)


def dot_cols(a, b):
    return lax.dot_general(flat(a), flat(b), CONTRACT_COLS, preferred_element_type=F32)


def gelu(a):
    return 0.5 * a * (1.0 + jnp.tanh(GELU_C * (a + 0.044715 * a * a * a)))


def hidden_rows(net, chip, u, up, a, s):
    at = pl.ds(chip * 2, 2)

    def body(_, wide, cols):
        pre = dot_rows(u[at], up[:, :, cols]).astype(BF16)
        a[at, :, cols] = pre.reshape(2, -1, wide)
        s[at, :, cols] = gelu(pre.astype(F32)).astype(BF16).reshape(2, -1, wide)

    wide_loop(up.shape[2], body)
    net.spend(1.7)


def down_rows(net, chip, s, down, part):
    at = pl.ds(chip * 2, 2)

    def body(_, wide, cols):
        part[:, :, cols] = dot_rows(s[at], down[:, :, cols]).reshape(2, -1, wide)

    wide_loop(down.shape[2], body)
    net.spend(1.76)


def hidden_back_rows(net, chip, dy, down, ds):
    at = pl.ds(chip * 2, 2)
    rows = down.shape[1]

    def body(k, wide, cols):
        blocks = pl.ds(k * (wide // rows), wide // rows)
        ds[at, :, cols] = dot_cols(dy[at], down[blocks]).astype(BF16).reshape(2, -1, wide)

    wide_loop(down.shape[0] * rows, body)
    net.spend(1.5)


def gelu_both(a):
    t = jnp.tanh(GELU_C * (a + 0.044715 * a * a * a))
    return 0.5 * a * (1.0 + t), 0.5 * (1.0 + t) + 0.5 * a * (1.0 - t * t) * (GELU_C * (1.0 + 3 * 0.044715 * a * a))


def hidden_turn_rows(net, chip, u, up, s, ds):
    at = pl.ds(chip * 2, 2)

    def body(_, wide, cols):
        pre = dot_rows(u[at], up[:, :, cols]).astype(BF16).astype(F32)
        value, slope = gelu_both(pre)
        s[at, :, cols] = value.astype(BF16).reshape(2, -1, wide)
        ds[at, :, cols] = (ds[at, :, cols].astype(F32) * slope.reshape(2, -1, wide)).astype(BF16)

    wide_loop(up.shape[2], body)
    net.spend(2.1)


def pre_back_rows(net, chip, dy, down, a, da):
    at = pl.ds(chip * 2, 2)
    rows = down.shape[1]

    def body(k, wide, cols):
        blocks = pl.ds(k * (wide // rows), wide // rows)
        ds = dot_cols(dy[at], down[blocks]).astype(BF16).astype(F32).reshape(2, -1, wide)
        da[at, :, cols] = (ds * gelu_both(a[at, :, cols].astype(F32))[1]).astype(BF16)

    wide_loop(down.shape[0] * rows, body)
    net.spend(1.95)


def input_back_rows(net, chip, da, up, part):
    at = pl.ds(chip * 2, 2)
    rows = up.shape[1]

    def body(k, wide, cols):
        blocks = pl.ds(k * (wide // rows), wide // rows)
        part[:, :, cols] = dot_cols(da[at], up[blocks]).reshape(2, -1, wide)

    wide_loop(up.shape[0] * rows, body)
    net.spend(1.9)


def stored_tiles(net, count, compute, stage, out):
    def store(t):
        return pltpu.make_async_copy(stage.at[lax.rem(t, 2)], out(t), net.tile_sems.at[lax.rem(t, 2)])

    def step(t, carry):
        @pl.when(t >= 2)
        def _():
            store(t - 2).wait()

        compute(t, stage.at[lax.rem(t, 2)])
        store(t).start()
        return carry

    lax.fori_loop(0, count, step, 0)
    for t in range(max(count - 2, 0), count):
        store(jnp.int32(t)).wait()


def dot_tokens(a, b):
    return lax.dot_general(flat(a), flat(b), CONTRACT_ROWS, preferred_element_type=F32)


def grad_tiles(net, lhs, rhs, stage, out):
    wide = stage.shape[1]

    def compute(t, slot):
        slot[...] = dot_tokens(lhs[:, :, pl.ds(pl.multiple_of(t * wide, wide), wide)], rhs[...])

    stored_tiles(net, lhs.shape[2] // wide, compute, stage, lambda t: out.at[pl.ds(pl.multiple_of(t * wide, wide), wide)])
    net.spend(4.35 * lhs.shape[2] / 1024)


def solution(mesh):
    nl, nd = mesh.shape['local'], mesh.shape['data']
    tok_spec = P(BOTH_AXES, None)
    w_spec = P(None, BOTH_AXES, None)

    def device_fn(tokens, grad_out, w_up, w_down):
        num_layers, ur, ffn = w_up.shape
        dr = w_down.shape[1]
        rows, width = tokens.shape
        hidden = nl * dr
        shape = jax.ShapeDtypeStruct
        up_full = shape((nl, nd * ur, hidden), BF16)
        down_full = shape((nl, dr, width), BF16)
        act_full = shape((nd, rows, width), BF16)
        hid_full = shape((nd, rows, hidden), BF16)
        own = shape((rows, width), BF16)
        part_vmem = pltpu.VMEM((RING, 2, rows, width), F32)
        rx = [part_vmem] + reduce_x_scratch(rows, width)
        sums = sums_scratch(dr, hidden) * 4 + sums_stage(dr, hidden) * 2

        def vmem(like):
            return pltpu.VMEM(like.shape, like.dtype)

        def step(net, x_in, x_halves, g_in, w_up_in, w_down_in,
                 x_out, dx_out, block_out, u_out, a_out, s_out, d_up0, d_down0, d_up1, d_down1, dw_up1, dw_down1, dw_up0, dw_down0,
                 x, u, g, up0, up1, down0, down1, ds, s, stage, part, *scratch):
            net.arrive('dyz')
            rx_scratch = scratch[:5]
            names = ('blocks', 'blocks1', 'sent_u', 'got_u', 'got_g', 'sent_up0', 'sent_down0', 'sent_up1', 'sent_down1', 'got_up0', 'got_down0',
                     'got_up1', 'got_down1', 'saved', 'free0', 'reduced0', 'ds_made', 'got_u1', 'hidden', 'all_du', 'reduced1', 'sent_dy', 'got_dy',
                     'back_up0', 'back_up0_rest', 'back_down0', 'd_down1', 'd_up1', 'y_reduced', 'acts', 'd_down0', 'da0', 'd_up0', 'du_reduced',
                     'out_up1', 'out_up0', 'got_u0', 'y_made', 'x_saved', 'weights_in', 'd_down1_0')
            ev = {name: Event(name=name) for name in names}
            for kind in ('up', 'down'):
                for layer in range(2):
                    for k in range(2):
                        ev['sum_%s%d%d' % (kind, layer, k)] = Event(name='sum_%s%d%d' % (kind, layer, k))
            ev['got_up0'].rank = R_HIDDEN
            hidden_made, made0, made1, y_made, du_made = ([Event(name='%s%d' % (name, k)) for k in range(RING)]
                                                          for name in ('hidden_', 'made0_', 'made1_', 'y_made_', 'du_made_'))
            wide = width // 2
            half_up = nd * ur // 2
            act_pool, rs_pool = Pool(), Pool()
            job_pools = [[Pool(), Pool()], [Pool(), Pool()]]
            pools = {'up0': [Pool(), Pool()], 'down0': [Pool(), Pool()], 'up1': job_pools[0], 'down1': job_pools[1]}
            stages = (scratch[21:24], scratch[24:27])
            job_scratch = [[scratch[5 + 8 * n + 4 * k:9 + 8 * n + 4 * k] for k in range(2)] for n in range(2)]
            frees = [[Event(0.0) for _ in range(3)] for _ in range(2)]
            freed = {k: Event() for k in range(10, 14)}

            def columns(h):
                return pl.ds(h * wide, wide)

            inputs = [net.load(x_in, x)]
            inputs += [net.load(w_up_in.at[l, :, pl.ds(k * hidden, hidden)], ds.at[k, pl.ds(l * ur, ur)]) for l in range(num_layers) for k in range(nd)]

            def gather(name, own, full, split):
                size = own.shape[0] // 2

                def join(kind, events):
                    yield events
                    if kind == 'got_':
                        ev[kind + name].copies = events[0].copies + events[1].copies
                    fire(net, ev[kind + name])

                got, sent = [Event(), Event()], [Event(), Event()]
                for k, first in enumerate('yz'):
                    net.spawn(gather_yz(net, own.at[pl.ds(k * size, size)], full, first, got[k], sent[k], k * size, split=split, pool=pools[name][k]))
                net.spawn(join('got_', got))
                net.spawn(join('sent_', sent))

            net.enter()
            gather('down0', w_down_in.at[0], down0, False)
            net.take(inputs)
            split_columns(ds, s, num_layers * ur)
            net.spend(0.5)
            net.spawn(exchange(net, lambda k: s.at[k, pl.ds(0, ur)], block_out.at[0], ev['blocks']))
            norm_rows(x, u.at[net.data])
            net.spend(0.7)
            own_grads = net.load(g_in, g.at[net.data])

            def up_first():
                yield [ev['blocks']]
                gather('up0', block_out.at[0], up0, True)
                net.spawn(gather_x(net, u, ev['got_u'], ev['sent_u'], pool=act_pool))
                yield [ev['sent_u']]
                net.spawn(exchange(net, lambda k: s.at[k, pl.ds(ur, ur)], block_out.at[1], ev['blocks1']))
                yield [own_grads]
                net.spawn(gather_x(net, g, ev['got_g']))

            def second():
                yield [ev['sent_up0'], ev['sent_down0'], ev['blocks1']]
                gather('down1', w_down_in.at[1], down1, False)
                yield [made0[EARLY]]
                gather('up1', block_out.at[1], up1, True)

            def hidden_flow():
                yield [ev['got_u'], ev['got_up0'], ev['blocks1']]
                for k, step in enumerate(STEPS):
                    hidden_rows(net, net.at('x', step), u, up0, ds, s)
                    fire(net, hidden_made[k])
                    yield [Event(net.now, R_HIDDEN)]
                yield [net.load(ds, a_out), net.load(s, s_out), net.load(u, u_out)]
                fire(net, ev['saved'])

            def down_flow():
                for k, step in enumerate(STEPS):
                    yield [hidden_made[k], ev['got_down0'], Event(0.0, R_DOWN)]
                    down_rows(net, net.at('x', step), s, down0, part.at[k])
                    fire(net, made0[k])
                fire(net, ev['free0'])

            net.spawn(reduce_x(net, part, made0, rx_scratch, ev['reduced0'], rs_pool))
            here = {step: Event(name='u%d' % step) for step in STEPS}
            dy_here = {step: Event() for step in STEPS}

            def next_layer():
                yield [ev['saved'], ev['got_g']]
                net.drain(ev['got_u'].copies + ev['got_g'].copies)
                credit = net.grant(3, 'xp')
                yield [ev['reduced0'], credit]
                add_rows(x, part.at[3, net.core], x)
                norm_rows(x, u.at[net.data])
                net.spend(1.0)
                net.spawn(gather_x(net, u, ev['got_u1'], chips=here, pool=act_pool.again()))
                net.drain(ev['reduced0'].copies)
                yield [net.grant(4, 'xp')]
                net.spawn(reduce_x(net, part, made1, rx_scratch, ev['reduced1'], rs_pool.again()))

            def back_flow():
                for k, step in enumerate(STEPS):
                    yield [ev['got_g'], ev['got_down1'], ev['saved'], Event(0.0, R_BACK)]
                    hidden_back_rows(net, net.at('x', step), g, down1, ds)
                fire(net, ev['ds_made'])

            def again():
                top = nd * ur * TOP // 8
                yield [ev['free0'], ev['ds_made']]
                net.drain(ev['got_up0'].copies + ev['got_down0'].copies)
                credit = net.grant(6, 'yz')
                yield [credit]
                net.spawn(gather_yz(net, w_down_in.at[0], down0, NEAR, ev['back_down0'], near=True, pool=pools['down0'][1].again()))
                net.spawn(gather_yz(net, block_out.at[0, pl.ds(0, top)], up0, 'y', ev['back_up0'], pool=pools['up0'][0].again()))
                net.spawn(gather_yz(net, block_out.at[0, pl.ds(top, nd * ur - top)], up0, 'z', ev['back_up0_rest'], offset=top, pool=pools['up0'][1].again()))

            def weights():
                yield [ev['got_up1'], ev['got_down1']]
                yield [net.grant(7, 'yz')]
                fire(net, ev['weights_in'])

            left = [RING, RING]

            def layer1(k, step):
                yield [here[step], ev['ds_made'], ev['got_up1'], Event(0.0, R_TURN)]
                hidden_turn_rows(net, net.at('x', step), u, up1, s, ds)
                left[0] -= 1
                if left[0] == 0:
                    fire(net, ev['hidden'])
                yield [Event(net.now, R_DU)]
                input_back_rows(net, net.at('x', step), ds, up1, part.at[k])
                fire(net, made1[k])
                left[1] -= 1
                if left[1] == 0:
                    fire(net, ev['all_du'])

            def grads1():
                for h in range(2):
                    yield [Event(0.0, R_DDOWN2 if h else R_DDOWN), ev['hidden']]
                    grad_tiles(net, s, g.at[:, :, columns(h)], stage, d_down1.at[:, columns(h)])
                    fire(net, ev['d_down1' if h else 'd_down1_0'])
                for h in range(2):
                    yield [Event(net.now, R_DUP)]
                    grad_tiles(net, u.at[:, :, columns(h)], ds, stage, d_up1.at[columns(h)])
                fire(net, ev['d_up1'])

            def act():
                yield [ev['d_up1'], ev['all_du'], ev['got_u1']]
                own_g = [net.load(g_in.at[:, columns(h)], ds.at[h]) for h in range(2)]
                net.drain(ev['got_u1'].copies)
                credit = net.grant(5, 'xp')
                yield [ev['reduced1'], credit] + own_g
                norm_back_rows(x, lambda at: jnp.concatenate([ds[h, at, :] for h in range(2)], axis=-1), part.at[3, net.core], u.at[net.data])
                net.spend(0.7)
                net.spawn(gather_x(net, u, ev['got_dy'], ev['sent_dy'], dy_here, pool=act_pool.again()))

            def layer1_out():
                yield [ev['reduced1'], Event(0.0, R_OUT)]
                net.drain(ev['reduced1'].copies)
                credit = net.grant(8, 'xp')
                for k, step in enumerate(STEPS):
                    down_rows(net, net.at('x', step), s, down1, part.at[k])
                    yield [Event(net.now, R_OUT)]
                fire(net, ev['y_made'])
                yield [ev['sent_dy'], credit]
                net.spawn(reduce_x(net, part, y_made, rx_scratch, ev['y_reduced'], rs_pool.again()))
                for k in range(RING):
                    fire(net, y_made[k])
                yield [ev['y_reduced']]
                add_rows(x, part.at[3, net.core], x)
                yield [net.load(x, x_out)]
                fire(net, ev['x_saved'])

            a0, s0 = up1.at[pl.ds(0, nd)], up1.at[pl.ds(nd, nd)]
            backs = [RING]

            def bring_back():
                yield [ev['d_down1']]
                yield [net.load(u_out, g)]
                fire(net, ev['got_u0'])

            def bring_acts():
                yield [ev['all_du']]
                net.drain(ev['got_up1'].copies)
                yield [net.load(a_out, a0), net.load(s_out, s0)]
                fire(net, ev['acts'])

            def layer0_hidden(step):
                yield [dy_here[step], ev['acts'], ev['back_down0'], ev['d_up1'], Event(0.0, R_PRE)]
                pre_back_rows(net, net.at('x', step), u, down0, a0, ds)
                backs[0] -= 1
                if backs[0] == 0:
                    fire(net, ev['da0'])

            def layer0():
                for h in range(2):
                    yield [ev['da0'], ev['got_u0'], Event(0.0, R_GUP)]
                    grad_tiles(net, g.at[:, :, columns(h)], ds, stage, d_up0.at[columns(h)])
                fire(net, ev['d_up0'])
                for h in range(2):
                    yield [ev['got_dy'], ev['acts'], Event(0.0, R_GDOWN)]
                    grad_tiles(net, s0, u.at[:, :, columns(h)], stage, d_down0.at[:, columns(h)])
                fire(net, ev['d_down0'])
                yield [ev['y_reduced'], ev['back_up0'], ev['back_up0_rest'], Event(0.0, R_DX)]
                net.drain(ev['y_reduced'].copies + ev['got_down1'].copies)
                x0 = down1.at[pl.ds(0, x_halves.shape[0])]
                yield [net.grant(9, 'xp'), net.load(x_halves, x0)]
                net.spawn(reduce_x(net, part, du_made, rx_scratch, ev['du_reduced'], rs_pool.again()))
                for k, step in enumerate(STEPS):
                    input_back_rows(net, net.at('x', step), ds, up0, part.at[k])
                    fire(net, du_made[k])
                    yield [Event(net.now, R_DX)]
                yield [ev['du_reduced'], ev['x_saved']]
                for q in range(x_halves.shape[0]):
                    rows_q = pl.ds(q * dr, dr)
                    dy_q = u.at[net.data, rows_q]
                    norm_back_rows(x0.at[q], lambda at, dy_q=dy_q: dy_q[at, :], part.at[3, net.core, rows_q], x.at[rows_q])
                yield [net.load(x, dx_out)]

            def up_place(ref, k):
                return lambda block, rows: ref.at[pl.ds(pl.multiple_of(block * (2 * half_up) + k * half_up + rows.start, rows.size), rows.size)]

            def down_place(ref, k):
                return lambda block, rows: ref.at[pl.ds(pl.multiple_of(block * dr + rows.start, rows.size), rows.size), columns(k)]

            def gate(event, items, pool):
                yield items
                pool.again()
                fire(net, event)

            def sum_job(job, place, ref, ready, name, credits=()):
                passed = [Event(), Event()]
                for k in range(2):
                    start = Event()
                    n = job % 2
                    net.spawn(gate(start, ready[k] + ([credits[k]] if credits else []), job_pools[n][k]))
                    sums = Sums(net, AXES[job][k], job_scratch[n][k], stages[k])
                    net.spawn(sums.run(place(ref, k), start, ev['sum_%s%d' % (name, k)], frees[k], passed[k], job_pools[n][k], WINDOWS[2 * job + k], LEAD[min(job, 2)]))
                return passed

            def out_down(layer, dw_down, credit):
                def one(k):
                    done = ev['sum_down%d%d' % (layer, k)]
                    yield [done]
                    yield [net.load(done.total, dw_down.at[:, columns(k)])]
                    if credit is not None:
                        net.drain(done.copies)
                        yield [net.grant(credit + k, 'yz')]
                        fire(net, freed[credit + k])

                for k in range(2):
                    net.spawn(one(k))

            def out_up(n, layer, dw_up, credit):
                totals = [ev['sum_up%d%d' % (layer, k)] for k in range(2)]
                yield totals
                net.drain(totals[0].copies + totals[1].copies)
                spare = job_scratch[n][0][0].at[0]
                for k, done in enumerate(totals):
                    for q in range(2):
                        copy_rows(net, done.total.at[pl.ds(q * spare.shape[1], spare.shape[1])], spare.at[2 * k + q])
                done = ev['out_up%d' % layer]
                net.spawn(exchange_back(net, spare, dw_up, done))
                if credit is not None:
                    yield [done]
                    for k in range(2):
                        yield [net.grant(credit + k, 'yz')]
                        fire(net, freed[credit + k])

            passed = sum_job(0, down_place, d_down1, [[ev['d_down1_0'], ev['weights_in']], [ev['d_down1'], ev['weights_in']]], 'down1')
            passed = sum_job(1, up_place, d_up1, [[ev['d_up1']] + passed] * 2, 'up1')
            passed = sum_job(2, up_place, d_up0, [[ev['d_up0']] + passed] * 2, 'up0', [freed[10], freed[11]])
            sum_job(3, down_place, d_down0, [[ev['d_down0']] + passed] * 2, 'down0', [freed[12], freed[13]])
            out_down(1, dw_down1, 10)
            net.spawn(out_up(1, 1, dw_up1, 12))
            net.spawn(out_up(0, 0, dw_up0, None))
            out_down(0, dw_down0, None)
            for k in (3, 2, 1, 0):
                net.spawn(layer1(k, STEPS[k]))
            for step in (0, -1, 1, 2):
                net.spawn(layer0_hidden(step))
            for flow in (up_first(), second(), hidden_flow(), down_flow(), next_layer(), back_flow(), again(), weights(), grads1(), act(), layer1_out(),
                         bring_back(), bring_acts(), layer0()):
                net.spawn(flow)
            net.run()

        def finish(*refs):
            sources, targets, held, ups, sems = refs[:6], refs[6:10], refs[10:16], refs[16:18], refs[18]
            x_out, dx_out, up_out, down_out = targets
            loads = [pltpu.make_async_copy(src, dst, sems.at[k]) for k, (src, dst) in enumerate(zip(sources, held))]
            stores = [(ups[1], up_out.at[1]), (ups[0], up_out.at[0]), (held[2], down_out.at[1]), (held[3], down_out.at[0]), (held[4], x_out), (held[5], dx_out)]
            stores = [pltpu.make_async_copy(src, dst, sems.at[6 + k]) for k, (src, dst) in enumerate(stores)]
            for load in loads:
                load.start()
            for k in (2, 3, 4, 5):
                loads[k].wait()
                stores[k].start()
            for k in (0, 1):
                loads[k].wait()
                join_columns(held[k], ups[1 - k])
                stores[k].start()
            for store in stores:
                store.wait()

        d_up_own, d_down_own = shape((nd, ur, hidden), F32), shape((dr, width), F32)

        d_up_full, d_down_full = shape((width, hidden), F32), shape((hidden, width), F32)
        x_out, dx, _, _, _, _, _, _, _, _, *grads = call(
            step, [own, own, shape((num_layers, nd * ur, hidden), BF16), act_full, hid_full, hid_full] + [d_up_full, d_down_full] * 2
            + [d_up_own, d_down_own] * 2, 'h' * 14, 'hhhhh',
            [vmem(own)] + [vmem(act_full)] * 2 + [vmem(up_full)] * 2 + [vmem(down_full)] * 2 + [vmem(hid_full)] * 2
            + [pltpu.VMEM((2, hidden // 4, width // 2), F32)] + rx + sums, TR, TS, TL, 0,
            tokens, tokens.reshape(rows // dr, dr, width), grad_out, w_up, w_down)
        up1_own, down1_own, up0_own, down0_own = grads
        held = [d_up_own, d_up_own, d_down_own, d_down_own, own, own]
        return pl.pallas_call(
            finish, out_shape=[own, own, shape(w_up.shape, F32), shape(w_down.shape, F32)], name='finish',
            in_specs=[pl.BlockSpec(memory_space=pl.ANY)] * 6, out_specs=[pl.BlockSpec(memory_space=pl.ANY)] * 4,
            scratch_shapes=[vmem(like) for like in held] + [pltpu.VMEM(w_up.shape[1:], F32)] * 2 + [pltpu.SemaphoreType.DMA((12,))],
        )(up1_own, up0_own, down1_own, down0_own, x_out, dx)

    return jax.shard_map(device_fn, mesh=mesh, in_specs=(tok_spec, tok_spec, w_spec, w_spec), out_specs=(tok_spec, tok_spec, w_spec, w_spec), check_vma=False)
```

```python
import contextlib

import jax
import jax.numpy as jnp
from jax import lax
from jax.experimental import pallas as pl
from jax.experimental.pallas import tpu as pltpu
from jax.sharding import PartitionSpec as P

NORM_EPS = 1e-6
BOTH_AXES = ('local', 'data')
CONTRACT_ROWS = (((0,), (0,)), ((), ()))
CONTRACT_COLS = (((1,), (1,)), ((), ()))
MESH = pl.DeviceIdType.MESH
RING = 4
F32, BF16 = jnp.float32, jnp.bfloat16

LINK_RATE = 46.0e3
PAIR_RATE = 600e3
LOCAL_RATE = 3000e3
HOP = 2.4
PAIR_HOP = 1.0
ENTRY = 4.0
GELU_C = 0.7978845608028654


def scope(label):
    return jax.named_scope(label) if SCOPES else contextlib.nullcontext()


class Event:
    def __init__(self, time=None, rank=0, name=''):
        self.time, self.rank, self.name = time, rank, name


class Copy:
    def __init__(self, desc, time, remote):
        self.desc, self.time, self.remote, self.rank, self.waited = desc, time, remote, 0, False

    def wait(self):
        if self.remote:
            self.desc.wait_recv()
        else:
            self.desc.wait()


class Credit:
    def __init__(self, semaphore, count, time):
        self.semaphore, self.count, self.time, self.rank, self.waited = semaphore, count, time, 0, False

    def wait(self):
        pl.semaphore_wait(self.semaphore, self.count)


class Pool:
    def __init__(self):
        self.slots, self.next = [], 0

    def again(self):
        self.next = 0
        return self


class Net:
    def __init__(self, send_sems, recv_sems, local_sems, credit_sems):
        self.send_sems, self.recv_sems, self.local_sems, self.credit_sems = send_sems, recv_sems, local_sems, credit_sems
        self.n_remote = self.n_local = 0
        self.free_sends = list(range(send_sems.shape[0]))
        self.free_locals = []
        self.now = 0.0
        self.free = {}
        self.sent = []
        self.flows = []
        self.labels = {}
        here, there = lax.axis_index('local'), lax.axis_index('data')
        pos = {'z': here // RING, 'y': lax.rem(here, RING), 'x': there // 2}
        self.data, self.core = there, lax.rem(there, 2)
        self.ring = {axis: [at] + [lax.rem(at + step, RING) for step in range(1, RING)] for axis, at in pos.items()}
        self.hops = [there] + [lax.rem(there + step, 2 * RING) for step in range(1, 2 * RING)]
        self.blocks = [at * 2 + self.core for at in self.ring['x']]
        self.places = [[z * RING + y for y in self.ring['y']] for z in self.ring['z']]
        self.partner = pos['x'] * 2 + (1 - self.core)
        self.other = 1 - self.core

    def at(self, axis, step):
        return self.ring[axis][step % RING]

    def block(self, step):
        return self.blocks[step % RING]

    def device(self, axis, step):
        if axis == 'p':
            return {'data': self.partner}
        if axis == 'd':
            return {'data': self.hops[step % (2 * RING)]}
        if axis == 'x':
            return {'data': self.block(step)}
        if axis == 'y':
            return {'local': self.places[0][step % RING]}
        return {'local': self.places[step % RING][0]}

    def peers(self, axes):
        return [(axis, step) for axis in axes for step in ((1, -1) if axis in 'xyz' else (1,) if axis == 'p' else range(1, 2 * RING))]

    def signal(self, semaphore, axes):
        for axis, step in self.peers(axes):
            pl.semaphore_signal(semaphore, inc=1, device_id=self.device(axis, step), device_id_type=MESH)

    def arrive(self, axes):
        self.entry, self.entered = pltpu.get_barrier_semaphore(), len(self.peers(axes))
        self.signal(self.entry, axes)

    def enter(self):
        pl.semaphore_wait(self.entry, self.entered)
        self.now = max(self.now, ENTRY)

    def take(self, copies):
        for copy in copies:
            copy.wait()
            copy.waited = True
            self.free_locals.append(copy.slot)
            self.now = max(self.now, copy.time)

    def grant(self, k, axes):
        self.signal(self.credit_sems.at[k], axes)
        return Credit(self.credit_sems.at[k], len(self.peers(axes)), self.now + HOP)

    def drain(self, copies):
        for copy in copies:
            if copy in self.sent:
                copy.desc.wait_send()
                self.sent.remove(copy)
                self.free_sends.append(copy.slot)

    def idle(self, gap):
        over = [copy for copy in self.sent if copy.time + 1.5 < self.now]
        self.drain(over[:int(gap / 0.05)])

    def send(self, src, dst, axis, step=1, pool=None):
        if pool is not None and pool.next < len(pool.slots):
            k = pool.slots[pool.next]
        else:
            k = self.n_remote
            self.n_remote += 1
            if pool is not None:
                pool.slots.append(k)
        if pool is not None:
            pool.next += 1
        if not self.free_sends:
            if PRINT:
                print('EXHAUSTED', round(self.now, 1))
            self.drain([min(self.sent, key=lambda copy: copy.time)])
        send_slot = self.free_sends.pop()
        desc = pltpu.make_async_remote_copy(
            src_ref=src, dst_ref=dst, send_sem=self.send_sems.at[send_slot], recv_sem=self.recv_sems.at[k],
            device_id=self.device(axis, step), device_id_type=MESH)
        desc.start()
        size = 1
        for n in dst.shape:
            size *= n
        size *= dst.dtype.itemsize
        rate = PAIR_RATE if axis == 'p' else LINK_RATE
        extra = 2.0 if axis == 'd' else 0.0
        if axis == 'd':
            axis, step, size = ('p', 1, size) if step == 1 else ('x', 1 if step < RING + 2 else -1, size)
        key = (axis, step)
        done = max(self.free.get(key, 0.0), self.now) + size / rate
        self.free[key] = done
        copy = Copy(desc, done + extra + (PAIR_HOP if axis == 'p' else HOP), True)
        copy.slot = send_slot
        self.sent.append(copy)
        return copy

    def load(self, src, dst):
        if not self.free_locals:
            self.free_locals.append(self.n_local)
            self.n_local += 1
        k = self.free_locals.pop()
        desc = pltpu.make_async_copy(src, dst, self.local_sems.at[k])
        desc.start()
        size = 1
        for n in dst.shape:
            size *= n
        done = max(self.free.get('hbm', 0.0), self.now) + size * dst.dtype.itemsize / LOCAL_RATE
        self.free['hbm'] = done
        copy = Copy(desc, done + 0.9, False)
        copy.slot = k
        return copy

    def save(self, src, dst):
        copy = self.load(src, dst)
        copy.time += 4.0
        return copy

    def spend(self, microseconds):
        self.now += microseconds

    def spawn(self, flow):
        self.step(flow)

    def step(self, flow):
        try:
            if flow not in self.labels:
                self.labels[flow] = [flow.__name__, len(self.labels), 0]
            self.labels[flow][2] += 1
            self.flows.append((flow, next(flow)))
        except StopIteration:
            pass

    def run(self):
        while self.flows:
            best = None
            for k, (_, items) in enumerate(self.flows):
                if any(item.time is None for item in items):
                    continue
                time = max([item.time for item in items] + [0.0])
                late = max([item.rank for item in items] + [0])
                rank = (max(time, self.now) + (SLACK if late else 0.0), late, time)
                if best is None or rank < best[0]:
                    best = (rank, k, time)
            _, k, time = best
            flow, items = self.flows.pop(k)
            self.idle(time - self.now)
            label = '%s_%d_%d' % tuple(self.labels[flow])
            with scope('w_' + label):
                for item in items:
                    if not isinstance(item, Event) and not item.waited:
                        item.wait()
                        item.waited = True
                        if isinstance(item, Copy) and not item.remote:
                            self.free_locals.append(item.slot)
            before = self.now
            self.now = max(self.now, time)
            if PRINT:
                print('STEP', label, round(before, 2), round(self.now, 2))
            with scope('s_' + label):
                self.step(flow)

    def finish(self):
        for copy in self.sent:
            copy.desc.wait_send()


def rows_loop(rows, chunk, body):
    chunk = min(chunk, rows)

    def step(k, carry):
        body(pl.ds(pl.multiple_of(k * chunk, chunk), chunk))
        return carry

    lax.fori_loop(0, rows // chunk, step, 0)


def add_into(net, dst, *others):
    rows, cols = dst.shape

    def body(at):
        total = dst[at, :]
        for other in others:
            total = total + other[at, :]
        dst[at, :] = total

    rows_loop(rows, 16, body)
    net.spend(rows * cols * 4 * (1 + len(others)) / 4e6)


def fire(net, event):
    event.time = net.now
    if PRINT and event.name:
        print('   %7.1f %s' % (net.now, event.name))


def exchange(net, source, dst, done, pool):
    rows = dst.shape[0] // (2 * RING)

    def mine():
        return dst.at[pl.ds(pl.multiple_of(net.data * rows, rows), rows)]

    own = net.load(source(net.data), mine())
    copies = [net.send(source(net.hops[k]), mine(), 'd', k, pool) for k in (4, 5, 2, 3, 6, 7, 1)]
    yield [own] + copies
    net.drain(copies)
    fire(net, done)


def exchange_back(net, src, dst, done, pool):
    rows = dst.shape[1]
    per = src.shape[1] // rows

    def block(k):
        return src.at[lax.div(k, per), pl.ds(pl.multiple_of(lax.rem(k, per) * rows, rows), rows)]

    own = net.load(block(net.data), dst.at[net.data])
    copies = [net.send(block(net.hops[k]), dst.at[net.data], 'd', k, pool) for k in (4, 5, 2, 3, 6, 7, 1)]
    yield [own] + copies
    net.drain(copies)
    fire(net, done)


def copy_rows(net, src, dst):
    def body(at):
        dst[at, :] = src[at, :]

    rows_loop(src.shape[0], 16, body)
    net.spend(0.2)


def gather_x(net, full, done, issued=None, chips=None, pool=None):
    half = full.shape[1] // 2
    lo, hi = pl.ds(0, half), pl.ds(half, half)
    chips = chips or {step: Event() for step in STEPS}
    left = [2]
    done.copies = []

    def send(*args):
        done.copies.append(net.send(*args, pool=pool))
        return done.copies[-1]

    def block(step):
        return full.at[net.block(step)]

    def part(step, rows):
        return full.at[net.block(step), rows]

    relays = []

    def side(step, first, second, mine):
        yield [mine[0]]
        relays.append(send(part(step, first), part(step, first), 'x', -step))
        left[0] -= 1
        if left[0] == 0:
            net.spawn(far())
            if issued is not None:
                fire(net, issued)
        yield [mine[1]]
        pair = send(block(step), block(step), 'p')
        yield [pair]
        fire(net, chips[step])

    def far():
        yield relays
        pair = send(block(2), block(2), 'p')
        yield [pair]
        fire(net, chips[2])

    forth = [send(part(0, rows), part(0, rows), 'x', 1) for rows in (lo, hi)]
    back = [send(part(0, rows), part(0, rows), 'x', -1) for rows in (hi, lo)]
    pair = send(block(0), block(0), 'p')
    net.spawn(side(-1, lo, hi, forth))
    net.spawn(side(1, hi, lo, back))
    yield [pair]
    fire(net, chips[0])
    yield [chips[step] for step in STEPS]
    fire(net, done)


def gather_yz(net, own, full, first, done, issued=None, offset=0, near=False, split=True, pool=None):
    second = 'y' if first == 'z' else 'z'
    done.copies = []

    def emit(*args):
        done.copies.append(net.send(*args, pool=pool))
        return done.copies[-1]

    size = own.shape[0]
    half = size // 2
    lo, hi, both = pl.ds(offset, half), pl.ds(offset + half, half), pl.ds(offset, size)
    forward, backward = ((lo, hi), (hi, lo)) if split and not near else ((both,), (both,))

    def part(one, two, rows):
        return full.at[yz_index(net, first, one, two), rows]

    left = [3 if near else RING, 3 if near else RING]

    def arrived(which):
        left[which] -= 1
        if left[which] == 0 and (done, issued)[which] is not None:
            fire(net, (done, issued)[which])

    def send(one, rows, axis, step):
        src = own.at[pl.ds(rows.start - offset, rows.size)] if one == 0 else part(one, 0, rows)
        return emit(src, part(one, 0, rows), axis, step)

    def column(one):
        forth = [send(one, rows, second, 1) for rows in forward]
        back = [send(one, rows, second, -1) for rows in backward]

        def finish():
            if near:
                arrived(1)
                yield forth + back
            else:
                yield [forth[0]]
                relays = [emit(part(one, -1, lo), part(one, -1, lo), second, 1)]
                yield [back[0]]
                relays.append(emit(part(one, 1, hi), part(one, 1, hi), second, -1))
                arrived(1)
                yield forth[1:] + back[1:] + relays
            arrived(0)

        net.spawn(finish())

    relays = []

    def side(step, first_half, mine):
        yield [mine[0]]
        if not near:
            relays.append(emit(part(step, 0, first_half), part(step, 0, first_half), first, -step))
            if len(relays) == 2:
                net.spawn(far())
        yield mine[1:]
        column(step)

    def far():
        yield relays
        column(2)

    mine = [net.load(own, part(0, 0, both))]
    forth = [send(0, rows, first, 1) for rows in forward]
    back = [send(0, rows, first, -1) for rows in backward]
    column(0)
    net.spawn(side(-1, lo, forth))
    net.spawn(side(1, hi, back))
    left[0] += 1
    yield mine
    arrived(0)


def yz_index(net, first, one, two):
    return net.places[one % RING][two % RING] if first == 'z' else net.places[two % RING][one % RING]


FAR = [(2, 0), (2, 1), (2, -1), (2, 2), (0, 2), (1, 2), (-1, 2)]


STEPS = (2, 1, -1, 0)


def reduce_x(net, part, made, scratch, done, pool=None):
    other, relay_f, relay_b, last_f, last_b = scratch
    half = part.shape[2] // 2
    lo, hi = pl.ds(0, half), pl.ds(half, half)

    def acc(k, rows=None):
        return part.at[k, net.core] if rows is None else part.at[k, net.core, rows]

    pairs = [None] * RING
    ready = [Event() for _ in STEPS]

    def pair(k):
        yield [made[k]]
        pairs[k] = net.send(part.at[k, net.other], other.at[k], 'p', pool=pool)
        yield [pairs[k]]
        add_into(net, acc(k), other.at[k])
        fire(net, ready[k])

    for k in range(RING):
        net.spawn(pair(k))
    sent = {}
    started, relayed = Event(), Event()

    def part_flow(k):
        yield [ready[k]] + ([relayed] if k else [])
        if k == 0:
            sent['first_f'] = net.send(acc(0, lo), relay_f, 'x', 1, pool=pool)
            sent['first_b'] = net.send(acc(0, hi), relay_b, 'x', -1, pool=pool)
            fire(net, relayed)
        elif k == 1:
            sent['direct_f'] = net.send(acc(1, hi), last_f.at[hi], 'x', 1, pool=pool)
        else:
            sent['direct_b'] = net.send(acc(2, lo), last_b.at[lo], 'x', -1, pool=pool)
        if len(sent) == 4:
            fire(net, started)

    for k in range(3):
        net.spawn(part_flow(k))
    yield [started]
    yield [sent['first_f']]
    add_into(net, acc(1, lo), relay_f)
    summed_f = net.send(acc(1, lo), last_f.at[lo], 'x', 1, pool=pool)
    yield [sent['first_b']]
    add_into(net, acc(2, hi), relay_b)
    summed_b = net.send(acc(2, hi), last_b.at[hi], 'x', -1, pool=pool)
    yield [ready[3], sent['direct_f'], sent['direct_b'], summed_f, summed_b]
    add_into(net, acc(3), last_f, last_b)
    done.copies = pairs + list(sent.values()) + [summed_f, summed_b]
    fire(net, done)


def reduce_x_scratch(rows, cols):
    return [pltpu.VMEM((RING, rows, cols), F32), pltpu.VMEM((rows // 2, cols), F32), pltpu.VMEM((rows // 2, cols), F32),
            pltpu.VMEM((rows, cols), F32), pltpu.VMEM((rows, cols), F32)]


def load_parts(net, src, part, made):
    for k, step in enumerate(STEPS):
        def bring(k=k, step=step):
            yield [net.load(src.at[pl.ds(net.at('x', step) * 2, 2)], part.at[k])]
            fire(net, made[k])

        net.spawn(bring())


class Sums:
    def __init__(self, net, first, scratch, stage):
        self.net, self.first, self.scratch, self.stage = net, first, scratch, stage
        self.second = 'y' if first == 'z' else 'z'

    def run(self, place, start, done, free, passed_all, pool, window, lead):
        net, first, second = self.net, self.first, self.second
        relay1, last1, relay2, last2 = self.scratch
        ahead, behind, mine = self.stage
        half = mine.shape[0] // 2
        lo, hi, all_rows = pl.ds(0, half), pl.ds(half, half), pl.ds(0, 2 * half)
        done.copies = []

        def send(*args):
            done.copies.append(net.send(*args, pool=pool))
            return done.copies[-1]

        def term(one, two, rows=all_rows):
            return place(yz_index(net, first, one, two), rows)

        def bring(gate, src, dst, got):
            yield [gate, start]
            yield [net.load(src, dst)]
            fire(net, got)

        chain = [[gate] + [Event() for _ in range(RING)] for gate in free]
        free[:] = [events[RING] for events in chain]
        got = [[Event() for _ in range(RING)] for _ in range(3)]
        ends = [Event() for _ in STEPS]
        passed = [Event() for _ in range(RING)]
        passed[lead] = passed_all

        def ring(k):
            two = STEPS[k]
            if k >= window:
                yield [passed[k - window]]
            net.spawn(bring(chain[0][k], term(1, two, lo), ahead, got[0][k]))
            net.spawn(bring(chain[1][k], term(-1, two, hi), behind, got[1][k]))
            net.spawn(bring(chain[2][k], term(0, two), mine, got[2][k]))
            first_f = send(term(2, two, lo), relay1.at[0, k], first, 1)
            first_b = send(term(2, two, hi), relay1.at[1, k], first, -1)
            direct_f = send(term(1, two, hi), last1.at[0, k, hi], first, 1)
            direct_b = send(term(-1, two, lo), last1.at[1, k, lo], first, -1)
            yield [first_f, got[0][k]]
            add_into(net, relay1.at[0, k], ahead)
            fire(net, chain[0][k + 1])
            summed_f = send(relay1.at[0, k], last1.at[0, k, lo], first, 1)
            yield [first_b, got[1][k]]
            add_into(net, relay1.at[1, k], behind)
            fire(net, chain[1][k + 1])
            summed_b = send(relay1.at[1, k], last1.at[1, k, hi], first, -1)
            fire(net, passed[k])
            yield [direct_f, direct_b, summed_f, summed_b, got[2][k]]
            add_into(net, last1.at[0, k], last1.at[1, k], mine)
            fire(net, chain[2][k + 1])
            fire(net, ends[k])

        def sums(k, rows=all_rows):
            return last1.at[0, k, rows]

        yield [start]
        for k in range(RING):
            net.spawn(ring(k))
        yield [ends[0]]
        first_f = send(sums(0, lo), relay2.at[0], second, 1)
        first_b = send(sums(0, hi), relay2.at[1], second, -1)
        yield [ends[1]]
        direct_f = send(sums(1, hi), last2.at[0, hi], second, 1)
        yield [ends[2]]
        direct_b = send(sums(2, lo), last2.at[1, lo], second, -1)
        yield [first_f]
        add_into(net, sums(1, lo), relay2.at[0])
        summed_f = send(sums(1, lo), last2.at[0, lo], second, 1)
        yield [first_b]
        add_into(net, sums(2, hi), relay2.at[1])
        summed_b = send(sums(2, hi), last2.at[1, hi], second, -1)
        yield [ends[3], direct_f, direct_b, summed_f, summed_b]
        add_into(net, sums(3), last2.at[0], last2.at[1])
        done.total = sums(3)
        fire(net, done)


def sums_scratch(rows, cols):
    return [pltpu.VMEM((2, RING, rows // 2, cols), F32), pltpu.VMEM((2, RING, rows, cols), F32),
            pltpu.VMEM((2, rows // 2, cols), F32), pltpu.VMEM((2, rows, cols), F32)]


def sums_stage(rows, cols):
    return [pltpu.VMEM((rows // 2, cols), F32), pltpu.VMEM((rows // 2, cols), F32), pltpu.VMEM((rows, cols), F32)]


def norm_rows(x_ref, u_ref):
    def body(at):
        x = x_ref[at, :].astype(F32)
        u_ref[at, :] = (x * lax.rsqrt(jnp.mean(x * x, axis=-1, keepdims=True) + NORM_EPS)).astype(BF16)

    rows_loop(x_ref.shape[0], 16, body)


def norm_back_rows(x_ref, dy_of, du_ref, dx_ref):
    def body(at):
        x = x_ref[at, :].astype(F32)
        du = du_ref[at, :]
        r = lax.rsqrt(jnp.mean(x * x, axis=-1, keepdims=True) + NORM_EPS)
        xr = x * r
        dx_ref[at, :] = (dy_of(at).astype(F32) + r * (du - xr * jnp.mean(xr * du, axis=-1, keepdims=True))).astype(BF16)

    rows_loop(x_ref.shape[0], 16, body)


def add_rows(x_ref, y_ref, out_ref):
    def body(at):
        out_ref[at, :] = (x_ref[at, :].astype(F32) + y_ref[at, :]).astype(BF16)

    rows_loop(x_ref.shape[0], 16, body)


def swap_halves(even, odd):
    low = lax.broadcasted_iota(jnp.int32, even.shape, len(even.shape) - 1) < even.shape[-1] // 2
    shift = even.shape[-1] // 2
    axis = len(even.shape) - 1
    return jnp.where(low, even, pltpu.roll(odd, shift, axis)), jnp.where(low, pltpu.roll(even, shift, axis), odd)


def split_columns(w_ref, cols_ref, layers):
    pieces, _, wide = w_ref.shape
    rows = layers
    tile = pieces * wide // (4 * RING * RING)
    for x in range(RING):
        for p in range(wide // tile):
            pair = []
            for i in (2 * p, 2 * p + 1):
                at = (i * RING + x) * tile
                pair.append(w_ref[at // wide, pl.ds(0, rows), pl.ds(at % wide, tile)].astype(F32))
            for c, value in enumerate(swap_halves(*pair)):
                cols_ref[2 * x + c, pl.ds(0, rows), pl.ds(p * tile, tile)] = value.astype(cols_ref.dtype)


def join_columns(cols_ref, w_ref):
    tile = w_ref.shape[1] // (4 * RING * RING)
    for x in range(RING):
        for p in range(cols_ref.shape[2] // tile):
            pair = [cols_ref[2 * x + c, :, pl.ds(p * tile, tile)] for c in range(2)]
            for i, value in zip((2 * p, 2 * p + 1), swap_halves(*pair)):
                w_ref[:, pl.ds((i * RING + x) * tile, tile)] = value


def call(body, out_shape, out_spaces, in_spaces, scratch, remote, sends, local, collective_id, *args):
    spaces = {'v': pl.BlockSpec(memory_space=pltpu.VMEM), 'h': pl.BlockSpec(memory_space=pl.ANY)}

    def kernel(*refs):
        net = Net(*refs[-5:-1])
        net.tile_sems = refs[-1]
        body(net, *refs[:-5])
        net.finish()
        assert net.n_remote <= remote and net.n_local <= local, (body.__name__, net.n_remote, net.n_local)
        if PRINT:
            print(body.__name__, net.n_remote, net.n_local, round(net.now, 1))

    return pl.pallas_call(
        kernel, out_shape=out_shape, in_specs=[spaces[s] for s in in_spaces], out_specs=[spaces[s] for s in out_spaces],
        scratch_shapes=list(scratch) + [pltpu.SemaphoreType.DMA((sends,)), pltpu.SemaphoreType.DMA((remote,)), pltpu.SemaphoreType.DMA((local,)),
                                               pltpu.SemaphoreType.REGULAR((14,)), pltpu.SemaphoreType.DMA((2,))],
        compiler_params=pltpu.CompilerParams(collective_id=collective_id, has_side_effects=True, vmem_limit_bytes=67000000),
        cost_estimate=pl.CostEstimate(flops=10**8, bytes_accessed=10**7, transcendentals=0),
        name=body.__name__)(*args)


PRINT = False
SCOPES = False


WIDE = 512
EARLY = 3
SLACK = 0.1
R_HIDDEN, R_DOWN, R_BACK, R_TURN, R_DDOWN, R_DDOWN2, R_DUP, R_OUT, R_PRE, R_GUP, R_GDOWN, R_DX = 2, 1, 3, 1, 2, 2, 4, 2, 2, 3, 3, 2
R_DU, HOLD = (3, 3.1, 3.2, 3.3), (0, 1, 2)
WINDOWS = (2, 2, 2, 2, 2, 2, 2, 2)
AXES = ('yz', 'yz', 'yz', 'yz')
TOP = 6
NEAR = 'z'
LEAD = (3, 3, 3)
TR, TS, TL = 264, 64, 9


def wide_loop(total, body):
    wide = min(WIDE, total)

    def step(k, carry):
        body(k, wide, pl.ds(pl.multiple_of(k * wide, wide), wide))
        return carry

    lax.fori_loop(0, total // wide, step, 0)


def flat(value):
    return value.reshape(value.shape[0] * value.shape[1], value.shape[2])


def dot_rows(a, b):
    return jnp.dot(flat(a), flat(b), preferred_element_type=F32)


def dot_cols(a, b):
    return lax.dot_general(flat(a), flat(b), CONTRACT_COLS, preferred_element_type=F32)


def gelu(a):
    return 0.5 * a * (1.0 + jnp.tanh(GELU_C * (a + 0.044715 * a * a * a)))


def hidden_rows(net, chip, u, up, a, s):
    at = pl.ds(chip * 2, 2)

    def body(_, wide, cols):
        pre = dot_rows(u[at], up[:, :, cols]).astype(BF16)
        a[at, :, cols] = pre.reshape(2, -1, wide)
        s[at, :, cols] = gelu(pre.astype(F32)).astype(BF16).reshape(2, -1, wide)

    wide_loop(up.shape[2], body)
    net.spend(1.7)


def down_rows(net, chip, s, down, part):
    at = pl.ds(chip * 2, 2)

    def body(_, wide, cols):
        part[:, :, cols] = dot_rows(s[at], down[:, :, cols]).reshape(2, -1, wide)

    wide_loop(down.shape[2], body)
    net.spend(1.76)


def hidden_back_rows(net, chip, dy, down, ds):
    at = pl.ds(chip * 2, 2)
    rows = down.shape[1]

    def body(k, wide, cols):
        blocks = pl.ds(k * (wide // rows), wide // rows)
        ds[at, :, cols] = dot_cols(dy[at], down[blocks]).astype(BF16).reshape(2, -1, wide)

    wide_loop(down.shape[0] * rows, body)
    net.spend(1.5)


def gelu_both(a):
    t = jnp.tanh(GELU_C * (a + 0.044715 * a * a * a))
    return 0.5 * a * (1.0 + t), 0.5 * (1.0 + t) + 0.5 * a * (1.0 - t * t) * (GELU_C * (1.0 + 3 * 0.044715 * a * a))


def hidden_turn_rows(net, chip, u, up, s, ds):
    at = pl.ds(chip * 2, 2)

    def body(_, wide, cols):
        pre = dot_rows(u[at], up[:, :, cols]).astype(BF16).astype(F32)
        value, slope = gelu_both(pre)
        s[at, :, cols] = value.astype(BF16).reshape(2, -1, wide)
        ds[at, :, cols] = (ds[at, :, cols].astype(F32) * slope.reshape(2, -1, wide)).astype(BF16)

    wide_loop(up.shape[2], body)
    net.spend(2.1)


def pre_back_rows(net, chip, dy, down, a, da):
    at = pl.ds(chip * 2, 2)
    rows = down.shape[1]

    def body(k, wide, cols):
        blocks = pl.ds(k * (wide // rows), wide // rows)
        ds = dot_cols(dy[at], down[blocks]).astype(BF16).astype(F32).reshape(2, -1, wide)
        da[at, :, cols] = (ds * gelu_both(a[at, :, cols].astype(F32))[1]).astype(BF16)

    wide_loop(down.shape[0] * rows, body)
    net.spend(1.95)


def input_back_rows(net, chip, da, up, part):
    at = pl.ds(chip * 2, 2)
    rows = up.shape[1]

    def body(k, wide, cols):
        blocks = pl.ds(k * (wide // rows), wide // rows)
        part[:, :, cols] = dot_cols(da[at], up[blocks]).reshape(2, -1, wide)

    wide_loop(up.shape[0] * rows, body)
    net.spend(1.9)


def stored_tiles(net, count, compute, stage, out):
    def store(t):
        return pltpu.make_async_copy(stage.at[lax.rem(t, 2)], out(t), net.tile_sems.at[lax.rem(t, 2)])

    def step(t, carry):
        @pl.when(t >= 2)
        def _():
            store(t - 2).wait()

        compute(t, stage.at[lax.rem(t, 2)])
        store(t).start()
        return carry

    lax.fori_loop(0, count, step, 0)
    for t in range(max(count - 2, 0), count):
        store(jnp.int32(t)).wait()


def dot_tokens(a, b):
    return lax.dot_general(flat(a), flat(b), CONTRACT_ROWS, preferred_element_type=F32)


def grad_tiles(net, lhs, rhs, stage, out):
    wide = stage.shape[1]

    def compute(t, slot):
        slot[...] = dot_tokens(lhs[:, :, pl.ds(pl.multiple_of(t * wide, wide), wide)], rhs[...])

    stored_tiles(net, lhs.shape[2] // wide, compute, stage, lambda t: out.at[pl.ds(pl.multiple_of(t * wide, wide), wide)])
    net.spend(4.35 * lhs.shape[2] / 1024)


def solution(mesh):
    nl, nd = mesh.shape['local'], mesh.shape['data']
    tok_spec = P(BOTH_AXES, None)
    w_spec = P(None, BOTH_AXES, None)

    def device_fn(tokens, grad_out, w_up, w_down):
        num_layers, ur, ffn = w_up.shape
        dr = w_down.shape[1]
        rows, width = tokens.shape
        hidden = nl * dr
        shape = jax.ShapeDtypeStruct
        up_full = shape((nl, nd * ur, hidden), BF16)
        down_full = shape((nl, dr, width), BF16)
        act_full = shape((nd, rows, width), BF16)
        hid_full = shape((nd, rows, hidden), BF16)
        own = shape((rows, width), BF16)
        part_vmem = pltpu.VMEM((RING, 2, rows, width), F32)
        rx = [part_vmem] + reduce_x_scratch(rows, width)
        sums = sums_scratch(dr, hidden) * 4 + sums_stage(dr, hidden) * 2

        def vmem(like):
            return pltpu.VMEM(like.shape, like.dtype)

        def step(net, x_in, x_halves, g_in, w_up_in, w_down_in,
                 x_out, dx_out, block_out, u_out, a_out, s_out, d_up0, d_down0, d_up1, d_down1, dw_up1, dw_down1, dw_up0, dw_down0,
                 x, u, g, up0, up1, down0, down1, ds, s, stage, part, *scratch):
            net.arrive('dyz')
            rx_scratch = scratch[:5]
            names = ('blocks', 'blocks1', 'sent_u', 'got_u', 'got_g', 'sent_up0', 'sent_down0', 'sent_up1', 'sent_down1', 'got_up0', 'got_down0',
                     'got_up1', 'got_down1', 'saved', 'free0', 'reduced0', 'ds_made', 'got_u1', 'hidden', 'all_du', 'reduced1', 'sent_dy', 'got_dy',
                     'back_up0', 'back_up0_rest', 'back_down0', 'd_down1', 'd_up1', 'y_reduced', 'acts', 'd_down0', 'da0', 'd_up0', 'du_reduced',
                     'out_up1', 'out_up0', 'got_u0', 'y_made', 'x_saved', 'weights_in', 'd_down1_0')
            ev = {name: Event(name=name) for name in names}
            for kind in ('up', 'down'):
                for layer in range(2):
                    for k in range(2):
                        ev['sum_%s%d%d' % (kind, layer, k)] = Event(name='sum_%s%d%d' % (kind, layer, k))
            ev['got_up0'].rank = R_HIDDEN
            hidden_made, made0, made1, y_made, du_made = ([Event(name='%s%d' % (name, k)) for k in range(RING)]
                                                          for name in ('hidden_', 'made0_', 'made1_', 'y_made_', 'du_made_'))
            wide = width // 2
            half_up = nd * ur // 2
            act_pool, rs_pool = Pool(), Pool()
            job_pools = [[Pool(), Pool()], [Pool(), Pool()]]
            pools = {'up0': [Pool(), Pool()], 'down0': [Pool(), Pool()], 'up1': job_pools[0], 'down1': job_pools[1], 'blocks': [Pool(), Pool()]}
            stages = (scratch[21:24], scratch[24:27])
            job_scratch = [[scratch[5 + 8 * n + 4 * k:9 + 8 * n + 4 * k] for k in range(2)] for n in range(2)]
            frees = [[Event(0.0) for _ in range(3)] for _ in range(2)]
            freed = {k: Event() for k in range(10, 14)}

            def columns(h):
                return pl.ds(h * wide, wide)

            inputs = [net.load(x_in, x)]
            inputs += [net.load(w_up_in.at[:, pl.ds(k * hidden, hidden)], ds.at[k, pl.ds(0, num_layers * ur)]) for k in range(nd)]

            def gather(name, own, full, split):
                size = own.shape[0] // 2

                def join(kind, events):
                    yield events
                    if kind == 'got_':
                        ev[kind + name].copies = events[0].copies + events[1].copies
                    fire(net, ev[kind + name])

                got, sent = [Event(), Event()], [Event(), Event()]
                for k, first in enumerate('yz'):
                    net.spawn(gather_yz(net, own.at[pl.ds(k * size, size)], full, first, got[k], sent[k], k * size, split=split, pool=pools[name][k]))
                net.spawn(join('got_', got))
                net.spawn(join('sent_', sent))

            net.take(inputs)
            split_columns(ds, s, num_layers * ur)
            norm_rows(x, u.at[net.data])
            net.enter()
            gather('down0', w_down_in.at[0], down0, False)
            net.spawn(exchange(net, lambda k: s.at[k, pl.ds(0, ur)], block_out.at[0], ev['blocks'], pools['blocks'][0]))
            own_grads = net.load(g_in, g.at[net.data])

            def up_first():
                yield [ev['blocks']]
                gather('up0', block_out.at[0], up0, True)
                net.spawn(gather_x(net, u, ev['got_u'], ev['sent_u'], pool=act_pool))
                yield [ev['sent_u']]
                net.spawn(exchange(net, lambda k: s.at[k, pl.ds(ur, ur)], block_out.at[1], ev['blocks1'], pools['blocks'][1]))
                yield [own_grads]
                net.spawn(gather_x(net, g, ev['got_g']))

            def second():
                yield [ev['sent_up0'], ev['sent_down0'], ev['blocks1']]
                gather('down1', w_down_in.at[1], down1, False)
                yield [made0[EARLY]]
                gather('up1', block_out.at[1], up1, True)

            def hidden_flow():
                yield [ev['got_u'], ev['got_up0'], ev['blocks1']]
                for k, step in enumerate(STEPS):
                    hidden_rows(net, net.at('x', step), u, up0, ds, s)
                    fire(net, hidden_made[k])
                    yield [Event(net.now, R_HIDDEN)]
                yield [net.load(ds, a_out), net.load(s, s_out), net.load(u, u_out)]
                fire(net, ev['saved'])

            def down_flow():
                for k, step in enumerate(STEPS):
                    yield [hidden_made[k], ev['got_down0'], Event(0.0, R_DOWN)]
                    down_rows(net, net.at('x', step), s, down0, part.at[k])
                    fire(net, made0[k])
                fire(net, ev['free0'])

            net.spawn(reduce_x(net, part, made0, rx_scratch, ev['reduced0'], rs_pool))
            here = {step: Event(name='u%d' % step) for step in STEPS}
            dy_here = {step: Event() for step in STEPS}

            def next_layer():
                yield [ev['saved'], ev['got_g']]
                net.drain(ev['got_u'].copies + ev['got_g'].copies)
                credit = net.grant(3, 'xp')
                yield [ev['reduced0'], credit]
                add_rows(x, part.at[3, net.core], x)
                norm_rows(x, u.at[net.data])
                net.spend(1.0)
                net.spawn(gather_x(net, u, ev['got_u1'], chips=here, pool=act_pool.again()))
                net.drain(ev['reduced0'].copies)
                yield [net.grant(4, 'xp')]
                net.spawn(reduce_x(net, part, made1, rx_scratch, ev['reduced1'], rs_pool.again()))

            def back_flow():
                for k, step in enumerate(STEPS):
                    yield [ev['got_g'], ev['got_down1'], ev['saved'], Event(0.0, R_BACK)]
                    hidden_back_rows(net, net.at('x', step), g, down1, ds)
                fire(net, ev['ds_made'])

            def again():
                top = nd * ur * TOP // 8
                yield [ev['free0'], ev['ds_made']]
                net.drain(ev['got_up0'].copies + ev['got_down0'].copies)
                credit = net.grant(6, 'yz')
                yield [credit]
                net.spawn(gather_yz(net, w_down_in.at[0], down0, NEAR, ev['back_down0'], near=True, pool=pools['down0'][1].again()))
                net.spawn(gather_yz(net, block_out.at[0, pl.ds(0, top)], up0, 'y', ev['back_up0'], pool=pools['up0'][0].again()))
                net.spawn(gather_yz(net, block_out.at[0, pl.ds(top, nd * ur - top)], up0, 'z', ev['back_up0_rest'], offset=top, pool=pools['up0'][1].again()))

            def weights():
                yield [ev['got_up1'], ev['got_down1']]
                yield [net.grant(7, 'yz')]
                fire(net, ev['weights_in'])

            left = [RING, RING]

            turned = [Event() for _ in STEPS]

            def layer1(k, step):
                yield [here[step], ev['ds_made'], ev['got_up1'], Event(0.0, R_TURN)]
                hidden_turn_rows(net, net.at('x', step), u, up1, s, ds)
                fire(net, turned[k])
                left[0] -= 1
                if left[0] == 0:
                    fire(net, ev['hidden'])

            def layer1_back(k, step):
                yield [turned[k], Event(0.0, R_DU[k])] + ([ev['hidden']] if k in HOLD else [])
                input_back_rows(net, net.at('x', step), ds, up1, part.at[k])
                fire(net, made1[k])
                left[1] -= 1
                if left[1] == 0:
                    fire(net, ev['all_du'])

            def grads1():
                for h in range(2):
                    yield [Event(0.0, R_DDOWN2 if h else R_DDOWN), ev['hidden']]
                    grad_tiles(net, s, g.at[:, :, columns(h)], stage, d_down1.at[:, columns(h)])
                    fire(net, ev['d_down1' if h else 'd_down1_0'])
                for h in range(2):
                    yield [Event(net.now, R_DUP)]
                    grad_tiles(net, u.at[:, :, columns(h)], ds, stage, d_up1.at[columns(h)])
                fire(net, ev['d_up1'])

            def act():
                yield [ev['d_up1'], ev['all_du'], ev['got_u1']]
                own_g = [net.load(g_in.at[:, columns(h)], ds.at[h]) for h in range(2)]
                net.drain(ev['got_u1'].copies)
                credit = net.grant(5, 'xp')
                yield [ev['reduced1'], credit] + own_g
                norm_back_rows(x, lambda at: jnp.concatenate([ds[h, at, :] for h in range(2)], axis=-1), part.at[3, net.core], u.at[net.data])
                net.spend(0.7)
                net.spawn(gather_x(net, u, ev['got_dy'], ev['sent_dy'], dy_here, pool=act_pool.again()))

            def layer1_out():
                yield [ev['reduced1'], Event(0.0, R_OUT)]
                net.drain(ev['reduced1'].copies)
                credit = net.grant(8, 'xp')
                for k, step in enumerate(STEPS):
                    down_rows(net, net.at('x', step), s, down1, part.at[k])
                    yield [Event(net.now, R_OUT)]
                fire(net, ev['y_made'])
                yield [ev['sent_dy'], credit]
                net.spawn(reduce_x(net, part, y_made, rx_scratch, ev['y_reduced'], rs_pool.again()))
                for k in range(RING):
                    fire(net, y_made[k])
                yield [ev['y_reduced']]
                add_rows(x, part.at[3, net.core], x)
                yield [net.load(x, x_out)]
                fire(net, ev['x_saved'])

            a0, s0 = up1.at[pl.ds(0, nd)], up1.at[pl.ds(nd, nd)]
            backs = [RING]

            def bring_back():
                yield [ev['d_down1']]
                yield [net.load(u_out, g)]
                fire(net, ev['got_u0'])

            def bring_acts():
                yield [ev['all_du']]
                net.drain(ev['got_up1'].copies)
                yield [net.load(a_out, a0), net.load(s_out, s0)]
                fire(net, ev['acts'])

            def layer0_hidden(step):
                yield [dy_here[step], ev['acts'], ev['back_down0'], ev['d_up1'], Event(0.0, R_PRE)]
                pre_back_rows(net, net.at('x', step), u, down0, a0, ds)
                backs[0] -= 1
                if backs[0] == 0:
                    fire(net, ev['da0'])

            def layer0():
                for h in range(2):
                    yield [ev['da0'], ev['got_u0'], Event(0.0, R_GUP)]
                    grad_tiles(net, g.at[:, :, columns(h)], ds, stage, d_up0.at[columns(h)])
                fire(net, ev['d_up0'])
                for h in range(2):
                    yield [ev['got_dy'], ev['acts'], Event(0.0, R_GDOWN)]
                    grad_tiles(net, s0, u.at[:, :, columns(h)], stage, d_down0.at[:, columns(h)])
                fire(net, ev['d_down0'])
                yield [ev['y_reduced'], ev['back_up0'], ev['back_up0_rest'], Event(0.0, R_DX)]
                net.drain(ev['y_reduced'].copies + ev['got_down1'].copies)
                x0 = down1.at[pl.ds(0, x_halves.shape[0])]
                yield [net.grant(9, 'xp'), net.load(x_halves, x0)]
                net.spawn(reduce_x(net, part, du_made, rx_scratch, ev['du_reduced'], rs_pool.again()))
                for k, step in enumerate(STEPS):
                    input_back_rows(net, net.at('x', step), ds, up0, part.at[k])
                    fire(net, du_made[k])
                    yield [Event(net.now, R_DX)]
                yield [ev['du_reduced'], ev['x_saved']]
                for q in range(x_halves.shape[0]):
                    rows_q = pl.ds(q * dr, dr)
                    dy_q = u.at[net.data, rows_q]
                    norm_back_rows(x0.at[q], lambda at, dy_q=dy_q: dy_q[at, :], part.at[3, net.core, rows_q], x.at[rows_q])
                yield [net.load(x, dx_out)]

            def up_place(ref, k):
                return lambda block, rows: ref.at[pl.ds(pl.multiple_of(block * (2 * half_up) + k * half_up + rows.start, rows.size), rows.size)]

            def down_place(ref, k):
                return lambda block, rows: ref.at[pl.ds(pl.multiple_of(block * dr + rows.start, rows.size), rows.size), columns(k)]

            def gate(event, items, pool):
                yield items
                pool.again()
                fire(net, event)

            def sum_job(job, place, ref, ready, name, credits=()):
                passed = [Event(), Event()]
                for k in range(2):
                    start = Event()
                    n = job % 2
                    net.spawn(gate(start, ready[k] + ([credits[k]] if credits else []), job_pools[n][k]))
                    sums = Sums(net, AXES[job][k], job_scratch[n][k], stages[k])
                    net.spawn(sums.run(place(ref, k), start, ev['sum_%s%d' % (name, k)], frees[k], passed[k], job_pools[n][k], WINDOWS[2 * job + k], LEAD[min(job, 2)]))
                return passed

            def out_down(layer, dw_down, credit):
                def one(k):
                    done = ev['sum_down%d%d' % (layer, k)]
                    yield [done]
                    yield [net.load(done.total, dw_down.at[:, columns(k)])]
                    if credit is not None:
                        net.drain(done.copies)
                        yield [net.grant(credit + k, 'yz')]
                        fire(net, freed[credit + k])

                for k in range(2):
                    net.spawn(one(k))

            def out_up(n, layer, dw_up, credit):
                totals = [ev['sum_up%d%d' % (layer, k)] for k in range(2)]
                yield totals
                net.drain(totals[0].copies + totals[1].copies)
                spare = job_scratch[n][0][0].at[0]
                for k, done in enumerate(totals):
                    for q in range(2):
                        copy_rows(net, done.total.at[pl.ds(q * spare.shape[1], spare.shape[1])], spare.at[2 * k + q])
                done = ev['out_up%d' % layer]
                net.spawn(exchange_back(net, spare, dw_up, done, pools['blocks'][layer].again()))
                if credit is not None:
                    yield [done]
                    for k in range(2):
                        yield [net.grant(credit + k, 'yz')]
                        fire(net, freed[credit + k])

            passed = sum_job(0, down_place, d_down1, [[ev['d_down1_0'], ev['weights_in']], [ev['d_down1'], ev['weights_in']]], 'down1')
            passed = sum_job(1, up_place, d_up1, [[ev['d_up1']] + passed] * 2, 'up1')
            passed = sum_job(2, up_place, d_up0, [[ev['d_up0']] + passed] * 2, 'up0', [freed[10], freed[11]])
            sum_job(3, down_place, d_down0, [[ev['d_down0']] + passed] * 2, 'down0', [freed[12], freed[13]])
            out_down(1, dw_down1, 10)
            net.spawn(out_up(1, 1, dw_up1, 12))
            net.spawn(out_up(0, 0, dw_up0, None))
            out_down(0, dw_down0, None)
            for k in (3, 2, 1, 0):
                net.spawn(layer1(k, STEPS[k]))
            for k in range(RING):
                net.spawn(layer1_back(k, STEPS[k]))
            for step in (0, -1, 1, 2):
                net.spawn(layer0_hidden(step))
            for flow in (up_first(), second(), hidden_flow(), down_flow(), next_layer(), back_flow(), again(), weights(), grads1(), act(), layer1_out(),
                         bring_back(), bring_acts(), layer0()):
                net.spawn(flow)
            net.run()

        def finish(*refs):
            sources, targets, held, ups, sems = refs[:6], refs[6:10], refs[10:16], refs[16:18], refs[18]
            x_out, dx_out, up_out, down_out = targets
            loads = [pltpu.make_async_copy(src, dst, sems.at[k]) for k, (src, dst) in enumerate(zip(sources, held))]
            stores = [(ups[1], up_out.at[1]), (ups[0], up_out.at[0]), (held[2], down_out.at[1]), (held[3], down_out.at[0]), (held[4], x_out), (held[5], dx_out)]
            stores = [pltpu.make_async_copy(src, dst, sems.at[6 + k]) for k, (src, dst) in enumerate(stores)]
            for load in loads:
                load.start()
            for k in (2, 3, 4, 5):
                loads[k].wait()
                stores[k].start()
            for k in (0, 1):
                loads[k].wait()
                join_columns(held[k], ups[1 - k])
                stores[k].start()
            for store in stores:
                store.wait()

        d_up_own, d_down_own = shape((nd, ur, hidden), F32), shape((dr, width), F32)

        d_up_full, d_down_full = shape((width, hidden), F32), shape((hidden, width), F32)
        x_out, dx, _, _, _, _, _, _, _, _, *grads = call(
            step, [own, own, shape((num_layers, nd * ur, hidden), BF16), act_full, hid_full, hid_full] + [d_up_full, d_down_full] * 2
            + [d_up_own, d_down_own] * 2, 'h' * 14, 'hhhhh',
            [vmem(own)] + [vmem(act_full)] * 2 + [vmem(up_full)] * 2 + [vmem(down_full)] * 2 + [vmem(hid_full)] * 2
            + [pltpu.VMEM((2, hidden // 4, width // 2), F32)] + rx + sums, TR, TS, TL, 0,
            tokens, tokens.reshape(rows // dr, dr, width), grad_out, w_up.reshape(num_layers * ur, ffn), w_down)
        up1_own, down1_own, up0_own, down0_own = grads
        held = [d_up_own, d_up_own, d_down_own, d_down_own, own, own]
        return pl.pallas_call(
            finish, out_shape=[own, own, shape(w_up.shape, F32), shape(w_down.shape, F32)], name='finish',
            in_specs=[pl.BlockSpec(memory_space=pl.ANY)] * 6, out_specs=[pl.BlockSpec(memory_space=pl.ANY)] * 4,
            scratch_shapes=[vmem(like) for like in held] + [pltpu.VMEM(w_up.shape[1:], F32)] * 2 + [pltpu.SemaphoreType.DMA((12,))],
        )(up1_own, up0_own, down1_own, down0_own, x_out, dx)

    return jax.shard_map(device_fn, mesh=mesh, in_specs=(tok_spec, tok_spec, w_spec, w_spec), out_specs=(tok_spec, tok_spec, w_spec, w_spec), check_vma=False)
```

```python
import contextlib

import jax
import jax.numpy as jnp
from jax import lax
from jax.experimental import pallas as pl
from jax.experimental.pallas import tpu as pltpu
from jax.sharding import PartitionSpec as P

NORM_EPS = 1e-6
BOTH_AXES = ('local', 'data')
CONTRACT_ROWS = (((0,), (0,)), ((), ()))
CONTRACT_COLS = (((1,), (1,)), ((), ()))
MESH = pl.DeviceIdType.MESH
RING = 4
F32, BF16 = jnp.float32, jnp.bfloat16

LINK_RATE = 46.0e3
PAIR_RATE = 600e3
LOCAL_RATE = 3000e3
HOP = 2.4
PAIR_HOP = 1.0
ENTRY = 4.0
GELU_C = 0.7978845608028654


def scope(label):
    return jax.named_scope(label) if SCOPES else contextlib.nullcontext()


class Event:
    def __init__(self, time=None, rank=0, name=''):
        self.time, self.rank, self.name = time, rank, name


class Copy:
    def __init__(self, desc, time, remote):
        self.desc, self.time, self.remote, self.rank, self.waited = desc, time, remote, 0, False

    def wait(self):
        if self.remote:
            self.desc.wait_recv()
        else:
            self.desc.wait()


class Credit:
    def __init__(self, semaphore, count, time):
        self.semaphore, self.count, self.time, self.rank, self.waited = semaphore, count, time, 0, False

    def wait(self):
        pl.semaphore_wait(self.semaphore, self.count)


class Pool:
    def __init__(self):
        self.slots, self.next = [], 0

    def again(self):
        self.next = 0
        return self


class Net:
    def __init__(self, send_sems, recv_sems, local_sems, credit_sems):
        self.send_sems, self.recv_sems, self.local_sems, self.credit_sems = send_sems, recv_sems, local_sems, credit_sems
        self.n_remote = self.n_local = 0
        self.free_sends = list(range(send_sems.shape[0]))
        self.free_locals = []
        self.now = 0.0
        self.free = {}
        self.sent = []
        self.flows = []
        self.labels = {}
        here, there = lax.axis_index('local'), lax.axis_index('data')
        pos = {'z': here // RING, 'y': lax.rem(here, RING), 'x': there // 2}
        self.data, self.core = there, lax.rem(there, 2)
        self.ring = {axis: [at] + [lax.rem(at + step, RING) for step in range(1, RING)] for axis, at in pos.items()}
        self.hops = [there] + [lax.rem(there + step, 2 * RING) for step in range(1, 2 * RING)]
        self.blocks = [at * 2 + self.core for at in self.ring['x']]
        self.places = [[z * RING + y for y in self.ring['y']] for z in self.ring['z']]
        self.partner = pos['x'] * 2 + (1 - self.core)
        self.other = 1 - self.core

    def at(self, axis, step):
        return self.ring[axis][step % RING]

    def block(self, step):
        return self.blocks[step % RING]

    def device(self, axis, step):
        if axis == 'p':
            return {'data': self.partner}
        if axis == 'd':
            return {'data': self.hops[step % (2 * RING)]}
        if axis == 'x':
            return {'data': self.block(step)}
        if axis == 'y':
            return {'local': self.places[0][step % RING]}
        return {'local': self.places[step % RING][0]}

    def peers(self, axes):
        return [(axis, step) for axis in axes for step in ((1, -1) if axis in 'xyz' else (1,) if axis == 'p' else range(1, 2 * RING))]

    def signal(self, semaphore, axes):
        for axis, step in self.peers(axes):
            pl.semaphore_signal(semaphore, inc=1, device_id=self.device(axis, step), device_id_type=MESH)

    def arrive(self, axes):
        self.entry, self.entered = pltpu.get_barrier_semaphore(), len(self.peers(axes))
        self.signal(self.entry, axes)

    def enter(self):
        pl.semaphore_wait(self.entry, self.entered)
        self.now = max(self.now, ENTRY)

    def take(self, copies):
        for copy in copies:
            copy.wait()
            copy.waited = True
            self.free_locals.append(copy.slot)
            self.now = max(self.now, copy.time)

    def grant(self, k, axes):
        self.signal(self.credit_sems.at[k], axes)
        return Credit(self.credit_sems.at[k], len(self.peers(axes)), self.now + HOP)

    def drain(self, copies):
        for copy in copies:
            if copy in self.sent:
                copy.desc.wait_send()
                self.sent.remove(copy)
                self.free_sends.append(copy.slot)

    def idle(self, gap):
        over = [copy for copy in self.sent if copy.time + 1.5 < self.now]
        self.drain(over[:int(gap / 0.05)])

    def send(self, src, dst, axis, step=1, pool=None):
        if pool is not None and pool.next < len(pool.slots):
            k = pool.slots[pool.next]
        else:
            k = self.n_remote
            self.n_remote += 1
            if pool is not None:
                pool.slots.append(k)
        if pool is not None:
            pool.next += 1
        if not self.free_sends:
            over = [copy for copy in self.sent if copy.time + 1.0 < self.now]
            if PRINT and not over:
                print('EXHAUSTED', round(self.now, 1))
            self.drain(over or [min(self.sent, key=lambda copy: copy.time)])
        send_slot = self.free_sends.pop()
        desc = pltpu.make_async_remote_copy(
            src_ref=src, dst_ref=dst, send_sem=self.send_sems.at[send_slot], recv_sem=self.recv_sems.at[k],
            device_id=self.device(axis, step), device_id_type=MESH)
        desc.start()
        size = 1
        for n in dst.shape:
            size *= n
        size *= dst.dtype.itemsize
        rate = PAIR_RATE if axis == 'p' else LINK_RATE
        extra = 2.0 if axis == 'd' else 0.0
        if axis == 'd':
            axis, step, size = ('p', 1, size) if step == 1 else ('x', 1 if step < RING + 2 else -1, size)
        key = (axis, step)
        done = max(self.free.get(key, 0.0), self.now) + size / rate
        self.free[key] = done
        copy = Copy(desc, done + extra + (PAIR_HOP if axis == 'p' else HOP), True)
        copy.slot = send_slot
        self.sent.append(copy)
        return copy

    def load(self, src, dst):
        if not self.free_locals:
            self.free_locals.append(self.n_local)
            self.n_local += 1
        k = self.free_locals.pop()
        desc = pltpu.make_async_copy(src, dst, self.local_sems.at[k])
        desc.start()
        size = 1
        for n in dst.shape:
            size *= n
        done = max(self.free.get('hbm', 0.0), self.now) + size * dst.dtype.itemsize / LOCAL_RATE
        self.free['hbm'] = done
        copy = Copy(desc, done + 0.9, False)
        copy.slot = k
        return copy

    def save(self, src, dst):
        copy = self.load(src, dst)
        copy.time += 4.0
        return copy

    def spend(self, microseconds):
        self.now += microseconds

    def spawn(self, flow):
        self.step(flow)

    def step(self, flow):
        try:
            if flow not in self.labels:
                self.labels[flow] = [flow.__name__, len(self.labels), 0]
            self.labels[flow][2] += 1
            self.flows.append((flow, next(flow)))
        except StopIteration:
            pass

    def run(self):
        while self.flows:
            best = None
            for k, (_, items) in enumerate(self.flows):
                if any(item.time is None for item in items):
                    continue
                time = max([item.time for item in items] + [0.0])
                late = max([item.rank for item in items] + [0])
                rank = (max(time, self.now) + (SLACK if late else 0.0), late, time)
                if best is None or rank < best[0]:
                    best = (rank, k, time)
            _, k, time = best
            flow, items = self.flows.pop(k)
            self.idle(time - self.now)
            label = '%s_%d_%d' % tuple(self.labels[flow])
            with scope('w_' + label):
                for item in items:
                    if not isinstance(item, Event) and not item.waited:
                        item.wait()
                        item.waited = True
                        if isinstance(item, Copy) and not item.remote:
                            self.free_locals.append(item.slot)
            before = self.now
            self.now = max(self.now, time)
            if PRINT:
                print('STEP', label, round(before, 2), round(self.now, 2))
            with scope('s_' + label):
                self.step(flow)

    def finish(self):
        for copy in self.sent:
            copy.desc.wait_send()


def rows_loop(rows, chunk, body):
    chunk = min(chunk, rows)

    def step(k, carry):
        body(pl.ds(pl.multiple_of(k * chunk, chunk), chunk))
        return carry

    lax.fori_loop(0, rows // chunk, step, 0)


def add_into(net, dst, *others):
    rows, cols = dst.shape

    def body(at):
        total = dst[at, :]
        for other in others:
            total = total + other[at, :]
        dst[at, :] = total

    rows_loop(rows, 16, body)
    net.spend(rows * cols * 4 * (1 + len(others)) / 4e6)


def fire(net, event):
    event.time = net.now
    if PRINT and event.name:
        print('   %7.1f %s' % (net.now, event.name))


def exchange(net, source, dst, done, pool):
    rows = dst.shape[0] // (2 * RING)

    def mine():
        return dst.at[pl.ds(pl.multiple_of(net.data * rows, rows), rows)]

    own = net.load(source(net.data), mine())
    copies = [net.send(source(net.hops[k]), mine(), 'd', k, pool) for k in (4, 5, 2, 3, 6, 7, 1)]
    yield [own] + copies
    net.drain(copies)
    fire(net, done)


def exchange_back(net, src, dst, done, pool):
    rows = dst.shape[1]
    per = src.shape[1] // rows

    def block(k):
        return src.at[lax.div(k, per), pl.ds(pl.multiple_of(lax.rem(k, per) * rows, rows), rows)]

    own = net.load(block(net.data), dst.at[net.data])
    copies = [net.send(block(net.hops[k]), dst.at[net.data], 'd', k, pool) for k in (4, 5, 2, 3, 6, 7, 1)]
    yield [own] + copies
    net.drain(copies)
    fire(net, done)


def copy_rows(net, src, dst):
    def body(at):
        dst[at, :] = src[at, :]

    rows_loop(src.shape[0], 16, body)
    net.spend(0.2)


def gather_x(net, full, done, issued=None, chips=None, pool=None):
    half = full.shape[1] // 2
    lo, hi = pl.ds(0, half), pl.ds(half, half)
    chips = chips or {step: Event() for step in STEPS}
    left = [2]
    done.copies = []

    def send(*args):
        done.copies.append(net.send(*args, pool=pool))
        return done.copies[-1]

    def block(step):
        return full.at[net.block(step)]

    def part(step, rows):
        return full.at[net.block(step), rows]

    relays = []

    def side(step, first, second, mine):
        yield [mine[0]]
        relays.append(send(part(step, first), part(step, first), 'x', -step))
        left[0] -= 1
        if left[0] == 0:
            net.spawn(far())
            if issued is not None:
                fire(net, issued)
        yield [mine[1]]
        pair = send(block(step), block(step), 'p')
        yield [pair]
        fire(net, chips[step])

    def far():
        yield relays
        pair = send(block(2), block(2), 'p')
        yield [pair]
        fire(net, chips[2])

    forth = [send(part(0, rows), part(0, rows), 'x', 1) for rows in (lo, hi)]
    back = [send(part(0, rows), part(0, rows), 'x', -1) for rows in (hi, lo)]
    pair = send(block(0), block(0), 'p')
    net.spawn(side(-1, lo, hi, forth))
    net.spawn(side(1, hi, lo, back))
    yield [pair]
    fire(net, chips[0])
    yield [chips[step] for step in STEPS]
    fire(net, done)


def gather_yz(net, own, full, first, done, issued=None, offset=0, near=False, split=True, pool=None):
    second = 'y' if first == 'z' else 'z'
    done.copies = []

    def emit(*args):
        done.copies.append(net.send(*args, pool=pool))
        return done.copies[-1]

    size = own.shape[0]
    half = size // 2
    lo, hi, both = pl.ds(offset, half), pl.ds(offset + half, half), pl.ds(offset, size)
    forward, backward = ((lo, hi), (hi, lo)) if split and not near else ((both,), (both,))

    def part(one, two, rows):
        return full.at[yz_index(net, first, one, two), rows]

    left = [3 if near else RING, 3 if near else RING]

    def arrived(which):
        left[which] -= 1
        if left[which] == 0 and (done, issued)[which] is not None:
            fire(net, (done, issued)[which])

    def send(one, rows, axis, step):
        src = own.at[pl.ds(rows.start - offset, rows.size)] if one == 0 else part(one, 0, rows)
        return emit(src, part(one, 0, rows), axis, step)

    def column(one):
        forth = [send(one, rows, second, 1) for rows in forward]
        back = [send(one, rows, second, -1) for rows in backward]

        def finish():
            if near:
                arrived(1)
                yield forth + back
            else:
                yield [forth[0]]
                relays = [emit(part(one, -1, lo), part(one, -1, lo), second, 1)]
                yield [back[0]]
                relays.append(emit(part(one, 1, hi), part(one, 1, hi), second, -1))
                arrived(1)
                yield forth[1:] + back[1:] + relays
            arrived(0)

        net.spawn(finish())

    relays = []

    def side(step, first_half, mine):
        yield [mine[0]]
        if not near:
            relays.append(emit(part(step, 0, first_half), part(step, 0, first_half), first, -step))
            if len(relays) == 2:
                net.spawn(far())
        yield mine[1:]
        column(step)

    def far():
        yield relays
        column(2)

    mine = [net.load(own, part(0, 0, both))]
    forth = [send(0, rows, first, 1) for rows in forward]
    back = [send(0, rows, first, -1) for rows in backward]
    column(0)
    net.spawn(side(-1, lo, forth))
    net.spawn(side(1, hi, back))
    left[0] += 1
    yield mine
    arrived(0)


def yz_index(net, first, one, two):
    return net.places[one % RING][two % RING] if first == 'z' else net.places[two % RING][one % RING]


FAR = [(2, 0), (2, 1), (2, -1), (2, 2), (0, 2), (1, 2), (-1, 2)]


STEPS = (2, 1, -1, 0)


def reduce_x(net, part, made, scratch, done, pool=None):
    other, relay_f, relay_b, last_f, last_b = scratch
    half = part.shape[2] // 2
    lo, hi = pl.ds(0, half), pl.ds(half, half)

    def acc(k, rows=None):
        return part.at[k, net.core] if rows is None else part.at[k, net.core, rows]

    pairs = [None] * RING
    ready = [Event() for _ in STEPS]

    def pair(k):
        yield [made[k]]
        pairs[k] = net.send(part.at[k, net.other], other.at[k], 'p', pool=pool)
        yield [pairs[k]]
        add_into(net, acc(k), other.at[k])
        fire(net, ready[k])

    for k in range(RING):
        net.spawn(pair(k))
    sent = {}
    started, relayed = Event(), Event()

    def part_flow(k):
        yield [ready[k]] + ([relayed] if k else [])
        if k == 0:
            sent['first_f'] = net.send(acc(0, lo), relay_f, 'x', 1, pool=pool)
            sent['first_b'] = net.send(acc(0, hi), relay_b, 'x', -1, pool=pool)
            fire(net, relayed)
        elif k == 1:
            sent['direct_f'] = net.send(acc(1, hi), last_f.at[hi], 'x', 1, pool=pool)
        else:
            sent['direct_b'] = net.send(acc(2, lo), last_b.at[lo], 'x', -1, pool=pool)
        if len(sent) == 4:
            fire(net, started)

    for k in range(3):
        net.spawn(part_flow(k))
    yield [started]
    yield [sent['first_f']]
    add_into(net, acc(1, lo), relay_f)
    summed_f = net.send(acc(1, lo), last_f.at[lo], 'x', 1, pool=pool)
    yield [sent['first_b']]
    add_into(net, acc(2, hi), relay_b)
    summed_b = net.send(acc(2, hi), last_b.at[hi], 'x', -1, pool=pool)
    yield [ready[3], sent['direct_f'], sent['direct_b'], summed_f, summed_b]
    add_into(net, acc(3), last_f, last_b)
    done.copies = pairs + list(sent.values()) + [summed_f, summed_b]
    fire(net, done)


def reduce_x_scratch(rows, cols):
    return [pltpu.VMEM((RING, rows, cols), F32), pltpu.VMEM((rows // 2, cols), F32), pltpu.VMEM((rows // 2, cols), F32),
            pltpu.VMEM((rows, cols), F32), pltpu.VMEM((rows, cols), F32)]


def load_parts(net, src, part, made):
    for k, step in enumerate(STEPS):
        def bring(k=k, step=step):
            yield [net.load(src.at[pl.ds(net.at('x', step) * 2, 2)], part.at[k])]
            fire(net, made[k])

        net.spawn(bring())


class Sums:
    def __init__(self, net, first, scratch, stage):
        self.net, self.first, self.scratch, self.stage = net, first, scratch, stage
        self.second = 'y' if first == 'z' else 'z'

    def run(self, place, start, done, free, passed_all, pool, window, lead):
        net, first, second = self.net, self.first, self.second
        relay1, last1, relay2, last2 = self.scratch
        ahead, behind, mine = self.stage
        half = mine.shape[0] // 2
        lo, hi, all_rows = pl.ds(0, half), pl.ds(half, half), pl.ds(0, 2 * half)
        done.copies = []

        def send(*args):
            done.copies.append(net.send(*args, pool=pool))
            return done.copies[-1]

        def term(one, two, rows=all_rows):
            return place(yz_index(net, first, one, two), rows)

        def bring(gate, src, dst, got):
            yield [gate, start]
            yield [net.load(src, dst)]
            fire(net, got)

        chain = [[gate] + [Event() for _ in range(RING)] for gate in free]
        free[:] = [events[RING] for events in chain]
        got = [[Event() for _ in range(RING)] for _ in range(3)]
        ends = [Event() for _ in STEPS]
        passed = [Event() for _ in range(RING)]
        passed[lead] = passed_all

        def ring(k):
            two = STEPS[k]
            if k >= window:
                yield [passed[k - window]]
            net.spawn(bring(chain[0][k], term(1, two, lo), ahead, got[0][k]))
            net.spawn(bring(chain[1][k], term(-1, two, hi), behind, got[1][k]))
            net.spawn(bring(chain[2][k], term(0, two), mine, got[2][k]))
            first_f = send(term(2, two, lo), relay1.at[0, k], first, 1)
            first_b = send(term(2, two, hi), relay1.at[1, k], first, -1)
            direct_f = send(term(1, two, hi), last1.at[0, k, hi], first, 1)
            direct_b = send(term(-1, two, lo), last1.at[1, k, lo], first, -1)
            yield [first_f, got[0][k]]
            add_into(net, relay1.at[0, k], ahead)
            fire(net, chain[0][k + 1])
            summed_f = send(relay1.at[0, k], last1.at[0, k, lo], first, 1)
            yield [first_b, got[1][k]]
            add_into(net, relay1.at[1, k], behind)
            fire(net, chain[1][k + 1])
            summed_b = send(relay1.at[1, k], last1.at[1, k, hi], first, -1)
            fire(net, passed[k])
            yield [direct_f, direct_b, summed_f, summed_b, got[2][k]]
            add_into(net, last1.at[0, k], last1.at[1, k], mine)
            fire(net, chain[2][k + 1])
            fire(net, ends[k])

        def sums(k, rows=all_rows):
            return last1.at[0, k, rows]

        yield [start]
        for k in range(RING):
            net.spawn(ring(k))
        yield [ends[0]]
        first_f = send(sums(0, lo), relay2.at[0], second, 1)
        first_b = send(sums(0, hi), relay2.at[1], second, -1)
        yield [ends[1]]
        direct_f = send(sums(1, hi), last2.at[0, hi], second, 1)
        yield [ends[2]]
        direct_b = send(sums(2, lo), last2.at[1, lo], second, -1)
        yield [first_f]
        add_into(net, sums(1, lo), relay2.at[0])
        summed_f = send(sums(1, lo), last2.at[0, lo], second, 1)
        yield [first_b]
        add_into(net, sums(2, hi), relay2.at[1])
        summed_b = send(sums(2, hi), last2.at[1, hi], second, -1)
        yield [ends[3], direct_f, direct_b, summed_f, summed_b]
        add_into(net, sums(3), last2.at[0], last2.at[1])
        done.total = sums(3)
        fire(net, done)


def sums_scratch(rows, cols):
    return [pltpu.VMEM((2, RING, rows // 2, cols), F32), pltpu.VMEM((2, RING, rows, cols), F32),
            pltpu.VMEM((2, rows // 2, cols), F32), pltpu.VMEM((2, rows, cols), F32)]


def sums_stage(rows, cols):
    return [pltpu.VMEM((rows // 2, cols), F32), pltpu.VMEM((rows // 2, cols), F32), pltpu.VMEM((rows, cols), F32)]


def norm_rows(x_ref, u_ref):
    def body(at):
        x = x_ref[at, :].astype(F32)
        u_ref[at, :] = (x * lax.rsqrt(jnp.mean(x * x, axis=-1, keepdims=True) + NORM_EPS)).astype(BF16)

    rows_loop(x_ref.shape[0], 16, body)


def norm_back_rows(x_ref, dy_of, du_ref, dx_ref):
    def body(at):
        x = x_ref[at, :].astype(F32)
        du = du_ref[at, :]
        r = lax.rsqrt(jnp.mean(x * x, axis=-1, keepdims=True) + NORM_EPS)
        xr = x * r
        dx_ref[at, :] = (dy_of(at).astype(F32) + r * (du - xr * jnp.mean(xr * du, axis=-1, keepdims=True))).astype(BF16)

    rows_loop(x_ref.shape[0], 16, body)


def add_rows(x_ref, y_ref, out_ref):
    def body(at):
        out_ref[at, :] = (x_ref[at, :].astype(F32) + y_ref[at, :]).astype(BF16)

    rows_loop(x_ref.shape[0], 16, body)


def swap_halves(even, odd):
    low = lax.broadcasted_iota(jnp.int32, even.shape, len(even.shape) - 1) < even.shape[-1] // 2
    shift = even.shape[-1] // 2
    axis = len(even.shape) - 1
    return jnp.where(low, even, pltpu.roll(odd, shift, axis)), jnp.where(low, pltpu.roll(even, shift, axis), odd)


def split_columns(w_ref, cols_ref, layers):
    pieces, _, wide = w_ref.shape
    rows = layers
    tile = pieces * wide // (4 * RING * RING)
    for x in range(RING):
        for p in range(wide // tile):
            pair = []
            for i in (2 * p, 2 * p + 1):
                at = (i * RING + x) * tile
                pair.append(w_ref[at // wide, pl.ds(0, rows), pl.ds(at % wide, tile)].astype(F32))
            for c, value in enumerate(swap_halves(*pair)):
                cols_ref[2 * x + c, pl.ds(0, rows), pl.ds(p * tile, tile)] = value.astype(cols_ref.dtype)


def join_columns(cols_ref, w_ref):
    tile = w_ref.shape[1] // (4 * RING * RING)
    for x in range(RING):
        for p in range(cols_ref.shape[2] // tile):
            pair = [cols_ref[2 * x + c, :, pl.ds(p * tile, tile)] for c in range(2)]
            for i, value in zip((2 * p, 2 * p + 1), swap_halves(*pair)):
                w_ref[:, pl.ds((i * RING + x) * tile, tile)] = value


def call(body, out_shape, out_spaces, in_spaces, scratch, remote, sends, local, collective_id, *args):
    spaces = {'v': pl.BlockSpec(memory_space=pltpu.VMEM), 'h': pl.BlockSpec(memory_space=pl.ANY)}

    def kernel(*refs):
        net = Net(*refs[-5:-1])
        net.tile_sems = refs[-1]
        body(net, *refs[:-5])
        net.finish()
        assert net.n_remote <= remote and net.n_local <= local, (body.__name__, net.n_remote, net.n_local)
        if PRINT:
            print(body.__name__, net.n_remote, net.n_local, round(net.now, 1))

    return pl.pallas_call(
        kernel, out_shape=out_shape, in_specs=[spaces[s] for s in in_spaces], out_specs=[spaces[s] for s in out_spaces],
        scratch_shapes=list(scratch) + [pltpu.SemaphoreType.DMA((sends,)), pltpu.SemaphoreType.DMA((remote,)), pltpu.SemaphoreType.DMA((local,)),
                                               pltpu.SemaphoreType.REGULAR((14,)), pltpu.SemaphoreType.DMA((2,))],
        compiler_params=pltpu.CompilerParams(collective_id=collective_id, has_side_effects=True, vmem_limit_bytes=67000000),
        cost_estimate=pl.CostEstimate(flops=10**8, bytes_accessed=10**7, transcendentals=0),
        name=body.__name__)(*args)


PRINT = False
SCOPES = False


WIDE = 512
EARLY = 3
GRAD_TIME = 3.4
SLACK = 0.1
R_HIDDEN, R_DOWN, R_BACK, R_TURN, R_DDOWN, R_DDOWN2, R_DUP, R_OUT, R_PRE, R_GUP, R_GDOWN, R_DX = 2, 1, 3, 1, 2, 2, 4, 2, 2, 3, 3, 2
R_DU, HOLD = (3, 3.1, 3.2, 3.3), (0, 1, 2)
WINDOWS = (2, 2, 2, 2, 2, 2, 2, 2)
AXES = ('yz', 'yz', 'yz', 'yz')
TOP = 6
NEAR = 'z'
LEAD = (3, 3, 3)
TR, TS, TL = 264, 56, 9


def wide_loop(total, body):
    wide = min(WIDE, total)

    def step(k, carry):
        body(k, wide, pl.ds(pl.multiple_of(k * wide, wide), wide))
        return carry

    lax.fori_loop(0, total // wide, step, 0)


def flat(value):
    return value.reshape(value.shape[0] * value.shape[1], value.shape[2])


def dot_rows(a, b):
    return jnp.dot(flat(a), flat(b), preferred_element_type=F32)


def dot_cols(a, b):
    return lax.dot_general(flat(a), flat(b), CONTRACT_COLS, preferred_element_type=F32)


def gelu(a):
    return 0.5 * a * (1.0 + jnp.tanh(GELU_C * (a + 0.044715 * a * a * a)))


def hidden_rows(net, chip, u, up, a, s):
    at = pl.ds(chip * 2, 2)

    def body(_, wide, cols):
        pre = dot_rows(u[at], up[:, :, cols]).astype(BF16)
        a[at, :, cols] = pre.reshape(2, -1, wide)
        s[at, :, cols] = gelu(pre.astype(F32)).astype(BF16).reshape(2, -1, wide)

    wide_loop(up.shape[2], body)
    net.spend(1.7)


def down_rows(net, chip, s, down, part):
    at = pl.ds(chip * 2, 2)

    def body(_, wide, cols):
        part[:, :, cols] = dot_rows(s[at], down[:, :, cols]).reshape(2, -1, wide)

    wide_loop(down.shape[2], body)
    net.spend(1.76)


def hidden_back_rows(net, chip, dy, down, ds):
    at = pl.ds(chip * 2, 2)
    rows = down.shape[1]

    def body(k, wide, cols):
        blocks = pl.ds(k * (wide // rows), wide // rows)
        ds[at, :, cols] = dot_cols(dy[at], down[blocks]).astype(BF16).reshape(2, -1, wide)

    wide_loop(down.shape[0] * rows, body)
    net.spend(1.5)


def gelu_both(a):
    t = jnp.tanh(GELU_C * (a + 0.044715 * a * a * a))
    return 0.5 * a * (1.0 + t), 0.5 * (1.0 + t) + 0.5 * a * (1.0 - t * t) * (GELU_C * (1.0 + 3 * 0.044715 * a * a))


def hidden_turn_rows(net, chip, u, up, s, ds):
    at = pl.ds(chip * 2, 2)

    def body(_, wide, cols):
        pre = dot_rows(u[at], up[:, :, cols]).astype(BF16).astype(F32)
        value, slope = gelu_both(pre)
        s[at, :, cols] = value.astype(BF16).reshape(2, -1, wide)
        ds[at, :, cols] = (ds[at, :, cols].astype(F32) * slope.reshape(2, -1, wide)).astype(BF16)

    wide_loop(up.shape[2], body)
    net.spend(2.1)


def pre_back_rows(net, chip, dy, down, a, da):
    at = pl.ds(chip * 2, 2)
    rows = down.shape[1]

    def body(k, wide, cols):
        blocks = pl.ds(k * (wide // rows), wide // rows)
        ds = dot_cols(dy[at], down[blocks]).astype(BF16).astype(F32).reshape(2, -1, wide)
        da[at, :, cols] = (ds * gelu_both(a[at, :, cols].astype(F32))[1]).astype(BF16)

    wide_loop(down.shape[0] * rows, body)
    net.spend(1.95)


def input_back_rows(net, chip, da, up, part):
    at = pl.ds(chip * 2, 2)
    rows = up.shape[1]

    def body(k, wide, cols):
        blocks = pl.ds(k * (wide // rows), wide // rows)
        part[:, :, cols] = dot_cols(da[at], up[blocks]).reshape(2, -1, wide)

    wide_loop(up.shape[0] * rows, body)
    net.spend(1.9)


def stored_tiles(net, count, compute, stage, out):
    def store(t):
        return pltpu.make_async_copy(stage.at[lax.rem(t, 2)], out(t), net.tile_sems.at[lax.rem(t, 2)])

    def step(t, carry):
        @pl.when(t >= 2)
        def _():
            store(t - 2).wait()

        compute(t, stage.at[lax.rem(t, 2)])
        store(t).start()
        return carry

    lax.fori_loop(0, count, step, 0)
    for t in range(max(count - 2, 0), count):
        store(jnp.int32(t)).wait()


def dot_tokens(a, b):
    return lax.dot_general(flat(a), flat(b), CONTRACT_ROWS, preferred_element_type=F32)


def grad_tiles(net, lhs, rhs, stage, out):
    _, high, wide = stage.shape
    across = rhs.shape[2] // wide

    def columns(t):
        return pl.ds(pl.multiple_of(lax.rem(t, across) * wide, wide), wide)

    def rows(t):
        return pl.ds(pl.multiple_of(lax.div(t, across) * high, high), high)

    def compute(t, slot):
        slot[...] = dot_tokens(lhs[:, :, rows(t)], rhs[:, :, columns(t)])

    stored_tiles(net, lhs.shape[2] // high * across, compute, stage, lambda t: out.at[rows(t), columns(t)])
    net.spend(GRAD_TIME * lhs.shape[2] / 1024)


def solution(mesh):
    nl, nd = mesh.shape['local'], mesh.shape['data']
    tok_spec = P(BOTH_AXES, None)
    w_spec = P(None, BOTH_AXES, None)

    def device_fn(tokens, grad_out, w_up, w_down):
        num_layers, ur, ffn = w_up.shape
        dr = w_down.shape[1]
        rows, width = tokens.shape
        hidden = nl * dr
        shape = jax.ShapeDtypeStruct
        up_full = shape((nl, nd * ur, hidden), BF16)
        down_full = shape((nl, dr, width), BF16)
        act_full = shape((nd, rows, width), BF16)
        hid_full = shape((nd, rows, hidden), BF16)
        own = shape((rows, width), BF16)
        part_vmem = pltpu.VMEM((RING, 2, rows, width), F32)
        rx = [part_vmem] + reduce_x_scratch(rows, width)
        sums = sums_scratch(dr, hidden) * 4 + sums_stage(dr, hidden) * 2

        def vmem(like):
            return pltpu.VMEM(like.shape, like.dtype)

        def step(net, x_in, x_halves, g_in, w_up_in, w_down_in,
                 x_out, dx_out, block_out, u_out, a_out, s_out, d_up0, d_down0, d_up1, d_down1, dw_up1, dw_down1, dw_up0, dw_down0,
                 x, u, g, up0, up1, down0, down1, ds, s, stage, part, *scratch):
            net.arrive('dyz')
            rx_scratch = scratch[:5]
            names = ('blocks', 'blocks1', 'sent_u', 'got_u', 'got_g', 'sent_up0', 'sent_down0', 'sent_up1', 'sent_down1', 'got_up0', 'got_down0',
                     'got_up1', 'got_down1', 'saved', 'free0', 'reduced0', 'ds_made', 'got_u1', 'hidden', 'all_du', 'reduced1', 'sent_dy', 'got_dy',
                     'back_up0', 'back_up0_rest', 'back_down0', 'd_down1', 'd_up1', 'y_reduced', 'acts', 'd_down0', 'da0', 'd_up0', 'du_reduced',
                     'out_up1', 'out_up0', 'got_u0', 'y_made', 'x_saved', 'weights_in', 'd_down1_0')
            ev = {name: Event(name=name) for name in names}
            for kind in ('up', 'down'):
                for layer in range(2):
                    for k in range(2):
                        ev['sum_%s%d%d' % (kind, layer, k)] = Event(name='sum_%s%d%d' % (kind, layer, k))
            ev['got_up0'].rank = R_HIDDEN
            hidden_made, made0, made1, y_made, du_made = ([Event(name='%s%d' % (name, k)) for k in range(RING)]
                                                          for name in ('hidden_', 'made0_', 'made1_', 'y_made_', 'du_made_'))
            wide = width // 2
            half_up = nd * ur // 2
            act_pool, rs_pool = Pool(), Pool()
            job_pools = [[Pool(), Pool()], [Pool(), Pool()]]
            pools = {'up0': [Pool(), Pool()], 'down0': [Pool(), Pool()], 'up1': job_pools[0], 'down1': job_pools[1], 'blocks': [Pool(), Pool()]}
            stages = (scratch[21:24], scratch[24:27])
            job_scratch = [[scratch[5 + 8 * n + 4 * k:9 + 8 * n + 4 * k] for k in range(2)] for n in range(2)]
            frees = [[Event(0.0) for _ in range(3)] for _ in range(2)]
            freed = {k: Event() for k in range(10, 14)}

            def columns(h):
                return pl.ds(h * wide, wide)

            inputs = [net.load(x_in, x)]
            inputs += [net.load(w_up_in.at[:, pl.ds(k * hidden, hidden)], ds.at[k, pl.ds(0, num_layers * ur)]) for k in range(nd)]

            def gather(name, own, full, split):
                size = own.shape[0] // 2

                def join(kind, events):
                    yield events
                    if kind == 'got_':
                        ev[kind + name].copies = events[0].copies + events[1].copies
                    fire(net, ev[kind + name])

                got, sent = [Event(), Event()], [Event(), Event()]
                for k, first in enumerate('yz'):
                    net.spawn(gather_yz(net, own.at[pl.ds(k * size, size)], full, first, got[k], sent[k], k * size, split=split, pool=pools[name][k]))
                net.spawn(join('got_', got))
                net.spawn(join('sent_', sent))

            net.take(inputs)
            split_columns(ds, s, num_layers * ur)
            norm_rows(x, u.at[net.data])
            net.enter()
            gather('down0', w_down_in.at[0], down0, False)
            net.spawn(exchange(net, lambda k: s.at[k, pl.ds(0, ur)], block_out.at[0], ev['blocks'], pools['blocks'][0]))
            own_grads = net.load(g_in, g.at[net.data])

            def up_first():
                yield [ev['blocks']]
                gather('up0', block_out.at[0], up0, True)
                net.spawn(gather_x(net, u, ev['got_u'], ev['sent_u'], pool=act_pool))
                yield [ev['sent_u']]
                net.spawn(exchange(net, lambda k: s.at[k, pl.ds(ur, ur)], block_out.at[1], ev['blocks1'], pools['blocks'][1]))
                yield [own_grads]
                net.spawn(gather_x(net, g, ev['got_g']))

            def second():
                yield [ev['sent_up0'], ev['sent_down0'], ev['blocks1']]
                gather('down1', w_down_in.at[1], down1, False)
                yield [made0[EARLY]]
                gather('up1', block_out.at[1], up1, True)

            def hidden_flow():
                yield [ev['got_u'], ev['got_up0'], ev['blocks1']]
                for k, step in enumerate(STEPS):
                    hidden_rows(net, net.at('x', step), u, up0, ds, s)
                    fire(net, hidden_made[k])
                    yield [Event(net.now, R_HIDDEN)]
                yield [net.load(ds, a_out), net.load(s, s_out), net.load(u, u_out)]
                fire(net, ev['saved'])

            def down_flow():
                for k, step in enumerate(STEPS):
                    yield [hidden_made[k], ev['got_down0'], Event(0.0, R_DOWN)]
                    down_rows(net, net.at('x', step), s, down0, part.at[k])
                    fire(net, made0[k])
                fire(net, ev['free0'])

            net.spawn(reduce_x(net, part, made0, rx_scratch, ev['reduced0'], rs_pool))
            here = {step: Event(name='u%d' % step) for step in STEPS}
            dy_here = {step: Event() for step in STEPS}

            def next_layer():
                yield [ev['saved'], ev['got_g']]
                net.drain(ev['got_u'].copies + ev['got_g'].copies)
                credit = net.grant(3, 'xp')
                yield [ev['reduced0'], credit]
                add_rows(x, part.at[3, net.core], x)
                norm_rows(x, u.at[net.data])
                net.spend(1.0)
                net.spawn(gather_x(net, u, ev['got_u1'], chips=here, pool=act_pool.again()))
                net.drain(ev['reduced0'].copies)
                yield [net.grant(4, 'xp')]
                net.spawn(reduce_x(net, part, made1, rx_scratch, ev['reduced1'], rs_pool.again()))

            def back_flow():
                for k, step in enumerate(STEPS):
                    yield [ev['got_g'], ev['got_down1'], ev['saved'], Event(0.0, R_BACK)]
                    hidden_back_rows(net, net.at('x', step), g, down1, ds)
                fire(net, ev['ds_made'])

            def again():
                top = nd * ur * TOP // 8
                yield [ev['free0'], ev['ds_made']]
                net.drain(ev['got_up0'].copies + ev['got_down0'].copies)
                credit = net.grant(6, 'yz')
                yield [credit]
                net.spawn(gather_yz(net, w_down_in.at[0], down0, NEAR, ev['back_down0'], near=True, pool=pools['down0'][1].again()))
                net.spawn(gather_yz(net, block_out.at[0, pl.ds(0, top)], up0, 'y', ev['back_up0'], pool=pools['up0'][0].again()))
                net.spawn(gather_yz(net, block_out.at[0, pl.ds(top, nd * ur - top)], up0, 'z', ev['back_up0_rest'], offset=top, pool=pools['up0'][1].again()))

            def weights():
                yield [ev['got_up1'], ev['got_down1']]
                yield [net.grant(7, 'yz')]
                fire(net, ev['weights_in'])

            left = [RING, RING]

            turned = [Event() for _ in STEPS]

            def layer1(k, step):
                yield [here[step], ev['ds_made'], ev['got_up1'], Event(0.0, R_TURN)]
                hidden_turn_rows(net, net.at('x', step), u, up1, s, ds)
                fire(net, turned[k])
                left[0] -= 1
                if left[0] == 0:
                    fire(net, ev['hidden'])

            def layer1_back(k, step):
                yield [turned[k], Event(0.0, R_DU[k])] + ([ev['hidden']] if k in HOLD else [])
                input_back_rows(net, net.at('x', step), ds, up1, part.at[k])
                fire(net, made1[k])
                left[1] -= 1
                if left[1] == 0:
                    fire(net, ev['all_du'])

            def grads1():
                for h in range(2):
                    yield [Event(0.0, R_DDOWN2 if h else R_DDOWN), ev['hidden']]
                    grad_tiles(net, s, g.at[:, :, columns(h)], stage, d_down1.at[:, columns(h)])
                    fire(net, ev['d_down1' if h else 'd_down1_0'])
                for h in range(2):
                    yield [Event(net.now, R_DUP)]
                    grad_tiles(net, u.at[:, :, columns(h)], ds, stage, d_up1.at[columns(h)])
                fire(net, ev['d_up1'])

            def act():
                yield [ev['d_up1'], ev['all_du'], ev['got_u1']]
                own_g = [net.load(g_in.at[:, columns(h)], ds.at[h]) for h in range(2)]
                net.drain(ev['got_u1'].copies)
                credit = net.grant(5, 'xp')
                yield [ev['reduced1'], credit] + own_g
                norm_back_rows(x, lambda at: jnp.concatenate([ds[h, at, :] for h in range(2)], axis=-1), part.at[3, net.core], u.at[net.data])
                net.spend(0.7)
                net.spawn(gather_x(net, u, ev['got_dy'], ev['sent_dy'], dy_here, pool=act_pool.again()))

            def layer1_out():
                yield [ev['reduced1'], Event(0.0, R_OUT)]
                net.drain(ev['reduced1'].copies)
                credit = net.grant(8, 'xp')
                for k, step in enumerate(STEPS):
                    down_rows(net, net.at('x', step), s, down1, part.at[k])
                    yield [Event(net.now, R_OUT)]
                fire(net, ev['y_made'])
                yield [ev['sent_dy'], credit]
                net.spawn(reduce_x(net, part, y_made, rx_scratch, ev['y_reduced'], rs_pool.again()))
                for k in range(RING):
                    fire(net, y_made[k])
                yield [ev['y_reduced']]
                add_rows(x, part.at[3, net.core], x)
                yield [net.load(x, x_out)]
                fire(net, ev['x_saved'])

            a0, s0 = up1.at[pl.ds(0, nd)], up1.at[pl.ds(nd, nd)]
            backs = [RING]

            def bring_back():
                yield [ev['d_down1']]
                yield [net.load(u_out, g)]
                fire(net, ev['got_u0'])

            def bring_acts():
                yield [ev['all_du']]
                net.drain(ev['got_up1'].copies)
                yield [net.load(a_out, a0), net.load(s_out, s0)]
                fire(net, ev['acts'])

            def layer0_hidden(step):
                yield [dy_here[step], ev['acts'], ev['back_down0'], ev['d_up1'], Event(0.0, R_PRE)]
                pre_back_rows(net, net.at('x', step), u, down0, a0, ds)
                backs[0] -= 1
                if backs[0] == 0:
                    fire(net, ev['da0'])

            def layer0():
                for h in range(2):
                    yield [ev['da0'], ev['got_u0'], Event(0.0, R_GUP)]
                    grad_tiles(net, g.at[:, :, columns(h)], ds, stage, d_up0.at[columns(h)])
                fire(net, ev['d_up0'])
                for h in range(2):
                    yield [ev['got_dy'], ev['acts'], Event(0.0, R_GDOWN)]
                    grad_tiles(net, s0, u.at[:, :, columns(h)], stage, d_down0.at[:, columns(h)])
                fire(net, ev['d_down0'])
                yield [ev['y_reduced'], ev['back_up0'], ev['back_up0_rest'], Event(0.0, R_DX)]
                net.drain(ev['y_reduced'].copies + ev['got_down1'].copies)
                x0 = down1.at[pl.ds(0, x_halves.shape[0])]
                yield [net.grant(9, 'xp'), net.load(x_halves, x0)]
                net.spawn(reduce_x(net, part, du_made, rx_scratch, ev['du_reduced'], rs_pool.again()))
                for k, step in enumerate(STEPS):
                    input_back_rows(net, net.at('x', step), ds, up0, part.at[k])
                    fire(net, du_made[k])
                    yield [Event(net.now, R_DX)]
                yield [ev['du_reduced'], ev['x_saved']]
                for q in range(x_halves.shape[0]):
                    rows_q = pl.ds(q * dr, dr)
                    dy_q = u.at[net.data, rows_q]
                    norm_back_rows(x0.at[q], lambda at, dy_q=dy_q: dy_q[at, :], part.at[3, net.core, rows_q], x.at[rows_q])
                yield [net.load(x, dx_out)]

            def up_place(ref, k):
                return lambda block, rows: ref.at[pl.ds(pl.multiple_of(block * (2 * half_up) + k * half_up + rows.start, rows.size), rows.size)]

            def down_place(ref, k):
                return lambda block, rows: ref.at[pl.ds(pl.multiple_of(block * dr + rows.start, rows.size), rows.size), columns(k)]

            def gate(event, items, pool):
                yield items
                pool.again()
                fire(net, event)

            def sum_job(job, place, ref, ready, name, credits=()):
                passed = [Event(), Event()]
                for k in range(2):
                    start = Event()
                    n = job % 2
                    net.spawn(gate(start, ready[k] + ([credits[k]] if credits else []), job_pools[n][k]))
                    sums = Sums(net, AXES[job][k], job_scratch[n][k], stages[k])
                    net.spawn(sums.run(place(ref, k), start, ev['sum_%s%d' % (name, k)], frees[k], passed[k], job_pools[n][k], WINDOWS[2 * job + k], LEAD[min(job, 2)]))
                return passed

            def out_down(layer, dw_down, credit):
                def one(k):
                    done = ev['sum_down%d%d' % (layer, k)]
                    yield [done]
                    yield [net.load(done.total, dw_down.at[:, columns(k)])]
                    if credit is not None:
                        net.drain(done.copies)
                        yield [net.grant(credit + k, 'yz')]
                        fire(net, freed[credit + k])

                for k in range(2):
                    net.spawn(one(k))

            def out_up(n, layer, dw_up, credit):
                totals = [ev['sum_up%d%d' % (layer, k)] for k in range(2)]
                yield totals
                net.drain(totals[0].copies + totals[1].copies)
                spare = job_scratch[n][0][0].at[0]
                for k, done in enumerate(totals):
                    for q in range(2):
                        copy_rows(net, done.total.at[pl.ds(q * spare.shape[1], spare.shape[1])], spare.at[2 * k + q])
                done = ev['out_up%d' % layer]
                net.spawn(exchange_back(net, spare, dw_up, done, pools['blocks'][layer].again()))
                if credit is not None:
                    yield [done]
                    for k in range(2):
                        yield [net.grant(credit + k, 'yz')]
                        fire(net, freed[credit + k])

            passed = sum_job(0, down_place, d_down1, [[ev['d_down1_0'], ev['weights_in']], [ev['d_down1'], ev['weights_in']]], 'down1')
            passed = sum_job(1, up_place, d_up1, [[ev['d_up1']] + passed] * 2, 'up1')
            passed = sum_job(2, up_place, d_up0, [[ev['d_up0']] + passed] * 2, 'up0', [freed[10], freed[11]])
            sum_job(3, down_place, d_down0, [[ev['d_down0']] + passed] * 2, 'down0', [freed[12], freed[13]])
            out_down(1, dw_down1, 10)
            net.spawn(out_up(1, 1, dw_up1, 12))
            net.spawn(out_up(0, 0, dw_up0, None))
            out_down(0, dw_down0, None)
            for k in (3, 2, 1, 0):
                net.spawn(layer1(k, STEPS[k]))
            for k in range(RING):
                net.spawn(layer1_back(k, STEPS[k]))
            for step in (0, -1, 1, 2):
                net.spawn(layer0_hidden(step))
            for flow in (up_first(), second(), hidden_flow(), down_flow(), next_layer(), back_flow(), again(), weights(), grads1(), act(), layer1_out(),
                         bring_back(), bring_acts(), layer0()):
                net.spawn(flow)
            net.run()

        def finish(*refs):
            sources, targets, held, ups, sems = refs[:6], refs[6:10], refs[10:16], refs[16:18], refs[18]
            x_out, dx_out, up_out, down_out = targets
            loads = [pltpu.make_async_copy(src, dst, sems.at[k]) for k, (src, dst) in enumerate(zip(sources, held))]
            stores = [(ups[1], up_out.at[1]), (ups[0], up_out.at[0]), (held[2], down_out.at[1]), (held[3], down_out.at[0]), (held[4], x_out), (held[5], dx_out)]
            stores = [pltpu.make_async_copy(src, dst, sems.at[6 + k]) for k, (src, dst) in enumerate(stores)]
            for load in loads:
                load.start()
            for k in (2, 3, 4, 5):
                loads[k].wait()
                stores[k].start()
            for k in (0, 1):
                loads[k].wait()
                join_columns(held[k], ups[1 - k])
                stores[k].start()
            for store in stores:
                store.wait()

        d_up_own, d_down_own = shape((nd, ur, hidden), F32), shape((dr, width), F32)

        d_up_full, d_down_full = shape((width, hidden), F32), shape((hidden, width), F32)
        x_out, dx, _, _, _, _, _, _, _, _, *grads = call(
            step, [own, own, shape((num_layers, nd * ur, hidden), BF16), act_full, hid_full, hid_full] + [d_up_full, d_down_full] * 2
            + [d_up_own, d_down_own] * 2, 'h' * 14, 'hhhhh',
            [vmem(own)] + [vmem(act_full)] * 2 + [vmem(up_full)] * 2 + [vmem(down_full)] * 2 + [vmem(hid_full)] * 2
            + [pltpu.VMEM((2, hidden // 2, width // 4), F32)] + rx + sums, TR, TS, TL, 0,
            tokens, tokens.reshape(rows // dr, dr, width), grad_out, w_up.reshape(num_layers * ur, ffn), w_down)
        up1_own, down1_own, up0_own, down0_own = grads
        held = [d_up_own, d_up_own, d_down_own, d_down_own, own, own]
        return pl.pallas_call(
            finish, out_shape=[own, own, shape(w_up.shape, F32), shape(w_down.shape, F32)], name='finish',
            in_specs=[pl.BlockSpec(memory_space=pl.ANY)] * 6, out_specs=[pl.BlockSpec(memory_space=pl.ANY)] * 4,
            scratch_shapes=[vmem(like) for like in held] + [pltpu.VMEM(w_up.shape[1:], F32)] * 2 + [pltpu.SemaphoreType.DMA((12,))],
        )(up1_own, up0_own, down1_own, down0_own, x_out, dx)

    return jax.shard_map(device_fn, mesh=mesh, in_specs=(tok_spec, tok_spec, w_spec, w_spec), out_specs=(tok_spec, tok_spec, w_spec, w_spec), check_vma=False)
```

```python
import jax
import jax.numpy as jnp
from jax import lax
from jax.experimental import pallas as pl
from jax.experimental.pallas import tpu as pltpu
from jax.sharding import PartitionSpec as P

NORM_EPS = 1e-6
BOTH_AXES = ('local', 'data')
CONTRACT_ROWS = (((0,), (0,)), ((), ()))
CONTRACT_COLS = (((1,), (1,)), ((), ()))
MESH = pl.DeviceIdType.MESH
RING = 4
F32, BF16 = jnp.float32, jnp.bfloat16

LINK_RATE = 46.0e3
PAIR_RATE = 600e3
LOCAL_RATE = 3000e3
HOP = 2.4
PAIR_HOP = 1.0
ENTRY = 4.2
GELU_C = 0.7978845608028654


class Event:
    def __init__(self, time=None, rank=0):
        self.time, self.rank = time, rank


class Copy:
    def __init__(self, desc, time, remote):
        self.desc, self.time, self.remote, self.rank, self.waited = desc, time, remote, 0, False

    def wait(self):
        if self.remote:
            self.desc.wait_recv()
        else:
            self.desc.wait()


class Credit:
    def __init__(self, semaphore, count, time):
        self.semaphore, self.count, self.time, self.rank, self.waited = semaphore, count, time, 0, False

    def wait(self):
        pl.semaphore_wait(self.semaphore, self.count)


class Pool:
    def __init__(self):
        self.slots, self.next = [], 0

    def again(self):
        self.next = 0
        return self


class Net:
    def __init__(self, send_sems, recv_sems, local_sems, credit_sems):
        self.send_sems, self.recv_sems, self.local_sems, self.credit_sems = send_sems, recv_sems, local_sems, credit_sems
        self.n_remote = self.n_local = 0
        self.free_sends = list(range(send_sems.shape[0]))
        self.free_locals = []
        self.now = 0.0
        self.free = {}
        self.sent = []
        self.flows = []
        here, there = lax.axis_index('local'), lax.axis_index('data')
        pos = {'z': here // RING, 'y': lax.rem(here, RING), 'x': there // 2}
        self.data, self.core = there, lax.rem(there, 2)
        self.ring = {axis: [at] + [lax.rem(at + step, RING) for step in range(1, RING)] for axis, at in pos.items()}
        self.hops = [there] + [lax.rem(there + step, 2 * RING) for step in range(1, 2 * RING)]
        self.blocks = [at * 2 + self.core for at in self.ring['x']]
        self.places = [[z * RING + y for y in self.ring['y']] for z in self.ring['z']]
        self.partner = pos['x'] * 2 + (1 - self.core)
        self.other = 1 - self.core

    def at(self, axis, step):
        return self.ring[axis][step % RING]

    def block(self, step):
        return self.blocks[step % RING]

    def device(self, axis, step):
        if axis == 'p':
            return {'data': self.partner}
        if axis == 'd':
            return {'data': self.hops[step % (2 * RING)]}
        if axis == 'x':
            return {'data': self.block(step)}
        if axis == 'y':
            return {'local': self.places[0][step % RING]}
        return {'local': self.places[step % RING][0]}

    def peers(self, axes):
        return [(axis, step) for axis in axes for step in ((1, -1) if axis in 'xyz' else (1,) if axis == 'p' else range(1, 2 * RING))]

    def signal(self, semaphore, axes):
        for axis, step in self.peers(axes):
            pl.semaphore_signal(semaphore, inc=1, device_id=self.device(axis, step), device_id_type=MESH)

    def arrive(self, axes):
        self.entry, self.entered = pltpu.get_barrier_semaphore(), len(self.peers(axes))
        self.signal(self.entry, axes)

    def enter(self):
        pl.semaphore_wait(self.entry, self.entered)
        self.now = max(self.now, ENTRY)

    def take(self, copies):
        for copy in copies:
            copy.wait()
            copy.waited = True
            self.free_locals.append(copy.slot)
            self.now = max(self.now, copy.time)

    def grant(self, k, axes):
        self.signal(self.credit_sems.at[k], axes)
        return Credit(self.credit_sems.at[k], len(self.peers(axes)), self.now + HOP)

    def drain(self, copies):
        for copy in copies:
            if copy in self.sent:
                copy.desc.wait_send()
                self.sent.remove(copy)
                self.free_sends.append(copy.slot)

    def idle(self, gap):
        over = [copy for copy in self.sent if copy.time + 1.5 < self.now]
        self.drain(over[:int(gap / 0.05)])

    def send(self, src, dst, axis, step=1, pool=None):
        if pool is not None and pool.next < len(pool.slots):
            k = pool.slots[pool.next]
        else:
            k = self.n_remote
            self.n_remote += 1
            if pool is not None:
                pool.slots.append(k)
        if pool is not None:
            pool.next += 1
        if not self.free_sends:
            over = [copy for copy in self.sent if copy.time + 1.0 < self.now]
            self.drain(over or [min(self.sent, key=lambda copy: copy.time)])
        send_slot = self.free_sends.pop()
        desc = pltpu.make_async_remote_copy(
            src_ref=src, dst_ref=dst, send_sem=self.send_sems.at[send_slot], recv_sem=self.recv_sems.at[k],
            device_id=self.device(axis, step), device_id_type=MESH)
        desc.start()
        size = 1
        for n in dst.shape:
            size *= n
        size *= dst.dtype.itemsize
        rate = PAIR_RATE if axis == 'p' else LINK_RATE
        extra = 4.4 if axis == 'd' else 0.0
        if axis == 'd':
            axis, step, size = ('p', 1, size) if step == 1 else ('x', 1 if step < RING + 2 else -1, size)
        key = (axis, step)
        done = max(self.free.get(key, 0.0), self.now) + size / rate
        self.free[key] = done
        copy = Copy(desc, done + extra + (PAIR_HOP if axis == 'p' else HOP), True)
        copy.slot = send_slot
        self.sent.append(copy)
        return copy

    def load(self, src, dst):
        if not self.free_locals:
            self.free_locals.append(self.n_local)
            self.n_local += 1
        k = self.free_locals.pop()
        desc = pltpu.make_async_copy(src, dst, self.local_sems.at[k])
        desc.start()
        size = 1
        for n in dst.shape:
            size *= n
        done = max(self.free.get('hbm', 0.0), self.now) + size * dst.dtype.itemsize / LOCAL_RATE
        self.free['hbm'] = done
        copy = Copy(desc, done + 0.9, False)
        copy.slot = k
        return copy

    def spend(self, microseconds):
        self.now += microseconds

    def spawn(self, flow):
        self.step(flow)

    def step(self, flow):
        try:
            self.flows.append((flow, next(flow)))
        except StopIteration:
            pass

    def run(self):
        while self.flows:
            best = None
            for k, (_, items) in enumerate(self.flows):
                if any(item.time is None for item in items):
                    continue
                time = max([item.time for item in items] + [0.0])
                late = max([item.rank for item in items] + [0])
                rank = (max(time, self.now) + (SLACK if late else 0.0), late, time)
                if best is None or rank < best[0]:
                    best = (rank, k, time)
            _, k, time = best
            flow, items = self.flows.pop(k)
            self.idle(time - self.now)
            for item in items:
                if not isinstance(item, Event) and not item.waited:
                    item.wait()
                    item.waited = True
                    if isinstance(item, Copy) and not item.remote:
                        self.free_locals.append(item.slot)
            self.now = max(self.now, time)
            self.step(flow)

    def finish(self):
        for copy in self.sent:
            copy.desc.wait_send()


def rows_loop(rows, chunk, body):
    chunk = min(chunk, rows)

    def step(k, carry):
        body(pl.ds(pl.multiple_of(k * chunk, chunk), chunk))
        return carry

    lax.fori_loop(0, rows // chunk, step, 0)


def add_into(net, dst, *others):
    rows, cols = dst.shape

    def body(at):
        total = dst[at, :]
        for other in others:
            total = total + other[at, :]
        dst[at, :] = total

    rows_loop(rows, 16, body)
    net.spend(rows * cols * 4 * (1 + len(others)) / 4e6)


def fire(net, event):
    event.time = net.now


def exchange(net, source, dst, done, pool):
    rows = dst.shape[0] // (2 * RING)

    def mine():
        return dst.at[pl.ds(pl.multiple_of(net.data * rows, rows), rows)]

    own = net.load(source(net.data), mine())
    copies = [net.send(source(net.hops[k]), mine(), 'd', k, pool) for k in (4, 5, 2, 3, 6, 7, 1)]
    yield [own] + copies
    net.drain(copies)
    fire(net, done)


def exchange_back(net, src, dst, done, pool):
    rows = dst.shape[1]
    per = src.shape[1] // rows

    def block(k):
        return src.at[lax.div(k, per), pl.ds(pl.multiple_of(lax.rem(k, per) * rows, rows), rows)]

    own = net.load(block(net.data), dst.at[net.data])
    copies = [net.send(block(net.hops[k]), dst.at[net.data], 'd', k, pool) for k in (4, 5, 2, 3, 6, 7, 1)]
    yield [own] + copies
    net.drain(copies)
    fire(net, done)


def copy_rows(net, src, dst):
    def body(at):
        dst[at, :] = src[at, :]

    rows_loop(src.shape[0], 16, body)
    net.spend(0.2)


def gather_x(net, full, done, issued=None, chips=None, pool=None):
    half = full.shape[1] // 2
    lo, hi = pl.ds(0, half), pl.ds(half, half)
    chips = chips or {step: Event() for step in STEPS}
    left = [2]
    done.copies = []

    def send(*args):
        done.copies.append(net.send(*args, pool=pool))
        return done.copies[-1]

    def block(step):
        return full.at[net.block(step)]

    def part(step, rows):
        return full.at[net.block(step), rows]

    relays = []

    def side(step, first, second, mine):
        yield [mine[0]]
        relays.append(send(part(step, first), part(step, first), 'x', -step))
        left[0] -= 1
        if left[0] == 0:
            net.spawn(far())
            if issued is not None:
                fire(net, issued)
        yield [mine[1]]
        pair = send(block(step), block(step), 'p')
        yield [pair]
        fire(net, chips[step])

    def far():
        yield relays
        pair = send(block(2), block(2), 'p')
        yield [pair]
        fire(net, chips[2])

    forth = [send(part(0, rows), part(0, rows), 'x', 1) for rows in (lo, hi)]
    back = [send(part(0, rows), part(0, rows), 'x', -1) for rows in (hi, lo)]
    pair = send(block(0), block(0), 'p')
    net.spawn(side(-1, lo, hi, forth))
    net.spawn(side(1, hi, lo, back))
    yield [pair]
    fire(net, chips[0])
    yield [chips[step] for step in STEPS]
    fire(net, done)


def gather_yz(net, own, full, first, done, issued=None, offset=0, near=False, split=True, pool=None):
    second = 'y' if first == 'z' else 'z'
    done.copies = []

    def emit(*args):
        done.copies.append(net.send(*args, pool=pool))
        return done.copies[-1]

    size = own.shape[0]
    half = size // 2
    lo, hi, both = pl.ds(offset, half), pl.ds(offset + half, half), pl.ds(offset, size)
    forward, backward = ((lo, hi), (hi, lo)) if split and not near else ((both,), (both,))

    def part(one, two, rows):
        return full.at[yz_index(net, first, one, two), rows]

    left = [3 if near else RING, 3 if near else RING]

    def arrived(which):
        left[which] -= 1
        if left[which] == 0 and (done, issued)[which] is not None:
            fire(net, (done, issued)[which])

    def send(one, rows, axis, step):
        src = own.at[pl.ds(rows.start - offset, rows.size)] if one == 0 else part(one, 0, rows)
        return emit(src, part(one, 0, rows), axis, step)

    def column(one):
        forth = [send(one, rows, second, 1) for rows in forward]
        back = [send(one, rows, second, -1) for rows in backward]

        def finish():
            if near:
                arrived(1)
                yield forth + back
            else:
                yield [forth[0]]
                relays = [emit(part(one, -1, lo), part(one, -1, lo), second, 1)]
                yield [back[0]]
                relays.append(emit(part(one, 1, hi), part(one, 1, hi), second, -1))
                arrived(1)
                yield forth[1:] + back[1:] + relays
            arrived(0)

        net.spawn(finish())

    relays = []

    def side(step, first_half, mine):
        yield [mine[0]]
        if not near:
            relays.append(emit(part(step, 0, first_half), part(step, 0, first_half), first, -step))
            if len(relays) == 2:
                net.spawn(far())
        yield mine[1:]
        column(step)

    def far():
        yield relays
        column(2)

    mine = [net.load(own, part(0, 0, both))]
    forth = [send(0, rows, first, 1) for rows in forward]
    back = [send(0, rows, first, -1) for rows in backward]
    column(0)
    net.spawn(side(-1, lo, forth))
    net.spawn(side(1, hi, back))
    left[0] += 1
    yield mine
    arrived(0)


def yz_index(net, first, one, two):
    return net.places[one % RING][two % RING] if first == 'z' else net.places[two % RING][one % RING]


STEPS = (2, 1, -1, 0)


def reduce_x(net, part, made, scratch, done, pool=None, relayed=None):
    other, relay_f, relay_b, last_f, last_b = scratch
    half = part.shape[2] // 2
    lo, hi = pl.ds(0, half), pl.ds(half, half)

    def acc(k, rows=None):
        return part.at[k, net.core] if rows is None else part.at[k, net.core, rows]

    pairs = [None] * RING
    ready = [Event() for _ in STEPS]

    def pair(k):
        yield [made[k]]
        pairs[k] = net.send(part.at[k, net.other], other.at[k], 'p', pool=pool)
        yield [pairs[k]]
        add_into(net, acc(k), other.at[k])
        fire(net, ready[k])

    for k in range(RING):
        net.spawn(pair(k))
    sent = {}
    started, relayed = Event(), relayed or Event()

    def part_flow(k):
        yield [ready[k]] + ([relayed] if k else [])
        if k == 0:
            sent['first_f'] = net.send(acc(0, lo), relay_f, 'x', 1, pool=pool)
            sent['first_b'] = net.send(acc(0, hi), relay_b, 'x', -1, pool=pool)
            fire(net, relayed)
        elif k == 1:
            sent['direct_f'] = net.send(acc(1, hi), last_f.at[hi], 'x', 1, pool=pool)
        else:
            sent['direct_b'] = net.send(acc(2, lo), last_b.at[lo], 'x', -1, pool=pool)
        if len(sent) == 4:
            fire(net, started)

    for k in range(3):
        net.spawn(part_flow(k))
    yield [started]
    yield [sent['first_f']]
    add_into(net, acc(1, lo), relay_f)
    summed_f = net.send(acc(1, lo), last_f.at[lo], 'x', 1, pool=pool)
    yield [sent['first_b']]
    add_into(net, acc(2, hi), relay_b)
    summed_b = net.send(acc(2, hi), last_b.at[hi], 'x', -1, pool=pool)
    yield [ready[3], sent['direct_f'], sent['direct_b'], summed_f, summed_b]
    add_into(net, acc(3), last_f, last_b)
    done.copies = pairs + list(sent.values()) + [summed_f, summed_b]
    fire(net, done)


def reduce_x_scratch(rows, cols):
    return [pltpu.VMEM((RING, rows, cols), F32), pltpu.VMEM((rows // 2, cols), F32), pltpu.VMEM((rows // 2, cols), F32),
            pltpu.VMEM((rows, cols), F32), pltpu.VMEM((rows, cols), F32)]


class Sums:
    def __init__(self, net, first, scratch, stage):
        self.net, self.first, self.scratch, self.stage = net, first, scratch, stage
        self.second = 'y' if first == 'z' else 'z'

    def run(self, place, start, done, free, passed_all, pool, window, lead):
        net, first, second = self.net, self.first, self.second
        relay1, last1, relay2, last2 = self.scratch
        ahead, behind, mine = self.stage
        half = mine.shape[0] // 2
        lo, hi, all_rows = pl.ds(0, half), pl.ds(half, half), pl.ds(0, 2 * half)
        done.copies = []

        def send(*args):
            done.copies.append(net.send(*args, pool=pool))
            return done.copies[-1]

        def term(one, two, rows=all_rows):
            return place(yz_index(net, first, one, two), rows)

        def bring(gate, src, dst, got):
            yield [gate, start]
            yield [net.load(src, dst)]
            fire(net, got)

        chain = [[gate] + [Event() for _ in range(RING)] for gate in free]
        free[:] = [events[RING] for events in chain]
        got = [[Event() for _ in range(RING)] for _ in range(3)]
        ends = [Event() for _ in STEPS]
        passed = [Event() for _ in range(RING)]
        passed[lead] = passed_all

        def ring(k):
            two = STEPS[k]
            if k >= window:
                yield [passed[k - window]]
            net.spawn(bring(chain[0][k], term(1, two, lo), ahead, got[0][k]))
            net.spawn(bring(chain[1][k], term(-1, two, hi), behind, got[1][k]))
            net.spawn(bring(chain[2][k], term(0, two), mine, got[2][k]))
            first_f = send(term(2, two, lo), relay1.at[0, k], first, 1)
            first_b = send(term(2, two, hi), relay1.at[1, k], first, -1)
            direct_f = send(term(1, two, hi), last1.at[0, k, hi], first, 1)
            direct_b = send(term(-1, two, lo), last1.at[1, k, lo], first, -1)
            yield [first_f, got[0][k]]
            add_into(net, relay1.at[0, k], ahead)
            fire(net, chain[0][k + 1])
            summed_f = send(relay1.at[0, k], last1.at[0, k, lo], first, 1)
            yield [first_b, got[1][k]]
            add_into(net, relay1.at[1, k], behind)
            fire(net, chain[1][k + 1])
            summed_b = send(relay1.at[1, k], last1.at[1, k, hi], first, -1)
            fire(net, passed[k])
            yield [direct_f, direct_b, summed_f, summed_b, got[2][k]]
            add_into(net, last1.at[0, k], last1.at[1, k], mine)
            fire(net, chain[2][k + 1])
            fire(net, ends[k])

        def sums(k, rows=all_rows):
            return last1.at[0, k, rows]

        yield [start]
        for k in range(RING):
            net.spawn(ring(k))
        yield [ends[0]]
        first_f = send(sums(0, lo), relay2.at[0], second, 1)
        first_b = send(sums(0, hi), relay2.at[1], second, -1)
        yield [ends[1]]
        direct_f = send(sums(1, hi), last2.at[0, hi], second, 1)
        yield [ends[2]]
        direct_b = send(sums(2, lo), last2.at[1, lo], second, -1)
        yield [first_f]
        add_into(net, sums(1, lo), relay2.at[0])
        summed_f = send(sums(1, lo), last2.at[0, lo], second, 1)
        yield [first_b]
        add_into(net, sums(2, hi), relay2.at[1])
        summed_b = send(sums(2, hi), last2.at[1, hi], second, -1)
        yield [ends[3], direct_f, direct_b, summed_f, summed_b]
        add_into(net, sums(3), last2.at[0], last2.at[1])
        done.total = sums(3)
        fire(net, done)


def sums_scratch(rows, cols):
    return [pltpu.VMEM((2, RING, rows // 2, cols), F32), pltpu.VMEM((2, RING, rows, cols), F32),
            pltpu.VMEM((2, rows // 2, cols), F32), pltpu.VMEM((2, rows, cols), F32)]


def sums_stage(rows, cols):
    return [pltpu.VMEM((rows // 2, cols), F32), pltpu.VMEM((rows // 2, cols), F32), pltpu.VMEM((rows, cols), F32)]


def norm_rows(x_ref, u_ref):
    def body(at):
        x = x_ref[at, :].astype(F32)
        u_ref[at, :] = (x * lax.rsqrt(jnp.mean(x * x, axis=-1, keepdims=True) + NORM_EPS)).astype(BF16)

    rows_loop(x_ref.shape[0], 16, body)


def norm_back_rows(x_ref, dy_of, du_ref, dx_ref):
    def body(at):
        x = x_ref[at, :].astype(F32)
        du = du_ref[at, :]
        r = lax.rsqrt(jnp.mean(x * x, axis=-1, keepdims=True) + NORM_EPS)
        xr = x * r
        dx_ref[at, :] = (dy_of(at).astype(F32) + r * (du - xr * jnp.mean(xr * du, axis=-1, keepdims=True))).astype(BF16)

    rows_loop(x_ref.shape[0], 16, body)


def add_rows(x_ref, y_ref, out_ref):
    def body(at):
        out_ref[at, :] = (x_ref[at, :].astype(F32) + y_ref[at, :]).astype(BF16)

    rows_loop(x_ref.shape[0], 16, body)


def swap_halves(even, odd):
    low = lax.broadcasted_iota(jnp.int32, even.shape, len(even.shape) - 1) < even.shape[-1] // 2
    shift = even.shape[-1] // 2
    axis = len(even.shape) - 1
    return jnp.where(low, even, pltpu.roll(odd, shift, axis)), jnp.where(low, pltpu.roll(even, shift, axis), odd)


def split_columns(w_ref, cols_ref, layers):
    pieces, _, wide = w_ref.shape
    rows = layers
    tile = pieces * wide // (4 * RING * RING)
    for x in range(RING):
        for p in range(wide // tile):
            pair = []
            for i in (2 * p, 2 * p + 1):
                at = (i * RING + x) * tile
                pair.append(w_ref[at // wide, pl.ds(0, rows), pl.ds(at % wide, tile)].astype(F32))
            for c, value in enumerate(swap_halves(*pair)):
                cols_ref[2 * x + c, pl.ds(0, rows), pl.ds(p * tile, tile)] = value.astype(cols_ref.dtype)


def join_columns(cols_ref, w_ref):
    tile = w_ref.shape[1] // (4 * RING * RING)
    for x in range(RING):
        for p in range(cols_ref.shape[2] // tile):
            pair = [cols_ref[2 * x + c, :, pl.ds(p * tile, tile)] for c in range(2)]
            for i, value in zip((2 * p, 2 * p + 1), swap_halves(*pair)):
                w_ref[:, pl.ds((i * RING + x) * tile, tile)] = value


def call(body, out_shape, out_spaces, in_spaces, scratch, remote, sends, local, collective_id, *args):
    spaces = {'v': pl.BlockSpec(memory_space=pltpu.VMEM), 'h': pl.BlockSpec(memory_space=pl.ANY)}

    def kernel(*refs):
        net = Net(*refs[-5:-1])
        net.tile_sems = refs[-1]
        body(net, *refs[:-5])
        net.finish()
        assert net.n_remote <= remote and net.n_local <= local, (body.__name__, net.n_remote, net.n_local)

    return pl.pallas_call(
        kernel, out_shape=out_shape, in_specs=[spaces[s] for s in in_spaces], out_specs=[spaces[s] for s in out_spaces],
        scratch_shapes=list(scratch) + [pltpu.SemaphoreType.DMA((sends,)), pltpu.SemaphoreType.DMA((remote,)), pltpu.SemaphoreType.DMA((local,)),
                                               pltpu.SemaphoreType.REGULAR((14,)), pltpu.SemaphoreType.DMA((2,))],
        compiler_params=pltpu.CompilerParams(collective_id=collective_id, has_side_effects=True, vmem_limit_bytes=67000000),
        cost_estimate=pl.CostEstimate(flops=10**8, bytes_accessed=10**7, transcendentals=0),
        name=body.__name__)(*args)


WIDE = 512
EARLY = 3
GRAD_TIME = 4.25
SLACK = 0.3
R_HIDDEN, R_DOWN, R_BACK, R_TURN, R_DDOWN, R_DDOWN2, R_DUP, R_OUT, R_PRE, R_GUP, R_GDOWN, R_DX = 2, 1, 3, 1, 2, 2, 4, 2, 2, 3, 3, 2
R_DU, HOLD = (3, 3.1, 3.2, 3.3), (0, 1, 2)
WINDOWS = (2, 2, 2, 2, 2, 2, 2, 2)
AXES = ('yz', 'yz', 'yz', 'yz')
TOP = 6
NEAR = 'z'
LEAD = (3, 3, 3)
TR, TS, TL = 264, 56, 9


def wide_loop(total, body):
    wide = min(WIDE, total)

    def step(k, carry):
        body(k, wide, pl.ds(pl.multiple_of(k * wide, wide), wide))
        return carry

    lax.fori_loop(0, total // wide, step, 0)


def flat(value):
    return value.reshape(value.shape[0] * value.shape[1], value.shape[2])


def dot_rows(a, b):
    return jnp.dot(flat(a), flat(b), preferred_element_type=F32)


def dot_cols(a, b):
    return lax.dot_general(flat(a), flat(b), CONTRACT_COLS, preferred_element_type=F32)


def gelu(a):
    return 0.5 * a * (1.0 + jnp.tanh(GELU_C * (a + 0.044715 * a * a * a)))


def hidden_rows(net, chip, u, up, a, s):
    at = pl.ds(chip * 2, 2)

    def body(_, wide, cols):
        pre = dot_rows(u[at], up[:, :, cols]).astype(BF16)
        a[at, :, cols] = pre.reshape(2, -1, wide)
        s[at, :, cols] = gelu(pre.astype(F32)).astype(BF16).reshape(2, -1, wide)

    wide_loop(up.shape[2], body)
    net.spend(1.7)


def down_rows(net, chip, s, down, part):
    at = pl.ds(chip * 2, 2)

    def body(_, wide, cols):
        part[:, :, cols] = dot_rows(s[at], down[:, :, cols]).reshape(2, -1, wide)

    wide_loop(down.shape[2], body)
    net.spend(1.76)


def hidden_back_rows(net, chip, dy, down, ds):
    at = pl.ds(chip * 2, 2)
    rows = down.shape[1]

    def body(k, wide, cols):
        blocks = pl.ds(k * (wide // rows), wide // rows)
        ds[at, :, cols] = dot_cols(dy[at], down[blocks]).astype(BF16).reshape(2, -1, wide)

    wide_loop(down.shape[0] * rows, body)
    net.spend(1.5)


def gelu_both(a):
    t = jnp.tanh(GELU_C * (a + 0.044715 * a * a * a))
    return 0.5 * a * (1.0 + t), 0.5 * (1.0 + t) + 0.5 * a * (1.0 - t * t) * (GELU_C * (1.0 + 3 * 0.044715 * a * a))


def hidden_turn_rows(net, chip, u, up, s, ds):
    at = pl.ds(chip * 2, 2)

    def body(_, wide, cols):
        pre = dot_rows(u[at], up[:, :, cols]).astype(BF16).astype(F32)
        value, slope = gelu_both(pre)
        s[at, :, cols] = value.astype(BF16).reshape(2, -1, wide)
        ds[at, :, cols] = (ds[at, :, cols].astype(F32) * slope.reshape(2, -1, wide)).astype(BF16)

    wide_loop(up.shape[2], body)
    net.spend(2.1)


def pre_back_rows(net, chip, dy, down, a, da):
    at = pl.ds(chip * 2, 2)
    rows = down.shape[1]

    def body(k, wide, cols):
        blocks = pl.ds(k * (wide // rows), wide // rows)
        ds = dot_cols(dy[at], down[blocks]).astype(BF16).astype(F32).reshape(2, -1, wide)
        da[at, :, cols] = (ds * gelu_both(a[at, :, cols].astype(F32))[1]).astype(BF16)

    wide_loop(down.shape[0] * rows, body)
    net.spend(1.95)


def input_back_rows(net, chip, da, up, part):
    at = pl.ds(chip * 2, 2)
    rows = up.shape[1]

    def body(k, wide, cols):
        blocks = pl.ds(k * (wide // rows), wide // rows)
        part[:, :, cols] = dot_cols(da[at], up[blocks]).reshape(2, -1, wide)

    wide_loop(up.shape[0] * rows, body)
    net.spend(1.9)


def stored_tiles(net, count, compute, stage, out):
    def store(t):
        return pltpu.make_async_copy(stage.at[lax.rem(t, 2)], out(t), net.tile_sems.at[lax.rem(t, 2)])

    def step(t, carry):
        @pl.when(t >= 2)
        def _():
            store(t - 2).wait()

        compute(t, stage.at[lax.rem(t, 2)])
        store(t).start()
        return carry

    lax.fori_loop(0, count, step, 0)
    for t in range(max(count - 2, 0), count):
        store(jnp.int32(t)).wait()


def dot_tokens(a, b):
    return lax.dot_general(flat(a), flat(b), CONTRACT_ROWS, preferred_element_type=F32)


def grad_tiles(net, lhs, rhs, stage, out):
    _, high, wide = stage.shape
    across = rhs.shape[2] // wide

    def columns(t):
        return pl.ds(pl.multiple_of(lax.rem(t, across) * wide, wide), wide)

    def rows(t):
        return pl.ds(pl.multiple_of(lax.div(t, across) * high, high), high)

    def compute(t, slot):
        slot[...] = dot_tokens(lhs[:, :, rows(t)], rhs[:, :, columns(t)])

    stored_tiles(net, lhs.shape[2] // high * across, compute, stage, lambda t: out.at[rows(t), columns(t)])
    net.spend(GRAD_TIME * lhs.shape[2] / 1024)


def solution(mesh):
    nl, nd = mesh.shape['local'], mesh.shape['data']
    tok_spec = P(BOTH_AXES, None)
    w_spec = P(None, BOTH_AXES, None)

    def device_fn(tokens, grad_out, w_up, w_down):
        num_layers, ur, ffn = w_up.shape
        dr = w_down.shape[1]
        rows, width = tokens.shape
        hidden = nl * dr
        shape = jax.ShapeDtypeStruct
        up_full = shape((nl, nd * ur, hidden), BF16)
        down_full = shape((nl, dr, width), BF16)
        act_full = shape((nd, rows, width), BF16)
        hid_full = shape((nd, rows, hidden), BF16)
        own = shape((rows, width), BF16)
        part_vmem = pltpu.VMEM((RING, 2, rows, width), F32)
        rx = [part_vmem] + reduce_x_scratch(rows, width)
        sums = sums_scratch(dr, hidden) * 4 + sums_stage(dr, hidden) * 2

        def vmem(like):
            return pltpu.VMEM(like.shape, like.dtype)

        def step(net, x_in, x_halves, g_in, w_up_in, w_down_in,
                 x_out, dx_out, block_out, u_out, a_out, s_out, d_up0, d_down0, d_up1, d_down1, dw_up1, dw_down1, dw_up0, dw_down0,
                 x, u, g, up0, up1, down0, down1, ds, s, stage, part, *scratch):
            net.arrive('dyz')
            rx_scratch = scratch[:5]
            names = ('blocks', 'blocks1', 'sent_u', 'got_u', 'got_g', 'sent_up0', 'sent_down0', 'sent_up1', 'sent_down1', 'got_up0', 'got_down0',
                     'got_up1', 'got_down1', 'saved', 'free0', 'reduced0', 'ds_made', 'got_u1', 'hidden', 'all_du', 'reduced1', 'sent_dy', 'got_dy',
                     'back_up0', 'back_up0_rest', 'back_down0', 'd_down1', 'd_up1', 'y_reduced', 'acts', 'd_down0', 'da0', 'd_up0', 'du_reduced',
                     'out_up1', 'out_up0', 'got_u0', 'y_made', 'x_saved', 'weights_in', 'd_down1_0', 'relayed0')
            ev = {name: Event() for name in names}
            for kind in ('up', 'down'):
                for layer in range(2):
                    for k in range(2):
                        ev['sum_%s%d%d' % (kind, layer, k)] = Event()
            ev['got_up0'].rank = R_HIDDEN
            hidden_made, made0, made1, y_made, du_made = ([Event() for _ in STEPS] for _ in range(5))
            wide = width // 2
            half_up = nd * ur // 2
            act_pool, rs_pool = Pool(), Pool()
            job_pools = [[Pool(), Pool()], [Pool(), Pool()]]
            pools = {'up0': [Pool(), Pool()], 'down0': [Pool(), Pool()], 'up1': job_pools[0], 'down1': job_pools[1], 'blocks': [Pool(), Pool()]}
            stages = (scratch[21:24], scratch[24:27])
            job_scratch = [[scratch[5 + 8 * n + 4 * k:9 + 8 * n + 4 * k] for k in range(2)] for n in range(2)]
            frees = [[Event(0.0) for _ in range(3)] for _ in range(2)]
            freed = {k: Event() for k in range(10, 14)}

            def columns(h):
                return pl.ds(h * wide, wide)

            inputs = [net.load(x_in, x)]
            inputs += [net.load(w_up_in.at[:, pl.ds(k * hidden, hidden)], ds.at[k, pl.ds(0, num_layers * ur)]) for k in range(nd)]

            def gather(name, own, full, split):
                size = own.shape[0] // 2

                def join(kind, events):
                    yield events
                    if kind == 'got_':
                        ev[kind + name].copies = events[0].copies + events[1].copies
                    fire(net, ev[kind + name])

                got, sent = [Event(), Event()], [Event(), Event()]
                for k, first in enumerate('yz'):
                    net.spawn(gather_yz(net, own.at[pl.ds(k * size, size)], full, first, got[k], sent[k], k * size, split=split, pool=pools[name][k]))
                net.spawn(join('got_', got))
                net.spawn(join('sent_', sent))

            net.take(inputs)
            split_columns(ds, s, num_layers * ur)
            norm_rows(x, u.at[net.data])
            net.enter()
            gather('down0', w_down_in.at[0], down0, False)
            net.spawn(exchange(net, lambda k: s.at[k, pl.ds(0, ur)], block_out.at[0], ev['blocks'], pools['blocks'][0]))
            own_grads = net.load(g_in, g.at[net.data])

            def up_first():
                yield [ev['blocks']]
                gather('up0', block_out.at[0], up0, True)
                net.spawn(gather_x(net, u, ev['got_u'], ev['sent_u'], pool=act_pool))
                yield [ev['sent_u']]
                net.spawn(exchange(net, lambda k: s.at[k, pl.ds(ur, ur)], block_out.at[1], ev['blocks1'], pools['blocks'][1]))
                yield [own_grads]
                net.spawn(gather_x(net, g, ev['got_g']))

            def second():
                yield [ev['sent_up0'], ev['sent_down0'], ev['blocks1']]
                gather('down1', w_down_in.at[1], down1, False)
                yield [made0[EARLY]]
                gather('up1', block_out.at[1], up1, True)

            def hidden_flow():
                yield [ev['got_u'], ev['got_up0'], ev['blocks1']]
                for k, step in enumerate(STEPS):
                    hidden_rows(net, net.at('x', step), u, up0, ds, s)
                    fire(net, hidden_made[k])
                    yield [Event(net.now, R_HIDDEN)] + ([ev['relayed0']] if k == 1 else [])
                yield [net.load(ds, a_out), net.load(s, s_out), net.load(u, u_out)]
                fire(net, ev['saved'])

            def down_flow():
                for k, step in enumerate(STEPS):
                    yield [hidden_made[k], ev['got_down0'], Event(0.0, R_DOWN)] + ([ev['relayed0']] if k == 1 else [])
                    down_rows(net, net.at('x', step), s, down0, part.at[k])
                    fire(net, made0[k])
                fire(net, ev['free0'])

            net.spawn(reduce_x(net, part, made0, rx_scratch, ev['reduced0'], rs_pool, ev['relayed0']))
            here = {step: Event() for step in STEPS}
            dy_here = {step: Event() for step in STEPS}

            def next_layer():
                yield [ev['saved'], ev['got_g']]
                net.drain(ev['got_u'].copies + ev['got_g'].copies)
                credit = net.grant(3, 'xp')
                yield [ev['reduced0'], credit]
                add_rows(x, part.at[3, net.core], x)
                norm_rows(x, u.at[net.data])
                net.spend(1.0)
                net.spawn(gather_x(net, u, ev['got_u1'], chips=here, pool=act_pool.again()))
                net.drain(ev['reduced0'].copies)
                yield [net.grant(4, 'xp')]
                net.spawn(reduce_x(net, part, made1, rx_scratch, ev['reduced1'], rs_pool.again()))

            def back_flow():
                for k, step in enumerate(STEPS):
                    yield [ev['got_g'], ev['got_down1'], ev['saved'], Event(0.0, R_BACK)]
                    hidden_back_rows(net, net.at('x', step), g, down1, ds)
                fire(net, ev['ds_made'])

            def again():
                top = nd * ur * TOP // 8
                yield [ev['free0'], ev['ds_made']]
                net.drain(ev['got_up0'].copies + ev['got_down0'].copies)
                credit = net.grant(6, 'yz')
                yield [credit]
                net.spawn(gather_yz(net, w_down_in.at[0], down0, NEAR, ev['back_down0'], near=True, pool=pools['down0'][1].again()))
                net.spawn(gather_yz(net, block_out.at[0, pl.ds(0, top)], up0, 'y', ev['back_up0'], pool=pools['up0'][0].again()))
                net.spawn(gather_yz(net, block_out.at[0, pl.ds(top, nd * ur - top)], up0, 'z', ev['back_up0_rest'], offset=top, pool=pools['up0'][1].again()))

            def weights():
                yield [ev['got_up1'], ev['got_down1']]
                yield [net.grant(7, 'yz')]
                fire(net, ev['weights_in'])

            left = [RING, RING]

            turned = [Event() for _ in STEPS]

            def layer1(k, step):
                yield [here[step], ev['ds_made'], ev['got_up1'], Event(0.0, R_TURN)]
                hidden_turn_rows(net, net.at('x', step), u, up1, s, ds)
                fire(net, turned[k])
                left[0] -= 1
                if left[0] == 0:
                    fire(net, ev['hidden'])

            def layer1_back(k, step):
                yield [turned[k], Event(0.0, R_DU[k])] + ([ev['hidden']] if k in HOLD else [])
                input_back_rows(net, net.at('x', step), ds, up1, part.at[k])
                fire(net, made1[k])
                left[1] -= 1
                if left[1] == 0:
                    fire(net, ev['all_du'])

            def grads1():
                for h in range(2):
                    yield [Event(0.0, R_DDOWN2 if h else R_DDOWN), ev['hidden']]
                    grad_tiles(net, s, g.at[:, :, columns(h)], stage, d_down1.at[:, columns(h)])
                    fire(net, ev['d_down1' if h else 'd_down1_0'])
                for h in range(2):
                    yield [Event(net.now, R_DUP)]
                    grad_tiles(net, u.at[:, :, columns(h)], ds, stage, d_up1.at[columns(h)])
                fire(net, ev['d_up1'])

            def act():
                yield [ev['d_up1'], ev['all_du'], ev['got_u1']]
                own_g = [net.load(g_in.at[:, columns(h)], ds.at[h]) for h in range(2)]
                net.drain(ev['got_u1'].copies)
                credit = net.grant(5, 'xp')
                yield [ev['reduced1'], credit] + own_g
                norm_back_rows(x, lambda at: jnp.concatenate([ds[h, at, :] for h in range(2)], axis=-1), part.at[3, net.core], u.at[net.data])
                net.spend(0.7)
                net.spawn(gather_x(net, u, ev['got_dy'], ev['sent_dy'], dy_here, pool=act_pool.again()))

            def layer1_out():
                yield [ev['reduced1'], Event(0.0, R_OUT)]
                net.drain(ev['reduced1'].copies)
                credit = net.grant(8, 'xp')
                for k, step in enumerate(STEPS):
                    down_rows(net, net.at('x', step), s, down1, part.at[k])
                    yield [Event(net.now, R_OUT)]
                fire(net, ev['y_made'])
                yield [ev['sent_dy'], credit]
                net.spawn(reduce_x(net, part, y_made, rx_scratch, ev['y_reduced'], rs_pool.again()))
                for k in range(RING):
                    fire(net, y_made[k])
                yield [ev['y_reduced']]
                add_rows(x, part.at[3, net.core], x)
                yield [net.load(x, x_out)]
                fire(net, ev['x_saved'])

            a0, s0 = up1.at[pl.ds(0, nd)], up1.at[pl.ds(nd, nd)]
            backs = [RING]

            def bring_back():
                yield [ev['d_down1']]
                yield [net.load(u_out, g)]
                fire(net, ev['got_u0'])

            def bring_acts():
                yield [ev['all_du']]
                net.drain(ev['got_up1'].copies)
                yield [net.load(a_out, a0), net.load(s_out, s0)]
                fire(net, ev['acts'])

            def layer0_hidden(step):
                yield [dy_here[step], ev['acts'], ev['back_down0'], ev['d_up1'], Event(0.0, R_PRE)]
                pre_back_rows(net, net.at('x', step), u, down0, a0, ds)
                backs[0] -= 1
                if backs[0] == 0:
                    fire(net, ev['da0'])

            def layer0():
                for h in range(2):
                    yield [ev['da0'], ev['got_u0'], Event(0.0, R_GUP)]
                    grad_tiles(net, g.at[:, :, columns(h)], ds, stage, d_up0.at[columns(h)])
                fire(net, ev['d_up0'])
                for h in range(2):
                    yield [ev['got_dy'], ev['acts'], Event(0.0, R_GDOWN)]
                    grad_tiles(net, s0, u.at[:, :, columns(h)], stage, d_down0.at[:, columns(h)])
                fire(net, ev['d_down0'])
                yield [ev['y_reduced'], ev['back_up0'], ev['back_up0_rest'], Event(0.0, R_DX)]
                net.drain(ev['y_reduced'].copies + ev['got_down1'].copies)
                x0 = down1.at[pl.ds(0, x_halves.shape[0])]
                yield [net.grant(9, 'xp'), net.load(x_halves, x0)]
                net.spawn(reduce_x(net, part, du_made, rx_scratch, ev['du_reduced'], rs_pool.again()))
                for k, step in enumerate(STEPS):
                    input_back_rows(net, net.at('x', step), ds, up0, part.at[k])
                    fire(net, du_made[k])
                    yield [Event(net.now, R_DX)]
                yield [ev['du_reduced'], ev['x_saved']]
                for q in range(x_halves.shape[0]):
                    rows_q = pl.ds(q * dr, dr)
                    dy_q = u.at[net.data, rows_q]
                    norm_back_rows(x0.at[q], lambda at, dy_q=dy_q: dy_q[at, :], part.at[3, net.core, rows_q], x.at[rows_q])
                yield [net.load(x, dx_out)]

            def up_place(ref, k):
                return lambda block, rows: ref.at[pl.ds(pl.multiple_of(block * (2 * half_up) + k * half_up + rows.start, rows.size), rows.size)]

            def down_place(ref, k):
                return lambda block, rows: ref.at[pl.ds(pl.multiple_of(block * dr + rows.start, rows.size), rows.size), columns(k)]

            def gate(event, items, pool):
                yield items
                pool.again()
                fire(net, event)

            def sum_job(job, place, ref, ready, name, credits=()):
                passed = [Event(), Event()]
                for k in range(2):
                    start = Event()
                    n = job % 2
                    net.spawn(gate(start, ready[k] + ([credits[k]] if credits else []), job_pools[n][k]))
                    sums = Sums(net, AXES[job][k], job_scratch[n][k], stages[k])
                    net.spawn(sums.run(place(ref, k), start, ev['sum_%s%d' % (name, k)], frees[k], passed[k], job_pools[n][k], WINDOWS[2 * job + k], LEAD[min(job, 2)]))
                return passed

            def out_down(layer, dw_down, credit):
                def one(k):
                    done = ev['sum_down%d%d' % (layer, k)]
                    yield [done]
                    yield [net.load(done.total, dw_down.at[:, columns(k)])]
                    if credit is not None:
                        net.drain(done.copies)
                        yield [net.grant(credit + k, 'yz')]
                        fire(net, freed[credit + k])

                for k in range(2):
                    net.spawn(one(k))

            def out_up(n, layer, dw_up, credit):
                totals = [ev['sum_up%d%d' % (layer, k)] for k in range(2)]
                yield totals
                net.drain(totals[0].copies + totals[1].copies)
                spare = job_scratch[n][0][0].at[0]
                for k, done in enumerate(totals):
                    for q in range(2):
                        copy_rows(net, done.total.at[pl.ds(q * spare.shape[1], spare.shape[1])], spare.at[2 * k + q])
                done = ev['out_up%d' % layer]
                net.spawn(exchange_back(net, spare, dw_up, done, pools['blocks'][layer].again()))
                if credit is not None:
                    yield [done]
                    for k in range(2):
                        yield [net.grant(credit + k, 'yz')]
                        fire(net, freed[credit + k])

            passed = sum_job(0, down_place, d_down1, [[ev['d_down1_0'], ev['weights_in']], [ev['d_down1'], ev['weights_in']]], 'down1')
            passed = sum_job(1, up_place, d_up1, [[ev['d_up1']] + passed] * 2, 'up1')
            passed = sum_job(2, up_place, d_up0, [[ev['d_up0']] + passed] * 2, 'up0', [freed[10], freed[11]])
            sum_job(3, down_place, d_down0, [[ev['d_down0']] + passed] * 2, 'down0', [freed[12], freed[13]])
            out_down(1, dw_down1, 10)
            net.spawn(out_up(1, 1, dw_up1, 12))
            net.spawn(out_up(0, 0, dw_up0, None))
            out_down(0, dw_down0, None)
            for k in (3, 2, 1, 0):
                net.spawn(layer1(k, STEPS[k]))
            for k in range(RING):
                net.spawn(layer1_back(k, STEPS[k]))
            for step in (0, -1, 1, 2):
                net.spawn(layer0_hidden(step))
            for flow in (up_first(), second(), hidden_flow(), down_flow(), next_layer(), back_flow(), again(), weights(), grads1(), act(), layer1_out(),
                         bring_back(), bring_acts(), layer0()):
                net.spawn(flow)
            net.run()

        def finish(*refs):
            sources, targets, held, ups, sems = refs[:6], refs[6:10], refs[10:16], refs[16:18], refs[18]
            x_out, dx_out, up_out, down_out = targets
            loads = [pltpu.make_async_copy(src, dst, sems.at[k]) for k, (src, dst) in enumerate(zip(sources, held))]
            stores = [(ups[1], up_out.at[1]), (ups[0], up_out.at[0]), (held[2], down_out.at[1]), (held[3], down_out.at[0]), (held[4], x_out), (held[5], dx_out)]
            stores = [pltpu.make_async_copy(src, dst, sems.at[6 + k]) for k, (src, dst) in enumerate(stores)]
            for load in loads:
                load.start()
            for k in (2, 3, 4, 5):
                loads[k].wait()
                stores[k].start()
            for k in (0, 1):
                loads[k].wait()
                join_columns(held[k], ups[1 - k])
                stores[k].start()
            for store in stores:
                store.wait()

        d_up_own, d_down_own = shape((nd, ur, hidden), F32), shape((dr, width), F32)

        d_up_full, d_down_full = shape((width, hidden), F32), shape((hidden, width), F32)
        x_out, dx, _, _, _, _, _, _, _, _, *grads = call(
            step, [own, own, shape((num_layers, nd * ur, hidden), BF16), act_full, hid_full, hid_full] + [d_up_full, d_down_full] * 2
            + [d_up_own, d_down_own] * 2, 'h' * 14, 'hhhhh',
            [vmem(own)] + [vmem(act_full)] * 2 + [vmem(up_full)] * 2 + [vmem(down_full)] * 2 + [vmem(hid_full)] * 2
            + [pltpu.VMEM((2, hidden // 2, width // 4), F32)] + rx + sums, TR, TS, TL, 0,
            tokens, tokens.reshape(rows // dr, dr, width), grad_out, w_up.reshape(num_layers * ur, ffn), w_down)
        up1_own, down1_own, up0_own, down0_own = grads
        held = [d_up_own, d_up_own, d_down_own, d_down_own, own, own]
        return pl.pallas_call(
            finish, out_shape=[own, own, shape(w_up.shape, F32), shape(w_down.shape, F32)], name='finish',
            in_specs=[pl.BlockSpec(memory_space=pl.ANY)] * 6, out_specs=[pl.BlockSpec(memory_space=pl.ANY)] * 4,
            scratch_shapes=[vmem(like) for like in held] + [pltpu.VMEM(w_up.shape[1:], F32)] * 2 + [pltpu.SemaphoreType.DMA((12,))],
        )(up1_own, up0_own, down1_own, down0_own, x_out, dx)

    return jax.shard_map(device_fn, mesh=mesh, in_specs=(tok_spec, tok_spec, w_spec, w_spec), out_specs=(tok_spec, tok_spec, w_spec, w_spec), check_vma=False)
```

```python
import jax
import jax.numpy as jnp
from jax import lax
from jax.experimental import pallas as pl
from jax.experimental.pallas import tpu as pltpu
from jax.sharding import PartitionSpec as P

NORM_EPS = 1e-6
BOTH_AXES = ('local', 'data')
CONTRACT_ROWS = (((0,), (0,)), ((), ()))
CONTRACT_COLS = (((1,), (1,)), ((), ()))
MESH = pl.DeviceIdType.MESH
RING = 4
F32, BF16 = jnp.float32, jnp.bfloat16

LINK_RATE = 46.0e3
PAIR_RATE = 600e3
LOCAL_RATE = 3000e3
HOP = 2.4
PAIR_HOP = 1.0
ENTRY = 4.2
GELU_C = 0.7978845608028654


class Event:
    def __init__(self, time=None, rank=0):
        self.time, self.rank = time, rank


class Copy:
    def __init__(self, desc, time, remote):
        self.desc, self.time, self.remote, self.rank, self.waited = desc, time, remote, 0, False

    def wait(self):
        if self.remote:
            self.desc.wait_recv()
        else:
            self.desc.wait()


class Credit:
    def __init__(self, semaphore, count, time):
        self.semaphore, self.count, self.time, self.rank, self.waited = semaphore, count, time, 0, False

    def wait(self):
        pl.semaphore_wait(self.semaphore, self.count)


class Pool:
    def __init__(self):
        self.slots, self.next = [], 0

    def again(self):
        self.next = 0
        return self


class Net:
    def __init__(self, send_sems, recv_sems, local_sems, credit_sems):
        self.send_sems, self.recv_sems, self.local_sems, self.credit_sems = send_sems, recv_sems, local_sems, credit_sems
        self.n_remote = self.n_local = 0
        self.free_sends = list(range(send_sems.shape[0]))
        self.free_locals = []
        self.now = 0.0
        self.free = {}
        self.sent = []
        self.flows = []
        here, there = lax.axis_index('local'), lax.axis_index('data')
        pos = {'z': here // RING, 'y': lax.rem(here, RING), 'x': there // 2}
        self.data, self.core = there, lax.rem(there, 2)
        self.ring = {axis: [at] + [lax.rem(at + step, RING) for step in range(1, RING)] for axis, at in pos.items()}
        self.hops = [there] + [lax.rem(there + step, 2 * RING) for step in range(1, 2 * RING)]
        self.blocks = [at * 2 + self.core for at in self.ring['x']]
        self.places = [[z * RING + y for y in self.ring['y']] for z in self.ring['z']]
        self.partner = pos['x'] * 2 + (1 - self.core)
        self.other = 1 - self.core

    def at(self, axis, step):
        return self.ring[axis][step % RING]

    def block(self, step):
        return self.blocks[step % RING]

    def device(self, axis, step):
        if axis == 'p':
            return {'data': self.partner}
        if axis == 'd':
            return {'data': self.hops[step % (2 * RING)]}
        if axis == 'x':
            return {'data': self.block(step)}
        if axis == 'y':
            return {'local': self.places[0][step % RING]}
        return {'local': self.places[step % RING][0]}

    def peers(self, axes):
        return [(axis, step) for axis in axes for step in ((1, -1) if axis in 'xyz' else (1,) if axis == 'p' else range(1, 2 * RING))]

    def signal(self, semaphore, axes):
        for axis, step in self.peers(axes):
            pl.semaphore_signal(semaphore, inc=1, device_id=self.device(axis, step), device_id_type=MESH)

    def arrive(self, axes):
        self.entry, self.entered = pltpu.get_barrier_semaphore(), len(self.peers(axes))
        self.signal(self.entry, axes)

    def enter(self):
        pl.semaphore_wait(self.entry, self.entered)
        self.now = max(self.now, ENTRY)

    def take(self, copies):
        for copy in copies:
            copy.wait()
            copy.waited = True
            self.free_locals.append(copy.slot)
            self.now = max(self.now, copy.time)

    def grant(self, k, axes):
        self.signal(self.credit_sems.at[k], axes)
        return Credit(self.credit_sems.at[k], len(self.peers(axes)), self.now + HOP)

    def drain(self, copies):
        for copy in copies:
            if copy in self.sent:
                copy.desc.wait_send()
                self.sent.remove(copy)
                self.free_sends.append(copy.slot)

    def idle(self, gap):
        over = [copy for copy in self.sent if copy.time + 1.5 < self.now]
        self.drain(over[:int(gap / 0.05)])

    def send(self, src, dst, axis, step=1, pool=None):
        if pool is not None and pool.next < len(pool.slots):
            k = pool.slots[pool.next]
        else:
            k = self.n_remote
            self.n_remote += 1
            if pool is not None:
                pool.slots.append(k)
        if pool is not None:
            pool.next += 1
        if not self.free_sends:
            over = [copy for copy in self.sent if copy.time + 1.0 < self.now]
            self.drain(over or [min(self.sent, key=lambda copy: copy.time)])
        send_slot = self.free_sends.pop()
        desc = pltpu.make_async_remote_copy(
            src_ref=src, dst_ref=dst, send_sem=self.send_sems.at[send_slot], recv_sem=self.recv_sems.at[k],
            device_id=self.device(axis, step), device_id_type=MESH)
        desc.start()
        size = 1
        for n in dst.shape:
            size *= n
        size *= dst.dtype.itemsize
        rate = PAIR_RATE if axis == 'p' else LINK_RATE
        extra = 4.4 if axis == 'd' else 0.0
        if axis == 'd':
            axis, step, size = ('p', 1, size) if step == 1 else ('x', 1 if step < RING + 2 else -1, size)
        key = (axis, step)
        done = max(self.free.get(key, 0.0), self.now) + size / rate
        self.free[key] = done
        copy = Copy(desc, done + extra + (PAIR_HOP if axis == 'p' else HOP), True)
        copy.slot = send_slot
        self.sent.append(copy)
        return copy

    def load(self, src, dst):
        if not self.free_locals:
            self.free_locals.append(self.n_local)
            self.n_local += 1
        k = self.free_locals.pop()
        desc = pltpu.make_async_copy(src, dst, self.local_sems.at[k])
        desc.start()
        size = 1
        for n in dst.shape:
            size *= n
        done = max(self.free.get('hbm', 0.0), self.now) + size * dst.dtype.itemsize / LOCAL_RATE
        self.free['hbm'] = done
        copy = Copy(desc, done + 0.9, False)
        copy.slot = k
        return copy

    def spend(self, microseconds):
        self.now += microseconds

    def spawn(self, flow):
        self.step(flow)

    def step(self, flow):
        try:
            self.flows.append((flow, next(flow)))
        except StopIteration:
            pass

    def run(self):
        while self.flows:
            best = None
            for k, (_, items) in enumerate(self.flows):
                if any(item.time is None for item in items):
                    continue
                time = max([item.time for item in items] + [0.0])
                late = max([item.rank for item in items] + [0])
                rank = (max(time, self.now) + (SLACK if late else 0.0), late, time)
                if best is None or rank < best[0]:
                    best = (rank, k, time)
            _, k, time = best
            flow, items = self.flows.pop(k)
            self.idle(time - self.now)
            for item in items:
                if not isinstance(item, Event) and not item.waited:
                    item.wait()
                    item.waited = True
                    if isinstance(item, Copy) and not item.remote:
                        self.free_locals.append(item.slot)
            self.now = max(self.now, time)
            self.step(flow)

    def finish(self):
        for copy in self.sent:
            copy.desc.wait_send()


def rows_loop(rows, chunk, body):
    chunk = min(chunk, rows)

    def step(k, carry):
        body(pl.ds(pl.multiple_of(k * chunk, chunk), chunk))
        return carry

    lax.fori_loop(0, rows // chunk, step, 0)


def add_into(net, dst, *others):
    rows, cols = dst.shape

    def body(at):
        total = dst[at, :]
        for other in others:
            total = total + other[at, :]
        dst[at, :] = total

    rows_loop(rows, 16, body)
    net.spend(rows * cols * 4 * (1 + len(others)) / 4e6)


def fire(net, event):
    event.time = net.now


def exchange(net, source, dst, done, pool):
    rows = dst.shape[0] // (2 * RING)

    def mine():
        return dst.at[pl.ds(pl.multiple_of(net.data * rows, rows), rows)]

    own = net.load(source(net.data), mine())
    copies = [net.send(source(net.hops[k]), mine(), 'd', k, pool) for k in (4, 5, 2, 3, 6, 7, 1)]
    yield [own] + copies
    net.drain(copies)
    fire(net, done)


def exchange_back(net, src, dst, done, pool):
    rows = dst.shape[1]
    per = src.shape[1] // rows

    def block(k):
        return src.at[lax.div(k, per), pl.ds(pl.multiple_of(lax.rem(k, per) * rows, rows), rows)]

    own = net.load(block(net.data), dst.at[net.data])
    copies = [net.send(block(net.hops[k]), dst.at[net.data], 'd', k, pool) for k in (4, 5, 2, 3, 6, 7, 1)]
    yield [own] + copies
    net.drain(copies)
    fire(net, done)


def copy_rows(net, src, dst):
    def body(at):
        dst[at, :] = src[at, :]

    rows_loop(src.shape[0], 16, body)
    net.spend(0.2)


def gather_x(net, full, done, issued=None, chips=None, pool=None, strip=(0, 1)):
    size = full.shape[1] // strip[1]
    base, half = strip[0] * size, size // 2
    lo, hi, both = pl.ds(base, half), pl.ds(base + half, half), pl.ds(base, size)
    chips = chips or {step: Event() for step in STEPS}
    left = [2]
    done.copies = []

    def send(*args):
        done.copies.append(net.send(*args, pool=pool))
        return done.copies[-1]

    def block(step):
        return full.at[net.block(step), both]

    def part(step, rows):
        return full.at[net.block(step), rows]

    relays = []

    def side(step, first, second, mine):
        yield [mine[0]]
        relays.append(send(part(step, first), part(step, first), 'x', -step))
        left[0] -= 1
        if left[0] == 0:
            net.spawn(far())
            if issued is not None:
                fire(net, issued)
        yield [mine[1]]
        pair = send(block(step), block(step), 'p')
        yield [pair]
        fire(net, chips[step])

    def far():
        yield relays
        pair = send(block(2), block(2), 'p')
        yield [pair]
        fire(net, chips[2])

    forth = [send(part(0, rows), part(0, rows), 'x', 1) for rows in (lo, hi)]
    back = [send(part(0, rows), part(0, rows), 'x', -1) for rows in (hi, lo)]
    pair = send(block(0), block(0), 'p')
    net.spawn(side(-1, lo, hi, forth))
    net.spawn(side(1, hi, lo, back))
    yield [pair]
    fire(net, chips[0])
    yield [chips[step] for step in STEPS]
    fire(net, done)


def gather_yz(net, own, full, first, done, issued=None, offset=0, near=False, split=True, pool=None):
    second = 'y' if first == 'z' else 'z'
    done.copies = []

    def emit(*args):
        done.copies.append(net.send(*args, pool=pool))
        return done.copies[-1]

    size = own.shape[0]
    half = size // 2
    lo, hi, both = pl.ds(offset, half), pl.ds(offset + half, half), pl.ds(offset, size)
    forward, backward = ((lo, hi), (hi, lo)) if split and not near else ((both,), (both,))

    def part(one, two, rows):
        return full.at[yz_index(net, first, one, two), rows]

    left = [3 if near else RING, 3 if near else RING]

    def arrived(which):
        left[which] -= 1
        if left[which] == 0 and (done, issued)[which] is not None:
            fire(net, (done, issued)[which])

    def send(one, rows, axis, step):
        src = own.at[pl.ds(rows.start - offset, rows.size)] if one == 0 else part(one, 0, rows)
        return emit(src, part(one, 0, rows), axis, step)

    def column(one):
        forth = [send(one, rows, second, 1) for rows in forward]
        back = [send(one, rows, second, -1) for rows in backward]

        def finish():
            if near:
                arrived(1)
                yield forth + back
            else:
                yield [forth[0]]
                relays = [emit(part(one, -1, lo), part(one, -1, lo), second, 1)]
                yield [back[0]]
                relays.append(emit(part(one, 1, hi), part(one, 1, hi), second, -1))
                arrived(1)
                yield forth[1:] + back[1:] + relays
            arrived(0)

        net.spawn(finish())

    relays = []

    def side(step, first_half, mine):
        yield [mine[0]]
        if not near:
            relays.append(emit(part(step, 0, first_half), part(step, 0, first_half), first, -step))
            if len(relays) == 2:
                net.spawn(far())
        yield mine[1:]
        column(step)

    def far():
        yield relays
        column(2)

    mine = [net.load(own, part(0, 0, both))]
    forth = [send(0, rows, first, 1) for rows in forward]
    back = [send(0, rows, first, -1) for rows in backward]
    column(0)
    net.spawn(side(-1, lo, forth))
    net.spawn(side(1, hi, back))
    left[0] += 1
    yield mine
    arrived(0)


def yz_index(net, first, one, two):
    return net.places[one % RING][two % RING] if first == 'z' else net.places[two % RING][one % RING]


STEPS = (2, 1, -1, 0)


def reduce_x(net, part, made, scratch, done, pool=None, relayed=None, strips=None):
    other, relay_f, relay_b, last_f, last_b = scratch
    strips = strips or [Event()]
    size = part.shape[2] // len(strips)
    done.copies = []

    def acc(k, rows=None):
        return part.at[k, net.core] if rows is None else part.at[k, net.core, rows]

    def send(*args):
        done.copies.append(net.send(*args, pool=pool))
        return done.copies[-1]

    ready = [Event() for _ in STEPS]

    def pair(k):
        yield [made[k]]
        yield [send(part.at[k, net.other], other.at[k], 'p')]
        add_into(net, acc(k), other.at[k])
        fire(net, ready[k])

    for k in range(RING):
        net.spawn(pair(k))

    def strip(n, end):
        half = size // 2
        lo, hi, both, relay_rows = pl.ds(n * size, half), pl.ds(n * size + half, half), pl.ds(n * size, size), pl.ds(n * half, half)
        sent = {}
        started, relay_sent = Event(), Event()

        def part_flow(k):
            yield [ready[k]] + ([relay_sent] if k else [])
            if k == 0:
                sent['first_f'] = send(acc(0, lo), relay_f.at[relay_rows], 'x', 1)
                sent['first_b'] = send(acc(0, hi), relay_b.at[relay_rows], 'x', -1)
                fire(net, relay_sent)
                if n == len(strips) - 1 and relayed is not None:
                    fire(net, relayed)
            elif k == 1:
                sent['direct_f'] = send(acc(1, hi), last_f.at[hi], 'x', 1)
            else:
                sent['direct_b'] = send(acc(2, lo), last_b.at[lo], 'x', -1)
            if len(sent) == 4:
                fire(net, started)

        for k in range(3):
            net.spawn(part_flow(k))
        yield [started]
        yield [sent['first_f']]
        add_into(net, acc(1, lo), relay_f.at[relay_rows])
        summed_f = send(acc(1, lo), last_f.at[lo], 'x', 1)
        yield [sent['first_b']]
        add_into(net, acc(2, hi), relay_b.at[relay_rows])
        summed_b = send(acc(2, hi), last_b.at[hi], 'x', -1)
        yield [ready[3], sent['direct_f'], sent['direct_b'], summed_f, summed_b]
        add_into(net, acc(3, both), last_f.at[both], last_b.at[both])
        fire(net, end)

    for n, end in enumerate(strips):
        net.spawn(strip(n, end))
    yield strips
    fire(net, done)


def reduce_x_scratch(rows, cols):
    return [pltpu.VMEM((RING, rows, cols), F32), pltpu.VMEM((rows // 2, cols), F32), pltpu.VMEM((rows // 2, cols), F32),
            pltpu.VMEM((rows, cols), F32), pltpu.VMEM((rows, cols), F32)]


class Sums:
    def __init__(self, net, first, scratch, stage):
        self.net, self.first, self.scratch, self.stage = net, first, scratch, stage
        self.second = 'y' if first == 'z' else 'z'

    def run(self, place, start, done, free, passed_all, pool, window, lead):
        net, first, second = self.net, self.first, self.second
        relay1, last1, relay2, last2 = self.scratch
        ahead, behind, mine = self.stage
        half = mine.shape[0] // 2
        lo, hi, all_rows = pl.ds(0, half), pl.ds(half, half), pl.ds(0, 2 * half)
        done.copies = []

        def send(*args):
            done.copies.append(net.send(*args, pool=pool))
            return done.copies[-1]

        def term(one, two, rows=all_rows):
            return place(yz_index(net, first, one, two), rows)

        def bring(gate, src, dst, got):
            yield [gate, start]
            yield [net.load(src, dst)]
            fire(net, got)

        chain = [[gate] + [Event() for _ in range(RING)] for gate in free]
        free[:] = [events[RING] for events in chain]
        got = [[Event() for _ in range(RING)] for _ in range(3)]
        ends = [Event() for _ in STEPS]
        passed = [Event() for _ in range(RING)]
        passed[lead] = passed_all

        def ring(k):
            two = STEPS[k]
            if k >= window:
                yield [passed[k - window]]
            net.spawn(bring(chain[0][k], term(1, two, lo), ahead, got[0][k]))
            net.spawn(bring(chain[1][k], term(-1, two, hi), behind, got[1][k]))
            net.spawn(bring(chain[2][k], term(0, two), mine, got[2][k]))
            first_f = send(term(2, two, lo), relay1.at[0, k], first, 1)
            first_b = send(term(2, two, hi), relay1.at[1, k], first, -1)
            direct_f = send(term(1, two, hi), last1.at[0, k, hi], first, 1)
            direct_b = send(term(-1, two, lo), last1.at[1, k, lo], first, -1)
            yield [first_f, got[0][k]]
            add_into(net, relay1.at[0, k], ahead)
            fire(net, chain[0][k + 1])
            summed_f = send(relay1.at[0, k], last1.at[0, k, lo], first, 1)
            yield [first_b, got[1][k]]
            add_into(net, relay1.at[1, k], behind)
            fire(net, chain[1][k + 1])
            summed_b = send(relay1.at[1, k], last1.at[1, k, hi], first, -1)
            fire(net, passed[k])
            yield [direct_f, direct_b, summed_f, summed_b, got[2][k]]
            add_into(net, last1.at[0, k], last1.at[1, k], mine)
            fire(net, chain[2][k + 1])
            fire(net, ends[k])

        def sums(k, rows=all_rows):
            return last1.at[0, k, rows]

        yield [start]
        for k in range(RING):
            net.spawn(ring(k))
        yield [ends[0]]
        first_f = send(sums(0, lo), relay2.at[0], second, 1)
        first_b = send(sums(0, hi), relay2.at[1], second, -1)
        yield [ends[1]]
        direct_f = send(sums(1, hi), last2.at[0, hi], second, 1)
        yield [ends[2]]
        direct_b = send(sums(2, lo), last2.at[1, lo], second, -1)
        yield [first_f]
        add_into(net, sums(1, lo), relay2.at[0])
        summed_f = send(sums(1, lo), last2.at[0, lo], second, 1)
        yield [first_b]
        add_into(net, sums(2, hi), relay2.at[1])
        summed_b = send(sums(2, hi), last2.at[1, hi], second, -1)
        yield [ends[3], direct_f, direct_b, summed_f, summed_b]
        add_into(net, sums(3), last2.at[0], last2.at[1])
        done.total = sums(3)
        fire(net, done)


def sums_scratch(rows, cols):
    return [pltpu.VMEM((2, RING, rows // 2, cols), F32), pltpu.VMEM((2, RING, rows, cols), F32),
            pltpu.VMEM((2, rows // 2, cols), F32), pltpu.VMEM((2, rows, cols), F32)]


def sums_stage(rows, cols):
    return [pltpu.VMEM((rows // 2, cols), F32), pltpu.VMEM((rows // 2, cols), F32), pltpu.VMEM((rows, cols), F32)]


def norm_rows(x_ref, u_ref):
    def body(at):
        x = x_ref[at, :].astype(F32)
        u_ref[at, :] = (x * lax.rsqrt(jnp.mean(x * x, axis=-1, keepdims=True) + NORM_EPS)).astype(BF16)

    rows_loop(x_ref.shape[0], 16, body)


def norm_back_rows(x_ref, dy_of, du_ref, dx_ref):
    def body(at):
        x = x_ref[at, :].astype(F32)
        du = du_ref[at, :]
        r = lax.rsqrt(jnp.mean(x * x, axis=-1, keepdims=True) + NORM_EPS)
        xr = x * r
        dx_ref[at, :] = (dy_of(at).astype(F32) + r * (du - xr * jnp.mean(xr * du, axis=-1, keepdims=True))).astype(BF16)

    rows_loop(x_ref.shape[0], 16, body)


def add_rows(x_ref, y_ref, out_ref):
    def body(at):
        out_ref[at, :] = (x_ref[at, :].astype(F32) + y_ref[at, :]).astype(BF16)

    rows_loop(x_ref.shape[0], 16, body)


def swap_halves(even, odd):
    low = lax.broadcasted_iota(jnp.int32, even.shape, len(even.shape) - 1) < even.shape[-1] // 2
    shift = even.shape[-1] // 2
    axis = len(even.shape) - 1
    return jnp.where(low, even, pltpu.roll(odd, shift, axis)), jnp.where(low, pltpu.roll(even, shift, axis), odd)


def split_columns(w_ref, cols_ref, layers):
    pieces, _, wide = w_ref.shape
    rows = layers
    tile = pieces * wide // (4 * RING * RING)
    for x in range(RING):
        for p in range(wide // tile):
            pair = []
            for i in (2 * p, 2 * p + 1):
                at = (i * RING + x) * tile
                pair.append(w_ref[at // wide, pl.ds(0, rows), pl.ds(at % wide, tile)].astype(F32))
            for c, value in enumerate(swap_halves(*pair)):
                cols_ref[2 * x + c, pl.ds(0, rows), pl.ds(p * tile, tile)] = value.astype(cols_ref.dtype)


def join_columns(cols_ref, w_ref):
    tile = w_ref.shape[1] // (4 * RING * RING)
    for x in range(RING):
        for p in range(cols_ref.shape[2] // tile):
            pair = [cols_ref[2 * x + c, :, pl.ds(p * tile, tile)] for c in range(2)]
            for i, value in zip((2 * p, 2 * p + 1), swap_halves(*pair)):
                w_ref[:, pl.ds((i * RING + x) * tile, tile)] = value


def call(body, out_shape, out_spaces, in_spaces, scratch, remote, sends, local, collective_id, *args):
    spaces = {'v': pl.BlockSpec(memory_space=pltpu.VMEM), 'h': pl.BlockSpec(memory_space=pl.ANY)}

    def kernel(*refs):
        net = Net(*refs[-5:-1])
        net.tile_sems = refs[-1]
        body(net, *refs[:-5])
        net.finish()
        assert net.n_remote <= remote and net.n_local <= local, (body.__name__, net.n_remote, net.n_local)

    return pl.pallas_call(
        kernel, out_shape=out_shape, in_specs=[spaces[s] for s in in_spaces], out_specs=[spaces[s] for s in out_spaces],
        scratch_shapes=list(scratch) + [pltpu.SemaphoreType.DMA((sends,)), pltpu.SemaphoreType.DMA((remote,)), pltpu.SemaphoreType.DMA((local,)),
                                               pltpu.SemaphoreType.REGULAR((14,)), pltpu.SemaphoreType.DMA((2,))],
        compiler_params=pltpu.CompilerParams(collective_id=collective_id, has_side_effects=True, vmem_limit_bytes=67000000),
        cost_estimate=pl.CostEstimate(flops=10**8, bytes_accessed=10**7, transcendentals=0),
        name=body.__name__)(*args)


WIDE = 512
EARLY = 3
STRIPS = 2
GRAD_TIME = 4.25
SLACK = 0.4
R_HIDDEN, R_DOWN, R_BACK, R_TURN, R_DDOWN, R_DDOWN2, R_DUP, R_OUT, R_PRE, R_GUP, R_GDOWN, R_DX = 2, 1, 3, 1, 2, 2, 4, 2, 2, 1, 3, 2
R_DU, HOLD = (3, 3.1, 3, 3.3), (0, 1, 2, 3)
WINDOWS = (2, 2, 3, 2, 1, 2, 3, 4)
AXES = ('yz', 'yz', 'yz', 'yz')
TOP = 6
NEAR = 'z'
LEAD = (3, 3, 3)
TR, TS, TL = 281, 64, 9


def wide_loop(total, body):
    wide = min(WIDE, total)

    def step(k, carry):
        body(k, wide, pl.ds(pl.multiple_of(k * wide, wide), wide))
        return carry

    lax.fori_loop(0, total // wide, step, 0)


def flat(value):
    return value.reshape(value.shape[0] * value.shape[1], value.shape[2])


def dot_rows(a, b):
    return jnp.dot(flat(a), flat(b), preferred_element_type=F32)


def dot_cols(a, b):
    return lax.dot_general(flat(a), flat(b), CONTRACT_COLS, preferred_element_type=F32)


def gelu(a):
    return 0.5 * a * (1.0 + jnp.tanh(GELU_C * (a + 0.044715 * a * a * a)))


def hidden_rows(net, chip, u, up, a, s):
    at = pl.ds(chip * 2, 2)

    def body(_, wide, cols):
        pre = dot_rows(u[at], up[:, :, cols]).astype(BF16)
        a[at, :, cols] = pre.reshape(2, -1, wide)
        s[at, :, cols] = gelu(pre.astype(F32)).astype(BF16).reshape(2, -1, wide)

    wide_loop(up.shape[2], body)
    net.spend(1.7)


def down_rows(net, chip, s, down, part):
    at = pl.ds(chip * 2, 2)

    def body(_, wide, cols):
        part[:, :, cols] = dot_rows(s[at], down[:, :, cols]).reshape(2, -1, wide)

    wide_loop(down.shape[2], body)
    net.spend(1.76)


def hidden_back_rows(net, chip, dy, down, ds):
    at = pl.ds(chip * 2, 2)
    rows = down.shape[1]

    def body(k, wide, cols):
        blocks = pl.ds(k * (wide // rows), wide // rows)
        ds[at, :, cols] = dot_cols(dy[at], down[blocks]).astype(BF16).reshape(2, -1, wide)

    wide_loop(down.shape[0] * rows, body)
    net.spend(1.5)


def gelu_both(a):
    t = jnp.tanh(GELU_C * (a + 0.044715 * a * a * a))
    return 0.5 * a * (1.0 + t), 0.5 * (1.0 + t) + 0.5 * a * (1.0 - t * t) * (GELU_C * (1.0 + 3 * 0.044715 * a * a))


def hidden_turn_rows(net, chip, u, up, s, ds):
    at = pl.ds(chip * 2, 2)

    def body(_, wide, cols):
        pre = dot_rows(u[at], up[:, :, cols]).astype(BF16).astype(F32)
        value, slope = gelu_both(pre)
        s[at, :, cols] = value.astype(BF16).reshape(2, -1, wide)
        ds[at, :, cols] = (ds[at, :, cols].astype(F32) * slope.reshape(2, -1, wide)).astype(BF16)

    wide_loop(up.shape[2], body)
    net.spend(2.1)


def pre_back_rows(net, chip, dy, down, a, da):
    at = pl.ds(chip * 2, 2)
    rows = down.shape[1]

    def body(k, wide, cols):
        blocks = pl.ds(k * (wide // rows), wide // rows)
        ds = dot_cols(dy[at], down[blocks]).astype(BF16).astype(F32).reshape(2, -1, wide)
        da[at, :, cols] = (ds * gelu_both(a[at, :, cols].astype(F32))[1]).astype(BF16)

    wide_loop(down.shape[0] * rows, body)
    net.spend(1.95)


def input_back_rows(net, chip, da, up, part):
    at = pl.ds(chip * 2, 2)
    rows = up.shape[1]

    def body(k, wide, cols):
        blocks = pl.ds(k * (wide // rows), wide // rows)
        part[:, :, cols] = dot_cols(da[at], up[blocks]).reshape(2, -1, wide)

    wide_loop(up.shape[0] * rows, body)
    net.spend(1.9)


def stored_tiles(net, count, compute, stage, out):
    def store(t):
        return pltpu.make_async_copy(stage.at[lax.rem(t, 2)], out(t), net.tile_sems.at[lax.rem(t, 2)])

    def step(t, carry):
        @pl.when(t >= 2)
        def _():
            store(t - 2).wait()

        compute(t, stage.at[lax.rem(t, 2)])
        store(t).start()
        return carry

    lax.fori_loop(0, count, step, 0)
    for t in range(max(count - 2, 0), count):
        store(jnp.int32(t)).wait()


def dot_tokens(a, b):
    return lax.dot_general(flat(a), flat(b), CONTRACT_ROWS, preferred_element_type=F32)


def grad_tiles(net, lhs, rhs, stage, out):
    _, high, wide = stage.shape
    across = rhs.shape[2] // wide

    def columns(t):
        return pl.ds(pl.multiple_of(lax.rem(t, across) * wide, wide), wide)

    def rows(t):
        return pl.ds(pl.multiple_of(lax.div(t, across) * high, high), high)

    def compute(t, slot):
        slot[...] = dot_tokens(lhs[:, :, rows(t)], rhs[:, :, columns(t)])

    stored_tiles(net, lhs.shape[2] // high * across, compute, stage, lambda t: out.at[rows(t), columns(t)])
    net.spend(GRAD_TIME * lhs.shape[2] / 1024)


def solution(mesh):
    nl, nd = mesh.shape['local'], mesh.shape['data']
    tok_spec = P(BOTH_AXES, None)
    w_spec = P(None, BOTH_AXES, None)

    def device_fn(tokens, grad_out, w_up, w_down):
        num_layers, ur, ffn = w_up.shape
        dr = w_down.shape[1]
        rows, width = tokens.shape
        hidden = nl * dr
        shape = jax.ShapeDtypeStruct
        up_full = shape((nl, nd * ur, hidden), BF16)
        down_full = shape((nl, dr, width), BF16)
        act_full = shape((nd, rows, width), BF16)
        hid_full = shape((nd, rows, hidden), BF16)
        own = shape((rows, width), BF16)
        part_vmem = pltpu.VMEM((RING, 2, rows, width), F32)
        rx = [part_vmem] + reduce_x_scratch(rows, width)
        sums = sums_scratch(dr, hidden) * 4 + sums_stage(dr, hidden) * 2

        def vmem(like):
            return pltpu.VMEM(like.shape, like.dtype)

        def step(net, x_in, x_halves, g_in, w_up_in, w_down_in,
                 x_out, dx_out, block_out, u_out, a_out, s_out, d_up0, d_down0, d_up1, d_down1, dw_up1, dw_down1, dw_up0, dw_down0,
                 x, u, g, up0, up1, down0, down1, ds, s, stage, part, *scratch):
            net.arrive('dyz')
            rx_scratch = scratch[:5]
            names = ('blocks', 'blocks1', 'sent_u', 'got_u', 'got_g', 'sent_up0', 'sent_down0', 'sent_up1', 'sent_down1', 'got_up0', 'got_down0',
                     'got_up1', 'got_down1', 'saved', 'free0', 'reduced0', 'ds_made', 'got_u1', 'hidden', 'all_du', 'reduced1', 'sent_dy', 'got_dy',
                     'back_up0', 'back_up0_rest', 'back_down0', 'd_down1', 'd_up1', 'y_reduced', 'acts', 'd_down0', 'da0', 'd_up0', 'du_reduced',
                     'out_up1', 'out_up0', 'got_u0', 'y_made', 'x_saved', 'weights_in', 'd_down1_0', 'relayed0')
            ev = {name: Event() for name in names}
            for kind in ('up', 'down'):
                for layer in range(2):
                    for k in range(2):
                        ev['sum_%s%d%d' % (kind, layer, k)] = Event()
            ev['got_up0'].rank = R_HIDDEN
            hidden_made, made0, made1, y_made, du_made = ([Event() for _ in STEPS] for _ in range(5))
            wide = width // 2
            half_up = nd * ur // 2
            act_pool, rs_pool = Pool(), Pool()
            job_pools = [[Pool(), Pool()], [Pool(), Pool()]]
            pools = {'up0': [Pool(), Pool()], 'down0': [Pool(), Pool()], 'up1': job_pools[0], 'down1': job_pools[1], 'blocks': [Pool(), Pool()]}
            stages = (scratch[21:24], scratch[24:27])
            job_scratch = [[scratch[5 + 8 * n + 4 * k:9 + 8 * n + 4 * k] for k in range(2)] for n in range(2)]
            frees = [[Event(0.0) for _ in range(3)] for _ in range(2)]
            freed = {k: Event() for k in range(10, 14)}

            def columns(h):
                return pl.ds(h * wide, wide)

            inputs = [net.load(x_in, x)]
            inputs += [net.load(w_up_in.at[:, pl.ds(k * hidden, hidden)], ds.at[k, pl.ds(0, num_layers * ur)]) for k in range(nd)]

            def gather(name, own, full, split):
                size = own.shape[0] // 2

                def join(kind, events):
                    yield events
                    if kind == 'got_':
                        ev[kind + name].copies = events[0].copies + events[1].copies
                    fire(net, ev[kind + name])

                got, sent = [Event(), Event()], [Event(), Event()]
                for k, first in enumerate('yz'):
                    net.spawn(gather_yz(net, own.at[pl.ds(k * size, size)], full, first, got[k], sent[k], k * size, split=split, pool=pools[name][k]))
                net.spawn(join('got_', got))
                net.spawn(join('sent_', sent))

            net.take(inputs)
            split_columns(ds, s, num_layers * ur)
            norm_rows(x, u.at[net.data])
            net.enter()
            gather('down0', w_down_in.at[0], down0, False)
            net.spawn(exchange(net, lambda k: s.at[k, pl.ds(0, ur)], block_out.at[0], ev['blocks'], pools['blocks'][0]))
            own_grads = net.load(g_in, g.at[net.data])

            def up_first():
                yield [ev['blocks']]
                gather('up0', block_out.at[0], up0, True)
                net.spawn(gather_x(net, u, ev['got_u'], ev['sent_u'], pool=act_pool))
                yield [ev['sent_u']]
                net.spawn(exchange(net, lambda k: s.at[k, pl.ds(ur, ur)], block_out.at[1], ev['blocks1'], pools['blocks'][1]))
                yield [own_grads]
                net.spawn(gather_x(net, g, ev['got_g']))

            def second():
                yield [ev['sent_up0'], ev['sent_down0'], ev['blocks1']]
                gather('down1', w_down_in.at[1], down1, False)
                yield [made0[EARLY]]
                gather('up1', block_out.at[1], up1, True)

            def hidden_flow():
                yield [ev['got_u'], ev['got_up0'], ev['blocks1']]
                for k, step in enumerate(STEPS):
                    hidden_rows(net, net.at('x', step), u, up0, ds, s)
                    fire(net, hidden_made[k])
                    yield [Event(net.now, R_HIDDEN)] + ([ev['relayed0']] if k == 1 else [])
                yield [net.load(ds, a_out), net.load(s, s_out), net.load(u, u_out)]
                fire(net, ev['saved'])

            def down_flow():
                for k, step in enumerate(STEPS):
                    yield [hidden_made[k], ev['got_down0'], Event(0.0, R_DOWN)] + ([ev['relayed0']] if k == 1 else [])
                    down_rows(net, net.at('x', step), s, down0, part.at[k])
                    fire(net, made0[k])
                fire(net, ev['free0'])

            here = {step: Event() for step in STEPS}
            dy_here = {step: Event() for step in STEPS}

            strips0 = [Event() for _ in range(STRIPS)]
            net.spawn(reduce_x(net, part, made0, rx_scratch, ev['reduced0'], rs_pool, ev['relayed0'], strips0))

            def next_layer():
                yield [ev['saved'], ev['got_g']]
                net.drain(ev['got_u'].copies + ev['got_g'].copies)
                credit = net.grant(3, 'xp')
                act_pool.again()
                got = [Event() for _ in strips0]
                chips = [{step: Event() for step in STEPS} for _ in strips0]

                def strip(n):
                    at = pl.ds(n * (rows // STRIPS), rows // STRIPS)
                    yield [strips0[n], credit]
                    add_rows(x.at[at], part.at[3, net.core, at], x.at[at])
                    norm_rows(x.at[at], u.at[net.data, at])
                    net.spend(1.0 / STRIPS)
                    net.spawn(gather_x(net, u, got[n], chips=chips[n], pool=act_pool, strip=(n, STRIPS)))

                def chip(step):
                    yield [arrived[step] for arrived in chips]
                    fire(net, here[step])

                for n in range(STRIPS):
                    net.spawn(strip(n))
                for step in STEPS:
                    net.spawn(chip(step))
                yield [ev['reduced0']]
                net.drain(ev['reduced0'].copies)
                yield [net.grant(4, 'xp')]
                net.spawn(reduce_x(net, part, made1, rx_scratch, ev['reduced1'], rs_pool.again()))
                yield got
                ev['got_u1'].copies = sum((event.copies for event in got), [])
                fire(net, ev['got_u1'])

            def back_flow():
                for k, step in enumerate(STEPS):
                    yield [ev['got_g'], ev['got_down1'], ev['saved'], Event(0.0, R_BACK)]
                    hidden_back_rows(net, net.at('x', step), g, down1, ds)
                fire(net, ev['ds_made'])

            def again():
                top = nd * ur * TOP // 8
                yield [ev['free0'], ev['ds_made']]
                net.drain(ev['got_up0'].copies + ev['got_down0'].copies)
                credit = net.grant(6, 'yz')
                yield [credit]
                net.spawn(gather_yz(net, w_down_in.at[0], down0, NEAR, ev['back_down0'], near=True, pool=pools['down0'][1].again()))
                net.spawn(gather_yz(net, block_out.at[0, pl.ds(0, top)], up0, 'y', ev['back_up0'], pool=pools['up0'][0].again()))
                net.spawn(gather_yz(net, block_out.at[0, pl.ds(top, nd * ur - top)], up0, 'z', ev['back_up0_rest'], offset=top, pool=pools['up0'][1].again()))

            def weights():
                yield [ev['got_up1'], ev['got_down1']]
                yield [net.grant(7, 'yz')]
                fire(net, ev['weights_in'])

            left = [RING, RING]

            turned = [Event() for _ in STEPS]

            def layer1(k, step):
                yield [here[step], ev['ds_made'], ev['got_up1'], Event(0.0, R_TURN)]
                hidden_turn_rows(net, net.at('x', step), u, up1, s, ds)
                fire(net, turned[k])
                left[0] -= 1
                if left[0] == 0:
                    fire(net, ev['hidden'])

            def layer1_back(k, step):
                yield [turned[k], Event(0.0, R_DU[k])] + ([ev['hidden']] if k in HOLD else [])
                input_back_rows(net, net.at('x', step), ds, up1, part.at[k])
                fire(net, made1[k])
                left[1] -= 1
                if left[1] == 0:
                    fire(net, ev['all_du'])

            def grads1():
                for h in range(2):
                    yield [Event(0.0, R_DDOWN2 if h else R_DDOWN), ev['hidden']]
                    grad_tiles(net, s, g.at[:, :, columns(h)], stage, d_down1.at[:, columns(h)])
                    fire(net, ev['d_down1' if h else 'd_down1_0'])
                for h in range(2):
                    yield [Event(net.now, R_DUP)]
                    grad_tiles(net, u.at[:, :, columns(h)], ds, stage, d_up1.at[columns(h)])
                fire(net, ev['d_up1'])

            def act():
                yield [ev['d_up1'], ev['all_du'], ev['got_u1']]
                own_g = [net.load(g_in.at[:, columns(h)], ds.at[h]) for h in range(2)]
                net.drain(ev['got_u1'].copies)
                credit = net.grant(5, 'xp')
                yield [ev['reduced1'], credit] + own_g
                norm_back_rows(x, lambda at: jnp.concatenate([ds[h, at, :] for h in range(2)], axis=-1), part.at[3, net.core], u.at[net.data])
                net.spend(0.7)
                net.spawn(gather_x(net, u, ev['got_dy'], ev['sent_dy'], dy_here, pool=act_pool.again()))

            def layer1_out():
                yield [ev['reduced1'], Event(0.0, R_OUT)]
                net.drain(ev['reduced1'].copies)
                credit = net.grant(8, 'xp')
                for k, step in enumerate(STEPS):
                    down_rows(net, net.at('x', step), s, down1, part.at[k])
                    yield [Event(net.now, R_OUT)]
                fire(net, ev['y_made'])
                yield [ev['sent_dy'], credit]
                net.spawn(reduce_x(net, part, y_made, rx_scratch, ev['y_reduced'], rs_pool.again()))
                for k in range(RING):
                    fire(net, y_made[k])
                yield [ev['y_reduced']]
                add_rows(x, part.at[3, net.core], x)
                yield [net.load(x, x_out)]
                fire(net, ev['x_saved'])

            a0, s0 = up1.at[pl.ds(0, nd)], up1.at[pl.ds(nd, nd)]
            backs = [RING]

            def bring_back():
                yield [ev['d_down1']]
                yield [net.load(u_out, g)]
                fire(net, ev['got_u0'])

            def bring_acts():
                yield [ev['all_du']]
                net.drain(ev['got_up1'].copies)
                yield [net.load(a_out, a0), net.load(s_out, s0)]
                fire(net, ev['acts'])

            def layer0_hidden(step):
                yield [dy_here[step], ev['acts'], ev['back_down0'], ev['d_up1'], Event(0.0, R_PRE)]
                pre_back_rows(net, net.at('x', step), u, down0, a0, ds)
                backs[0] -= 1
                if backs[0] == 0:
                    fire(net, ev['da0'])

            def layer0():
                for h in range(2):
                    yield [ev['da0'], ev['got_u0'], Event(0.0, R_GUP)]
                    grad_tiles(net, g.at[:, :, columns(h)], ds, stage, d_up0.at[columns(h)])
                fire(net, ev['d_up0'])
                for h in range(2):
                    yield [ev['got_dy'], ev['acts'], Event(0.0, R_GDOWN)]
                    grad_tiles(net, s0, u.at[:, :, columns(h)], stage, d_down0.at[:, columns(h)])
                fire(net, ev['d_down0'])
                yield [ev['y_reduced'], ev['back_up0'], ev['back_up0_rest'], Event(0.0, R_DX)]
                net.drain(ev['y_reduced'].copies + ev['got_down1'].copies)
                x0 = down1.at[pl.ds(0, x_halves.shape[0])]
                yield [net.grant(9, 'xp'), net.load(x_halves, x0)]
                net.spawn(reduce_x(net, part, du_made, rx_scratch, ev['du_reduced'], rs_pool.again()))
                for k, step in enumerate(STEPS):
                    input_back_rows(net, net.at('x', step), ds, up0, part.at[k])
                    fire(net, du_made[k])
                    yield [Event(net.now, R_DX)]
                yield [ev['du_reduced'], ev['x_saved']]
                for q in range(x_halves.shape[0]):
                    rows_q = pl.ds(q * dr, dr)
                    dy_q = u.at[net.data, rows_q]
                    norm_back_rows(x0.at[q], lambda at, dy_q=dy_q: dy_q[at, :], part.at[3, net.core, rows_q], x.at[rows_q])
                yield [net.load(x, dx_out)]

            def up_place(ref, k):
                return lambda block, rows: ref.at[pl.ds(pl.multiple_of(block * (2 * half_up) + k * half_up + rows.start, rows.size), rows.size)]

            def down_place(ref, k):
                return lambda block, rows: ref.at[pl.ds(pl.multiple_of(block * dr + rows.start, rows.size), rows.size), columns(k)]

            def gate(event, items, pool):
                yield items
                pool.again()
                fire(net, event)

            def sum_job(job, place, ref, ready, name, credits=()):
                passed = [Event(), Event()]
                for k in range(2):
                    start = Event()
                    n = job % 2
                    net.spawn(gate(start, ready[k] + ([credits[k]] if credits else []), job_pools[n][k]))
                    sums = Sums(net, AXES[job][k], job_scratch[n][k], stages[k])
                    net.spawn(sums.run(place(ref, k), start, ev['sum_%s%d' % (name, k)], frees[k], passed[k], job_pools[n][k], WINDOWS[2 * job + k], LEAD[min(job, 2)]))
                return passed

            def out_down(layer, dw_down, credit):
                def one(k):
                    done = ev['sum_down%d%d' % (layer, k)]
                    yield [done]
                    yield [net.load(done.total, dw_down.at[:, columns(k)])]
                    if credit is not None:
                        net.drain(done.copies)
                        yield [net.grant(credit + k, 'yz')]
                        fire(net, freed[credit + k])

                for k in range(2):
                    net.spawn(one(k))

            def out_up(n, layer, dw_up, credit):
                totals = [ev['sum_up%d%d' % (layer, k)] for k in range(2)]
                yield totals
                net.drain(totals[0].copies + totals[1].copies)
                spare = job_scratch[n][0][0].at[0]
                for k, done in enumerate(totals):
                    for q in range(2):
                        copy_rows(net, done.total.at[pl.ds(q * spare.shape[1], spare.shape[1])], spare.at[2 * k + q])
                done = ev['out_up%d' % layer]
                net.spawn(exchange_back(net, spare, dw_up, done, pools['blocks'][layer].again()))
                if credit is not None:
                    yield [done]
                    for k in range(2):
                        yield [net.grant(credit + k, 'yz')]
                        fire(net, freed[credit + k])

            passed = sum_job(0, down_place, d_down1, [[ev['d_down1_0'], ev['weights_in']], [ev['d_down1'], ev['weights_in']]], 'down1')
            passed = sum_job(1, up_place, d_up1, [[ev['d_up1']] + passed] * 2, 'up1')
            passed = sum_job(2, up_place, d_up0, [[ev['d_up0']] + passed] * 2, 'up0', [freed[10], freed[11]])
            sum_job(3, down_place, d_down0, [[ev['d_down0']] + passed] * 2, 'down0', [freed[12], freed[13]])
            out_down(1, dw_down1, 10)
            net.spawn(out_up(1, 1, dw_up1, 12))
            net.spawn(out_up(0, 0, dw_up0, None))
            out_down(0, dw_down0, None)
            for k in (3, 2, 1, 0):
                net.spawn(layer1(k, STEPS[k]))
            for k in range(RING):
                net.spawn(layer1_back(k, STEPS[k]))
            for step in (0, -1, 1, 2):
                net.spawn(layer0_hidden(step))
            for flow in (up_first(), second(), hidden_flow(), down_flow(), next_layer(), back_flow(), again(), weights(), grads1(), act(), layer1_out(),
                         bring_back(), bring_acts(), layer0()):
                net.spawn(flow)
            net.run()

        def finish(*refs):
            sources, targets, held, ups, sems = refs[:6], refs[6:10], refs[10:16], refs[16:18], refs[18]
            x_out, dx_out, up_out, down_out = targets
            loads = [pltpu.make_async_copy(src, dst, sems.at[k]) for k, (src, dst) in enumerate(zip(sources, held))]
            stores = [(ups[1], up_out.at[1]), (ups[0], up_out.at[0]), (held[2], down_out.at[1]), (held[3], down_out.at[0]), (held[4], x_out), (held[5], dx_out)]
            stores = [pltpu.make_async_copy(src, dst, sems.at[6 + k]) for k, (src, dst) in enumerate(stores)]
            for load in loads:
                load.start()
            for k in (2, 3, 4, 5):
                loads[k].wait()
                stores[k].start()
            for k in (0, 1):
                loads[k].wait()
                join_columns(held[k], ups[1 - k])
                stores[k].start()
            for store in stores:
                store.wait()

        d_up_own, d_down_own = shape((nd, ur, hidden), F32), shape((dr, width), F32)

        d_up_full, d_down_full = shape((width, hidden), F32), shape((hidden, width), F32)
        x_out, dx, _, _, _, _, _, _, _, _, *grads = call(
            step, [own, own, shape((num_layers, nd * ur, hidden), BF16), act_full, hid_full, hid_full] + [d_up_full, d_down_full] * 2
            + [d_up_own, d_down_own] * 2, 'h' * 14, 'hhhhh',
            [vmem(own)] + [vmem(act_full)] * 2 + [vmem(up_full)] * 2 + [vmem(down_full)] * 2 + [vmem(hid_full)] * 2
            + [pltpu.VMEM((2, hidden // 2, width // 4), F32)] + rx + sums, TR, TS, TL, 0,
            tokens, tokens.reshape(rows // dr, dr, width), grad_out, w_up.reshape(num_layers * ur, ffn), w_down)
        up1_own, down1_own, up0_own, down0_own = grads
        held = [d_up_own, d_up_own, d_down_own, d_down_own, own, own]
        return pl.pallas_call(
            finish, out_shape=[own, own, shape(w_up.shape, F32), shape(w_down.shape, F32)], name='finish',
            in_specs=[pl.BlockSpec(memory_space=pl.ANY)] * 6, out_specs=[pl.BlockSpec(memory_space=pl.ANY)] * 4,
            scratch_shapes=[vmem(like) for like in held] + [pltpu.VMEM(w_up.shape[1:], F32)] * 2 + [pltpu.SemaphoreType.DMA((12,))],
        )(up1_own, up0_own, down1_own, down0_own, x_out, dx)

    return jax.shard_map(device_fn, mesh=mesh, in_specs=(tok_spec, tok_spec, w_spec, w_spec), out_specs=(tok_spec, tok_spec, w_spec, w_spec), check_vma=False)
```

```python
import jax
import jax.numpy as jnp
from jax import lax
from jax.experimental import pallas as pl
from jax.experimental.pallas import tpu as pltpu
from jax.sharding import PartitionSpec as P

NORM_EPS = 1e-6
BOTH_AXES = ('local', 'data')
CONTRACT_ROWS = (((0,), (0,)), ((), ()))
CONTRACT_COLS = (((1,), (1,)), ((), ()))
MESH = pl.DeviceIdType.MESH
RING = 4
F32, BF16 = jnp.float32, jnp.bfloat16

LINK_RATE = 46.0e3
PAIR_RATE = 600e3
LOCAL_RATE = 3000e3
HOP = 2.4
PAIR_HOP = 1.0
ENTRY = 3.2
GELU_C = 0.7978845608028654


class Event:
    def __init__(self, time=None, rank=0):
        self.time, self.rank = time, rank


class Copy:
    def __init__(self, desc, time, remote):
        self.desc, self.time, self.remote, self.rank, self.waited = desc, time, remote, 0, False

    def wait(self):
        if self.remote:
            self.desc.wait_recv()
        else:
            self.desc.wait()


class Credit:
    def __init__(self, semaphore, count, time):
        self.semaphore, self.count, self.time, self.rank, self.waited = semaphore, count, time, 0, False

    def wait(self):
        pl.semaphore_wait(self.semaphore, self.count)


class Both:
    def __init__(self, net, dst, one, two):
        self.desc = pltpu.make_async_remote_copy(
            src_ref=dst, dst_ref=dst, send_sem=net.send_sems.at[one.slot], recv_sem=net.recv_sems.at[one.receive],
            device_id=net.device('p', 1), device_id_type=MESH)
        self.time, self.rank, self.waited = max(one.time, two.time), 0, False

    def wait(self):
        self.desc.wait_recv()


class Pool:
    def __init__(self):
        self.slots, self.next = [], 0

    def again(self):
        self.next = 0
        return self


class Net:
    def __init__(self, send_sems, recv_sems, local_sems, credit_sems):
        self.send_sems, self.recv_sems, self.local_sems, self.credit_sems = send_sems, recv_sems, local_sems, credit_sems
        self.n_remote = self.n_local = 0
        self.free_sends = list(range(send_sems.shape[0]))
        self.free_locals = []
        self.now = 0.0
        self.free = {}
        self.sent = []
        self.flows = []
        here, there = lax.axis_index('local'), lax.axis_index('data')
        pos = {'z': here // RING, 'y': lax.rem(here, RING), 'x': there // 2}
        self.data, self.core = there, lax.rem(there, 2)
        self.ring = {axis: [at] + [lax.rem(at + step, RING) for step in range(1, RING)] for axis, at in pos.items()}
        self.hops = [there] + [lax.rem(there + step, 2 * RING) for step in range(1, 2 * RING)]
        self.blocks = [at * 2 + self.core for at in self.ring['x']]
        self.places = [[z * RING + y for y in self.ring['y']] for z in self.ring['z']]
        self.partner = pos['x'] * 2 + (1 - self.core)
        self.other = 1 - self.core

    def at(self, axis, step):
        return self.ring[axis][step % RING]

    def block(self, step):
        return self.blocks[step % RING]

    def device(self, axis, step):
        if axis == 'p':
            return {'data': self.partner}
        if axis == 'd':
            return {'data': self.hops[step % (2 * RING)]}
        if axis == 'x':
            return {'data': self.block(step)}
        if axis == 'y':
            return {'local': self.places[0][step % RING]}
        return {'local': self.places[step % RING][0]}

    def peers(self, axes):
        return [(axis, step) for axis in axes for step in ((1, -1) if axis in 'xyz' else (1,) if axis == 'p' else range(1, 2 * RING))]

    def signal(self, semaphore, axes):
        for axis, step in self.peers(axes):
            pl.semaphore_signal(semaphore, inc=1, device_id=self.device(axis, step), device_id_type=MESH)

    def arrive(self, axes):
        self.entry, self.entered = pltpu.get_barrier_semaphore(), len(self.peers(axes))
        self.signal(self.entry, axes)

    def enter(self):
        pl.semaphore_wait(self.entry, self.entered)
        self.now = max(self.now, ENTRY)

    def take(self, copies):
        for copy in copies:
            copy.wait()
            copy.waited = True
            self.free_locals.append(copy.slot)
            self.now = max(self.now, copy.time)

    def grant(self, k, axes):
        self.signal(self.credit_sems.at[k], axes)
        return Credit(self.credit_sems.at[k], len(self.peers(axes)), self.now + HOP)

    def drain(self, copies):
        for copy in copies:
            if copy in self.sent:
                copy.desc.wait_send()
                self.sent.remove(copy)
                self.free_sends.append(copy.slot)

    def idle(self, gap):
        over = [copy for copy in self.sent if copy.time + 1.5 < self.now]
        self.drain(over[:int(gap / 0.05)])

    def send(self, src, dst, axis, step=1, pool=None, partner=None):
        if partner is not None:
            k = partner.receive
        elif pool is not None and pool.next < len(pool.slots):
            k = pool.slots[pool.next]
        else:
            k = self.n_remote
            self.n_remote += 1
            if pool is not None:
                pool.slots.append(k)
        if pool is not None and partner is None:
            pool.next += 1
        if not self.free_sends:
            over = [copy for copy in self.sent if copy.time + 1.0 < self.now]
            self.drain(over or [min(self.sent, key=lambda copy: copy.time)])
        send_slot = self.free_sends.pop()
        desc = pltpu.make_async_remote_copy(
            src_ref=src, dst_ref=dst, send_sem=self.send_sems.at[send_slot], recv_sem=self.recv_sems.at[k],
            device_id=self.device(axis, step), device_id_type=MESH)
        desc.start()
        size = 1
        for n in dst.shape:
            size *= n
        size *= dst.dtype.itemsize
        rate = PAIR_RATE if axis == 'p' else LINK_RATE
        extra = 4.4 if axis == 'd' else 0.0
        if axis == 'd':
            axis, step, size = ('p', 1, size) if step == 1 else ('x', 1 if step < RING + 2 else -1, size)
        key = (axis, step)
        done = max(self.free.get(key, 0.0), self.now) + size / rate
        self.free[key] = done
        copy = Copy(desc, done + extra + (PAIR_HOP if axis == 'p' else HOP), True)
        copy.slot, copy.receive = send_slot, k
        self.sent.append(copy)
        return copy

    def load(self, src, dst):
        if not self.free_locals:
            self.free_locals.append(self.n_local)
            self.n_local += 1
        k = self.free_locals.pop()
        desc = pltpu.make_async_copy(src, dst, self.local_sems.at[k])
        desc.start()
        size = 1
        for n in dst.shape:
            size *= n
        done = max(self.free.get('hbm', 0.0), self.now) + size * dst.dtype.itemsize / LOCAL_RATE
        self.free['hbm'] = done
        copy = Copy(desc, done + 0.9, False)
        copy.slot = k
        return copy

    def spend(self, microseconds):
        self.now += microseconds

    def spawn(self, flow):
        self.step(flow)

    def step(self, flow):
        try:
            self.flows.append((flow, next(flow)))
        except StopIteration:
            pass

    def run(self):
        while self.flows:
            best = None
            for k, (_, items) in enumerate(self.flows):
                if any(item.time is None for item in items):
                    continue
                time = max([item.time for item in items] + [0.0])
                late = max([item.rank for item in items] + [0])
                rank = (max(time, self.now) + (SLACK if late else 0.0), late, time)
                if best is None or rank < best[0]:
                    best = (rank, k, time)
            _, k, time = best
            flow, items = self.flows.pop(k)
            self.idle(time - self.now)
            for item in items:
                if not isinstance(item, Event) and not item.waited:
                    item.wait()
                    item.waited = True
                    if isinstance(item, Copy) and not item.remote:
                        self.free_locals.append(item.slot)
            self.now = max(self.now, time)
            self.step(flow)

    def finish(self):
        for copy in self.sent:
            copy.desc.wait_send()


def rows_loop(rows, chunk, body):
    chunk = min(chunk, rows)

    def step(k, carry):
        body(pl.ds(pl.multiple_of(k * chunk, chunk), chunk))
        return carry

    lax.fori_loop(0, rows // chunk, step, 0)


def add_into(net, dst, *others):
    rows, cols = dst.shape

    def body(at):
        total = dst[at, :]
        for other in others:
            total = total + other[at, :]
        dst[at, :] = total

    rows_loop(rows, 16, body)
    net.spend(rows * cols * 4 * (1 + len(others)) / 4e6)


def fire(net, event):
    event.time = net.now


def exchange(net, source, dst, done, pool):
    rows = dst.shape[0] // (2 * RING)

    def mine():
        return dst.at[pl.ds(pl.multiple_of(net.data * rows, rows), rows)]

    own = net.load(source(net.data), mine())
    copies = [net.send(source(net.hops[k]), mine(), 'd', k, pool) for k in (4, 5, 2, 3, 6, 7, 1)]
    yield [own] + copies
    net.drain(copies)
    fire(net, done)


def exchange_back(net, src, dst, done, pool):
    rows = dst.shape[1]
    per = src.shape[1] // rows

    def block(k):
        return src.at[lax.div(k, per), pl.ds(pl.multiple_of(lax.rem(k, per) * rows, rows), rows)]

    own = net.load(block(net.data), dst.at[net.data])
    copies = [net.send(block(net.hops[k]), dst.at[net.data], 'd', k, pool) for k in (4, 5, 2, 3, 6, 7, 1)]
    yield [own] + copies
    net.drain(copies)
    fire(net, done)


def copy_rows(net, src, dst):
    def body(at):
        dst[at, :] = src[at, :]

    rows_loop(src.shape[0], 16, body)
    net.spend(0.2)


def gather_x(net, full, done, issued=None, chips=None, pool=None, strip=(0, 1)):
    size = full.shape[1] // strip[1]
    base, half = strip[0] * size, size // 2
    lo, hi, both = pl.ds(base, half), pl.ds(base + half, half), pl.ds(base, size)
    chips = chips or {step: Event() for step in STEPS}
    left = [2]
    done.copies = []

    def send(*args):
        done.copies.append(net.send(*args, pool=pool))
        return done.copies[-1]

    def block(step):
        return full.at[net.block(step), both]

    def part(step, rows):
        return full.at[net.block(step), rows]

    relays = []

    def side(step, first, second, mine):
        yield [mine[0]]
        relays.append(send(part(step, first), part(step, first), 'x', -step))
        left[0] -= 1
        if left[0] == 0:
            net.spawn(far())
            if issued is not None:
                fire(net, issued)
        yield [mine[1]]
        pair = send(block(step), block(step), 'p')
        yield [pair]
        fire(net, chips[step])

    def far():
        yield relays
        pair = send(block(2), block(2), 'p')
        yield [pair]
        fire(net, chips[2])

    forth = [send(part(0, rows), part(0, rows), 'x', 1) for rows in (lo, hi)]
    back = [send(part(0, rows), part(0, rows), 'x', -1) for rows in (hi, lo)]
    pair = send(block(0), block(0), 'p')
    net.spawn(side(-1, lo, hi, forth))
    net.spawn(side(1, hi, lo, back))
    yield [pair]
    fire(net, chips[0])
    yield [chips[step] for step in STEPS]
    fire(net, done)


def gather_yz(net, own, full, first, done, issued=None, offset=0, near=False, split=True, pool=None):
    second = 'y' if first == 'z' else 'z'
    done.copies = []

    def emit(*args):
        done.copies.append(net.send(*args, pool=pool))
        return done.copies[-1]

    size = own.shape[0]
    half = size // 2
    lo, hi, both = pl.ds(offset, half), pl.ds(offset + half, half), pl.ds(offset, size)
    forward, backward = ((lo, hi), (hi, lo)) if split and not near else ((both,), (both,))

    def part(one, two, rows):
        return full.at[yz_index(net, first, one, two), rows]

    left = [3 if near else RING, 3 if near else RING]

    def arrived(which):
        left[which] -= 1
        if left[which] == 0 and (done, issued)[which] is not None:
            fire(net, (done, issued)[which])

    def send(one, rows, axis, step):
        src = own.at[pl.ds(rows.start - offset, rows.size)] if one == 0 else part(one, 0, rows)
        return emit(src, part(one, 0, rows), axis, step)

    def column(one):
        forth = [send(one, rows, second, 1) for rows in forward]
        back = [send(one, rows, second, -1) for rows in backward]

        def finish():
            if near:
                arrived(1)
                yield forth + back
            else:
                yield [forth[0]]
                relays = [emit(part(one, -1, lo), part(one, -1, lo), second, 1)]
                yield [back[0]]
                relays.append(emit(part(one, 1, hi), part(one, 1, hi), second, -1))
                arrived(1)
                yield forth[1:] + back[1:] + relays
            arrived(0)

        net.spawn(finish())

    relays = []

    def side(step, first_half, mine):
        yield [mine[0]]
        if not near:
            relays.append(emit(part(step, 0, first_half), part(step, 0, first_half), first, -step))
            if len(relays) == 2:
                net.spawn(far())
        yield mine[1:]
        column(step)

    def far():
        yield relays
        column(2)

    mine = [net.load(own, part(0, 0, both))]
    forth = [send(0, rows, first, 1) for rows in forward]
    back = [send(0, rows, first, -1) for rows in backward]
    column(0)
    net.spawn(side(-1, lo, forth))
    net.spawn(side(1, hi, back))
    left[0] += 1
    yield mine
    arrived(0)


def yz_index(net, first, one, two):
    return net.places[one % RING][two % RING] if first == 'z' else net.places[two % RING][one % RING]


STEPS = (2, 1, -1, 0)


def reduce_x(net, part, made, scratch, done, pool=None, relayed=None, strips=None):
    other, relay_f, relay_b, last_f, last_b = scratch
    strips = strips or [Event()]
    size = part.shape[2] // len(strips)
    done.copies = []

    def acc(k, rows=None):
        return part.at[k, net.core] if rows is None else part.at[k, net.core, rows]

    def send(*args):
        done.copies.append(net.send(*args, pool=pool))
        return done.copies[-1]

    ready = [Event() for _ in STEPS]

    def pair(k):
        yield [made[k]]
        yield [send(part.at[k, net.other], other.at[k], 'p')]
        add_into(net, acc(k), other.at[k])
        fire(net, ready[k])

    for k in range(RING):
        net.spawn(pair(k))

    def strip(n, end):
        half = size // 2
        lo, hi, both, relay_rows = pl.ds(n * size, half), pl.ds(n * size + half, half), pl.ds(n * size, size), pl.ds(n * half, half)
        sent = {}
        started, relay_sent = Event(), Event()

        def part_flow(k):
            yield [ready[k]] + ([relay_sent] if k else [])
            if k == 0:
                sent['first_f'] = send(acc(0, lo), relay_f.at[relay_rows], 'x', 1)
                sent['first_b'] = send(acc(0, hi), relay_b.at[relay_rows], 'x', -1)
                fire(net, relay_sent)
                if n == len(strips) - 1 and relayed is not None:
                    fire(net, relayed)
            elif k == 1:
                sent['direct_f'] = send(acc(1, hi), last_f.at[hi], 'x', 1)
            else:
                sent['direct_b'] = send(acc(2, lo), last_b.at[lo], 'x', -1)
            if len(sent) == 4:
                fire(net, started)

        for k in range(3):
            net.spawn(part_flow(k))
        yield [started]
        yield [sent['first_f']]
        add_into(net, acc(1, lo), relay_f.at[relay_rows])
        summed_f = send(acc(1, lo), last_f.at[lo], 'x', 1)
        yield [sent['first_b']]
        add_into(net, acc(2, hi), relay_b.at[relay_rows])
        summed_b = send(acc(2, hi), last_b.at[hi], 'x', -1)
        yield [ready[3], sent['direct_f'], sent['direct_b'], summed_f, summed_b]
        add_into(net, acc(3, both), last_f.at[both], last_b.at[both])
        fire(net, end)

    for n, end in enumerate(strips):
        net.spawn(strip(n, end))
    yield strips
    fire(net, done)


def reduce_x_scratch(rows, cols):
    return [pltpu.VMEM((RING, rows, cols), F32), pltpu.VMEM((rows // 2, cols), F32), pltpu.VMEM((rows // 2, cols), F32),
            pltpu.VMEM((rows, cols), F32), pltpu.VMEM((rows, cols), F32)]


class Sums:
    def __init__(self, net, first, scratch, stage):
        self.net, self.first, self.scratch, self.stage = net, first, scratch, stage
        self.second = 'y' if first == 'z' else 'z'

    def run(self, place, start, done, free, passed_all, pool, window, lead):
        net, first, second = self.net, self.first, self.second
        relay1, last1, relay2, last2 = self.scratch
        ahead, behind, mine = self.stage
        half = mine.shape[0] // 2
        lo, hi, all_rows = pl.ds(0, half), pl.ds(half, half), pl.ds(0, 2 * half)
        done.copies = []

        def send(*args, partner=None):
            done.copies.append(net.send(*args, pool=pool, partner=partner))
            return done.copies[-1]

        def term(one, two, rows=all_rows):
            return place(yz_index(net, first, one, two), rows)

        def bring(gate, src, dst, got):
            yield [gate, start]
            yield [net.load(src, dst)]
            fire(net, got)

        chain = [[gate] + [Event() for _ in range(RING)] for gate in free]
        free[:] = [events[RING] for events in chain]
        got = [[Event() for _ in range(RING)] for _ in range(3)]
        ends = [Event() for _ in STEPS]
        passed = [Event() for _ in range(RING)]
        passed[lead] = passed_all

        def ring(k):
            two = STEPS[k]
            if k >= window:
                yield [passed[k - window]]
            net.spawn(bring(chain[0][k], term(1, two, lo), ahead, got[0][k]))
            net.spawn(bring(chain[1][k], term(-1, two, hi), behind, got[1][k]))
            net.spawn(bring(chain[2][k], term(0, two), mine, got[2][k]))
            first_f = send(term(2, two, lo), relay1.at[0, k], first, 1)
            first_b = send(term(2, two, hi), relay1.at[1, k], first, -1)
            direct_f = send(term(1, two, hi), last1.at[0, k, hi], first, 1)
            direct_b = send(term(-1, two, lo), last1.at[1, k, lo], first, -1)
            yield [first_f, got[0][k]]
            add_into(net, relay1.at[0, k], ahead)
            fire(net, chain[0][k + 1])
            summed_f = send(relay1.at[0, k], last1.at[0, k, lo], first, 1, partner=direct_f)
            yield [first_b, got[1][k]]
            add_into(net, relay1.at[1, k], behind)
            fire(net, chain[1][k + 1])
            summed_b = send(relay1.at[1, k], last1.at[1, k, hi], first, -1, partner=direct_b)
            fire(net, passed[k])
            yield [Both(net, last1.at[0, k], direct_f, summed_f), Both(net, last1.at[1, k], direct_b, summed_b), got[2][k]]
            add_into(net, last1.at[0, k], last1.at[1, k], mine)
            fire(net, chain[2][k + 1])
            fire(net, ends[k])

        def sums(k, rows=all_rows):
            return last1.at[0, k, rows]

        yield [start]
        for k in range(RING):
            net.spawn(ring(k))
        yield [ends[0]]
        first_f = send(sums(0, lo), relay2.at[0], second, 1)
        first_b = send(sums(0, hi), relay2.at[1], second, -1)
        yield [ends[1]]
        direct_f = send(sums(1, hi), last2.at[0, hi], second, 1)
        yield [ends[2]]
        direct_b = send(sums(2, lo), last2.at[1, lo], second, -1)
        yield [first_f]
        add_into(net, sums(1, lo), relay2.at[0])
        summed_f = send(sums(1, lo), last2.at[0, lo], second, 1, partner=direct_f)
        yield [first_b]
        add_into(net, sums(2, hi), relay2.at[1])
        summed_b = send(sums(2, hi), last2.at[1, hi], second, -1, partner=direct_b)
        yield [ends[3], Both(net, last2.at[0], direct_f, summed_f), Both(net, last2.at[1], direct_b, summed_b)]
        add_into(net, sums(3), last2.at[0], last2.at[1])
        done.total = sums(3)
        fire(net, done)


def sums_scratch(rows, cols):
    return [pltpu.VMEM((2, RING, rows // 2, cols), F32), pltpu.VMEM((2, RING, rows, cols), F32),
            pltpu.VMEM((2, rows // 2, cols), F32), pltpu.VMEM((2, rows, cols), F32)]


def sums_stage(rows, cols):
    return [pltpu.VMEM((rows // 2, cols), F32), pltpu.VMEM((rows // 2, cols), F32), pltpu.VMEM((rows, cols), F32)]


def norm_rows(x_ref, u_ref):
    def body(at):
        x = x_ref[at, :].astype(F32)
        u_ref[at, :] = (x * lax.rsqrt(jnp.mean(x * x, axis=-1, keepdims=True) + NORM_EPS)).astype(BF16)

    rows_loop(x_ref.shape[0], 16, body)


def norm_back_rows(x_ref, dy_of, du_ref, dx_ref):
    def body(at):
        x = x_ref[at, :].astype(F32)
        du = du_ref[at, :]
        r = lax.rsqrt(jnp.mean(x * x, axis=-1, keepdims=True) + NORM_EPS)
        xr = x * r
        dx_ref[at, :] = (dy_of(at).astype(F32) + r * (du - xr * jnp.mean(xr * du, axis=-1, keepdims=True))).astype(BF16)

    rows_loop(x_ref.shape[0], 16, body)


def add_rows(x_ref, y_ref, out_ref):
    def body(at):
        out_ref[at, :] = (x_ref[at, :].astype(F32) + y_ref[at, :]).astype(BF16)

    rows_loop(x_ref.shape[0], 16, body)


def swap_halves(even, odd):
    low = lax.broadcasted_iota(jnp.int32, even.shape, len(even.shape) - 1) < even.shape[-1] // 2
    shift = even.shape[-1] // 2
    axis = len(even.shape) - 1
    return jnp.where(low, even, pltpu.roll(odd, shift, axis)), jnp.where(low, pltpu.roll(even, shift, axis), odd)


def split_columns(w_ref, cols_ref, layers):
    pieces, _, wide = w_ref.shape
    rows = layers
    tile = pieces * wide // (4 * RING * RING)
    for x in range(RING):
        for p in range(wide // tile):
            pair = []
            for i in (2 * p, 2 * p + 1):
                at = (i * RING + x) * tile
                pair.append(w_ref[at // wide, pl.ds(0, rows), pl.ds(at % wide, tile)].astype(F32))
            for c, value in enumerate(swap_halves(*pair)):
                cols_ref[2 * x + c, pl.ds(0, rows), pl.ds(p * tile, tile)] = value.astype(cols_ref.dtype)


def join_columns(cols_ref, w_ref):
    tile = w_ref.shape[1] // (4 * RING * RING)
    for x in range(RING):
        for p in range(cols_ref.shape[2] // tile):
            pair = [cols_ref[2 * x + c, :, pl.ds(p * tile, tile)] for c in range(2)]
            for i, value in zip((2 * p, 2 * p + 1), swap_halves(*pair)):
                w_ref[:, pl.ds((i * RING + x) * tile, tile)] = value


def call(body, out_shape, out_spaces, in_spaces, scratch, remote, sends, local, collective_id, *args):
    spaces = {'v': pl.BlockSpec(memory_space=pltpu.VMEM), 'h': pl.BlockSpec(memory_space=pl.ANY)}

    def kernel(*refs):
        net = Net(*refs[-5:-1])
        net.tile_sems = refs[-1]
        body(net, *refs[:-5])
        net.finish()
        assert net.n_remote <= remote and net.n_local <= local, (body.__name__, net.n_remote, net.n_local)

    return pl.pallas_call(
        kernel, out_shape=out_shape, in_specs=[spaces[s] for s in in_spaces], out_specs=[spaces[s] for s in out_spaces],
        scratch_shapes=list(scratch) + [pltpu.SemaphoreType.DMA((sends,)), pltpu.SemaphoreType.DMA((remote,)), pltpu.SemaphoreType.DMA((local,)),
                                               pltpu.SemaphoreType.REGULAR((14,)), pltpu.SemaphoreType.DMA((2,))],
        compiler_params=pltpu.CompilerParams(collective_id=collective_id, has_side_effects=True, vmem_limit_bytes=67000000),
        cost_estimate=pl.CostEstimate(flops=10**8, bytes_accessed=10**7, transcendentals=0),
        name=body.__name__)(*args)


WIDE = 512
EARLY = 3
STRIPS = 2
GRAD_TIME = 4.25
SLACK = 0.4
R_HIDDEN, R_DOWN, R_BACK, R_TURN, R_DDOWN, R_DDOWN2, R_DUP, R_OUT, R_PRE, R_GUP, R_GDOWN, R_DX = 2, 1, 3, 1, 2, 2, 4, 2, 2, 1, 3, 2
R_DU, HOLD = (3, 3.1, 3, 3.3), (0, 1, 2, 3)
WINDOWS = (2, 2, 3, 2, 1, 2, 3, 4)
AXES = ('yz', 'yz', 'yz', 'yz')
TOP = 6
NEAR = 'z'
LEAD = (3, 3, 3)
TR, TS, TL = 260, 64, 11


def wide_loop(total, body):
    wide = min(WIDE, total)

    def step(k, carry):
        body(k, wide, pl.ds(pl.multiple_of(k * wide, wide), wide))
        return carry

    lax.fori_loop(0, total // wide, step, 0)


def flat(value):
    return value.reshape(value.shape[0] * value.shape[1], value.shape[2])


def dot_rows(a, b):
    return jnp.dot(flat(a), flat(b), preferred_element_type=F32)


def dot_cols(a, b):
    return lax.dot_general(flat(a), flat(b), CONTRACT_COLS, preferred_element_type=F32)


def gelu(a):
    return 0.5 * a * (1.0 + jnp.tanh(GELU_C * (a + 0.044715 * a * a * a)))


def hidden_rows(net, chip, u, up, a, s):
    at = pl.ds(chip * 2, 2)

    def body(_, wide, cols):
        pre = dot_rows(u[at], up[:, :, cols]).astype(BF16)
        a[at, :, cols] = pre.reshape(2, -1, wide)
        s[at, :, cols] = gelu(pre.astype(F32)).astype(BF16).reshape(2, -1, wide)

    wide_loop(up.shape[2], body)
    net.spend(1.7)


def down_rows(net, chip, s, down, part):
    at = pl.ds(chip * 2, 2)

    def body(_, wide, cols):
        part[:, :, cols] = dot_rows(s[at], down[:, :, cols]).reshape(2, -1, wide)

    wide_loop(down.shape[2], body)
    net.spend(1.76)


def hidden_back_rows(net, chip, dy, down, ds):
    at = pl.ds(chip * 2, 2)
    rows = down.shape[1]

    def body(k, wide, cols):
        blocks = pl.ds(k * (wide // rows), wide // rows)
        ds[at, :, cols] = dot_cols(dy[at], down[blocks]).astype(BF16).reshape(2, -1, wide)

    wide_loop(down.shape[0] * rows, body)
    net.spend(1.5)


def gelu_both(a):
    t = jnp.tanh(GELU_C * (a + 0.044715 * a * a * a))
    return 0.5 * a * (1.0 + t), 0.5 * (1.0 + t) + 0.5 * a * (1.0 - t * t) * (GELU_C * (1.0 + 3 * 0.044715 * a * a))


def hidden_turn_rows(net, chip, u, up, s, ds):
    at = pl.ds(chip * 2, 2)

    def body(_, wide, cols):
        pre = dot_rows(u[at], up[:, :, cols]).astype(BF16).astype(F32)
        value, slope = gelu_both(pre)
        s[at, :, cols] = value.astype(BF16).reshape(2, -1, wide)
        ds[at, :, cols] = (ds[at, :, cols].astype(F32) * slope.reshape(2, -1, wide)).astype(BF16)

    wide_loop(up.shape[2], body)
    net.spend(2.1)


def pre_back_rows(net, chip, dy, down, a, da):
    at = pl.ds(chip * 2, 2)
    rows = down.shape[1]

    def body(k, wide, cols):
        blocks = pl.ds(k * (wide // rows), wide // rows)
        ds = dot_cols(dy[at], down[blocks]).astype(BF16).astype(F32).reshape(2, -1, wide)
        da[at, :, cols] = (ds * gelu_both(a[at, :, cols].astype(F32))[1]).astype(BF16)

    wide_loop(down.shape[0] * rows, body)
    net.spend(1.95)


def input_back_rows(net, chip, da, up, part):
    at = pl.ds(chip * 2, 2)
    rows = up.shape[1]

    def body(k, wide, cols):
        blocks = pl.ds(k * (wide // rows), wide // rows)
        part[:, :, cols] = dot_cols(da[at], up[blocks]).reshape(2, -1, wide)

    wide_loop(up.shape[0] * rows, body)
    net.spend(1.9)


def stored_tiles(net, count, compute, stage, out):
    def store(t):
        return pltpu.make_async_copy(stage.at[lax.rem(t, 2)], out(t), net.tile_sems.at[lax.rem(t, 2)])

    def step(t, carry):
        @pl.when(t >= 2)
        def _():
            store(t - 2).wait()

        compute(t, stage.at[lax.rem(t, 2)])
        store(t).start()
        return carry

    lax.fori_loop(0, count, step, 0)
    for t in range(max(count - 2, 0), count):
        store(jnp.int32(t)).wait()


def dot_tokens(a, b):
    return lax.dot_general(flat(a), flat(b), CONTRACT_ROWS, preferred_element_type=F32)


def grad_tiles(net, lhs, rhs, stage, out):
    _, high, wide = stage.shape
    across = rhs.shape[2] // wide

    def columns(t):
        return pl.ds(pl.multiple_of(lax.rem(t, across) * wide, wide), wide)

    def rows(t):
        return pl.ds(pl.multiple_of(lax.div(t, across) * high, high), high)

    def compute(t, slot):
        slot[...] = dot_tokens(lhs[:, :, rows(t)], rhs[:, :, columns(t)])

    stored_tiles(net, lhs.shape[2] // high * across, compute, stage, lambda t: out.at[rows(t), columns(t)])
    net.spend(GRAD_TIME * lhs.shape[2] / 1024)


def solution(mesh):
    nl, nd = mesh.shape['local'], mesh.shape['data']
    tok_spec = P(BOTH_AXES, None)
    w_spec = P(None, BOTH_AXES, None)

    def device_fn(tokens, grad_out, w_up, w_down):
        num_layers, ur, ffn = w_up.shape
        dr = w_down.shape[1]
        rows, width = tokens.shape
        hidden = nl * dr
        shape = jax.ShapeDtypeStruct
        up_full = shape((nl, nd * ur, hidden), BF16)
        down_full = shape((nl, dr, width), BF16)
        act_full = shape((nd, rows, width), BF16)
        hid_full = shape((nd, rows, hidden), BF16)
        own = shape((rows, width), BF16)
        part_vmem = pltpu.VMEM((RING, 2, rows, width), F32)
        rx = [part_vmem] + reduce_x_scratch(rows, width)
        sums = sums_scratch(dr, hidden) * 4 + sums_stage(dr, hidden) * 2

        def vmem(like):
            return pltpu.VMEM(like.shape, like.dtype)

        def step(net, x_in, x_halves, g_in, w_up_in, w_down_in,
                 x_out, dx_out, block_out, u_out, a_out, s_out, d_up0, d_down0, d_up1, d_down1, dw_up1, dw_down1, dw_up0, dw_down0,
                 x, u, g, up0, up1, down0, down1, ds, s, stage, part, *scratch):
            net.arrive('dyz')
            rx_scratch = scratch[:5]
            names = ('blocks', 'blocks1', 'sent_u', 'got_u', 'got_g', 'sent_up0', 'sent_down0', 'sent_up1', 'sent_down1', 'got_up0', 'got_down0',
                     'got_up1', 'got_down1', 'saved', 'free0', 'reduced0', 'ds_made', 'got_u1', 'hidden', 'all_du', 'reduced1', 'sent_dy', 'got_dy',
                     'back_up0', 'back_up0_rest', 'back_down0', 'd_down1', 'd_up1', 'y_reduced', 'acts', 'd_down0', 'da0', 'd_up0', 'du_reduced',
                     'out_up1', 'out_up0', 'got_u0', 'y_made', 'x_saved', 'weights_in', 'd_down1_0', 'relayed0')
            ev = {name: Event() for name in names}
            for kind in ('up', 'down'):
                for layer in range(2):
                    for k in range(2):
                        ev['sum_%s%d%d' % (kind, layer, k)] = Event()
            ev['got_up0'].rank = R_HIDDEN
            hidden_made, made0, made1, y_made, du_made = ([Event() for _ in STEPS] for _ in range(5))
            wide = width // 2
            half_up = nd * ur // 2
            act_pool, rs_pool = Pool(), Pool()
            job_pools = [[Pool(), Pool()], [Pool(), Pool()]]
            pools = {'up0': [Pool(), Pool()], 'down0': [Pool(), Pool()], 'up1': job_pools[0], 'down1': job_pools[1], 'blocks': [Pool(), Pool()]}
            stages = (scratch[21:24], scratch[24:27])
            job_scratch = [[scratch[5 + 8 * n + 4 * k:9 + 8 * n + 4 * k] for k in range(2)] for n in range(2)]
            frees = [[Event(0.0) for _ in range(3)] for _ in range(2)]
            freed = {k: Event() for k in range(10, 14)}

            def columns(h):
                return pl.ds(h * wide, wide)

            inputs = [net.load(x_in, x)]
            inputs += [net.load(w_up_in.at[:, pl.ds(k * hidden, hidden)], ds.at[k, pl.ds(0, num_layers * ur)]) for k in range(nd)]

            def gather(name, own, full, split):
                size = own.shape[0] // 2

                def join(kind, events):
                    yield events
                    if kind == 'got_':
                        ev[kind + name].copies = events[0].copies + events[1].copies
                    fire(net, ev[kind + name])

                got, sent = [Event(), Event()], [Event(), Event()]
                for k, first in enumerate('yz'):
                    net.spawn(gather_yz(net, own.at[pl.ds(k * size, size)], full, first, got[k], sent[k], k * size, split=split, pool=pools[name][k]))
                net.spawn(join('got_', got))
                net.spawn(join('sent_', sent))

            net.enter()
            gather('down0', w_down_in.at[0], down0, False)
            net.take(inputs)
            split_columns(ds, s, num_layers * ur)
            net.spend(0.6)
            net.spawn(exchange(net, lambda k: s.at[k, pl.ds(0, ur)], block_out.at[0], ev['blocks'], pools['blocks'][0]))
            norm_rows(x, u.at[net.data])
            net.spend(0.7)
            own_grads = net.load(g_in, g.at[net.data])

            def up_first():
                yield [ev['blocks']]
                gather('up0', block_out.at[0], up0, True)
                net.spawn(gather_x(net, u, ev['got_u'], ev['sent_u'], pool=act_pool))
                yield [ev['sent_u']]
                net.spawn(exchange(net, lambda k: s.at[k, pl.ds(ur, ur)], block_out.at[1], ev['blocks1'], pools['blocks'][1]))
                yield [own_grads]
                net.spawn(gather_x(net, g, ev['got_g']))

            def second():
                yield [ev['sent_up0'], ev['sent_down0'], ev['blocks1']]
                gather('down1', w_down_in.at[1], down1, False)
                yield [made0[EARLY]]
                gather('up1', block_out.at[1], up1, True)

            def hidden_flow():
                yield [ev['got_u'], ev['got_up0'], ev['blocks1']]
                for k, step in enumerate(STEPS):
                    hidden_rows(net, net.at('x', step), u, up0, ds, s)
                    fire(net, hidden_made[k])
                    yield [Event(net.now, R_HIDDEN)] + ([ev['relayed0']] if k == 1 else [])
                yield [net.load(ds, a_out), net.load(s, s_out), net.load(u, u_out)]
                fire(net, ev['saved'])

            def down_flow():
                for k, step in enumerate(STEPS):
                    yield [hidden_made[k], ev['got_down0'], Event(0.0, R_DOWN)] + ([ev['relayed0']] if k == 1 else [])
                    down_rows(net, net.at('x', step), s, down0, part.at[k])
                    fire(net, made0[k])
                fire(net, ev['free0'])

            here = {step: Event() for step in STEPS}
            dy_here = {step: Event() for step in STEPS}

            strips0 = [Event() for _ in range(STRIPS)]
            net.spawn(reduce_x(net, part, made0, rx_scratch, ev['reduced0'], rs_pool, ev['relayed0'], strips0))

            def next_layer():
                yield [ev['saved'], ev['got_g']]
                net.drain(ev['got_u'].copies + ev['got_g'].copies)
                credit = net.grant(3, 'xp')
                act_pool.again()
                got = [Event() for _ in strips0]
                chips = [{step: Event() for step in STEPS} for _ in strips0]

                def strip(n):
                    at = pl.ds(n * (rows // STRIPS), rows // STRIPS)
                    yield [strips0[n], credit]
                    add_rows(x.at[at], part.at[3, net.core, at], x.at[at])
                    norm_rows(x.at[at], u.at[net.data, at])
                    net.spend(1.0 / STRIPS)
                    net.spawn(gather_x(net, u, got[n], chips=chips[n], pool=act_pool, strip=(n, STRIPS)))

                def chip(step):
                    yield [arrived[step] for arrived in chips]
                    fire(net, here[step])

                for n in range(STRIPS):
                    net.spawn(strip(n))
                for step in STEPS:
                    net.spawn(chip(step))
                yield [ev['reduced0']]
                net.drain(ev['reduced0'].copies)
                yield [net.grant(4, 'xp')]
                net.spawn(reduce_x(net, part, made1, rx_scratch, ev['reduced1'], rs_pool.again()))
                yield got
                ev['got_u1'].copies = sum((event.copies for event in got), [])
                fire(net, ev['got_u1'])

            def back_flow():
                for k, step in enumerate(STEPS):
                    yield [ev['got_g'], ev['got_down1'], ev['saved'], Event(0.0, R_BACK)]
                    hidden_back_rows(net, net.at('x', step), g, down1, ds)
                fire(net, ev['ds_made'])

            def again():
                top = nd * ur * TOP // 8
                yield [ev['free0'], ev['ds_made']]
                net.drain(ev['got_up0'].copies + ev['got_down0'].copies)
                credit = net.grant(6, 'yz')
                yield [credit]
                net.spawn(gather_yz(net, w_down_in.at[0], down0, NEAR, ev['back_down0'], near=True, pool=pools['down0'][1].again()))
                net.spawn(gather_yz(net, block_out.at[0, pl.ds(0, top)], up0, 'y', ev['back_up0'], pool=pools['up0'][0].again()))
                net.spawn(gather_yz(net, block_out.at[0, pl.ds(top, nd * ur - top)], up0, 'z', ev['back_up0_rest'], offset=top, pool=pools['up0'][1].again()))

            def weights():
                yield [ev['got_up1'], ev['got_down1']]
                yield [net.grant(7, 'yz')]
                fire(net, ev['weights_in'])

            left = [RING, RING]

            turned = [Event() for _ in STEPS]

            def layer1(k, step):
                yield [here[step], ev['ds_made'], ev['got_up1'], Event(0.0, R_TURN)]
                hidden_turn_rows(net, net.at('x', step), u, up1, s, ds)
                fire(net, turned[k])
                left[0] -= 1
                if left[0] == 0:
                    fire(net, ev['hidden'])

            def layer1_back(k, step):
                yield [turned[k], Event(0.0, R_DU[k])] + ([ev['hidden']] if k in HOLD else [])
                input_back_rows(net, net.at('x', step), ds, up1, part.at[k])
                fire(net, made1[k])
                left[1] -= 1
                if left[1] == 0:
                    fire(net, ev['all_du'])

            def grads1():
                for h in range(2):
                    yield [Event(0.0, R_DDOWN2 if h else R_DDOWN), ev['hidden']]
                    grad_tiles(net, s, g.at[:, :, columns(h)], stage, d_down1.at[:, columns(h)])
                    fire(net, ev['d_down1' if h else 'd_down1_0'])
                for h in range(2):
                    yield [Event(net.now, R_DUP)]
                    grad_tiles(net, u.at[:, :, columns(h)], ds, stage, d_up1.at[columns(h)])
                fire(net, ev['d_up1'])

            def act():
                yield [ev['d_up1'], ev['all_du'], ev['got_u1']]
                own_g = [net.load(g_in.at[:, columns(h)], ds.at[h]) for h in range(2)]
                net.drain(ev['got_u1'].copies)
                credit = net.grant(5, 'xp')
                yield [ev['reduced1'], credit] + own_g
                norm_back_rows(x, lambda at: jnp.concatenate([ds[h, at, :] for h in range(2)], axis=-1), part.at[3, net.core], u.at[net.data])
                net.spend(0.7)
                net.spawn(gather_x(net, u, ev['got_dy'], ev['sent_dy'], dy_here, pool=act_pool.again()))

            def layer1_out():
                yield [ev['reduced1'], Event(0.0, R_OUT)]
                net.drain(ev['reduced1'].copies)
                credit = net.grant(8, 'xp')
                for k, step in enumerate(STEPS):
                    down_rows(net, net.at('x', step), s, down1, part.at[k])
                    yield [Event(net.now, R_OUT)]
                fire(net, ev['y_made'])
                yield [ev['sent_dy'], credit]
                net.spawn(reduce_x(net, part, y_made, rx_scratch, ev['y_reduced'], rs_pool.again()))
                for k in range(RING):
                    fire(net, y_made[k])
                yield [ev['y_reduced']]
                add_rows(x, part.at[3, net.core], x)
                yield [net.load(x, x_out)]
                fire(net, ev['x_saved'])

            a0, s0 = up1.at[pl.ds(0, nd)], up1.at[pl.ds(nd, nd)]
            backs = [RING]

            def bring_back():
                yield [ev['d_down1']]
                yield [net.load(u_out, g)]
                fire(net, ev['got_u0'])

            def bring_acts():
                yield [ev['all_du']]
                net.drain(ev['got_up1'].copies)
                yield [net.load(a_out, a0), net.load(s_out, s0)]
                fire(net, ev['acts'])

            def layer0_hidden(step):
                yield [dy_here[step], ev['acts'], ev['back_down0'], ev['d_up1'], Event(0.0, R_PRE)]
                pre_back_rows(net, net.at('x', step), u, down0, a0, ds)
                backs[0] -= 1
                if backs[0] == 0:
                    fire(net, ev['da0'])

            def layer0():
                for h in range(2):
                    yield [ev['da0'], ev['got_u0'], Event(0.0, R_GUP)]
                    grad_tiles(net, g.at[:, :, columns(h)], ds, stage, d_up0.at[columns(h)])
                fire(net, ev['d_up0'])
                for h in range(2):
                    yield [ev['got_dy'], ev['acts'], Event(0.0, R_GDOWN)]
                    grad_tiles(net, s0, u.at[:, :, columns(h)], stage, d_down0.at[:, columns(h)])
                fire(net, ev['d_down0'])
                yield [ev['y_reduced'], ev['back_up0'], ev['back_up0_rest'], Event(0.0, R_DX)]
                net.drain(ev['y_reduced'].copies + ev['got_down1'].copies)
                x0 = down1.at[pl.ds(0, x_halves.shape[0])]
                yield [net.grant(9, 'xp'), net.load(x_halves, x0)]
                net.spawn(reduce_x(net, part, du_made, rx_scratch, ev['du_reduced'], rs_pool.again()))
                for k, step in enumerate(STEPS):
                    input_back_rows(net, net.at('x', step), ds, up0, part.at[k])
                    fire(net, du_made[k])
                    yield [Event(net.now, R_DX)]
                yield [ev['du_reduced'], ev['x_saved']]
                for q in range(x_halves.shape[0]):
                    rows_q = pl.ds(q * dr, dr)
                    dy_q = u.at[net.data, rows_q]
                    norm_back_rows(x0.at[q], lambda at, dy_q=dy_q: dy_q[at, :], part.at[3, net.core, rows_q], x.at[rows_q])
                yield [net.load(x, dx_out)]

            def up_place(ref, k):
                return lambda block, rows: ref.at[pl.ds(pl.multiple_of(block * (2 * half_up) + k * half_up + rows.start, rows.size), rows.size)]

            def down_place(ref, k):
                return lambda block, rows: ref.at[pl.ds(pl.multiple_of(block * dr + rows.start, rows.size), rows.size), columns(k)]

            def gate(event, items, pool):
                yield items
                pool.again()
                fire(net, event)

            def sum_job(job, place, ref, ready, name, credits=()):
                passed = [Event(), Event()]
                for k in range(2):
                    start = Event()
                    n = job % 2
                    net.spawn(gate(start, ready[k] + ([credits[k]] if credits else []), job_pools[n][k]))
                    sums = Sums(net, AXES[job][k], job_scratch[n][k], stages[k])
                    net.spawn(sums.run(place(ref, k), start, ev['sum_%s%d' % (name, k)], frees[k], passed[k], job_pools[n][k], WINDOWS[2 * job + k], LEAD[min(job, 2)]))
                return passed

            def out_down(layer, dw_down, credit):
                def one(k):
                    done = ev['sum_down%d%d' % (layer, k)]
                    yield [done]
                    yield [net.load(done.total, dw_down.at[:, columns(k)])]
                    if credit is not None:
                        net.drain(done.copies)
                        yield [net.grant(credit + k, 'yz')]
                        fire(net, freed[credit + k])

                for k in range(2):
                    net.spawn(one(k))

            def out_up(n, layer, dw_up, credit):
                totals = [ev['sum_up%d%d' % (layer, k)] for k in range(2)]
                yield totals
                net.drain(totals[0].copies + totals[1].copies)
                spare = job_scratch[n][0][0].at[0]
                for k, done in enumerate(totals):
                    for q in range(2):
                        copy_rows(net, done.total.at[pl.ds(q * spare.shape[1], spare.shape[1])], spare.at[2 * k + q])
                done = ev['out_up%d' % layer]
                net.spawn(exchange_back(net, spare, dw_up, done, pools['blocks'][layer].again()))
                if credit is not None:
                    yield [done]
                    for k in range(2):
                        yield [net.grant(credit + k, 'yz')]
                        fire(net, freed[credit + k])

            passed = sum_job(0, down_place, d_down1, [[ev['d_down1_0'], ev['weights_in']], [ev['d_down1'], ev['weights_in']]], 'down1')
            passed = sum_job(1, up_place, d_up1, [[ev['d_up1']] + passed] * 2, 'up1')
            passed = sum_job(2, up_place, d_up0, [[ev['d_up0']] + passed] * 2, 'up0', [freed[10], freed[11]])
            sum_job(3, down_place, d_down0, [[ev['d_down0']] + passed] * 2, 'down0', [freed[12], freed[13]])
            out_down(1, dw_down1, 10)
            net.spawn(out_up(1, 1, dw_up1, 12))
            net.spawn(out_up(0, 0, dw_up0, None))
            out_down(0, dw_down0, None)
            for k in (3, 2, 1, 0):
                net.spawn(layer1(k, STEPS[k]))
            for k in range(RING):
                net.spawn(layer1_back(k, STEPS[k]))
            for step in (0, -1, 1, 2):
                net.spawn(layer0_hidden(step))
            for flow in (up_first(), second(), hidden_flow(), down_flow(), next_layer(), back_flow(), again(), weights(), grads1(), act(), layer1_out(),
                         bring_back(), bring_acts(), layer0()):
                net.spawn(flow)
            net.run()

        def finish(*refs):
            sources, targets, held, ups, sems = refs[:6], refs[6:10], refs[10:16], refs[16:18], refs[18]
            x_out, dx_out, up_out, down_out = targets
            loads = [pltpu.make_async_copy(src, dst, sems.at[k]) for k, (src, dst) in enumerate(zip(sources, held))]
            stores = [(ups[1], up_out.at[1]), (ups[0], up_out.at[0]), (held[2], down_out.at[1]), (held[3], down_out.at[0]), (held[4], x_out), (held[5], dx_out)]
            stores = [pltpu.make_async_copy(src, dst, sems.at[6 + k]) for k, (src, dst) in enumerate(stores)]
            for load in loads:
                load.start()
            for k in (2, 3, 4, 5):
                loads[k].wait()
                stores[k].start()
            for k in (0, 1):
                loads[k].wait()
                join_columns(held[k], ups[1 - k])
                stores[k].start()
            for store in stores:
                store.wait()

        d_up_own, d_down_own = shape((nd, ur, hidden), F32), shape((dr, width), F32)

        d_up_full, d_down_full = shape((width, hidden), F32), shape((hidden, width), F32)
        x_out, dx, _, _, _, _, _, _, _, _, *grads = call(
            step, [own, own, shape((num_layers, nd * ur, hidden), BF16), act_full, hid_full, hid_full] + [d_up_full, d_down_full] * 2
            + [d_up_own, d_down_own] * 2, 'h' * 14, 'hhhhh',
            [vmem(own)] + [vmem(act_full)] * 2 + [vmem(up_full)] * 2 + [vmem(down_full)] * 2 + [vmem(hid_full)] * 2
            + [pltpu.VMEM((2, hidden // 2, width // 4), F32)] + rx + sums, TR, TS, TL, 0,
            tokens, tokens.reshape(rows // dr, dr, width), grad_out, w_up.reshape(num_layers * ur, ffn), w_down)
        up1_own, down1_own, up0_own, down0_own = grads
        held = [d_up_own, d_up_own, d_down_own, d_down_own, own, own]
        return pl.pallas_call(
            finish, out_shape=[own, own, shape(w_up.shape, F32), shape(w_down.shape, F32)], name='finish',
            in_specs=[pl.BlockSpec(memory_space=pl.ANY)] * 6, out_specs=[pl.BlockSpec(memory_space=pl.ANY)] * 4,
            scratch_shapes=[vmem(like) for like in held] + [pltpu.VMEM(w_up.shape[1:], F32)] * 2 + [pltpu.SemaphoreType.DMA((12,))],
        )(up1_own, up0_own, down1_own, down0_own, x_out, dx)

    return jax.shard_map(device_fn, mesh=mesh, in_specs=(tok_spec, tok_spec, w_spec, w_spec), out_specs=(tok_spec, tok_spec, w_spec, w_spec), check_vma=False)
```

```python
import jax
import jax.numpy as jnp
from jax import lax
from jax.experimental import pallas as pl
from jax.experimental.pallas import tpu as pltpu
from jax.sharding import PartitionSpec as P

NORM_EPS = 1e-6
BOTH_AXES = ('local', 'data')
CONTRACT_ROWS = (((0,), (0,)), ((), ()))
CONTRACT_COLS = (((1,), (1,)), ((), ()))
MESH = pl.DeviceIdType.MESH
RING = 4
F32, BF16 = jnp.float32, jnp.bfloat16

LINK_RATE = 46.0e3
PAIR_RATE = 600e3
LOCAL_RATE = 3000e3
HOP = 2.4
PAIR_HOP = 1.0
ENTRY = 4.2
GELU_C = 0.7978845608028654


class Event:
    def __init__(self, time=None, rank=0):
        self.time, self.rank = time, rank


class Copy:
    def __init__(self, desc, time, remote):
        self.desc, self.time, self.remote, self.rank, self.waited = desc, time, remote, 0, False

    def wait(self):
        if self.remote:
            self.desc.wait_recv()
        else:
            self.desc.wait()


class Credit:
    def __init__(self, semaphore, count, time):
        self.semaphore, self.count, self.time, self.rank, self.waited = semaphore, count, time, 0, False

    def wait(self):
        pl.semaphore_wait(self.semaphore, self.count)


class Both:
    def __init__(self, net, dst, one, two):
        self.desc = pltpu.make_async_remote_copy(
            src_ref=dst, dst_ref=dst, send_sem=net.send_sems.at[one.slot], recv_sem=net.recv_sems.at[one.receive],
            device_id=net.device('p', 1), device_id_type=MESH)
        self.time, self.rank, self.waited = max(one.time, two.time), 0, False

    def wait(self):
        self.desc.wait_recv()


class Pool:
    def __init__(self):
        self.slots, self.next = [], 0

    def again(self):
        self.next = 0
        return self


class Net:
    def __init__(self, send_sems, recv_sems, local_sems, credit_sems):
        self.send_sems, self.recv_sems, self.local_sems, self.credit_sems = send_sems, recv_sems, local_sems, credit_sems
        self.n_remote = self.n_local = 0
        self.free_sends = list(range(send_sems.shape[0]))
        self.free_locals = []
        self.now = 0.0
        self.free = {}
        self.sent = []
        self.flows = []
        here, there = lax.axis_index('local'), lax.axis_index('data')
        pos = {'z': here // RING, 'y': lax.rem(here, RING), 'x': there // 2}
        self.data, self.core = there, lax.rem(there, 2)
        self.ring = {axis: [at] + [lax.rem(at + step, RING) for step in range(1, RING)] for axis, at in pos.items()}
        self.hops = [there] + [lax.rem(there + step, 2 * RING) for step in range(1, 2 * RING)]
        self.blocks = [at * 2 + self.core for at in self.ring['x']]
        self.places = [[z * RING + y for y in self.ring['y']] for z in self.ring['z']]
        self.partner = pos['x'] * 2 + (1 - self.core)
        self.other = 1 - self.core

    def at(self, axis, step):
        return self.ring[axis][step % RING]

    def block(self, step):
        return self.blocks[step % RING]

    def device(self, axis, step):
        if axis == 'p':
            return {'data': self.partner}
        if axis == 'd':
            return {'data': self.hops[step % (2 * RING)]}
        if axis == 'x':
            return {'data': self.block(step)}
        if axis == 'y':
            return {'local': self.places[0][step % RING]}
        return {'local': self.places[step % RING][0]}

    def peers(self, axes):
        return [(axis, step) for axis in axes for step in ((1, -1) if axis in 'xyz' else (1,) if axis == 'p' else range(1, 2 * RING))]

    def signal(self, semaphore, axes):
        for axis, step in self.peers(axes):
            pl.semaphore_signal(semaphore, inc=1, device_id=self.device(axis, step), device_id_type=MESH)

    def arrive(self, axes):
        self.entry, self.entered = pltpu.get_barrier_semaphore(), len(self.peers(axes))
        self.signal(self.entry, axes)

    def enter(self):
        pl.semaphore_wait(self.entry, self.entered)
        self.now = max(self.now, ENTRY)

    def take(self, copies):
        for copy in copies:
            copy.wait()
            copy.waited = True
            self.free_locals.append(copy.slot)
            self.now = max(self.now, copy.time)

    def grant(self, k, axes):
        self.signal(self.credit_sems.at[k], axes)
        return Credit(self.credit_sems.at[k], len(self.peers(axes)), self.now + HOP)

    def drain(self, copies):
        for copy in copies:
            if copy in self.sent:
                copy.desc.wait_send()
                self.sent.remove(copy)
                self.free_sends.append(copy.slot)

    def idle(self, gap):
        over = [copy for copy in self.sent if copy.time + 1.5 < self.now]
        self.drain(over[:int(gap / 0.05)])

    def send(self, src, dst, axis, step=1, pool=None, partner=None):
        if partner is not None:
            k = partner.receive
        elif pool is not None and pool.next < len(pool.slots):
            k = pool.slots[pool.next]
        else:
            k = self.n_remote
            self.n_remote += 1
            if pool is not None:
                pool.slots.append(k)
        if pool is not None and partner is None:
            pool.next += 1
        if not self.free_sends:
            over = [copy for copy in self.sent if copy.time + 1.0 < self.now]
            self.drain(over or [min(self.sent, key=lambda copy: copy.time)])
        send_slot = self.free_sends.pop()
        desc = pltpu.make_async_remote_copy(
            src_ref=src, dst_ref=dst, send_sem=self.send_sems.at[send_slot], recv_sem=self.recv_sems.at[k],
            device_id=self.device(axis, step), device_id_type=MESH)
        desc.start()
        size = 1
        for n in dst.shape:
            size *= n
        size *= dst.dtype.itemsize
        rate = PAIR_RATE if axis == 'p' else LINK_RATE
        extra = 4.4 if axis == 'd' else 0.0
        if axis == 'd':
            axis, step, size = ('p', 1, size) if step == 1 else ('x', 1 if step < RING + 2 else -1, size)
        key = (axis, step)
        done = max(self.free.get(key, 0.0), self.now) + size / rate
        self.free[key] = done
        copy = Copy(desc, done + extra + (PAIR_HOP if axis == 'p' else HOP), True)
        copy.slot, copy.receive = send_slot, k
        self.sent.append(copy)
        return copy

    def load(self, src, dst):
        if not self.free_locals:
            self.free_locals.append(self.n_local)
            self.n_local += 1
        k = self.free_locals.pop()
        desc = pltpu.make_async_copy(src, dst, self.local_sems.at[k])
        desc.start()
        size = 1
        for n in dst.shape:
            size *= n
        done = max(self.free.get('hbm', 0.0), self.now) + size * dst.dtype.itemsize / LOCAL_RATE
        self.free['hbm'] = done
        copy = Copy(desc, done + 0.9, False)
        copy.slot = k
        return copy

    def spend(self, microseconds):
        self.now += microseconds

    def spawn(self, flow):
        self.step(flow)

    def step(self, flow):
        try:
            self.flows.append((flow, next(flow)))
        except StopIteration:
            pass

    def run(self):
        while self.flows:
            best = None
            for k, (_, items) in enumerate(self.flows):
                if any(item.time is None for item in items):
                    continue
                time = max([item.time for item in items] + [0.0])
                late = max([item.rank for item in items] + [0])
                rank = (max(time, self.now) + (SLACK if late else 0.0), late, time)
                if best is None or rank < best[0]:
                    best = (rank, k, time)
            _, k, time = best
            flow, items = self.flows.pop(k)
            self.idle(time - self.now)
            for item in items:
                if not isinstance(item, Event) and not item.waited:
                    item.wait()
                    item.waited = True
                    if isinstance(item, Copy) and not item.remote:
                        self.free_locals.append(item.slot)
            self.now = max(self.now, time)
            self.step(flow)

    def finish(self):
        for copy in self.sent:
            copy.desc.wait_send()


def rows_loop(rows, chunk, body):
    chunk = min(chunk, rows)

    def step(k, carry):
        body(pl.ds(pl.multiple_of(k * chunk, chunk), chunk))
        return carry

    lax.fori_loop(0, rows // chunk, step, 0)


def add_into(net, dst, *others):
    rows, cols = dst.shape

    def body(at):
        total = dst[at, :]
        for other in others:
            total = total + other[at, :]
        dst[at, :] = total

    rows_loop(rows, 16, body)
    net.spend(rows * cols * 4 * (1 + len(others)) / 4e6)


def fire(net, event):
    event.time = net.now


def exchange(net, source, dst, done, pool):
    rows = dst.shape[0] // (2 * RING)

    def mine():
        return dst.at[pl.ds(pl.multiple_of(net.data * rows, rows), rows)]

    own = net.load(source(net.data), mine())
    copies = [net.send(source(net.hops[k]), mine(), 'd', k, pool) for k in (4, 5, 2, 3, 6, 7, 1)]
    yield [own] + copies
    net.drain(copies)
    fire(net, done)


def exchange_back(net, src, dst, done, pool):
    rows = dst.shape[1]
    per = src.shape[1] // rows

    def block(k):
        return src.at[lax.div(k, per), pl.ds(pl.multiple_of(lax.rem(k, per) * rows, rows), rows)]

    own = net.load(block(net.data), dst.at[net.data])
    copies = [net.send(block(net.hops[k]), dst.at[net.data], 'd', k, pool) for k in (4, 5, 2, 3, 6, 7, 1)]
    yield [own] + copies
    net.drain(copies)
    fire(net, done)


def copy_rows(net, src, dst):
    def body(at):
        dst[at, :] = src[at, :]

    rows_loop(src.shape[0], 16, body)
    net.spend(0.2)


def gather_x(net, full, done, issued=None, chips=None, pool=None, strip=(0, 1)):
    size = full.shape[1] // strip[1]
    base, half = strip[0] * size, size // 2
    lo, hi, both = pl.ds(base, half), pl.ds(base + half, half), pl.ds(base, size)
    chips = chips or {step: Event() for step in STEPS}
    left = [2]
    done.copies = []

    def send(*args):
        done.copies.append(net.send(*args, pool=pool))
        return done.copies[-1]

    def block(step):
        return full.at[net.block(step), both]

    def part(step, rows):
        return full.at[net.block(step), rows]

    relays = []

    def side(step, first, second, mine):
        yield [mine[0]]
        relays.append(send(part(step, first), part(step, first), 'x', -step))
        left[0] -= 1
        if left[0] == 0:
            net.spawn(far())
            if issued is not None:
                fire(net, issued)
        yield [mine[1]]
        pair = send(block(step), block(step), 'p')
        yield [pair]
        fire(net, chips[step])

    def far():
        yield relays
        pair = send(block(2), block(2), 'p')
        yield [pair]
        fire(net, chips[2])

    forth = [send(part(0, rows), part(0, rows), 'x', 1) for rows in (lo, hi)]
    back = [send(part(0, rows), part(0, rows), 'x', -1) for rows in (hi, lo)]
    pair = send(block(0), block(0), 'p')
    net.spawn(side(-1, lo, hi, forth))
    net.spawn(side(1, hi, lo, back))
    yield [pair]
    fire(net, chips[0])
    yield [chips[step] for step in STEPS]
    fire(net, done)


def gather_yz(net, own, full, first, done, issued=None, offset=0, near=False, split=True, pool=None):
    second = 'y' if first == 'z' else 'z'
    done.copies = []

    def emit(*args):
        done.copies.append(net.send(*args, pool=pool))
        return done.copies[-1]

    size = own.shape[0]
    half = size // 2
    lo, hi, both = pl.ds(offset, half), pl.ds(offset + half, half), pl.ds(offset, size)
    forward, backward = ((lo, hi), (hi, lo)) if split and not near else ((both,), (both,))

    def part(one, two, rows):
        return full.at[yz_index(net, first, one, two), rows]

    left = [3 if near else RING, 3 if near else RING]

    def arrived(which):
        left[which] -= 1
        if left[which] == 0 and (done, issued)[which] is not None:
            fire(net, (done, issued)[which])

    def send(one, rows, axis, step):
        src = own.at[pl.ds(rows.start - offset, rows.size)] if one == 0 else part(one, 0, rows)
        return emit(src, part(one, 0, rows), axis, step)

    def column(one):
        forth = [send(one, rows, second, 1) for rows in forward]
        back = [send(one, rows, second, -1) for rows in backward]

        def finish():
            if near:
                arrived(1)
                yield forth + back
            else:
                yield [forth[0]]
                relays = [emit(part(one, -1, lo), part(one, -1, lo), second, 1)]
                yield [back[0]]
                relays.append(emit(part(one, 1, hi), part(one, 1, hi), second, -1))
                arrived(1)
                yield forth[1:] + back[1:] + relays
            arrived(0)

        net.spawn(finish())

    relays = []

    def side(step, first_half, mine):
        yield [mine[0]]
        if not near:
            relays.append(emit(part(step, 0, first_half), part(step, 0, first_half), first, -step))
            if len(relays) == 2:
                net.spawn(far())
        yield mine[1:]
        column(step)

    def far():
        yield relays
        column(2)

    mine = [net.load(own, part(0, 0, both))]
    forth = [send(0, rows, first, 1) for rows in forward]
    back = [send(0, rows, first, -1) for rows in backward]
    column(0)
    net.spawn(side(-1, lo, forth))
    net.spawn(side(1, hi, back))
    left[0] += 1
    yield mine
    arrived(0)


def yz_index(net, first, one, two):
    return net.places[one % RING][two % RING] if first == 'z' else net.places[two % RING][one % RING]


STEPS = (2, 1, -1, 0)


def reduce_x(net, part, made, scratch, done, pool=None, relayed=None, strips=None):
    other, relay_f, relay_b, last_f, last_b = scratch
    strips = strips or [Event()]
    size = part.shape[2] // len(strips)
    done.copies = []

    def acc(k, rows=None):
        return part.at[k, net.core] if rows is None else part.at[k, net.core, rows]

    def send(*args):
        done.copies.append(net.send(*args, pool=pool))
        return done.copies[-1]

    ready = [Event() for _ in STEPS]

    def pair(k):
        yield [made[k]]
        yield [send(part.at[k, net.other], other.at[k], 'p')]
        add_into(net, acc(k), other.at[k])
        fire(net, ready[k])

    for k in range(RING):
        net.spawn(pair(k))

    def strip(n, end):
        half = size // 2
        lo, hi, both, relay_rows = pl.ds(n * size, half), pl.ds(n * size + half, half), pl.ds(n * size, size), pl.ds(n * half, half)
        sent = {}
        started, relay_sent = Event(), Event()

        def part_flow(k):
            yield [ready[k]] + ([relay_sent] if k else [])
            if k == 0:
                sent['first_f'] = send(acc(0, lo), relay_f.at[relay_rows], 'x', 1)
                sent['first_b'] = send(acc(0, hi), relay_b.at[relay_rows], 'x', -1)
                fire(net, relay_sent)
                if n == len(strips) - 1 and relayed is not None:
                    fire(net, relayed)
            elif k == 1:
                sent['direct_f'] = send(acc(1, hi), last_f.at[hi], 'x', 1)
            else:
                sent['direct_b'] = send(acc(2, lo), last_b.at[lo], 'x', -1)
            if len(sent) == 4:
                fire(net, started)

        for k in range(3):
            net.spawn(part_flow(k))
        yield [started]
        yield [sent['first_f']]
        add_into(net, acc(1, lo), relay_f.at[relay_rows])
        summed_f = send(acc(1, lo), last_f.at[lo], 'x', 1)
        yield [sent['first_b']]
        add_into(net, acc(2, hi), relay_b.at[relay_rows])
        summed_b = send(acc(2, hi), last_b.at[hi], 'x', -1)
        yield [ready[3], sent['direct_f'], sent['direct_b'], summed_f, summed_b]
        add_into(net, acc(3, both), last_f.at[both], last_b.at[both])
        fire(net, end)

    for n, end in enumerate(strips):
        net.spawn(strip(n, end))
    yield strips
    fire(net, done)


def reduce_x_scratch(rows, cols):
    return [pltpu.VMEM((RING, rows, cols), F32), pltpu.VMEM((rows // 2, cols), F32), pltpu.VMEM((rows // 2, cols), F32),
            pltpu.VMEM((rows, cols), F32), pltpu.VMEM((rows, cols), F32)]


class Sums:
    def __init__(self, net, first, scratch, stage):
        self.net, self.first, self.scratch, self.stage = net, first, scratch, stage
        self.second = 'y' if first == 'z' else 'z'

    def run(self, place, start, done, free, passed_all, pool, window, lead):
        net, first, second = self.net, self.first, self.second
        relay1, last1, relay2, last2 = self.scratch
        ahead, behind, mine = self.stage
        half = mine.shape[0] // 2
        lo, hi, all_rows = pl.ds(0, half), pl.ds(half, half), pl.ds(0, 2 * half)
        done.copies = []

        def send(*args, partner=None):
            done.copies.append(net.send(*args, pool=pool, partner=partner))
            return done.copies[-1]

        def term(one, two, rows=all_rows):
            return place(yz_index(net, first, one, two), rows)

        def bring(gate, src, dst, got):
            yield [gate, start]
            yield [net.load(src, dst)]
            fire(net, got)

        chain = [[gate] + [Event() for _ in range(RING)] for gate in free]
        free[:] = [events[RING] for events in chain]
        got = [[Event() for _ in range(RING)] for _ in range(3)]
        ends = [Event() for _ in STEPS]
        passed = [Event() for _ in range(RING)]
        passed[lead] = passed_all

        def ring(k):
            two = STEPS[k]
            if k >= window:
                yield [passed[k - window]]
            net.spawn(bring(chain[0][k], term(1, two, lo), ahead, got[0][k]))
            net.spawn(bring(chain[1][k], term(-1, two, hi), behind, got[1][k]))
            net.spawn(bring(chain[2][k], term(0, two), mine, got[2][k]))
            first_f = send(term(2, two, lo), relay1.at[0, k], first, 1)
            first_b = send(term(2, two, hi), relay1.at[1, k], first, -1)
            direct_f = send(term(1, two, hi), last1.at[0, k, hi], first, 1)
            direct_b = send(term(-1, two, lo), last1.at[1, k, lo], first, -1)
            yield [first_f, got[0][k]]
            add_into(net, relay1.at[0, k], ahead)
            fire(net, chain[0][k + 1])
            summed_f = send(relay1.at[0, k], last1.at[0, k, lo], first, 1, partner=direct_f)
            yield [first_b, got[1][k]]
            add_into(net, relay1.at[1, k], behind)
            fire(net, chain[1][k + 1])
            summed_b = send(relay1.at[1, k], last1.at[1, k, hi], first, -1, partner=direct_b)
            fire(net, passed[k])
            yield [Both(net, last1.at[0, k], direct_f, summed_f), Both(net, last1.at[1, k], direct_b, summed_b), got[2][k]]
            add_into(net, last1.at[0, k], last1.at[1, k], mine)
            fire(net, chain[2][k + 1])
            fire(net, ends[k])

        def sums(k, rows=all_rows):
            return last1.at[0, k, rows]

        yield [start]
        for k in range(RING):
            net.spawn(ring(k))
        yield [ends[0]]
        first_f = send(sums(0, lo), relay2.at[0], second, 1)
        first_b = send(sums(0, hi), relay2.at[1], second, -1)
        yield [ends[1]]
        direct_f = send(sums(1, hi), last2.at[0, hi], second, 1)
        yield [ends[2]]
        direct_b = send(sums(2, lo), last2.at[1, lo], second, -1)
        yield [first_f]
        add_into(net, sums(1, lo), relay2.at[0])
        summed_f = send(sums(1, lo), last2.at[0, lo], second, 1, partner=direct_f)
        yield [first_b]
        add_into(net, sums(2, hi), relay2.at[1])
        summed_b = send(sums(2, hi), last2.at[1, hi], second, -1, partner=direct_b)
        yield [ends[3], Both(net, last2.at[0], direct_f, summed_f), Both(net, last2.at[1], direct_b, summed_b)]
        add_into(net, sums(3), last2.at[0], last2.at[1])
        done.total = sums(3)
        fire(net, done)


def sums_scratch(rows, cols):
    return [pltpu.VMEM((2, RING, rows // 2, cols), F32), pltpu.VMEM((2, RING, rows, cols), F32),
            pltpu.VMEM((2, rows // 2, cols), F32), pltpu.VMEM((2, rows, cols), F32)]


def sums_stage(rows, cols):
    return [pltpu.VMEM((rows // 2, cols), F32), pltpu.VMEM((rows // 2, cols), F32), pltpu.VMEM((rows, cols), F32)]


def norm_rows(x_ref, u_ref):
    def body(at):
        x = x_ref[at, :].astype(F32)
        u_ref[at, :] = (x * lax.rsqrt(jnp.mean(x * x, axis=-1, keepdims=True) + NORM_EPS)).astype(BF16)

    rows_loop(x_ref.shape[0], 16, body)


def norm_back_rows(x_ref, dy_of, du_ref, dx_ref):
    def body(at):
        x = x_ref[at, :].astype(F32)
        du = du_ref[at, :]
        r = lax.rsqrt(jnp.mean(x * x, axis=-1, keepdims=True) + NORM_EPS)
        xr = x * r
        dx_ref[at, :] = (dy_of(at).astype(F32) + r * (du - xr * jnp.mean(xr * du, axis=-1, keepdims=True))).astype(BF16)

    rows_loop(x_ref.shape[0], 16, body)


def add_rows(x_ref, y_ref, out_ref):
    def body(at):
        out_ref[at, :] = (x_ref[at, :].astype(F32) + y_ref[at, :]).astype(BF16)

    rows_loop(x_ref.shape[0], 16, body)


def swap_halves(even, odd):
    low = lax.broadcasted_iota(jnp.int32, even.shape, len(even.shape) - 1) < even.shape[-1] // 2
    shift = even.shape[-1] // 2
    axis = len(even.shape) - 1
    return jnp.where(low, even, pltpu.roll(odd, shift, axis)), jnp.where(low, pltpu.roll(even, shift, axis), odd)


def split_columns(w_ref, cols_ref, layers):
    pieces, _, wide = w_ref.shape
    rows = layers
    tile = pieces * wide // (4 * RING * RING)
    for x in range(RING):
        for p in range(wide // tile):
            pair = []
            for i in (2 * p, 2 * p + 1):
                at = (i * RING + x) * tile
                pair.append(w_ref[at // wide, pl.ds(0, rows), pl.ds(at % wide, tile)].astype(F32))
            for c, value in enumerate(swap_halves(*pair)):
                cols_ref[2 * x + c, pl.ds(0, rows), pl.ds(p * tile, tile)] = value.astype(cols_ref.dtype)


def join_columns(cols_ref, w_ref):
    tile = w_ref.shape[1] // (4 * RING * RING)
    for x in range(RING):
        for p in range(cols_ref.shape[2] // tile):
            pair = [cols_ref[2 * x + c, :, pl.ds(p * tile, tile)] for c in range(2)]
            for i, value in zip((2 * p, 2 * p + 1), swap_halves(*pair)):
                w_ref[:, pl.ds((i * RING + x) * tile, tile)] = value


def call(body, out_shape, out_spaces, in_spaces, scratch, remote, sends, local, collective_id, *args):
    spaces = {'v': pl.BlockSpec(memory_space=pltpu.VMEM), 'h': pl.BlockSpec(memory_space=pl.ANY)}

    def kernel(*refs):
        net = Net(*refs[-5:-1])
        net.tile_sems = refs[-1]
        body(net, *refs[:-5])
        net.finish()
        assert net.n_remote <= remote and net.n_local <= local, (body.__name__, net.n_remote, net.n_local)

    return pl.pallas_call(
        kernel, out_shape=out_shape, in_specs=[spaces[s] for s in in_spaces], out_specs=[spaces[s] for s in out_spaces],
        scratch_shapes=list(scratch) + [pltpu.SemaphoreType.DMA((sends,)), pltpu.SemaphoreType.DMA((remote,)), pltpu.SemaphoreType.DMA((local,)),
                                               pltpu.SemaphoreType.REGULAR((14,)), pltpu.SemaphoreType.DMA((2,))],
        compiler_params=pltpu.CompilerParams(collective_id=collective_id, has_side_effects=True, vmem_limit_bytes=67000000),
        cost_estimate=pl.CostEstimate(flops=10**8, bytes_accessed=10**7, transcendentals=0),
        name=body.__name__)(*args)


WIDE = 512
EARLY = 3
STRIPS = 2
GRAD_TIME = 4.25
SLACK = 0.4
R_HIDDEN, R_DOWN, R_BACK, R_TURN, R_DDOWN, R_DDOWN2, R_DUP, R_OUT, R_PRE, R_GUP, R_GDOWN, R_DX = 2, 1, 3, 1, 2, 2, 4, 2, 2, 1, 3, 2
R_DU, HOLD = (3, 3.1, 3, 3.3), (0, 1, 2, 3)
WINDOWS = (2, 2, 3, 2, 1, 2, 3, 4)
AXES = ('yz', 'yz', 'yz', 'yz')
TOP = 6
NEAR = 'z'
LEAD = (3, 3, 3)
TR, TS, TL = 260, 64, 9


def wide_loop(total, body):
    wide = min(WIDE, total)

    def step(k, carry):
        body(k, wide, pl.ds(pl.multiple_of(k * wide, wide), wide))
        return carry

    lax.fori_loop(0, total // wide, step, 0)


def flat(value):
    return value.reshape(value.shape[0] * value.shape[1], value.shape[2])


def dot_rows(a, b):
    return jnp.dot(flat(a), flat(b), preferred_element_type=F32)


def dot_cols(a, b):
    return lax.dot_general(flat(a), flat(b), CONTRACT_COLS, preferred_element_type=F32)


def gelu(a):
    return 0.5 * a * (1.0 + jnp.tanh(GELU_C * (a + 0.044715 * a * a * a)))


def hidden_rows(net, chip, u, up, a, s):
    at = pl.ds(chip * 2, 2)

    def body(_, wide, cols):
        pre = dot_rows(u[at], up[:, :, cols]).astype(BF16)
        a[at, :, cols] = pre.reshape(2, -1, wide)
        s[at, :, cols] = gelu(pre.astype(F32)).astype(BF16).reshape(2, -1, wide)

    wide_loop(up.shape[2], body)
    net.spend(1.7)


def down_rows(net, chip, s, down, part):
    at = pl.ds(chip * 2, 2)

    def body(_, wide, cols):
        part[:, :, cols] = dot_rows(s[at], down[:, :, cols]).reshape(2, -1, wide)

    wide_loop(down.shape[2], body)
    net.spend(1.76)


def hidden_back_rows(net, chip, dy, down, ds):
    at = pl.ds(chip * 2, 2)
    rows = down.shape[1]

    def body(k, wide, cols):
        blocks = pl.ds(k * (wide // rows), wide // rows)
        ds[at, :, cols] = dot_cols(dy[at], down[blocks]).astype(BF16).reshape(2, -1, wide)

    wide_loop(down.shape[0] * rows, body)
    net.spend(1.5)


def gelu_both(a):
    t = jnp.tanh(GELU_C * (a + 0.044715 * a * a * a))
    return 0.5 * a * (1.0 + t), 0.5 * (1.0 + t) + 0.5 * a * (1.0 - t * t) * (GELU_C * (1.0 + 3 * 0.044715 * a * a))


def hidden_turn_rows(net, chip, u, up, s, ds):
    at = pl.ds(chip * 2, 2)

    def body(_, wide, cols):
        pre = dot_rows(u[at], up[:, :, cols]).astype(BF16).astype(F32)
        value, slope = gelu_both(pre)
        s[at, :, cols] = value.astype(BF16).reshape(2, -1, wide)
        ds[at, :, cols] = (ds[at, :, cols].astype(F32) * slope.reshape(2, -1, wide)).astype(BF16)

    wide_loop(up.shape[2], body)
    net.spend(2.1)


def pre_back_rows(net, chip, dy, down, a, da):
    at = pl.ds(chip * 2, 2)
    rows = down.shape[1]

    def body(k, wide, cols):
        blocks = pl.ds(k * (wide // rows), wide // rows)
        ds = dot_cols(dy[at], down[blocks]).astype(BF16).astype(F32).reshape(2, -1, wide)
        da[at, :, cols] = (ds * gelu_both(a[at, :, cols].astype(F32))[1]).astype(BF16)

    wide_loop(down.shape[0] * rows, body)
    net.spend(1.95)


def input_back_rows(net, chip, da, up, part):
    at = pl.ds(chip * 2, 2)
    rows = up.shape[1]

    def body(k, wide, cols):
        blocks = pl.ds(k * (wide // rows), wide // rows)
        part[:, :, cols] = dot_cols(da[at], up[blocks]).reshape(2, -1, wide)

    wide_loop(up.shape[0] * rows, body)
    net.spend(1.9)


def stored_tiles(net, count, compute, stage, out):
    def store(t):
        return pltpu.make_async_copy(stage.at[lax.rem(t, 2)], out(t), net.tile_sems.at[lax.rem(t, 2)])

    def step(t, carry):
        @pl.when(t >= 2)
        def _():
            store(t - 2).wait()

        compute(t, stage.at[lax.rem(t, 2)])
        store(t).start()
        return carry

    lax.fori_loop(0, count, step, 0)
    for t in range(max(count - 2, 0), count):
        store(jnp.int32(t)).wait()


def dot_tokens(a, b):
    return lax.dot_general(flat(a), flat(b), CONTRACT_ROWS, preferred_element_type=F32)


def grad_tiles(net, lhs, rhs, stage, out):
    _, high, wide = stage.shape
    across = rhs.shape[2] // wide

    def columns(t):
        return pl.ds(pl.multiple_of(lax.rem(t, across) * wide, wide), wide)

    def rows(t):
        return pl.ds(pl.multiple_of(lax.div(t, across) * high, high), high)

    def compute(t, slot):
        slot[...] = dot_tokens(lhs[:, :, rows(t)], rhs[:, :, columns(t)])

    stored_tiles(net, lhs.shape[2] // high * across, compute, stage, lambda t: out.at[rows(t), columns(t)])
    net.spend(GRAD_TIME * lhs.shape[2] / 1024)


def solution(mesh):
    nl, nd = mesh.shape['local'], mesh.shape['data']
    tok_spec = P(BOTH_AXES, None)
    w_spec = P(None, BOTH_AXES, None)

    def device_fn(tokens, grad_out, w_up, w_down):
        num_layers, ur, ffn = w_up.shape
        dr = w_down.shape[1]
        rows, width = tokens.shape
        hidden = nl * dr
        shape = jax.ShapeDtypeStruct
        up_full = shape((nl, nd * ur, hidden), BF16)
        down_full = shape((nl, dr, width), BF16)
        act_full = shape((nd, rows, width), BF16)
        hid_full = shape((nd, rows, hidden), BF16)
        own = shape((rows, width), BF16)
        part_vmem = pltpu.VMEM((RING, 2, rows, width), F32)
        rx = [part_vmem] + reduce_x_scratch(rows, width)
        sums = sums_scratch(dr, hidden) * 4 + sums_stage(dr, hidden) * 2

        def vmem(like):
            return pltpu.VMEM(like.shape, like.dtype)

        def step(net, x_in, x_halves, g_in, w_up_in, w_down_in,
                 x_out, dx_out, block_out, u_out, a_out, s_out, d_up0, d_down0, d_up1, d_down1, dw_up1, dw_down1, dw_up0, dw_down0,
                 x, u, g, up0, up1, down0, down1, ds, s, stage, part, *scratch):
            net.arrive('dyz')
            rx_scratch = scratch[:5]
            names = ('blocks', 'blocks1', 'sent_u', 'got_u', 'got_g', 'sent_up0', 'sent_down0', 'sent_up1', 'sent_down1', 'got_up0', 'got_down0',
                     'got_up1', 'got_down1', 'saved', 'free0', 'reduced0', 'ds_made', 'got_u1', 'hidden', 'all_du', 'reduced1', 'sent_dy', 'got_dy',
                     'back_up0', 'back_up0_rest', 'back_down0', 'd_down1', 'd_up1', 'y_reduced', 'acts', 'd_down0', 'da0', 'd_up0', 'du_reduced',
                     'out_up1', 'out_up0', 'got_u0', 'y_made', 'x_saved', 'weights_in', 'd_down1_0', 'relayed0')
            ev = {name: Event() for name in names}
            for kind in ('up', 'down'):
                for layer in range(2):
                    for k in range(2):
                        ev['sum_%s%d%d' % (kind, layer, k)] = Event()
            ev['got_up0'].rank = R_HIDDEN
            hidden_made, made0, made1, y_made, du_made = ([Event() for _ in STEPS] for _ in range(5))
            wide = width // 2
            half_up = nd * ur // 2
            act_pool, rs_pool = Pool(), Pool()
            job_pools = [[Pool(), Pool()], [Pool(), Pool()]]
            pools = {'up0': [Pool(), Pool()], 'down0': [Pool(), Pool()], 'up1': job_pools[0], 'down1': job_pools[1], 'blocks': [Pool(), Pool()]}
            stages = (scratch[21:24], scratch[24:27])
            job_scratch = [[scratch[5 + 8 * n + 4 * k:9 + 8 * n + 4 * k] for k in range(2)] for n in range(2)]
            frees = [[Event(0.0) for _ in range(3)] for _ in range(2)]
            freed = {k: Event() for k in range(10, 14)}

            def columns(h):
                return pl.ds(h * wide, wide)

            inputs = [net.load(x_in, x)]
            inputs += [net.load(w_up_in.at[:, pl.ds(k * hidden, hidden)], ds.at[k, pl.ds(0, num_layers * ur)]) for k in range(nd)]

            def gather(name, own, full, split):
                size = own.shape[0] // 2

                def join(kind, events):
                    yield events
                    if kind == 'got_':
                        ev[kind + name].copies = events[0].copies + events[1].copies
                    fire(net, ev[kind + name])

                got, sent = [Event(), Event()], [Event(), Event()]
                for k, first in enumerate('yz'):
                    net.spawn(gather_yz(net, own.at[pl.ds(k * size, size)], full, first, got[k], sent[k], k * size, split=split, pool=pools[name][k]))
                net.spawn(join('got_', got))
                net.spawn(join('sent_', sent))

            net.take(inputs)
            split_columns(ds, s, num_layers * ur)
            net.enter()
            net.spawn(exchange(net, lambda k: s.at[k, pl.ds(0, ur)], block_out.at[0], ev['blocks'], pools['blocks'][0]))
            gather('down0', w_down_in.at[0], down0, False)
            norm_rows(x, u.at[net.data])
            net.spend(0.7)
            own_grads = net.load(g_in, g.at[net.data])

            def up_first():
                yield [ev['blocks']]
                gather('up0', block_out.at[0], up0, True)
                net.spawn(gather_x(net, u, ev['got_u'], ev['sent_u'], pool=act_pool))
                yield [ev['sent_u']]
                net.spawn(exchange(net, lambda k: s.at[k, pl.ds(ur, ur)], block_out.at[1], ev['blocks1'], pools['blocks'][1]))
                yield [own_grads]
                net.spawn(gather_x(net, g, ev['got_g']))

            def second():
                yield [ev['sent_up0'], ev['sent_down0'], ev['blocks1']]
                gather('down1', w_down_in.at[1], down1, False)
                yield [made0[EARLY]]
                gather('up1', block_out.at[1], up1, True)

            def hidden_flow():
                yield [ev['got_u'], ev['got_up0'], ev['blocks1']]
                for k, step in enumerate(STEPS):
                    hidden_rows(net, net.at('x', step), u, up0, ds, s)
                    fire(net, hidden_made[k])
                    yield [Event(net.now, R_HIDDEN)] + ([ev['relayed0']] if k == 1 else [])
                yield [net.load(ds, a_out), net.load(s, s_out), net.load(u, u_out)]
                fire(net, ev['saved'])

            def down_flow():
                for k, step in enumerate(STEPS):
                    yield [hidden_made[k], ev['got_down0'], Event(0.0, R_DOWN)] + ([ev['relayed0']] if k == 1 else [])
                    down_rows(net, net.at('x', step), s, down0, part.at[k])
                    fire(net, made0[k])
                fire(net, ev['free0'])

            here = {step: Event() for step in STEPS}
            dy_here = {step: Event() for step in STEPS}

            strips0 = [Event() for _ in range(STRIPS)]
            net.spawn(reduce_x(net, part, made0, rx_scratch, ev['reduced0'], rs_pool, ev['relayed0'], strips0))

            def next_layer():
                yield [ev['saved'], ev['got_g']]
                net.drain(ev['got_u'].copies + ev['got_g'].copies)
                credit = net.grant(3, 'xp')
                act_pool.again()
                got = [Event() for _ in strips0]
                chips = [{step: Event() for step in STEPS} for _ in strips0]

                def strip(n):
                    at = pl.ds(n * (rows // STRIPS), rows // STRIPS)
                    yield [strips0[n], credit]
                    add_rows(x.at[at], part.at[3, net.core, at], x.at[at])
                    norm_rows(x.at[at], u.at[net.data, at])
                    net.spend(1.0 / STRIPS)
                    net.spawn(gather_x(net, u, got[n], chips=chips[n], pool=act_pool, strip=(n, STRIPS)))

                def chip(step):
                    yield [arrived[step] for arrived in chips]
                    fire(net, here[step])

                for n in range(STRIPS):
                    net.spawn(strip(n))
                for step in STEPS:
                    net.spawn(chip(step))
                yield [ev['reduced0']]
                net.drain(ev['reduced0'].copies)
                yield [net.grant(4, 'xp')]
                net.spawn(reduce_x(net, part, made1, rx_scratch, ev['reduced1'], rs_pool.again()))
                yield got
                ev['got_u1'].copies = sum((event.copies for event in got), [])
                fire(net, ev['got_u1'])

            def back_flow():
                for k, step in enumerate(STEPS):
                    yield [ev['got_g'], ev['got_down1'], ev['saved'], Event(0.0, R_BACK)]
                    hidden_back_rows(net, net.at('x', step), g, down1, ds)
                fire(net, ev['ds_made'])

            def again():
                top = nd * ur * TOP // 8
                yield [ev['free0'], ev['ds_made']]
                net.drain(ev['got_up0'].copies + ev['got_down0'].copies)
                credit = net.grant(6, 'yz')
                yield [credit]
                net.spawn(gather_yz(net, w_down_in.at[0], down0, NEAR, ev['back_down0'], near=True, pool=pools['down0'][1].again()))
                net.spawn(gather_yz(net, block_out.at[0, pl.ds(0, top)], up0, 'y', ev['back_up0'], pool=pools['up0'][0].again()))
                net.spawn(gather_yz(net, block_out.at[0, pl.ds(top, nd * ur - top)], up0, 'z', ev['back_up0_rest'], offset=top, pool=pools['up0'][1].again()))

            def weights():
                yield [ev['got_up1'], ev['got_down1']]
                yield [net.grant(7, 'yz')]
                fire(net, ev['weights_in'])

            left = [RING, RING]

            turned = [Event() for _ in STEPS]

            def layer1(k, step):
                yield [here[step], ev['ds_made'], ev['got_up1'], Event(0.0, R_TURN)]
                hidden_turn_rows(net, net.at('x', step), u, up1, s, ds)
                fire(net, turned[k])
                left[0] -= 1
                if left[0] == 0:
                    fire(net, ev['hidden'])

            def layer1_back(k, step):
                yield [turned[k], Event(0.0, R_DU[k])] + ([ev['hidden']] if k in HOLD else [])
                input_back_rows(net, net.at('x', step), ds, up1, part.at[k])
                fire(net, made1[k])
                left[1] -= 1
                if left[1] == 0:
                    fire(net, ev['all_du'])

            def grads1():
                for h in range(2):
                    yield [Event(0.0, R_DDOWN2 if h else R_DDOWN), ev['hidden']]
                    grad_tiles(net, s, g.at[:, :, columns(h)], stage, d_down1.at[:, columns(h)])
                    fire(net, ev['d_down1' if h else 'd_down1_0'])
                for h in range(2):
                    yield [Event(net.now, R_DUP)]
                    grad_tiles(net, u.at[:, :, columns(h)], ds, stage, d_up1.at[columns(h)])
                fire(net, ev['d_up1'])

            def act():
                yield [ev['d_up1'], ev['all_du'], ev['got_u1']]
                own_g = [net.load(g_in.at[:, columns(h)], ds.at[h]) for h in range(2)]
                net.drain(ev['got_u1'].copies)
                credit = net.grant(5, 'xp')
                yield [ev['reduced1'], credit] + own_g
                norm_back_rows(x, lambda at: jnp.concatenate([ds[h, at, :] for h in range(2)], axis=-1), part.at[3, net.core], u.at[net.data])
                net.spend(0.7)
                net.spawn(gather_x(net, u, ev['got_dy'], ev['sent_dy'], dy_here, pool=act_pool.again()))

            def layer1_out():
                yield [ev['reduced1'], Event(0.0, R_OUT)]
                net.drain(ev['reduced1'].copies)
                credit = net.grant(8, 'xp')
                for k, step in enumerate(STEPS):
                    down_rows(net, net.at('x', step), s, down1, part.at[k])
                    yield [Event(net.now, R_OUT)]
                fire(net, ev['y_made'])
                yield [ev['sent_dy'], credit]
                net.spawn(reduce_x(net, part, y_made, rx_scratch, ev['y_reduced'], rs_pool.again()))
                for k in range(RING):
                    fire(net, y_made[k])
                yield [ev['y_reduced']]
                add_rows(x, part.at[3, net.core], x)
                yield [net.load(x, x_out)]
                fire(net, ev['x_saved'])

            a0, s0 = up1.at[pl.ds(0, nd)], up1.at[pl.ds(nd, nd)]
            backs = [RING]

            def bring_back():
                yield [ev['d_down1']]
                yield [net.load(u_out, g)]
                fire(net, ev['got_u0'])

            def bring_acts():
                yield [ev['all_du']]
                net.drain(ev['got_up1'].copies)
                yield [net.load(a_out, a0), net.load(s_out, s0)]
                fire(net, ev['acts'])

            def layer0_hidden(step):
                yield [dy_here[step], ev['acts'], ev['back_down0'], ev['d_up1'], Event(0.0, R_PRE)]
                pre_back_rows(net, net.at('x', step), u, down0, a0, ds)
                backs[0] -= 1
                if backs[0] == 0:
                    fire(net, ev['da0'])

            def layer0():
                for h in range(2):
                    yield [ev['da0'], ev['got_u0'], Event(0.0, R_GUP)]
                    grad_tiles(net, g.at[:, :, columns(h)], ds, stage, d_up0.at[columns(h)])
                fire(net, ev['d_up0'])
                for h in range(2):
                    yield [ev['got_dy'], ev['acts'], Event(0.0, R_GDOWN)]
                    grad_tiles(net, s0, u.at[:, :, columns(h)], stage, d_down0.at[:, columns(h)])
                fire(net, ev['d_down0'])
                yield [ev['y_reduced'], ev['back_up0'], ev['back_up0_rest'], Event(0.0, R_DX)]
                net.drain(ev['y_reduced'].copies + ev['got_down1'].copies)
                x0 = down1.at[pl.ds(0, x_halves.shape[0])]
                yield [net.grant(9, 'xp'), net.load(x_halves, x0)]
                net.spawn(reduce_x(net, part, du_made, rx_scratch, ev['du_reduced'], rs_pool.again()))
                for k, step in enumerate(STEPS):
                    input_back_rows(net, net.at('x', step), ds, up0, part.at[k])
                    fire(net, du_made[k])
                    yield [Event(net.now, R_DX)]
                yield [ev['du_reduced'], ev['x_saved']]
                for q in range(x_halves.shape[0]):
                    rows_q = pl.ds(q * dr, dr)
                    dy_q = u.at[net.data, rows_q]
                    norm_back_rows(x0.at[q], lambda at, dy_q=dy_q: dy_q[at, :], part.at[3, net.core, rows_q], x.at[rows_q])
                yield [net.load(x, dx_out)]

            def up_place(ref, k):
                return lambda block, rows: ref.at[pl.ds(pl.multiple_of(block * (2 * half_up) + k * half_up + rows.start, rows.size), rows.size)]

            def down_place(ref, k):
                return lambda block, rows: ref.at[pl.ds(pl.multiple_of(block * dr + rows.start, rows.size), rows.size), columns(k)]

            def gate(event, items, pool):
                yield items
                pool.again()
                fire(net, event)

            def sum_job(job, place, ref, ready, name, credits=()):
                passed = [Event(), Event()]
                for k in range(2):
                    start = Event()
                    n = job % 2
                    net.spawn(gate(start, ready[k] + ([credits[k]] if credits else []), job_pools[n][k]))
                    sums = Sums(net, AXES[job][k], job_scratch[n][k], stages[k])
                    net.spawn(sums.run(place(ref, k), start, ev['sum_%s%d' % (name, k)], frees[k], passed[k], job_pools[n][k], WINDOWS[2 * job + k], LEAD[min(job, 2)]))
                return passed

            def out_down(layer, dw_down, credit):
                def one(k):
                    done = ev['sum_down%d%d' % (layer, k)]
                    yield [done]
                    yield [net.load(done.total, dw_down.at[:, columns(k)])]
                    if credit is not None:
                        net.drain(done.copies)
                        yield [net.grant(credit + k, 'yz')]
                        fire(net, freed[credit + k])

                for k in range(2):
                    net.spawn(one(k))

            def out_up(n, layer, dw_up, credit):
                totals = [ev['sum_up%d%d' % (layer, k)] for k in range(2)]
                yield totals
                net.drain(totals[0].copies + totals[1].copies)
                spare = job_scratch[n][0][0].at[0]
                for k, done in enumerate(totals):
                    for q in range(2):
                        copy_rows(net, done.total.at[pl.ds(q * spare.shape[1], spare.shape[1])], spare.at[2 * k + q])
                done = ev['out_up%d' % layer]
                net.spawn(exchange_back(net, spare, dw_up, done, pools['blocks'][layer].again()))
                if credit is not None:
                    yield [done]
                    for k in range(2):
                        yield [net.grant(credit + k, 'yz')]
                        fire(net, freed[credit + k])

            passed = sum_job(0, down_place, d_down1, [[ev['d_down1_0'], ev['weights_in']], [ev['d_down1'], ev['weights_in']]], 'down1')
            passed = sum_job(1, up_place, d_up1, [[ev['d_up1']] + passed] * 2, 'up1')
            passed = sum_job(2, up_place, d_up0, [[ev['d_up0']] + passed] * 2, 'up0', [freed[10], freed[11]])
            sum_job(3, down_place, d_down0, [[ev['d_down0']] + passed] * 2, 'down0', [freed[12], freed[13]])
            out_down(1, dw_down1, 10)
            net.spawn(out_up(1, 1, dw_up1, 12))
            net.spawn(out_up(0, 0, dw_up0, None))
            out_down(0, dw_down0, None)
            for k in (3, 2, 1, 0):
                net.spawn(layer1(k, STEPS[k]))
            for k in range(RING):
                net.spawn(layer1_back(k, STEPS[k]))
            for step in (0, -1, 1, 2):
                net.spawn(layer0_hidden(step))
            for flow in (up_first(), second(), hidden_flow(), down_flow(), next_layer(), back_flow(), again(), weights(), grads1(), act(), layer1_out(),
                         bring_back(), bring_acts(), layer0()):
                net.spawn(flow)
            net.run()

        def finish(*refs):
            sources, targets, held, ups, sems = refs[:6], refs[6:10], refs[10:16], refs[16:18], refs[18]
            x_out, dx_out, up_out, down_out = targets
            loads = [pltpu.make_async_copy(src, dst, sems.at[k]) for k, (src, dst) in enumerate(zip(sources, held))]
            stores = [(ups[1], up_out.at[1]), (ups[0], up_out.at[0]), (held[2], down_out.at[1]), (held[3], down_out.at[0]), (held[4], x_out), (held[5], dx_out)]
            stores = [pltpu.make_async_copy(src, dst, sems.at[6 + k]) for k, (src, dst) in enumerate(stores)]
            for load in loads:
                load.start()
            for k in (2, 3, 4, 5):
                loads[k].wait()
                stores[k].start()
            for k in (0, 1):
                loads[k].wait()
                join_columns(held[k], ups[1 - k])
                stores[k].start()
            for store in stores:
                store.wait()

        d_up_own, d_down_own = shape((nd, ur, hidden), F32), shape((dr, width), F32)

        d_up_full, d_down_full = shape((width, hidden), F32), shape((hidden, width), F32)
        x_out, dx, _, _, _, _, _, _, _, _, *grads = call(
            step, [own, own, shape((num_layers, nd * ur, hidden), BF16), act_full, hid_full, hid_full] + [d_up_full, d_down_full] * 2
            + [d_up_own, d_down_own] * 2, 'h' * 14, 'hhhhh',
            [vmem(own)] + [vmem(act_full)] * 2 + [vmem(up_full)] * 2 + [vmem(down_full)] * 2 + [vmem(hid_full)] * 2
            + [pltpu.VMEM((2, hidden // 2, width // 4), F32)] + rx + sums, TR, TS, TL, 0,
            tokens, tokens.reshape(rows // dr, dr, width), grad_out, w_up.reshape(num_layers * ur, ffn), w_down)
        up1_own, down1_own, up0_own, down0_own = grads
        held = [d_up_own, d_up_own, d_down_own, d_down_own, own, own]
        return pl.pallas_call(
            finish, out_shape=[own, own, shape(w_up.shape, F32), shape(w_down.shape, F32)], name='finish',
            in_specs=[pl.BlockSpec(memory_space=pl.ANY)] * 6, out_specs=[pl.BlockSpec(memory_space=pl.ANY)] * 4,
            scratch_shapes=[vmem(like) for like in held] + [pltpu.VMEM(w_up.shape[1:], F32)] * 2 + [pltpu.SemaphoreType.DMA((12,))],
        )(up1_own, up0_own, down1_own, down0_own, x_out, dx)

    return jax.shard_map(device_fn, mesh=mesh, in_specs=(tok_spec, tok_spec, w_spec, w_spec), out_specs=(tok_spec, tok_spec, w_spec, w_spec), check_vma=False)
```

```python
import jax
import jax.numpy as jnp
from jax import lax
from jax.experimental import pallas as pl
from jax.experimental.pallas import tpu as pltpu
from jax.sharding import PartitionSpec as P

NORM_EPS = 1e-6
BOTH_AXES = ('local', 'data')
CONTRACT_ROWS = (((0,), (0,)), ((), ()))
CONTRACT_COLS = (((1,), (1,)), ((), ()))
MESH = pl.DeviceIdType.MESH
RING = 4
F32, BF16 = jnp.float32, jnp.bfloat16

LINK_RATE = 46.0e3
PAIR_RATE = 600e3
LOCAL_RATE = 3000e3
HOP = 2.4
PAIR_HOP = 1.0
ENTRY = 4.2
GELU_C = 0.7978845608028654


class Event:
    def __init__(self, time=None, rank=0):
        self.time, self.rank = time, rank


class Copy:
    def __init__(self, desc, time, remote):
        self.desc, self.time, self.remote, self.rank, self.waited = desc, time, remote, 0, False

    def wait(self):
        if self.remote:
            self.desc.wait_recv()
        else:
            self.desc.wait()


class Credit:
    def __init__(self, semaphore, count, time):
        self.semaphore, self.count, self.time, self.rank, self.waited = semaphore, count, time, 0, False

    def wait(self):
        pl.semaphore_wait(self.semaphore, self.count)


class Both:
    def __init__(self, net, dst, one, two):
        self.desc = pltpu.make_async_remote_copy(
            src_ref=dst, dst_ref=dst, send_sem=net.send_sems.at[one.slot], recv_sem=net.recv_sems.at[one.receive],
            device_id=net.device('p', 1), device_id_type=MESH)
        self.time, self.rank, self.waited = max(one.time, two.time), 0, False

    def wait(self):
        self.desc.wait_recv()


class Pool:
    def __init__(self):
        self.slots, self.next = [], 0

    def again(self):
        self.next = 0
        return self


class Net:
    def __init__(self, send_sems, recv_sems, local_sems, credit_sems):
        self.send_sems, self.recv_sems, self.local_sems, self.credit_sems = send_sems, recv_sems, local_sems, credit_sems
        self.n_remote = self.n_local = 0
        self.free_sends = list(range(send_sems.shape[0]))
        self.free_locals = []
        self.now = 0.0
        self.free = {}
        self.sent = []
        self.flows = []
        here, there = lax.axis_index('local'), lax.axis_index('data')
        pos = {'z': here // RING, 'y': lax.rem(here, RING), 'x': there // 2}
        self.data, self.core = there, lax.rem(there, 2)
        self.ring = {axis: [at] + [lax.rem(at + step, RING) for step in range(1, RING)] for axis, at in pos.items()}
        self.hops = [there] + [lax.rem(there + step, 2 * RING) for step in range(1, 2 * RING)]
        self.blocks = [at * 2 + self.core for at in self.ring['x']]
        self.places = [[z * RING + y for y in self.ring['y']] for z in self.ring['z']]
        self.partner = pos['x'] * 2 + (1 - self.core)
        self.other = 1 - self.core

    def at(self, axis, step):
        return self.ring[axis][step % RING]

    def block(self, step):
        return self.blocks[step % RING]

    def device(self, axis, step):
        if axis == 'p':
            return {'data': self.partner}
        if axis == 'd':
            return {'data': self.hops[step % (2 * RING)]}
        if axis == 'x':
            return {'data': self.block(step)}
        if axis == 'y':
            return {'local': self.places[0][step % RING]}
        return {'local': self.places[step % RING][0]}

    def peers(self, axes):
        return [(axis, step) for axis in axes for step in ((1, -1) if axis in 'xyz' else (1,) if axis == 'p' else range(1, 2 * RING))]

    def signal(self, semaphore, axes):
        for axis, step in self.peers(axes):
            pl.semaphore_signal(semaphore, inc=1, device_id=self.device(axis, step), device_id_type=MESH)

    def arrive(self, axes):
        self.entry, self.entered = pltpu.get_barrier_semaphore(), len(self.peers(axes))
        self.signal(self.entry, axes)

    def enter(self):
        pl.semaphore_wait(self.entry, self.entered)
        self.now = max(self.now, ENTRY)

    def take(self, copies):
        for copy in copies:
            copy.wait()
            copy.waited = True
            self.free_locals.append(copy.slot)
            self.now = max(self.now, copy.time)

    def grant(self, k, axes):
        self.signal(self.credit_sems.at[k], axes)
        return Credit(self.credit_sems.at[k], len(self.peers(axes)), self.now + HOP)

    def drain(self, copies):
        for copy in copies:
            if copy in self.sent:
                copy.desc.wait_send()
                self.sent.remove(copy)
                self.free_sends.append(copy.slot)

    def idle(self, gap):
        over = [copy for copy in self.sent if copy.time + 1.5 < self.now]
        self.drain(over[:int(gap / 0.05)])

    def send(self, src, dst, axis, step=1, pool=None, partner=None):
        if partner is not None:
            k = partner.receive
        elif pool is not None and pool.next < len(pool.slots):
            k = pool.slots[pool.next]
        else:
            k = self.n_remote
            self.n_remote += 1
            if pool is not None:
                pool.slots.append(k)
        if pool is not None and partner is None:
            pool.next += 1
        if not self.free_sends:
            over = [copy for copy in self.sent if copy.time + 1.0 < self.now]
            self.drain(over or [min(self.sent, key=lambda copy: copy.time)])
        send_slot = self.free_sends.pop()
        desc = pltpu.make_async_remote_copy(
            src_ref=src, dst_ref=dst, send_sem=self.send_sems.at[send_slot], recv_sem=self.recv_sems.at[k],
            device_id=self.device(axis, step), device_id_type=MESH)
        desc.start()
        size = 1
        for n in dst.shape:
            size *= n
        size *= dst.dtype.itemsize
        rate = PAIR_RATE if axis == 'p' else LINK_RATE
        extra = 4.4 if axis == 'd' else 0.0
        if axis == 'd':
            axis, step, size = ('p', 1, size) if step == 1 else ('x', 1 if step < RING + 2 else -1, size)
        key = (axis, step)
        done = max(self.free.get(key, 0.0), self.now) + size / rate
        self.free[key] = done
        copy = Copy(desc, done + extra + (PAIR_HOP if axis == 'p' else HOP), True)
        copy.slot, copy.receive = send_slot, k
        self.sent.append(copy)
        return copy

    def load(self, src, dst):
        if not self.free_locals:
            self.free_locals.append(self.n_local)
            self.n_local += 1
        k = self.free_locals.pop()
        desc = pltpu.make_async_copy(src, dst, self.local_sems.at[k])
        desc.start()
        size = 1
        for n in dst.shape:
            size *= n
        done = max(self.free.get('hbm', 0.0), self.now) + size * dst.dtype.itemsize / LOCAL_RATE
        self.free['hbm'] = done
        copy = Copy(desc, done + 0.9, False)
        copy.slot = k
        return copy

    def spend(self, microseconds):
        self.now += microseconds

    def spawn(self, flow):
        self.step(flow)

    def step(self, flow):
        try:
            self.flows.append((flow, next(flow)))
        except StopIteration:
            pass

    def run(self):
        while self.flows:
            best = None
            for k, (_, items) in enumerate(self.flows):
                if any(item.time is None for item in items):
                    continue
                time = max([item.time for item in items] + [0.0])
                late = max([item.rank for item in items] + [0])
                rank = (max(time, self.now) + (SLACK if late else 0.0), late, time)
                if best is None or rank < best[0]:
                    best = (rank, k, time)
            _, k, time = best
            flow, items = self.flows.pop(k)
            self.idle(time - self.now)
            for item in items:
                if not isinstance(item, Event) and not item.waited:
                    item.wait()
                    item.waited = True
                    if isinstance(item, Copy) and not item.remote:
                        self.free_locals.append(item.slot)
            self.now = max(self.now, time)
            self.step(flow)

    def finish(self):
        for copy in self.sent:
            copy.desc.wait_send()


def rows_loop(rows, chunk, body):
    chunk = min(chunk, rows)

    def step(k, carry):
        body(pl.ds(pl.multiple_of(k * chunk, chunk), chunk))
        return carry

    lax.fori_loop(0, rows // chunk, step, 0)


def add_into(net, dst, *others):
    rows, cols = dst.shape

    def body(at):
        total = dst[at, :]
        for other in others:
            total = total + other[at, :]
        dst[at, :] = total

    rows_loop(rows, 16, body)
    net.spend(rows * cols * 4 * (1 + len(others)) / 4e6)


def fire(net, event):
    event.time = net.now


def exchange(net, source, dst, done, pool):
    rows = dst.shape[0] // (2 * RING)

    def mine():
        return dst.at[pl.ds(pl.multiple_of(net.data * rows, rows), rows)]

    own = net.load(source(net.data), mine())
    copies = [net.send(source(net.hops[k]), mine(), 'd', k, pool) for k in (4, 5, 2, 3, 6, 7, 1)]
    yield [own] + copies
    net.drain(copies)
    fire(net, done)


def exchange_back(net, src, dst, done, pool):
    rows = dst.shape[1]
    per = src.shape[1] // rows

    def block(k):
        return src.at[lax.div(k, per), pl.ds(pl.multiple_of(lax.rem(k, per) * rows, rows), rows)]

    own = net.load(block(net.data), dst.at[net.data])
    copies = [net.send(block(net.hops[k]), dst.at[net.data], 'd', k, pool) for k in (4, 5, 2, 3, 6, 7, 1)]
    yield [own] + copies
    net.drain(copies)
    fire(net, done)


def copy_rows(net, src, dst):
    def body(at):
        dst[at, :] = src[at, :]

    rows_loop(src.shape[0], 16, body)
    net.spend(0.2)


def gather_x(net, full, done, issued=None, chips=None, pool=None, strip=(0, 1)):
    size = full.shape[1] // strip[1]
    base, half = strip[0] * size, size // 2
    lo, hi, both = pl.ds(base, half), pl.ds(base + half, half), pl.ds(base, size)
    chips = chips or {step: Event() for step in STEPS}
    left = [2]
    done.copies = []

    def send(*args):
        done.copies.append(net.send(*args, pool=pool))
        return done.copies[-1]

    def block(step):
        return full.at[net.block(step), both]

    def part(step, rows):
        return full.at[net.block(step), rows]

    relays = []

    def side(step, first, second, mine):
        yield [mine[0]]
        relays.append(send(part(step, first), part(step, first), 'x', -step))
        left[0] -= 1
        if left[0] == 0:
            net.spawn(far())
            if issued is not None:
                fire(net, issued)
        yield [mine[1]]
        pair = send(block(step), block(step), 'p')
        yield [pair]
        fire(net, chips[step])

    def far():
        yield relays
        pair = send(block(2), block(2), 'p')
        yield [pair]
        fire(net, chips[2])

    forth = [send(part(0, rows), part(0, rows), 'x', 1) for rows in (lo, hi)]
    back = [send(part(0, rows), part(0, rows), 'x', -1) for rows in (hi, lo)]
    pair = send(block(0), block(0), 'p')
    net.spawn(side(-1, lo, hi, forth))
    net.spawn(side(1, hi, lo, back))
    yield [pair]
    fire(net, chips[0])
    yield [chips[step] for step in STEPS]
    fire(net, done)


def gather_yz(net, own, full, first, done, issued=None, offset=0, near=False, split=True, pool=None):
    second = 'y' if first == 'z' else 'z'
    done.copies = []

    def emit(*args):
        done.copies.append(net.send(*args, pool=pool))
        return done.copies[-1]

    size = own.shape[0]
    half = size // 2
    lo, hi, both = pl.ds(offset, half), pl.ds(offset + half, half), pl.ds(offset, size)
    forward, backward = ((lo, hi), (hi, lo)) if split and not near else ((both,), (both,))

    def part(one, two, rows):
        return full.at[yz_index(net, first, one, two), rows]

    left = [3 if near else RING, 3 if near else RING]

    def arrived(which):
        left[which] -= 1
        if left[which] == 0 and (done, issued)[which] is not None:
            fire(net, (done, issued)[which])

    def send(one, rows, axis, step):
        src = own.at[pl.ds(rows.start - offset, rows.size)] if one == 0 else part(one, 0, rows)
        return emit(src, part(one, 0, rows), axis, step)

    def column(one):
        forth = [send(one, rows, second, 1) for rows in forward]
        back = [send(one, rows, second, -1) for rows in backward]

        def finish():
            if near:
                arrived(1)
                yield forth + back
            else:
                yield [forth[0]]
                relays = [emit(part(one, -1, lo), part(one, -1, lo), second, 1)]
                yield [back[0]]
                relays.append(emit(part(one, 1, hi), part(one, 1, hi), second, -1))
                arrived(1)
                yield forth[1:] + back[1:] + relays
            arrived(0)

        net.spawn(finish())

    relays = []

    def side(step, first_half, mine):
        yield [mine[0]]
        if not near:
            relays.append(emit(part(step, 0, first_half), part(step, 0, first_half), first, -step))
            if len(relays) == 2:
                net.spawn(far())
        yield mine[1:]
        column(step)

    def far():
        yield relays
        column(2)

    mine = [net.load(own, part(0, 0, both))]
    forth = [send(0, rows, first, 1) for rows in forward]
    back = [send(0, rows, first, -1) for rows in backward]
    column(0)
    net.spawn(side(-1, lo, forth))
    net.spawn(side(1, hi, back))
    left[0] += 1
    yield mine
    arrived(0)


def yz_index(net, first, one, two):
    return net.places[one % RING][two % RING] if first == 'z' else net.places[two % RING][one % RING]


STEPS = (2, 1, -1, 0)


def reduce_x(net, part, made, scratch, done, pool=None, relayed=None, strips=None):
    other, relay_f, relay_b, last_f, last_b = scratch
    strips = strips or [Event()]
    size = part.shape[2] // len(strips)
    done.copies = []

    def acc(k, rows=None):
        return part.at[k, net.core] if rows is None else part.at[k, net.core, rows]

    def send(*args):
        done.copies.append(net.send(*args, pool=pool))
        return done.copies[-1]

    ready = [Event() for _ in STEPS]

    def pair(k):
        yield [made[k]]
        yield [send(part.at[k, net.other], other.at[k], 'p')]
        add_into(net, acc(k), other.at[k])
        fire(net, ready[k])

    for k in range(RING):
        net.spawn(pair(k))

    def strip(n, end):
        half = size // 2
        lo, hi, both, relay_rows = pl.ds(n * size, half), pl.ds(n * size + half, half), pl.ds(n * size, size), pl.ds(n * half, half)
        sent = {}
        started, relay_sent = Event(), Event()

        def part_flow(k):
            yield [ready[k]] + ([relay_sent] if k else [])
            if k == 0:
                sent['first_f'] = send(acc(0, lo), relay_f.at[relay_rows], 'x', 1)
                sent['first_b'] = send(acc(0, hi), relay_b.at[relay_rows], 'x', -1)
                fire(net, relay_sent)
                if n == len(strips) - 1 and relayed is not None:
                    fire(net, relayed)
            elif k == 1:
                sent['direct_f'] = send(acc(1, hi), last_f.at[hi], 'x', 1)
            else:
                sent['direct_b'] = send(acc(2, lo), last_b.at[lo], 'x', -1)
            if len(sent) == 4:
                fire(net, started)

        for k in range(3):
            net.spawn(part_flow(k))
        yield [started]
        yield [sent['first_f']]
        add_into(net, acc(1, lo), relay_f.at[relay_rows])
        summed_f = send(acc(1, lo), last_f.at[lo], 'x', 1)
        yield [sent['first_b']]
        add_into(net, acc(2, hi), relay_b.at[relay_rows])
        summed_b = send(acc(2, hi), last_b.at[hi], 'x', -1)
        yield [ready[3], sent['direct_f'], sent['direct_b'], summed_f, summed_b]
        add_into(net, acc(3, both), last_f.at[both], last_b.at[both])
        fire(net, end)

    for n, end in enumerate(strips):
        net.spawn(strip(n, end))
    yield strips
    fire(net, done)


def reduce_x_scratch(rows, cols):
    return [pltpu.VMEM((RING, rows, cols), F32), pltpu.VMEM((rows // 2, cols), F32), pltpu.VMEM((rows // 2, cols), F32),
            pltpu.VMEM((rows, cols), F32), pltpu.VMEM((rows, cols), F32)]


class Sums:
    def __init__(self, net, first, scratch, stage):
        self.net, self.first, self.scratch, self.stage = net, first, scratch, stage
        self.second = 'y' if first == 'z' else 'z'

    def run(self, place, start, done, free, passed_all, pool, window, lead):
        net, first, second = self.net, self.first, self.second
        relay1, last1, relay2, last2 = self.scratch
        ahead, behind, mine = self.stage
        half = mine.shape[0] // 2
        lo, hi, all_rows = pl.ds(0, half), pl.ds(half, half), pl.ds(0, 2 * half)
        done.copies = []

        def send(*args, partner=None):
            done.copies.append(net.send(*args, pool=pool, partner=partner))
            return done.copies[-1]

        def term(one, two, rows=all_rows):
            return place(yz_index(net, first, one, two), rows)

        def bring(gate, src, dst, got):
            yield [gate, start]
            yield [net.load(src, dst)]
            fire(net, got)

        chain = [[gate] + [Event() for _ in range(RING)] for gate in free]
        free[:] = [events[RING] for events in chain]
        got = [[Event() for _ in range(RING)] for _ in range(3)]
        ends = [Event() for _ in STEPS]
        passed = [Event() for _ in range(RING)]
        passed[lead] = passed_all

        def ring(k):
            two = STEPS[k]
            if k >= window:
                yield [passed[k - window]]
            net.spawn(bring(chain[0][k], term(1, two, lo), ahead, got[0][k]))
            net.spawn(bring(chain[1][k], term(-1, two, hi), behind, got[1][k]))
            net.spawn(bring(chain[2][k], term(0, two), mine, got[2][k]))
            first_f = send(term(2, two, lo), relay1.at[0, k], first, 1)
            first_b = send(term(2, two, hi), relay1.at[1, k], first, -1)
            direct_f = send(term(1, two, hi), last1.at[0, k, hi], first, 1)
            direct_b = send(term(-1, two, lo), last1.at[1, k, lo], first, -1)
            yield [first_f, got[0][k]]
            add_into(net, relay1.at[0, k], ahead)
            fire(net, chain[0][k + 1])
            summed_f = send(relay1.at[0, k], last1.at[0, k, lo], first, 1, partner=direct_f)
            yield [first_b, got[1][k]]
            add_into(net, relay1.at[1, k], behind)
            fire(net, chain[1][k + 1])
            summed_b = send(relay1.at[1, k], last1.at[1, k, hi], first, -1, partner=direct_b)
            fire(net, passed[k])
            yield [Both(net, last1.at[0, k], direct_f, summed_f), Both(net, last1.at[1, k], direct_b, summed_b), got[2][k]]
            add_into(net, last1.at[0, k], last1.at[1, k], mine)
            fire(net, chain[2][k + 1])
            fire(net, ends[k])

        def sums(k, rows=all_rows):
            return last1.at[0, k, rows]

        yield [start]
        for k in range(RING):
            net.spawn(ring(k))
        yield [ends[0]]
        first_f = send(sums(0, lo), relay2.at[0], second, 1)
        first_b = send(sums(0, hi), relay2.at[1], second, -1)
        yield [ends[1]]
        direct_f = send(sums(1, hi), last2.at[0, hi], second, 1)
        yield [ends[2]]
        direct_b = send(sums(2, lo), last2.at[1, lo], second, -1)
        yield [first_f]
        add_into(net, sums(1, lo), relay2.at[0])
        summed_f = send(sums(1, lo), last2.at[0, lo], second, 1, partner=direct_f)
        yield [first_b]
        add_into(net, sums(2, hi), relay2.at[1])
        summed_b = send(sums(2, hi), last2.at[1, hi], second, -1, partner=direct_b)
        yield [ends[3], Both(net, last2.at[0], direct_f, summed_f), Both(net, last2.at[1], direct_b, summed_b)]
        add_into(net, sums(3), last2.at[0], last2.at[1])
        done.total = sums(3)
        fire(net, done)


def sums_scratch(rows, cols):
    return [pltpu.VMEM((2, RING, rows // 2, cols), F32), pltpu.VMEM((2, RING, rows, cols), F32),
            pltpu.VMEM((2, rows // 2, cols), F32), pltpu.VMEM((2, rows, cols), F32)]


def sums_stage(rows, cols):
    return [pltpu.VMEM((rows // 2, cols), F32), pltpu.VMEM((rows // 2, cols), F32), pltpu.VMEM((rows, cols), F32)]


def norm_rows(x_ref, u_ref):
    def body(at):
        x = x_ref[at, :].astype(F32)
        u_ref[at, :] = (x * lax.rsqrt(jnp.mean(x * x, axis=-1, keepdims=True) + NORM_EPS)).astype(BF16)

    rows_loop(x_ref.shape[0], 16, body)


def norm_back_rows(x_ref, dy_of, du_ref, dx_ref):
    def body(at):
        x = x_ref[at, :].astype(F32)
        du = du_ref[at, :]
        r = lax.rsqrt(jnp.mean(x * x, axis=-1, keepdims=True) + NORM_EPS)
        xr = x * r
        dx_ref[at, :] = (dy_of(at).astype(F32) + r * (du - xr * jnp.mean(xr * du, axis=-1, keepdims=True))).astype(BF16)

    rows_loop(x_ref.shape[0], 16, body)


def add_rows(x_ref, y_ref, out_ref):
    def body(at):
        out_ref[at, :] = (x_ref[at, :].astype(F32) + y_ref[at, :]).astype(BF16)

    rows_loop(x_ref.shape[0], 16, body)


def swap_halves(even, odd):
    low = lax.broadcasted_iota(jnp.int32, even.shape, len(even.shape) - 1) < even.shape[-1] // 2
    shift = even.shape[-1] // 2
    axis = len(even.shape) - 1
    return jnp.where(low, even, pltpu.roll(odd, shift, axis)), jnp.where(low, pltpu.roll(even, shift, axis), odd)


def split_columns(w_ref, cols_ref, layers):
    pieces, _, wide = w_ref.shape
    rows = layers
    tile = pieces * wide // (4 * RING * RING)
    for x in range(RING):
        for p in range(wide // tile):
            pair = []
            for i in (2 * p, 2 * p + 1):
                at = (i * RING + x) * tile
                pair.append(w_ref[at // wide, pl.ds(0, rows), pl.ds(at % wide, tile)].astype(F32))
            for c, value in enumerate(swap_halves(*pair)):
                cols_ref[2 * x + c, pl.ds(0, rows), pl.ds(p * tile, tile)] = value.astype(cols_ref.dtype)


def join_columns(cols_ref, w_ref):
    tile = w_ref.shape[1] // (4 * RING * RING)
    for x in range(RING):
        for p in range(cols_ref.shape[2] // tile):
            pair = [cols_ref[2 * x + c, :, pl.ds(p * tile, tile)] for c in range(2)]
            for i, value in zip((2 * p, 2 * p + 1), swap_halves(*pair)):
                w_ref[:, pl.ds((i * RING + x) * tile, tile)] = value


def call(body, out_shape, out_spaces, in_spaces, scratch, remote, sends, local, collective_id, *args):
    spaces = {'v': pl.BlockSpec(memory_space=pltpu.VMEM), 'h': pl.BlockSpec(memory_space=pl.ANY)}

    def kernel(*refs):
        net = Net(*refs[-5:-1])
        net.tile_sems = refs[-1]
        body(net, *refs[:-5])
        net.finish()
        assert net.n_remote <= remote and net.n_local <= local, (body.__name__, net.n_remote, net.n_local)

    return pl.pallas_call(
        kernel, out_shape=out_shape, in_specs=[spaces[s] for s in in_spaces], out_specs=[spaces[s] for s in out_spaces],
        scratch_shapes=list(scratch) + [pltpu.SemaphoreType.DMA((sends,)), pltpu.SemaphoreType.DMA((remote,)), pltpu.SemaphoreType.DMA((local,)),
                                               pltpu.SemaphoreType.REGULAR((14,)), pltpu.SemaphoreType.DMA((2,))],
        compiler_params=pltpu.CompilerParams(collective_id=collective_id, has_side_effects=True, vmem_limit_bytes=67000000),
        cost_estimate=pl.CostEstimate(flops=10**8, bytes_accessed=10**7, transcendentals=0),
        name=body.__name__)(*args)


WIDE = 512
EARLY = 3
STRIPS = 2
GRAD_TIME = 4.25
SLACK = 0.3
R_HIDDEN, R_DOWN, R_BACK, R_TURN, R_DDOWN, R_DDOWN2, R_DUP, R_OUT, R_PRE, R_GUP, R_GDOWN, R_DX = 2, 1, 3, 1, 2, 2, 4, 2, 2, 3, 3, 2
R_DU, HOLD = (3, 3.1, 3, 3.3), (0, 1, 2, 3)
WINDOWS = (2, 2, 2, 2, 2, 2, 2, 4)
AXES = ('yz', 'yz', 'yz', 'yz')
TOP = 6
NEAR = 'z'
LEAD = (3, 3, 3)
TR, TS, TL = 260, 64, 9


def wide_loop(total, body):
    wide = min(WIDE, total)

    def step(k, carry):
        body(k, wide, pl.ds(pl.multiple_of(k * wide, wide), wide))
        return carry

    lax.fori_loop(0, total // wide, step, 0)


def flat(value):
    return value.reshape(value.shape[0] * value.shape[1], value.shape[2])


def dot_rows(a, b):
    return jnp.dot(flat(a), flat(b), preferred_element_type=F32)


def dot_cols(a, b):
    return lax.dot_general(flat(a), flat(b), CONTRACT_COLS, preferred_element_type=F32)


def gelu(a):
    return 0.5 * a * (1.0 + jnp.tanh(GELU_C * (a + 0.044715 * a * a * a)))


def hidden_rows(net, chip, u, up, a, s):
    at = pl.ds(chip * 2, 2)

    def body(_, wide, cols):
        pre = dot_rows(u[at], up[:, :, cols]).astype(BF16)
        a[at, :, cols] = pre.reshape(2, -1, wide)
        s[at, :, cols] = gelu(pre.astype(F32)).astype(BF16).reshape(2, -1, wide)

    wide_loop(up.shape[2], body)
    net.spend(1.7)


def down_rows(net, chip, s, down, part):
    at = pl.ds(chip * 2, 2)

    def body(_, wide, cols):
        part[:, :, cols] = dot_rows(s[at], down[:, :, cols]).reshape(2, -1, wide)

    wide_loop(down.shape[2], body)
    net.spend(1.76)


def hidden_back_rows(net, chip, dy, down, ds):
    at = pl.ds(chip * 2, 2)
    rows = down.shape[1]

    def body(k, wide, cols):
        blocks = pl.ds(k * (wide // rows), wide // rows)
        ds[at, :, cols] = dot_cols(dy[at], down[blocks]).astype(BF16).reshape(2, -1, wide)

    wide_loop(down.shape[0] * rows, body)
    net.spend(1.5)


def gelu_both(a):
    t = jnp.tanh(GELU_C * (a + 0.044715 * a * a * a))
    return 0.5 * a * (1.0 + t), 0.5 * (1.0 + t) + 0.5 * a * (1.0 - t * t) * (GELU_C * (1.0 + 3 * 0.044715 * a * a))


def hidden_turn_rows(net, chip, u, up, s, ds):
    at = pl.ds(chip * 2, 2)

    def body(_, wide, cols):
        pre = dot_rows(u[at], up[:, :, cols]).astype(BF16).astype(F32)
        value, slope = gelu_both(pre)
        s[at, :, cols] = value.astype(BF16).reshape(2, -1, wide)
        ds[at, :, cols] = (ds[at, :, cols].astype(F32) * slope.reshape(2, -1, wide)).astype(BF16)

    wide_loop(up.shape[2], body)
    net.spend(2.1)


def pre_back_rows(net, chip, dy, down, a, da):
    at = pl.ds(chip * 2, 2)
    rows = down.shape[1]

    def body(k, wide, cols):
        blocks = pl.ds(k * (wide // rows), wide // rows)
        ds = dot_cols(dy[at], down[blocks]).astype(BF16).astype(F32).reshape(2, -1, wide)
        da[at, :, cols] = (ds * gelu_both(a[at, :, cols].astype(F32))[1]).astype(BF16)

    wide_loop(down.shape[0] * rows, body)
    net.spend(1.95)


def input_back_rows(net, chip, da, up, part):
    at = pl.ds(chip * 2, 2)
    rows = up.shape[1]

    def body(k, wide, cols):
        blocks = pl.ds(k * (wide // rows), wide // rows)
        part[:, :, cols] = dot_cols(da[at], up[blocks]).reshape(2, -1, wide)

    wide_loop(up.shape[0] * rows, body)
    net.spend(1.9)


def stored_tiles(net, count, compute, stage, out):
    def store(t):
        return pltpu.make_async_copy(stage.at[lax.rem(t, 2)], out(t), net.tile_sems.at[lax.rem(t, 2)])

    def step(t, carry):
        @pl.when(t >= 2)
        def _():
            store(t - 2).wait()

        compute(t, stage.at[lax.rem(t, 2)])
        store(t).start()
        return carry

    lax.fori_loop(0, count, step, 0)
    for t in range(max(count - 2, 0), count):
        store(jnp.int32(t)).wait()


def dot_tokens(a, b):
    return lax.dot_general(flat(a), flat(b), CONTRACT_ROWS, preferred_element_type=F32)


def grad_tiles(net, lhs, rhs, stage, out):
    _, high, wide = stage.shape
    across = rhs.shape[2] // wide

    def columns(t):
        return pl.ds(pl.multiple_of(lax.rem(t, across) * wide, wide), wide)

    def rows(t):
        return pl.ds(pl.multiple_of(lax.div(t, across) * high, high), high)

    def compute(t, slot):
        slot[...] = dot_tokens(lhs[:, :, rows(t)], rhs[:, :, columns(t)])

    stored_tiles(net, lhs.shape[2] // high * across, compute, stage, lambda t: out.at[rows(t), columns(t)])
    net.spend(GRAD_TIME * lhs.shape[2] / 1024)


def solution(mesh):
    nl, nd = mesh.shape['local'], mesh.shape['data']
    tok_spec = P(BOTH_AXES, None)
    w_spec = P(None, BOTH_AXES, None)

    def device_fn(tokens, grad_out, w_up, w_down):
        num_layers, ur, ffn = w_up.shape
        dr = w_down.shape[1]
        rows, width = tokens.shape
        hidden = nl * dr
        shape = jax.ShapeDtypeStruct
        up_full = shape((nl, nd * ur, hidden), BF16)
        down_full = shape((nl, dr, width), BF16)
        act_full = shape((nd, rows, width), BF16)
        hid_full = shape((nd, rows, hidden), BF16)
        own = shape((rows, width), BF16)
        part_vmem = pltpu.VMEM((RING, 2, rows, width), F32)
        rx = [part_vmem] + reduce_x_scratch(rows, width)
        sums = sums_scratch(dr, hidden) * 4 + sums_stage(dr, hidden) * 2

        def vmem(like):
            return pltpu.VMEM(like.shape, like.dtype)

        def step(net, x_in, x_halves, g_in, w_up_in, w_down_in,
                 x_out, dx_out, block_out, u_out, a_out, s_out, d_up0, d_down0, d_up1, d_down1, dw_up1, dw_down1, dw_up0, dw_down0,
                 x, u, g, up0, up1, down0, down1, ds, s, stage, part, *scratch):
            net.arrive('dyz')
            rx_scratch = scratch[:5]
            names = ('blocks', 'blocks1', 'sent_u', 'got_u', 'got_g', 'sent_up0', 'sent_down0', 'sent_up1', 'sent_down1', 'got_up0', 'got_down0',
                     'got_up1', 'got_down1', 'saved', 'free0', 'reduced0', 'ds_made', 'got_u1', 'hidden', 'all_du', 'reduced1', 'sent_dy', 'got_dy',
                     'back_up0', 'back_up0_rest', 'back_down0', 'd_down1', 'd_up1', 'y_reduced', 'acts', 'd_down0', 'da0', 'd_up0', 'du_reduced',
                     'out_up1', 'out_up0', 'got_u0', 'y_made', 'x_saved', 'weights_in', 'd_down1_0', 'relayed0')
            ev = {name: Event() for name in names}
            for kind in ('up', 'down'):
                for layer in range(2):
                    for k in range(2):
                        ev['sum_%s%d%d' % (kind, layer, k)] = Event()
            ev['got_up0'].rank = R_HIDDEN
            hidden_made, made0, made1, y_made, du_made = ([Event() for _ in STEPS] for _ in range(5))
            wide = width // 2
            half_up = nd * ur // 2
            act_pool, rs_pool = Pool(), Pool()
            job_pools = [[Pool(), Pool()], [Pool(), Pool()]]
            pools = {'up0': [Pool(), Pool()], 'down0': [Pool(), Pool()], 'up1': job_pools[0], 'down1': job_pools[1], 'blocks': [Pool(), Pool()]}
            stages = (scratch[21:24], scratch[24:27])
            job_scratch = [[scratch[5 + 8 * n + 4 * k:9 + 8 * n + 4 * k] for k in range(2)] for n in range(2)]
            frees = [[Event(0.0) for _ in range(3)] for _ in range(2)]
            freed = {k: Event() for k in range(10, 14)}

            def columns(h):
                return pl.ds(h * wide, wide)

            inputs = [net.load(x_in, x)]
            inputs += [net.load(w_up_in.at[:, pl.ds(k * hidden, hidden)], ds.at[k, pl.ds(0, num_layers * ur)]) for k in range(nd)]

            def gather(name, own, full, split):
                size = own.shape[0] // 2

                def join(kind, events):
                    yield events
                    if kind == 'got_':
                        ev[kind + name].copies = events[0].copies + events[1].copies
                    fire(net, ev[kind + name])

                got, sent = [Event(), Event()], [Event(), Event()]
                for k, first in enumerate('yz'):
                    net.spawn(gather_yz(net, own.at[pl.ds(k * size, size)], full, first, got[k], sent[k], k * size, split=split, pool=pools[name][k]))
                net.spawn(join('got_', got))
                net.spawn(join('sent_', sent))

            net.take(inputs)
            split_columns(ds, s, num_layers * ur)
            net.enter()
            net.spawn(exchange(net, lambda k: s.at[k, pl.ds(0, ur)], block_out.at[0], ev['blocks'], pools['blocks'][0]))
            gather('down0', w_down_in.at[0], down0, False)
            norm_rows(x, u.at[net.data])
            net.spend(0.7)
            own_grads = net.load(g_in, g.at[net.data])

            def up_first():
                yield [ev['blocks']]
                gather('up0', block_out.at[0], up0, True)
                net.spawn(gather_x(net, u, ev['got_u'], ev['sent_u'], pool=act_pool))
                yield [ev['sent_u']]
                net.spawn(exchange(net, lambda k: s.at[k, pl.ds(ur, ur)], block_out.at[1], ev['blocks1'], pools['blocks'][1]))
                yield [own_grads]
                net.spawn(gather_x(net, g, ev['got_g']))

            def second():
                yield [ev['sent_up0'], ev['sent_down0'], ev['blocks1']]
                gather('down1', w_down_in.at[1], down1, False)
                yield [made0[EARLY]]
                gather('up1', block_out.at[1], up1, True)

            def hidden_flow():
                yield [ev['got_u'], ev['got_up0'], ev['blocks1']]
                for k, step in enumerate(STEPS):
                    hidden_rows(net, net.at('x', step), u, up0, ds, s)
                    fire(net, hidden_made[k])
                    yield [Event(net.now, R_HIDDEN)] + ([ev['relayed0']] if k == 1 else [])
                yield [net.load(ds, a_out), net.load(s, s_out), net.load(u, u_out)]
                fire(net, ev['saved'])

            def down_flow():
                for k, step in enumerate(STEPS):
                    yield [hidden_made[k], ev['got_down0'], Event(0.0, R_DOWN)] + ([ev['relayed0']] if k == 1 else [])
                    down_rows(net, net.at('x', step), s, down0, part.at[k])
                    fire(net, made0[k])
                fire(net, ev['free0'])

            here = {step: Event() for step in STEPS}
            dy_here = {step: Event() for step in STEPS}

            strips0 = [Event() for _ in range(STRIPS)]
            net.spawn(reduce_x(net, part, made0, rx_scratch, ev['reduced0'], rs_pool, ev['relayed0'], strips0))

            def next_layer():
                yield [ev['saved'], ev['got_g']]
                net.drain(ev['got_u'].copies + ev['got_g'].copies)
                credit = net.grant(3, 'xp')
                act_pool.again()
                got = [Event() for _ in strips0]
                chips = [{step: Event() for step in STEPS} for _ in strips0]

                def strip(n):
                    at = pl.ds(n * (rows // STRIPS), rows // STRIPS)
                    yield [strips0[n], credit]
                    add_rows(x.at[at], part.at[3, net.core, at], x.at[at])
                    norm_rows(x.at[at], u.at[net.data, at])
                    net.spend(1.0 / STRIPS)
                    net.spawn(gather_x(net, u, got[n], chips=chips[n], pool=act_pool, strip=(n, STRIPS)))

                def chip(step):
                    yield [arrived[step] for arrived in chips]
                    fire(net, here[step])

                for n in range(STRIPS):
                    net.spawn(strip(n))
                for step in STEPS:
                    net.spawn(chip(step))
                yield [ev['reduced0']]
                net.drain(ev['reduced0'].copies)
                yield [net.grant(4, 'xp')]
                net.spawn(reduce_x(net, part, made1, rx_scratch, ev['reduced1'], rs_pool.again()))
                yield got
                ev['got_u1'].copies = sum((event.copies for event in got), [])
                fire(net, ev['got_u1'])

            def back_flow():
                for k, step in enumerate(STEPS):
                    yield [ev['got_g'], ev['got_down1'], ev['saved'], Event(0.0, R_BACK)]
                    hidden_back_rows(net, net.at('x', step), g, down1, ds)
                fire(net, ev['ds_made'])

            def again():
                top = nd * ur * TOP // 8
                yield [ev['free0'], ev['ds_made']]
                net.drain(ev['got_up0'].copies + ev['got_down0'].copies)
                credit = net.grant(6, 'yz')
                yield [credit]
                net.spawn(gather_yz(net, w_down_in.at[0], down0, NEAR, ev['back_down0'], near=True, pool=pools['down0'][1].again()))
                net.spawn(gather_yz(net, block_out.at[0, pl.ds(0, top)], up0, 'y', ev['back_up0'], pool=pools['up0'][0].again()))
                net.spawn(gather_yz(net, block_out.at[0, pl.ds(top, nd * ur - top)], up0, 'z', ev['back_up0_rest'], offset=top, pool=pools['up0'][1].again()))

            def weights():
                yield [ev['got_up1'], ev['got_down1']]
                yield [net.grant(7, 'yz')]
                fire(net, ev['weights_in'])

            left = [RING, RING]

            turned = [Event() for _ in STEPS]

            def layer1(k, step):
                yield [here[step], ev['ds_made'], ev['got_up1'], Event(0.0, R_TURN)]
                hidden_turn_rows(net, net.at('x', step), u, up1, s, ds)
                fire(net, turned[k])
                left[0] -= 1
                if left[0] == 0:
                    fire(net, ev['hidden'])

            def layer1_back(k, step):
                yield [turned[k], Event(0.0, R_DU[k])] + ([ev['hidden']] if k in HOLD else [])
                input_back_rows(net, net.at('x', step), ds, up1, part.at[k])
                fire(net, made1[k])
                left[1] -= 1
                if left[1] == 0:
                    fire(net, ev['all_du'])

            def grads1():
                for h in range(2):
                    yield [Event(0.0, R_DDOWN2 if h else R_DDOWN), ev['hidden']]
                    grad_tiles(net, s, g.at[:, :, columns(h)], stage, d_down1.at[:, columns(h)])
                    fire(net, ev['d_down1' if h else 'd_down1_0'])
                for h in range(2):
                    yield [Event(net.now, R_DUP)]
                    grad_tiles(net, u.at[:, :, columns(h)], ds, stage, d_up1.at[columns(h)])
                fire(net, ev['d_up1'])

            def act():
                yield [ev['d_up1'], ev['all_du'], ev['got_u1']]
                own_g = [net.load(g_in.at[:, columns(h)], ds.at[h]) for h in range(2)]
                net.drain(ev['got_u1'].copies)
                credit = net.grant(5, 'xp')
                yield [ev['reduced1'], credit] + own_g
                norm_back_rows(x, lambda at: jnp.concatenate([ds[h, at, :] for h in range(2)], axis=-1), part.at[3, net.core], u.at[net.data])
                net.spend(0.7)
                net.spawn(gather_x(net, u, ev['got_dy'], ev['sent_dy'], dy_here, pool=act_pool.again()))

            def layer1_out():
                yield [ev['reduced1'], Event(0.0, R_OUT)]
                net.drain(ev['reduced1'].copies)
                credit = net.grant(8, 'xp')
                for k, step in enumerate(STEPS):
                    down_rows(net, net.at('x', step), s, down1, part.at[k])
                    yield [Event(net.now, R_OUT)]
                fire(net, ev['y_made'])
                yield [ev['sent_dy'], credit]
                net.spawn(reduce_x(net, part, y_made, rx_scratch, ev['y_reduced'], rs_pool.again()))
                for k in range(RING):
                    fire(net, y_made[k])
                yield [ev['y_reduced']]
                add_rows(x, part.at[3, net.core], x)
                yield [net.load(x, x_out)]
                fire(net, ev['x_saved'])

            a0, s0 = up1.at[pl.ds(0, nd)], up1.at[pl.ds(nd, nd)]
            backs = [RING]

            def bring_back():
                yield [ev['d_down1']]
                yield [net.load(u_out, g)]
                fire(net, ev['got_u0'])

            def bring_acts():
                yield [ev['all_du']]
                net.drain(ev['got_up1'].copies)
                yield [net.load(a_out, a0), net.load(s_out, s0)]
                fire(net, ev['acts'])

            def layer0_hidden(step):
                yield [dy_here[step], ev['acts'], ev['back_down0'], ev['d_up1'], Event(0.0, R_PRE)]
                pre_back_rows(net, net.at('x', step), u, down0, a0, ds)
                backs[0] -= 1
                if backs[0] == 0:
                    fire(net, ev['da0'])

            def layer0():
                for h in range(2):
                    yield [ev['da0'], ev['got_u0'], Event(0.0, R_GUP)]
                    grad_tiles(net, g.at[:, :, columns(h)], ds, stage, d_up0.at[columns(h)])
                fire(net, ev['d_up0'])
                for h in range(2):
                    yield [ev['got_dy'], ev['acts'], Event(0.0, R_GDOWN)]
                    grad_tiles(net, s0, u.at[:, :, columns(h)], stage, d_down0.at[:, columns(h)])
                fire(net, ev['d_down0'])
                yield [ev['y_reduced'], ev['back_up0'], ev['back_up0_rest'], Event(0.0, R_DX)]
                net.drain(ev['y_reduced'].copies + ev['got_down1'].copies)
                x0 = down1.at[pl.ds(0, x_halves.shape[0])]
                yield [net.grant(9, 'xp'), net.load(x_halves, x0)]
                net.spawn(reduce_x(net, part, du_made, rx_scratch, ev['du_reduced'], rs_pool.again()))
                for k, step in enumerate(STEPS):
                    input_back_rows(net, net.at('x', step), ds, up0, part.at[k])
                    fire(net, du_made[k])
                    yield [Event(net.now, R_DX)]
                yield [ev['du_reduced'], ev['x_saved']]
                for q in range(x_halves.shape[0]):
                    rows_q = pl.ds(q * dr, dr)
                    dy_q = u.at[net.data, rows_q]
                    norm_back_rows(x0.at[q], lambda at, dy_q=dy_q: dy_q[at, :], part.at[3, net.core, rows_q], x.at[rows_q])
                yield [net.load(x, dx_out)]

            def up_place(ref, k):
                return lambda block, rows: ref.at[pl.ds(pl.multiple_of(block * (2 * half_up) + k * half_up + rows.start, rows.size), rows.size)]

            def down_place(ref, k):
                return lambda block, rows: ref.at[pl.ds(pl.multiple_of(block * dr + rows.start, rows.size), rows.size), columns(k)]

            def gate(event, items, pool):
                yield items
                pool.again()
                fire(net, event)

            def sum_job(job, place, ref, ready, name, credits=()):
                passed = [Event(), Event()]
                for k in range(2):
                    start = Event()
                    n = job % 2
                    net.spawn(gate(start, ready[k] + ([credits[k]] if credits else []), job_pools[n][k]))
                    sums = Sums(net, AXES[job][k], job_scratch[n][k], stages[k])
                    net.spawn(sums.run(place(ref, k), start, ev['sum_%s%d' % (name, k)], frees[k], passed[k], job_pools[n][k], WINDOWS[2 * job + k], LEAD[min(job, 2)]))
                return passed

            def out_down(layer, dw_down, credit):
                def one(k):
                    done = ev['sum_down%d%d' % (layer, k)]
                    yield [done]
                    yield [net.load(done.total, dw_down.at[:, columns(k)])]
                    if credit is not None:
                        net.drain(done.copies)
                        yield [net.grant(credit + k, 'yz')]
                        fire(net, freed[credit + k])

                for k in range(2):
                    net.spawn(one(k))

            def out_up(n, layer, dw_up, credit):
                totals = [ev['sum_up%d%d' % (layer, k)] for k in range(2)]
                yield totals
                net.drain(totals[0].copies + totals[1].copies)
                spare = job_scratch[n][0][0].at[0]
                for k, done in enumerate(totals):
                    for q in range(2):
                        copy_rows(net, done.total.at[pl.ds(q * spare.shape[1], spare.shape[1])], spare.at[2 * k + q])
                done = ev['out_up%d' % layer]
                net.spawn(exchange_back(net, spare, dw_up, done, pools['blocks'][layer].again()))
                if credit is not None:
                    yield [done]
                    for k in range(2):
                        yield [net.grant(credit + k, 'yz')]
                        fire(net, freed[credit + k])

            passed = sum_job(0, down_place, d_down1, [[ev['d_down1_0'], ev['weights_in']], [ev['d_down1'], ev['weights_in']]], 'down1')
            passed = sum_job(1, up_place, d_up1, [[ev['d_up1']] + passed] * 2, 'up1')
            passed = sum_job(2, up_place, d_up0, [[ev['d_up0']] + passed] * 2, 'up0', [freed[10], freed[11]])
            sum_job(3, down_place, d_down0, [[ev['d_down0']] + passed] * 2, 'down0', [freed[12], freed[13]])
            out_down(1, dw_down1, 10)
            net.spawn(out_up(1, 1, dw_up1, 12))
            net.spawn(out_up(0, 0, dw_up0, None))
            out_down(0, dw_down0, None)
            for k in (3, 2, 1, 0):
                net.spawn(layer1(k, STEPS[k]))
            for k in range(RING):
                net.spawn(layer1_back(k, STEPS[k]))
            for step in (0, -1, 1, 2):
                net.spawn(layer0_hidden(step))
            for flow in (up_first(), second(), hidden_flow(), down_flow(), next_layer(), back_flow(), again(), weights(), grads1(), act(), layer1_out(),
                         bring_back(), bring_acts(), layer0()):
                net.spawn(flow)
            net.run()

        def finish(*refs):
            sources, targets, held, ups, sems = refs[:6], refs[6:10], refs[10:16], refs[16:18], refs[18]
            x_out, dx_out, up_out, down_out = targets
            loads = [pltpu.make_async_copy(src, dst, sems.at[k]) for k, (src, dst) in enumerate(zip(sources, held))]
            stores = [(ups[1], up_out.at[1]), (ups[0], up_out.at[0]), (held[2], down_out.at[1]), (held[3], down_out.at[0]), (held[4], x_out), (held[5], dx_out)]
            stores = [pltpu.make_async_copy(src, dst, sems.at[6 + k]) for k, (src, dst) in enumerate(stores)]
            for load in loads:
                load.start()
            for k in (2, 3, 4, 5):
                loads[k].wait()
                stores[k].start()
            for k in (0, 1):
                loads[k].wait()
                join_columns(held[k], ups[1 - k])
                stores[k].start()
            for store in stores:
                store.wait()

        d_up_own, d_down_own = shape((nd, ur, hidden), F32), shape((dr, width), F32)

        d_up_full, d_down_full = shape((width, hidden), F32), shape((hidden, width), F32)
        x_out, dx, _, _, _, _, _, _, _, _, *grads = call(
            step, [own, own, shape((num_layers, nd * ur, hidden), BF16), act_full, hid_full, hid_full] + [d_up_full, d_down_full] * 2
            + [d_up_own, d_down_own] * 2, 'h' * 14, 'hhhhh',
            [vmem(own)] + [vmem(act_full)] * 2 + [vmem(up_full)] * 2 + [vmem(down_full)] * 2 + [vmem(hid_full)] * 2
            + [pltpu.VMEM((2, hidden // 2, width // 4), F32)] + rx + sums, TR, TS, TL, 0,
            tokens, tokens.reshape(rows // dr, dr, width), grad_out, w_up.reshape(num_layers * ur, ffn), w_down)
        up1_own, down1_own, up0_own, down0_own = grads
        held = [d_up_own, d_up_own, d_down_own, d_down_own, own, own]
        return pl.pallas_call(
            finish, out_shape=[own, own, shape(w_up.shape, F32), shape(w_down.shape, F32)], name='finish',
            in_specs=[pl.BlockSpec(memory_space=pl.ANY)] * 6, out_specs=[pl.BlockSpec(memory_space=pl.ANY)] * 4,
            scratch_shapes=[vmem(like) for like in held] + [pltpu.VMEM(w_up.shape[1:], F32)] * 2 + [pltpu.SemaphoreType.DMA((12,))],
        )(up1_own, up0_own, down1_own, down0_own, x_out, dx)

    return jax.shard_map(device_fn, mesh=mesh, in_specs=(tok_spec, tok_spec, w_spec, w_spec), out_specs=(tok_spec, tok_spec, w_spec, w_spec), check_vma=False)
```

```python
import jax
import jax.numpy as jnp
from jax import lax
from jax.experimental import pallas as pl
from jax.experimental.pallas import tpu as pltpu
from jax.sharding import PartitionSpec as P

NORM_EPS = 1e-6
BOTH_AXES = ('local', 'data')
CONTRACT_ROWS = (((0,), (0,)), ((), ()))
CONTRACT_COLS = (((1,), (1,)), ((), ()))
MESH = pl.DeviceIdType.MESH
RING = 4
F32, BF16 = jnp.float32, jnp.bfloat16

LINK_RATE = 46.0e3
PAIR_RATE = 600e3
LOCAL_RATE = 3000e3
HOP = 2.4
PAIR_HOP = 1.0
ENTRY = 4.2
GELU_C = 0.7978845608028654


class Event:
    def __init__(self, time=None, rank=0):
        self.time, self.rank = time, rank


class Copy:
    def __init__(self, desc, time, remote):
        self.desc, self.time, self.remote, self.rank, self.waited = desc, time, remote, 0, False

    def wait(self):
        if self.remote:
            self.desc.wait_recv()
        else:
            self.desc.wait()


class Credit:
    def __init__(self, semaphore, count, time):
        self.semaphore, self.count, self.time, self.rank, self.waited = semaphore, count, time, 0, False

    def wait(self):
        pl.semaphore_wait(self.semaphore, self.count)


class Both:
    def __init__(self, net, dst, one, two):
        self.desc = pltpu.make_async_remote_copy(
            src_ref=dst, dst_ref=dst, send_sem=net.send_sems.at[one.slot], recv_sem=net.recv_sems.at[one.receive],
            device_id=net.device('p', 1), device_id_type=MESH)
        self.time, self.rank, self.waited = max(one.time, two.time), 0, False

    def wait(self):
        self.desc.wait_recv()


class Pool:
    def __init__(self):
        self.slots, self.next = [], 0

    def again(self):
        self.next = 0
        return self


class Net:
    def __init__(self, send_sems, recv_sems, local_sems, credit_sems):
        self.send_sems, self.recv_sems, self.local_sems, self.credit_sems = send_sems, recv_sems, local_sems, credit_sems
        self.n_remote = self.n_local = 0
        self.free_sends = list(range(send_sems.shape[0]))
        self.free_locals = []
        self.now = 0.0
        self.free = {}
        self.sent = []
        self.flows = []
        here, there = lax.axis_index('local'), lax.axis_index('data')
        pos = {'z': here // RING, 'y': lax.rem(here, RING), 'x': there // 2}
        self.data, self.core = there, lax.rem(there, 2)
        self.ring = {axis: [at] + [lax.rem(at + step, RING) for step in range(1, RING)] for axis, at in pos.items()}
        self.hops = [there] + [lax.rem(there + step, 2 * RING) for step in range(1, 2 * RING)]
        self.blocks = [at * 2 + self.core for at in self.ring['x']]
        self.places = [[z * RING + y for y in self.ring['y']] for z in self.ring['z']]
        self.partner = pos['x'] * 2 + (1 - self.core)
        self.other = 1 - self.core

    def at(self, axis, step):
        return self.ring[axis][step % RING]

    def block(self, step):
        return self.blocks[step % RING]

    def device(self, axis, step):
        if axis == 'p':
            return {'data': self.partner}
        if axis == 'd':
            return {'data': self.hops[step % (2 * RING)]}
        if axis == 'x':
            return {'data': self.block(step)}
        if axis == 'y':
            return {'local': self.places[0][step % RING]}
        return {'local': self.places[step % RING][0]}

    def peers(self, axes):
        return [(axis, step) for axis in axes for step in ((1, -1) if axis in 'xyz' else (1,) if axis == 'p' else range(1, 2 * RING))]

    def signal(self, semaphore, axes):
        for axis, step in self.peers(axes):
            pl.semaphore_signal(semaphore, inc=1, device_id=self.device(axis, step), device_id_type=MESH)

    def arrive(self, axes):
        self.entry, self.entered = pltpu.get_barrier_semaphore(), len(self.peers(axes))
        self.signal(self.entry, axes)

    def enter(self):
        pl.semaphore_wait(self.entry, self.entered)
        self.now = max(self.now, ENTRY)

    def take(self, copies):
        for copy in copies:
            copy.wait()
            copy.waited = True
            self.free_locals.append(copy.slot)
            self.now = max(self.now, copy.time)

    def grant(self, k, axes):
        self.signal(self.credit_sems.at[k], axes)
        return Credit(self.credit_sems.at[k], len(self.peers(axes)), self.now + HOP)

    def drain(self, copies):
        for copy in copies:
            if copy in self.sent:
                copy.desc.wait_send()
                self.sent.remove(copy)
                self.free_sends.append(copy.slot)

    def idle(self, gap):
        over = [copy for copy in self.sent if copy.time + 1.5 < self.now]
        self.drain(over[:int(gap / 0.05)])

    def send(self, src, dst, axis, step=1, pool=None, partner=None):
        if partner is not None:
            k = partner.receive
        elif pool is not None and pool.next < len(pool.slots):
            k = pool.slots[pool.next]
        else:
            k = self.n_remote
            self.n_remote += 1
            if pool is not None:
                pool.slots.append(k)
        if pool is not None and partner is None:
            pool.next += 1
        if not self.free_sends:
            over = [copy for copy in self.sent if copy.time + 1.0 < self.now]
            self.drain(over or [min(self.sent, key=lambda copy: copy.time)])
        send_slot = self.free_sends.pop()
        desc = pltpu.make_async_remote_copy(
            src_ref=src, dst_ref=dst, send_sem=self.send_sems.at[send_slot], recv_sem=self.recv_sems.at[k],
            device_id=self.device(axis, step), device_id_type=MESH)
        desc.start()
        size = 1
        for n in dst.shape:
            size *= n
        size *= dst.dtype.itemsize
        rate = PAIR_RATE if axis == 'p' else LINK_RATE
        extra = 4.4 if axis == 'd' else 0.0
        if axis == 'd':
            axis, step, size = ('p', 1, size) if step == 1 else ('x', 1 if step < RING + 2 else -1, size)
        key = (axis, step)
        done = max(self.free.get(key, 0.0), self.now) + size / rate
        self.free[key] = done
        copy = Copy(desc, done + extra + (PAIR_HOP if axis == 'p' else HOP), True)
        copy.slot, copy.receive = send_slot, k
        self.sent.append(copy)
        return copy

    def load(self, src, dst):
        if not self.free_locals:
            self.free_locals.append(self.n_local)
            self.n_local += 1
        k = self.free_locals.pop()
        desc = pltpu.make_async_copy(src, dst, self.local_sems.at[k])
        desc.start()
        size = 1
        for n in dst.shape:
            size *= n
        done = max(self.free.get('hbm', 0.0), self.now) + size * dst.dtype.itemsize / LOCAL_RATE
        self.free['hbm'] = done
        copy = Copy(desc, done + 0.9, False)
        copy.slot = k
        return copy

    def spend(self, microseconds):
        self.now += microseconds

    def spawn(self, flow):
        self.step(flow)

    def step(self, flow):
        try:
            self.flows.append((flow, next(flow)))
        except StopIteration:
            pass

    def run(self):
        while self.flows:
            best = None
            for k, (_, items) in enumerate(self.flows):
                if any(item.time is None for item in items):
                    continue
                time = max([item.time for item in items] + [0.0])
                late = max([item.rank for item in items] + [0])
                rank = (max(time, self.now) + (SLACK if late else 0.0), late, time)
                if best is None or rank < best[0]:
                    best = (rank, k, time)
            _, k, time = best
            flow, items = self.flows.pop(k)
            self.idle(time - self.now)
            for item in items:
                if not isinstance(item, Event) and not item.waited:
                    item.wait()
                    item.waited = True
                    if isinstance(item, Copy) and not item.remote:
                        self.free_locals.append(item.slot)
            self.now = max(self.now, time)
            self.step(flow)

    def finish(self):
        for copy in self.sent:
            copy.desc.wait_send()


def rows_loop(rows, chunk, body):
    chunk = min(chunk, rows)

    def step(k, carry):
        body(pl.ds(pl.multiple_of(k * chunk, chunk), chunk))
        return carry

    lax.fori_loop(0, rows // chunk, step, 0)


def add_into(net, dst, *others):
    rows, cols = dst.shape

    def body(at):
        total = dst[at, :]
        for other in others:
            total = total + other[at, :]
        dst[at, :] = total

    rows_loop(rows, 16, body)
    net.spend(rows * cols * 4 * (1 + len(others)) / 4e6)


def fire(net, event):
    event.time = net.now


def exchange(net, source, dst, done, pool):
    rows = dst.shape[0] // (2 * RING)

    def mine():
        return dst.at[pl.ds(pl.multiple_of(net.data * rows, rows), rows)]

    own = net.load(source(net.data), mine())
    copies = [net.send(source(net.hops[k]), mine(), 'd', k, pool) for k in (4, 5, 2, 3, 6, 7, 1)]
    yield [own] + copies
    net.drain(copies)
    fire(net, done)


def exchange_back(net, src, dst, done, pool):
    rows = dst.shape[1]
    per = src.shape[1] // rows

    def block(k):
        return src.at[lax.div(k, per), pl.ds(pl.multiple_of(lax.rem(k, per) * rows, rows), rows)]

    own = net.load(block(net.data), dst.at[net.data])
    copies = [net.send(block(net.hops[k]), dst.at[net.data], 'd', k, pool) for k in (4, 5, 2, 3, 6, 7, 1)]
    yield [own] + copies
    net.drain(copies)
    fire(net, done)


def copy_rows(net, src, dst):
    def body(at):
        dst[at, :] = src[at, :]

    rows_loop(src.shape[0], 16, body)
    net.spend(0.2)


def gather_x(net, full, done, issued=None, chips=None, pool=None, strip=(0, 1)):
    size = full.shape[1] // strip[1]
    base, half = strip[0] * size, size // 2
    lo, hi, both = pl.ds(base, half), pl.ds(base + half, half), pl.ds(base, size)
    chips = chips or {step: Event() for step in STEPS}
    left = [2]
    done.copies = []

    def send(*args):
        done.copies.append(net.send(*args, pool=pool))
        return done.copies[-1]

    def block(step):
        return full.at[net.block(step), both]

    def part(step, rows):
        return full.at[net.block(step), rows]

    relays = []

    def side(step, first, second, mine):
        yield [mine[0]]
        relays.append(send(part(step, first), part(step, first), 'x', -step))
        left[0] -= 1
        if left[0] == 0:
            net.spawn(far())
            if issued is not None:
                fire(net, issued)
        yield [mine[1]]
        pair = send(block(step), block(step), 'p')
        yield [pair]
        fire(net, chips[step])

    def far():
        yield relays
        pair = send(block(2), block(2), 'p')
        yield [pair]
        fire(net, chips[2])

    forth = [send(part(0, rows), part(0, rows), 'x', 1) for rows in (lo, hi)]
    back = [send(part(0, rows), part(0, rows), 'x', -1) for rows in (hi, lo)]
    pair = send(block(0), block(0), 'p')
    net.spawn(side(-1, lo, hi, forth))
    net.spawn(side(1, hi, lo, back))
    yield [pair]
    fire(net, chips[0])
    yield [chips[step] for step in STEPS]
    fire(net, done)


def gather_yz(net, own, full, first, done, issued=None, offset=0, near=False, split=True, pool=None):
    second = 'y' if first == 'z' else 'z'
    done.copies = []

    def emit(*args):
        done.copies.append(net.send(*args, pool=pool))
        return done.copies[-1]

    size = own.shape[0]
    half = size // 2
    lo, hi, both = pl.ds(offset, half), pl.ds(offset + half, half), pl.ds(offset, size)
    forward, backward = ((lo, hi), (hi, lo)) if split and not near else ((both,), (both,))

    def part(one, two, rows):
        return full.at[yz_index(net, first, one, two), rows]

    left = [3 if near else RING, 3 if near else RING]

    def arrived(which):
        left[which] -= 1
        if left[which] == 0 and (done, issued)[which] is not None:
            fire(net, (done, issued)[which])

    def send(one, rows, axis, step):
        src = own.at[pl.ds(rows.start - offset, rows.size)] if one == 0 else part(one, 0, rows)
        return emit(src, part(one, 0, rows), axis, step)

    def column(one):
        forth = [send(one, rows, second, 1) for rows in forward]
        back = [send(one, rows, second, -1) for rows in backward]

        def finish():
            if near:
                arrived(1)
                yield forth + back
            else:
                yield [forth[0]]
                relays = [emit(part(one, -1, lo), part(one, -1, lo), second, 1)]
                yield [back[0]]
                relays.append(emit(part(one, 1, hi), part(one, 1, hi), second, -1))
                arrived(1)
                yield forth[1:] + back[1:] + relays
            arrived(0)

        net.spawn(finish())

    relays = []

    def side(step, first_half, mine):
        yield [mine[0]]
        if not near:
            relays.append(emit(part(step, 0, first_half), part(step, 0, first_half), first, -step))
            if len(relays) == 2:
                net.spawn(far())
        yield mine[1:]
        column(step)

    def far():
        yield relays
        column(2)

    mine = [net.load(own, part(0, 0, both))]
    forth = [send(0, rows, first, 1) for rows in forward]
    back = [send(0, rows, first, -1) for rows in backward]
    column(0)
    net.spawn(side(-1, lo, forth))
    net.spawn(side(1, hi, back))
    left[0] += 1
    yield mine
    arrived(0)


def yz_index(net, first, one, two):
    return net.places[one % RING][two % RING] if first == 'z' else net.places[two % RING][one % RING]


STEPS = (2, 1, -1, 0)


def reduce_x(net, part, made, scratch, done, pool=None, relayed=None, strips=None):
    other, relay_f, relay_b, last_f, last_b = scratch
    strips = strips or [Event()]
    size = part.shape[2] // len(strips)
    done.copies = []

    def acc(k, rows=None):
        return part.at[k, net.core] if rows is None else part.at[k, net.core, rows]

    def send(*args):
        done.copies.append(net.send(*args, pool=pool))
        return done.copies[-1]

    ready = [Event() for _ in STEPS]

    def pair(k):
        yield [made[k]]
        yield [send(part.at[k, net.other], other.at[k], 'p')]
        add_into(net, acc(k), other.at[k])
        fire(net, ready[k])

    for k in range(RING):
        net.spawn(pair(k))

    def strip(n, end):
        half = size // 2
        lo, hi, both, relay_rows = pl.ds(n * size, half), pl.ds(n * size + half, half), pl.ds(n * size, size), pl.ds(n * half, half)
        sent = {}
        started, relay_sent = Event(), Event()

        def part_flow(k):
            yield [ready[k]] + ([relay_sent] if k else [])
            if k == 0:
                sent['first_f'] = send(acc(0, lo), relay_f.at[relay_rows], 'x', 1)
                sent['first_b'] = send(acc(0, hi), relay_b.at[relay_rows], 'x', -1)
                fire(net, relay_sent)
                if n == len(strips) - 1 and relayed is not None:
                    fire(net, relayed)
            elif k == 1:
                sent['direct_f'] = send(acc(1, hi), last_f.at[hi], 'x', 1)
            else:
                sent['direct_b'] = send(acc(2, lo), last_b.at[lo], 'x', -1)
            if len(sent) == 4:
                fire(net, started)

        for k in range(3):
            net.spawn(part_flow(k))
        yield [started]
        yield [sent['first_f']]
        add_into(net, acc(1, lo), relay_f.at[relay_rows])
        summed_f = send(acc(1, lo), last_f.at[lo], 'x', 1)
        yield [sent['first_b']]
        add_into(net, acc(2, hi), relay_b.at[relay_rows])
        summed_b = send(acc(2, hi), last_b.at[hi], 'x', -1)
        yield [ready[3], sent['direct_f'], sent['direct_b'], summed_f, summed_b]
        add_into(net, acc(3, both), last_f.at[both], last_b.at[both])
        fire(net, end)

    for n, end in enumerate(strips):
        net.spawn(strip(n, end))
    yield strips
    fire(net, done)


def reduce_x_scratch(rows, cols):
    return [pltpu.VMEM((RING, rows, cols), F32), pltpu.VMEM((rows // 2, cols), F32), pltpu.VMEM((rows // 2, cols), F32),
            pltpu.VMEM((rows, cols), F32), pltpu.VMEM((rows, cols), F32)]


class Sums:
    def __init__(self, net, first, scratch, stage):
        self.net, self.first, self.scratch, self.stage = net, first, scratch, stage
        self.second = 'y' if first == 'z' else 'z'

    def run(self, place, start, done, free, passed_all, pool, window, lead):
        net, first, second = self.net, self.first, self.second
        relay1, last1, relay2, last2 = self.scratch
        ahead, behind, mine = self.stage
        half = mine.shape[0] // 2
        lo, hi, all_rows = pl.ds(0, half), pl.ds(half, half), pl.ds(0, 2 * half)
        done.copies = []

        def send(*args, partner=None):
            done.copies.append(net.send(*args, pool=pool, partner=partner))
            return done.copies[-1]

        def term(one, two, rows=all_rows):
            return place(yz_index(net, first, one, two), rows)

        def bring(gate, src, dst, got):
            yield [gate, start]
            yield [net.load(src, dst)]
            fire(net, got)

        chain = [[gate] + [Event() for _ in range(RING)] for gate in free]
        free[:] = [events[RING] for events in chain]
        got = [[Event() for _ in range(RING)] for _ in range(3)]
        ends = [Event() for _ in STEPS]
        passed = [Event() for _ in range(RING)]
        passed[lead] = passed_all

        def ring(k):
            two = STEPS[k]
            if k >= window:
                yield [passed[k - window]]
            net.spawn(bring(chain[0][k], term(1, two, lo), ahead, got[0][k]))
            net.spawn(bring(chain[1][k], term(-1, two, hi), behind, got[1][k]))
            net.spawn(bring(chain[2][k], term(0, two), mine, got[2][k]))
            first_f = send(term(2, two, lo), relay1.at[0, k], first, 1)
            first_b = send(term(2, two, hi), relay1.at[1, k], first, -1)
            direct_f = send(term(1, two, hi), last1.at[0, k, hi], first, 1)
            direct_b = send(term(-1, two, lo), last1.at[1, k, lo], first, -1)
            yield [first_f, got[0][k]]
            add_into(net, relay1.at[0, k], ahead)
            fire(net, chain[0][k + 1])
            summed_f = send(relay1.at[0, k], last1.at[0, k, lo], first, 1, partner=direct_f)
            yield [first_b, got[1][k]]
            add_into(net, relay1.at[1, k], behind)
            fire(net, chain[1][k + 1])
            summed_b = send(relay1.at[1, k], last1.at[1, k, hi], first, -1, partner=direct_b)
            fire(net, passed[k])
            yield [Both(net, last1.at[0, k], direct_f, summed_f), Both(net, last1.at[1, k], direct_b, summed_b), got[2][k]]
            add_into(net, last1.at[0, k], last1.at[1, k], mine)
            fire(net, chain[2][k + 1])
            fire(net, ends[k])

        def sums(k, rows=all_rows):
            return last1.at[0, k, rows]

        yield [start]
        for k in range(RING):
            net.spawn(ring(k))
        yield [ends[0]]
        first_f = send(sums(0, lo), relay2.at[0], second, 1)
        first_b = send(sums(0, hi), relay2.at[1], second, -1)
        yield [ends[1]]
        direct_f = send(sums(1, hi), last2.at[0, hi], second, 1)
        yield [ends[2]]
        direct_b = send(sums(2, lo), last2.at[1, lo], second, -1)
        yield [first_f]
        add_into(net, sums(1, lo), relay2.at[0])
        summed_f = send(sums(1, lo), last2.at[0, lo], second, 1, partner=direct_f)
        yield [first_b]
        add_into(net, sums(2, hi), relay2.at[1])
        summed_b = send(sums(2, hi), last2.at[1, hi], second, -1, partner=direct_b)
        yield [ends[3], Both(net, last2.at[0], direct_f, summed_f), Both(net, last2.at[1], direct_b, summed_b)]
        add_into(net, sums(3), last2.at[0], last2.at[1])
        done.total = sums(3)
        fire(net, done)


def sums_scratch(rows, cols):
    return [pltpu.VMEM((2, RING, rows // 2, cols), F32), pltpu.VMEM((2, RING, rows, cols), F32),
            pltpu.VMEM((2, rows // 2, cols), F32), pltpu.VMEM((2, rows, cols), F32)]


def sums_stage(rows, cols):
    return [pltpu.VMEM((rows // 2, cols), F32), pltpu.VMEM((rows // 2, cols), F32), pltpu.VMEM((rows, cols), F32)]


def norm_rows(x_ref, u_ref):
    def body(at):
        x = x_ref[at, :].astype(F32)
        u_ref[at, :] = (x * lax.rsqrt(jnp.mean(x * x, axis=-1, keepdims=True) + NORM_EPS)).astype(BF16)

    rows_loop(x_ref.shape[0], 16, body)


def norm_back_rows(x_ref, dy_of, du_ref, dx_ref):
    def body(at):
        x = x_ref[at, :].astype(F32)
        du = du_ref[at, :]
        r = lax.rsqrt(jnp.mean(x * x, axis=-1, keepdims=True) + NORM_EPS)
        xr = x * r
        dx_ref[at, :] = (dy_of(at).astype(F32) + r * (du - xr * jnp.mean(xr * du, axis=-1, keepdims=True))).astype(BF16)

    rows_loop(x_ref.shape[0], 16, body)


def add_rows(x_ref, y_ref, out_ref):
    def body(at):
        out_ref[at, :] = (x_ref[at, :].astype(F32) + y_ref[at, :]).astype(BF16)

    rows_loop(x_ref.shape[0], 16, body)


def swap_halves(even, odd):
    low = lax.broadcasted_iota(jnp.int32, even.shape, len(even.shape) - 1) < even.shape[-1] // 2
    shift = even.shape[-1] // 2
    axis = len(even.shape) - 1
    return jnp.where(low, even, pltpu.roll(odd, shift, axis)), jnp.where(low, pltpu.roll(even, shift, axis), odd)


def split_columns(w_ref, cols_ref, layers):
    pieces, _, wide = w_ref.shape
    rows = layers
    tile = pieces * wide // (4 * RING * RING)
    for x in range(RING):
        for p in range(wide // tile):
            pair = []
            for i in (2 * p, 2 * p + 1):
                at = (i * RING + x) * tile
                pair.append(w_ref[at // wide, pl.ds(0, rows), pl.ds(at % wide, tile)].astype(F32))
            for c, value in enumerate(swap_halves(*pair)):
                cols_ref[2 * x + c, pl.ds(0, rows), pl.ds(p * tile, tile)] = value.astype(cols_ref.dtype)


def join_columns(cols_ref, w_ref):
    tile = w_ref.shape[1] // (4 * RING * RING)
    for x in range(RING):
        for p in range(cols_ref.shape[2] // tile):
            pair = [cols_ref[2 * x + c, :, pl.ds(p * tile, tile)] for c in range(2)]
            for i, value in zip((2 * p, 2 * p + 1), swap_halves(*pair)):
                w_ref[:, pl.ds((i * RING + x) * tile, tile)] = value


def call(body, out_shape, out_spaces, in_spaces, scratch, remote, sends, local, collective_id, *args):
    spaces = {'v': pl.BlockSpec(memory_space=pltpu.VMEM), 'h': pl.BlockSpec(memory_space=pl.ANY)}

    def kernel(*refs):
        net = Net(*refs[-5:-1])
        net.tile_sems = refs[-1]
        body(net, *refs[:-5])
        net.finish()
        assert net.n_remote <= remote and net.n_local <= local, (body.__name__, net.n_remote, net.n_local)

    return pl.pallas_call(
        kernel, out_shape=out_shape, in_specs=[spaces[s] for s in in_spaces], out_specs=[spaces[s] for s in out_spaces],
        scratch_shapes=list(scratch) + [pltpu.SemaphoreType.DMA((sends,)), pltpu.SemaphoreType.DMA((remote,)), pltpu.SemaphoreType.DMA((local,)),
                                               pltpu.SemaphoreType.REGULAR((14,)), pltpu.SemaphoreType.DMA((2,))],
        compiler_params=pltpu.CompilerParams(collective_id=collective_id, has_side_effects=True, vmem_limit_bytes=67000000),
        cost_estimate=pl.CostEstimate(flops=10**8, bytes_accessed=10**7, transcendentals=0),
        name=body.__name__)(*args)


WIDE = 512
EARLY = 3
STRIPS = 2
GRAD_TIME = 4.25
SLACK = 0.2
R_HIDDEN, R_DOWN, R_BACK, R_TURN, R_DDOWN, R_DDOWN2, R_DUP, R_OUT, R_PRE, R_GUP, R_GDOWN, R_DX = 2, 1, 3, 1, 2, 2, 4, 2, 2, 3, 3, 2
R_DU, HOLD = (3, 3.1, 3, 3.3), (0, 1, 2, 3)
WINDOWS = (2, 2, 2, 2, 2, 2, 2, 2)
AXES = ('yz', 'yz', 'yz', 'yz')
TOP = 6
NEAR = 'z'
LEAD = (3, 3, 3)
TR, TS, TL = 260, 64, 9


def wide_loop(total, body):
    wide = min(WIDE, total)

    def step(k, carry):
        body(k, wide, pl.ds(pl.multiple_of(k * wide, wide), wide))
        return carry

    lax.fori_loop(0, total // wide, step, 0)


def flat(value):
    return value.reshape(value.shape[0] * value.shape[1], value.shape[2])


def dot_rows(a, b):
    return jnp.dot(flat(a), flat(b), preferred_element_type=F32)


def dot_cols(a, b):
    return lax.dot_general(flat(a), flat(b), CONTRACT_COLS, preferred_element_type=F32)


def gelu(a):
    return 0.5 * a * (1.0 + jnp.tanh(GELU_C * (a + 0.044715 * a * a * a)))


def hidden_rows(net, chip, u, up, a, s):
    at = pl.ds(chip * 2, 2)

    def body(_, wide, cols):
        pre = dot_rows(u[at], up[:, :, cols]).astype(BF16)
        a[at, :, cols] = pre.reshape(2, -1, wide)
        s[at, :, cols] = gelu(pre.astype(F32)).astype(BF16).reshape(2, -1, wide)

    wide_loop(up.shape[2], body)
    net.spend(1.7)


def down_rows(net, chip, s, down, part):
    at = pl.ds(chip * 2, 2)

    def body(_, wide, cols):
        part[:, :, cols] = dot_rows(s[at], down[:, :, cols]).reshape(2, -1, wide)

    wide_loop(down.shape[2], body)
    net.spend(1.76)


def hidden_back_rows(net, chip, dy, down, ds):
    at = pl.ds(chip * 2, 2)
    rows = down.shape[1]

    def body(k, wide, cols):
        blocks = pl.ds(k * (wide // rows), wide // rows)
        ds[at, :, cols] = dot_cols(dy[at], down[blocks]).astype(BF16).reshape(2, -1, wide)

    wide_loop(down.shape[0] * rows, body)
    net.spend(1.5)


def gelu_both(a):
    t = jnp.tanh(GELU_C * (a + 0.044715 * a * a * a))
    return 0.5 * a * (1.0 + t), 0.5 * (1.0 + t) + 0.5 * a * (1.0 - t * t) * (GELU_C * (1.0 + 3 * 0.044715 * a * a))


def hidden_turn_rows(net, chip, u, up, s, ds):
    at = pl.ds(chip * 2, 2)

    def body(_, wide, cols):
        pre = dot_rows(u[at], up[:, :, cols]).astype(BF16).astype(F32)
        value, slope = gelu_both(pre)
        s[at, :, cols] = value.astype(BF16).reshape(2, -1, wide)
        ds[at, :, cols] = (ds[at, :, cols].astype(F32) * slope.reshape(2, -1, wide)).astype(BF16)

    wide_loop(up.shape[2], body)
    net.spend(2.1)


def pre_back_rows(net, chip, dy, down, a, da):
    at = pl.ds(chip * 2, 2)
    rows = down.shape[1]

    def body(k, wide, cols):
        blocks = pl.ds(k * (wide // rows), wide // rows)
        ds = dot_cols(dy[at], down[blocks]).astype(BF16).astype(F32).reshape(2, -1, wide)
        da[at, :, cols] = (ds * gelu_both(a[at, :, cols].astype(F32))[1]).astype(BF16)

    wide_loop(down.shape[0] * rows, body)
    net.spend(1.95)


def input_back_rows(net, chip, da, up, part):
    at = pl.ds(chip * 2, 2)
    rows = up.shape[1]

    def body(k, wide, cols):
        blocks = pl.ds(k * (wide // rows), wide // rows)
        part[:, :, cols] = dot_cols(da[at], up[blocks]).reshape(2, -1, wide)

    wide_loop(up.shape[0] * rows, body)
    net.spend(1.9)


def stored_tiles(net, count, compute, stage, out):
    def store(t):
        return pltpu.make_async_copy(stage.at[lax.rem(t, 2)], out(t), net.tile_sems.at[lax.rem(t, 2)])

    def step(t, carry):
        @pl.when(t >= 2)
        def _():
            store(t - 2).wait()

        compute(t, stage.at[lax.rem(t, 2)])
        store(t).start()
        return carry

    lax.fori_loop(0, count, step, 0)
    for t in range(max(count - 2, 0), count):
        store(jnp.int32(t)).wait()


def dot_tokens(a, b):
    return lax.dot_general(flat(a), flat(b), CONTRACT_ROWS, preferred_element_type=F32)


def grad_tiles(net, lhs, rhs, stage, out):
    _, high, wide = stage.shape
    across = rhs.shape[2] // wide

    def columns(t):
        return pl.ds(pl.multiple_of(lax.rem(t, across) * wide, wide), wide)

    def rows(t):
        return pl.ds(pl.multiple_of(lax.div(t, across) * high, high), high)

    def compute(t, slot):
        slot[...] = dot_tokens(lhs[:, :, rows(t)], rhs[:, :, columns(t)])

    stored_tiles(net, lhs.shape[2] // high * across, compute, stage, lambda t: out.at[rows(t), columns(t)])
    net.spend(GRAD_TIME * lhs.shape[2] / 1024)


def solution(mesh):
    nl, nd = mesh.shape['local'], mesh.shape['data']
    tok_spec = P(BOTH_AXES, None)
    w_spec = P(None, BOTH_AXES, None)

    def device_fn(tokens, grad_out, w_up, w_down):
        num_layers, ur, ffn = w_up.shape
        dr = w_down.shape[1]
        rows, width = tokens.shape
        hidden = nl * dr
        shape = jax.ShapeDtypeStruct
        up_full = shape((nl, nd * ur, hidden), BF16)
        down_full = shape((nl, dr, width), BF16)
        act_full = shape((nd, rows, width), BF16)
        hid_full = shape((nd, rows, hidden), BF16)
        own = shape((rows, width), BF16)
        part_vmem = pltpu.VMEM((RING, 2, rows, width), F32)
        rx = [part_vmem] + reduce_x_scratch(rows, width)
        sums = sums_scratch(dr, hidden) * 4 + sums_stage(dr, hidden) * 2

        def vmem(like):
            return pltpu.VMEM(like.shape, like.dtype)

        def step(net, x_in, x_halves, g_in, w_up_in, w_down_in,
                 x_out, dx_out, block_out, u_out, a_out, s_out, d_up0, d_down0, d_up1, d_down1, dw_up1, dw_down1, dw_up0, dw_down0,
                 x, u, g, up0, up1, down0, down1, ds, s, stage, part, *scratch):
            net.arrive('dyz')
            rx_scratch = scratch[:5]
            names = ('blocks', 'blocks1', 'sent_u', 'got_u', 'got_g', 'sent_up0', 'sent_down0', 'sent_up1', 'sent_down1', 'got_up0', 'got_down0',
                     'got_up1', 'got_down1', 'saved', 'free0', 'reduced0', 'ds_made', 'got_u1', 'hidden', 'all_du', 'reduced1', 'sent_dy', 'got_dy',
                     'back_up0', 'back_up0_rest', 'back_down0', 'd_down1', 'd_up1', 'y_reduced', 'acts', 'd_down0', 'da0', 'd_up0', 'du_reduced',
                     'out_up1', 'out_up0', 'got_u0', 'y_made', 'x_saved', 'weights_in', 'd_down1_0', 'relayed0')
            ev = {name: Event() for name in names}
            for kind in ('up', 'down'):
                for layer in range(2):
                    for k in range(2):
                        ev['sum_%s%d%d' % (kind, layer, k)] = Event()
            ev['got_up0'].rank = R_HIDDEN
            hidden_made, made0, made1, y_made, du_made = ([Event() for _ in STEPS] for _ in range(5))
            wide = width // 2
            half_up = nd * ur // 2
            act_pool, rs_pool = Pool(), Pool()
            job_pools = [[Pool(), Pool()], [Pool(), Pool()]]
            pools = {'up0': [Pool(), Pool()], 'down0': [Pool(), Pool()], 'up1': job_pools[0], 'down1': job_pools[1], 'blocks': [Pool(), Pool()]}
            stages = (scratch[21:24], scratch[24:27])
            job_scratch = [[scratch[5 + 8 * n + 4 * k:9 + 8 * n + 4 * k] for k in range(2)] for n in range(2)]
            frees = [[Event(0.0) for _ in range(3)] for _ in range(2)]
            freed = {k: Event() for k in range(10, 14)}

            def columns(h):
                return pl.ds(h * wide, wide)

            inputs = [net.load(x_in, x)]
            inputs += [net.load(w_up_in.at[:, pl.ds(k * hidden, hidden)], ds.at[k, pl.ds(0, num_layers * ur)]) for k in range(nd)]

            def gather(name, own, full, split):
                size = own.shape[0] // 2

                def join(kind, events):
                    yield events
                    if kind == 'got_':
                        ev[kind + name].copies = events[0].copies + events[1].copies
                    fire(net, ev[kind + name])

                got, sent = [Event(), Event()], [Event(), Event()]
                for k, first in enumerate('yz'):
                    net.spawn(gather_yz(net, own.at[pl.ds(k * size, size)], full, first, got[k], sent[k], k * size, split=split, pool=pools[name][k]))
                net.spawn(join('got_', got))
                net.spawn(join('sent_', sent))

            net.take(inputs)
            split_columns(ds, s, num_layers * ur)
            net.enter()
            net.spawn(exchange(net, lambda k: s.at[k, pl.ds(0, ur)], block_out.at[0], ev['blocks'], pools['blocks'][0]))
            gather('down0', w_down_in.at[0], down0, False)
            norm_rows(x, u.at[net.data])
            net.spend(0.7)
            own_grads = net.load(g_in, g.at[net.data])

            def up_first():
                yield [ev['blocks']]
                gather('up0', block_out.at[0], up0, True)
                net.spawn(gather_x(net, u, ev['got_u'], ev['sent_u'], pool=act_pool))
                yield [ev['sent_u']]
                net.spawn(exchange(net, lambda k: s.at[k, pl.ds(ur, ur)], block_out.at[1], ev['blocks1'], pools['blocks'][1]))
                yield [own_grads]
                net.spawn(gather_x(net, g, ev['got_g']))

            def second():
                yield [ev['sent_up0'], ev['sent_down0'], ev['blocks1']]
                gather('down1', w_down_in.at[1], down1, False)
                yield [made0[EARLY]]
                gather('up1', block_out.at[1], up1, True)

            def hidden_flow():
                yield [ev['got_u'], ev['got_up0'], ev['blocks1']]
                for k, step in enumerate(STEPS):
                    hidden_rows(net, net.at('x', step), u, up0, ds, s)
                    fire(net, hidden_made[k])
                    yield [Event(net.now, R_HIDDEN)] + ([ev['relayed0']] if k == 1 else [])
                yield [net.load(ds, a_out), net.load(s, s_out), net.load(u, u_out)]
                fire(net, ev['saved'])

            def down_flow():
                for k, step in enumerate(STEPS):
                    yield [hidden_made[k], ev['got_down0'], Event(0.0, R_DOWN)] + ([ev['relayed0']] if k == 1 else [])
                    down_rows(net, net.at('x', step), s, down0, part.at[k])
                    fire(net, made0[k])
                fire(net, ev['free0'])

            here = {step: Event() for step in STEPS}
            dy_here = {step: Event() for step in STEPS}

            strips0 = [Event() for _ in range(STRIPS)]
            net.spawn(reduce_x(net, part, made0, rx_scratch, ev['reduced0'], rs_pool, ev['relayed0'], strips0))

            def next_layer():
                yield [ev['saved'], ev['got_g']]
                net.drain(ev['got_u'].copies + ev['got_g'].copies)
                credit = net.grant(3, 'xp')
                act_pool.again()
                got = [Event() for _ in strips0]
                chips = [{step: Event() for step in STEPS} for _ in strips0]

                def strip(n):
                    at = pl.ds(n * (rows // STRIPS), rows // STRIPS)
                    yield [strips0[n], credit]
                    add_rows(x.at[at], part.at[3, net.core, at], x.at[at])
                    norm_rows(x.at[at], u.at[net.data, at])
                    net.spend(1.0 / STRIPS)
                    net.spawn(gather_x(net, u, got[n], chips=chips[n], pool=act_pool, strip=(n, STRIPS)))

                def chip(step):
                    yield [arrived[step] for arrived in chips]
                    fire(net, here[step])

                for n in range(STRIPS):
                    net.spawn(strip(n))
                for step in STEPS:
                    net.spawn(chip(step))
                yield [ev['reduced0']]
                net.drain(ev['reduced0'].copies)
                yield [net.grant(4, 'xp')]
                net.spawn(reduce_x(net, part, made1, rx_scratch, ev['reduced1'], rs_pool.again()))
                yield got
                ev['got_u1'].copies = sum((event.copies for event in got), [])
                fire(net, ev['got_u1'])

            def back_flow():
                for k, step in enumerate(STEPS):
                    yield [ev['got_g'], ev['got_down1'], ev['saved'], Event(0.0, R_BACK)]
                    hidden_back_rows(net, net.at('x', step), g, down1, ds)
                fire(net, ev['ds_made'])

            def again():
                top = nd * ur * TOP // 8
                yield [ev['free0'], ev['ds_made']]
                net.drain(ev['got_up0'].copies + ev['got_down0'].copies)
                credit = net.grant(6, 'yz')
                yield [credit]
                net.spawn(gather_yz(net, w_down_in.at[0], down0, NEAR, ev['back_down0'], near=True, pool=pools['down0'][1].again()))
                net.spawn(gather_yz(net, block_out.at[0, pl.ds(0, top)], up0, 'y', ev['back_up0'], pool=pools['up0'][0].again()))
                net.spawn(gather_yz(net, block_out.at[0, pl.ds(top, nd * ur - top)], up0, 'z', ev['back_up0_rest'], offset=top, pool=pools['up0'][1].again()))

            def weights():
                yield [ev['got_up1'], ev['got_down1']]
                yield [net.grant(7, 'yz')]
                fire(net, ev['weights_in'])

            left = [RING, RING]

            turned = [Event() for _ in STEPS]

            def layer1(k, step):
                yield [here[step], ev['ds_made'], ev['got_up1'], Event(0.0, R_TURN)]
                hidden_turn_rows(net, net.at('x', step), u, up1, s, ds)
                fire(net, turned[k])
                left[0] -= 1
                if left[0] == 0:
                    fire(net, ev['hidden'])

            def layer1_back(k, step):
                yield [turned[k], Event(0.0, R_DU[k])] + ([ev['hidden']] if k in HOLD else [])
                input_back_rows(net, net.at('x', step), ds, up1, part.at[k])
                fire(net, made1[k])
                left[1] -= 1
                if left[1] == 0:
                    fire(net, ev['all_du'])

            def grads1():
                for h in range(2):
                    yield [Event(0.0, R_DDOWN2 if h else R_DDOWN), ev['hidden']]
                    grad_tiles(net, s, g.at[:, :, columns(h)], stage, d_down1.at[:, columns(h)])
                    fire(net, ev['d_down1' if h else 'd_down1_0'])
                for h in range(2):
                    yield [Event(net.now, R_DUP)]
                    grad_tiles(net, u.at[:, :, columns(h)], ds, stage, d_up1.at[columns(h)])
                fire(net, ev['d_up1'])

            def act():
                yield [ev['d_up1'], ev['all_du'], ev['got_u1']]
                own_g = [net.load(g_in.at[:, columns(h)], ds.at[h]) for h in range(2)]
                net.drain(ev['got_u1'].copies)
                credit = net.grant(5, 'xp')
                yield [ev['reduced1'], credit] + own_g
                norm_back_rows(x, lambda at: jnp.concatenate([ds[h, at, :] for h in range(2)], axis=-1), part.at[3, net.core], u.at[net.data])
                net.spend(0.7)
                net.spawn(gather_x(net, u, ev['got_dy'], ev['sent_dy'], dy_here, pool=act_pool.again()))

            def layer1_out():
                yield [ev['reduced1'], Event(0.0, R_OUT)]
                net.drain(ev['reduced1'].copies)
                credit = net.grant(8, 'xp')
                for k, step in enumerate(STEPS):
                    down_rows(net, net.at('x', step), s, down1, part.at[k])
                    yield [Event(net.now, R_OUT)]
                fire(net, ev['y_made'])
                yield [ev['sent_dy'], credit]
                net.spawn(reduce_x(net, part, y_made, rx_scratch, ev['y_reduced'], rs_pool.again()))
                for k in range(RING):
                    fire(net, y_made[k])
                yield [ev['y_reduced']]
                add_rows(x, part.at[3, net.core], x)
                yield [net.load(x, x_out)]
                fire(net, ev['x_saved'])

            a0, s0 = up1.at[pl.ds(0, nd)], up1.at[pl.ds(nd, nd)]
            backs = [RING]

            def bring_back():
                yield [ev['d_down1']]
                yield [net.load(u_out, g)]
                fire(net, ev['got_u0'])

            def bring_acts():
                yield [ev['all_du']]
                net.drain(ev['got_up1'].copies)
                yield [net.load(a_out, a0), net.load(s_out, s0)]
                fire(net, ev['acts'])

            def layer0_hidden(step):
                yield [dy_here[step], ev['acts'], ev['back_down0'], ev['d_up1'], Event(0.0, R_PRE)]
                pre_back_rows(net, net.at('x', step), u, down0, a0, ds)
                backs[0] -= 1
                if backs[0] == 0:
                    fire(net, ev['da0'])

            def layer0():
                for h in range(2):
                    yield [ev['da0'], ev['got_u0'], Event(0.0, R_GUP)]
                    grad_tiles(net, g.at[:, :, columns(h)], ds, stage, d_up0.at[columns(h)])
                fire(net, ev['d_up0'])
                for h in range(2):
                    yield [ev['got_dy'], ev['acts'], Event(0.0, R_GDOWN)]
                    grad_tiles(net, s0, u.at[:, :, columns(h)], stage, d_down0.at[:, columns(h)])
                fire(net, ev['d_down0'])
                yield [ev['y_reduced'], ev['back_up0'], ev['back_up0_rest'], Event(0.0, R_DX)]
                net.drain(ev['y_reduced'].copies + ev['got_down1'].copies)
                x0 = down1.at[pl.ds(0, x_halves.shape[0])]
                yield [net.grant(9, 'xp'), net.load(x_halves, x0)]
                net.spawn(reduce_x(net, part, du_made, rx_scratch, ev['du_reduced'], rs_pool.again()))
                for k, step in enumerate(STEPS):
                    input_back_rows(net, net.at('x', step), ds, up0, part.at[k])
                    fire(net, du_made[k])
                    yield [Event(net.now, R_DX)]
                yield [ev['du_reduced'], ev['x_saved']]
                for q in range(x_halves.shape[0]):
                    rows_q = pl.ds(q * dr, dr)
                    dy_q = u.at[net.data, rows_q]
                    norm_back_rows(x0.at[q], lambda at, dy_q=dy_q: dy_q[at, :], part.at[3, net.core, rows_q], x.at[rows_q])
                yield [net.load(x, dx_out)]

            def up_place(ref, k):
                return lambda block, rows: ref.at[pl.ds(pl.multiple_of(block * (2 * half_up) + k * half_up + rows.start, rows.size), rows.size)]

            def down_place(ref, k):
                return lambda block, rows: ref.at[pl.ds(pl.multiple_of(block * dr + rows.start, rows.size), rows.size), columns(k)]

            def gate(event, items, pool):
                yield items
                pool.again()
                fire(net, event)

            def sum_job(job, place, ref, ready, name, credits=()):
                passed = [Event(), Event()]
                for k in range(2):
                    start = Event()
                    n = job % 2
                    net.spawn(gate(start, ready[k] + ([credits[k]] if credits else []), job_pools[n][k]))
                    sums = Sums(net, AXES[job][k], job_scratch[n][k], stages[k])
                    net.spawn(sums.run(place(ref, k), start, ev['sum_%s%d' % (name, k)], frees[k], passed[k], job_pools[n][k], WINDOWS[2 * job + k], LEAD[min(job, 2)]))
                return passed

            def out_down(layer, dw_down, credit):
                def one(k):
                    done = ev['sum_down%d%d' % (layer, k)]
                    yield [done]
                    yield [net.load(done.total, dw_down.at[:, columns(k)])]
                    if credit is not None:
                        net.drain(done.copies)
                        yield [net.grant(credit + k, 'yz')]
                        fire(net, freed[credit + k])

                for k in range(2):
                    net.spawn(one(k))

            def out_up(n, layer, dw_up, credit):
                totals = [ev['sum_up%d%d' % (layer, k)] for k in range(2)]
                yield totals
                net.drain(totals[0].copies + totals[1].copies)
                spare = job_scratch[n][0][0].at[0]
                for k, done in enumerate(totals):
                    for q in range(2):
                        copy_rows(net, done.total.at[pl.ds(q * spare.shape[1], spare.shape[1])], spare.at[2 * k + q])
                done = ev['out_up%d' % layer]
                net.spawn(exchange_back(net, spare, dw_up, done, pools['blocks'][layer].again()))
                if credit is not None:
                    yield [done]
                    for k in range(2):
                        yield [net.grant(credit + k, 'yz')]
                        fire(net, freed[credit + k])

            passed = sum_job(0, down_place, d_down1, [[ev['d_down1_0'], ev['weights_in']], [ev['d_down1'], ev['weights_in']]], 'down1')
            passed = sum_job(1, up_place, d_up1, [[ev['d_up1']] + passed] * 2, 'up1')
            passed = sum_job(2, up_place, d_up0, [[ev['d_up0']] + passed] * 2, 'up0', [freed[10], freed[11]])
            sum_job(3, down_place, d_down0, [[ev['d_down0']] + passed] * 2, 'down0', [freed[12], freed[13]])
            out_down(1, dw_down1, 10)
            net.spawn(out_up(1, 1, dw_up1, 12))
            net.spawn(out_up(0, 0, dw_up0, None))
            out_down(0, dw_down0, None)
            for k in (3, 2, 1, 0):
                net.spawn(layer1(k, STEPS[k]))
            for k in range(RING):
                net.spawn(layer1_back(k, STEPS[k]))
            for step in (0, -1, 1, 2):
                net.spawn(layer0_hidden(step))
            for flow in (up_first(), second(), hidden_flow(), down_flow(), next_layer(), back_flow(), again(), weights(), grads1(), act(), layer1_out(),
                         bring_back(), bring_acts(), layer0()):
                net.spawn(flow)
            net.run()

        def finish(*refs):
            sources, targets, held, ups, sems = refs[:6], refs[6:10], refs[10:16], refs[16:18], refs[18]
            x_out, dx_out, up_out, down_out = targets
            loads = [pltpu.make_async_copy(src, dst, sems.at[k]) for k, (src, dst) in enumerate(zip(sources, held))]
            stores = [(ups[1], up_out.at[1]), (ups[0], up_out.at[0]), (held[2], down_out.at[1]), (held[3], down_out.at[0]), (held[4], x_out), (held[5], dx_out)]
            stores = [pltpu.make_async_copy(src, dst, sems.at[6 + k]) for k, (src, dst) in enumerate(stores)]
            for load in loads:
                load.start()
            for k in (2, 3, 4, 5):
                loads[k].wait()
                stores[k].start()
            for k in (0, 1):
                loads[k].wait()
                join_columns(held[k], ups[1 - k])
                stores[k].start()
            for store in stores:
                store.wait()

        d_up_own, d_down_own = shape((nd, ur, hidden), F32), shape((dr, width), F32)

        d_up_full, d_down_full = shape((width, hidden), F32), shape((hidden, width), F32)
        x_out, dx, _, _, _, _, _, _, _, _, *grads = call(
            step, [own, own, shape((num_layers, nd * ur, hidden), BF16), act_full, hid_full, hid_full] + [d_up_full, d_down_full] * 2
            + [d_up_own, d_down_own] * 2, 'h' * 14, 'hhhhh',
            [vmem(own)] + [vmem(act_full)] * 2 + [vmem(up_full)] * 2 + [vmem(down_full)] * 2 + [vmem(hid_full)] * 2
            + [pltpu.VMEM((2, hidden // 2, width // 4), F32)] + rx + sums, TR, TS, TL, 0,
            tokens, tokens.reshape(rows // dr, dr, width), grad_out, w_up.reshape(num_layers * ur, ffn), w_down)
        up1_own, down1_own, up0_own, down0_own = grads
        held = [d_up_own, d_up_own, d_down_own, d_down_own, own, own]
        return pl.pallas_call(
            finish, out_shape=[own, own, shape(w_up.shape, F32), shape(w_down.shape, F32)], name='finish',
            in_specs=[pl.BlockSpec(memory_space=pl.ANY)] * 6, out_specs=[pl.BlockSpec(memory_space=pl.ANY)] * 4,
            scratch_shapes=[vmem(like) for like in held] + [pltpu.VMEM(w_up.shape[1:], F32)] * 2 + [pltpu.SemaphoreType.DMA((12,))],
        )(up1_own, up0_own, down1_own, down0_own, x_out, dx)

    return jax.shard_map(device_fn, mesh=mesh, in_specs=(tok_spec, tok_spec, w_spec, w_spec), out_specs=(tok_spec, tok_spec, w_spec, w_spec), check_vma=False)
```
